128 devices in a mesh: grp: 4 (over y), dev: 32 (over x, z, core).
Axes of the slice: x: 4, y: 4, z: 4, core: 2. Of those that a mesh axis runs over, the one named last changes fastest.
Arguments:
- displacement: float32 [3, 64, 32, 32], P(None, 'dev')
- external_force: float32 [3, 64, 32, 32], P(None, 'dev'), may hold values from -6 to 6
- element_sample: int32 [64, 32, 32], P('dev'), may hold values from 0 to 127, as said below
- lame_field: bfloat16 [128, 32, 1024], P('grp', 'dev'), may hold values from 0.5 to 2
- shear_field: bfloat16 [128, 32, 1024], P('grp', 'dev'), may hold values from 0.29882812 to 3
- plastic_steps: int32 [128], replicated, may hold values from 1 to 4
- owner_slot: int32 [128], replicated, may hold values from 0 to 31, as said below
Outputs:
- displacement_next: float32 [3, 64, 32, 32], P(None, 'dev')
- sample_response: float32 [128, 8], P(('grp', 'dev'))
- micro_strain: float32 [6, 128, 32, 1024], P(None, 'grp', 'dev')
The draws below stay inside these ranges and needn't reach their ends.
Inputs may be any that keep to these rules, and one draw needn't show every extreme that they name: `element_sample`: every value from 0 to 127 is taken by at least one element. `owner_slot`: within each aligned block of 32 RVEs a permutation of 0 to 31; slot s of a block belongs to the block's owner s.
All inputs are finite; a program needn't handle non-finite values.
Results may differ from the reference program's by a relative error of at most 0.0009.
Values may be sent and summed in bfloat16 or wider, within the bound.
A program may use at most 64 MiB of HBM per device.

```python
import math
import jax
import jax.numpy as jnp
from jax import lax

VOX = 32
RVE_DEV = 1
RVE_GRP = 32
RVES = 128
MY = 32
MZ = 32
NX = 64
ITERS = 1
KMAX = 4
CG_STEPS = 3


def draw_displacement(key, part):
    keys = jax.random.split(jax.random.fold_in(key, 37), 4)
    waves = jax.random.randint(keys[0], (6, 3), 1, 4).astype(jnp.float32)
    amplitude = 2.0 * jax.random.normal(keys[1], (3, 6), jnp.float32)
    phase = jax.random.uniform(keys[2], (6,), jnp.float32, 0.0, 2.0 * jnp.pi)
    along_x = jnp.arange(NX, dtype=jnp.float32) / NX
    along_y = jnp.arange(MY, dtype=jnp.float32) / MY
    along_z = jnp.arange(MZ, dtype=jnp.float32) / MZ
    angle = 2.0 * jnp.pi * (waves[:, 0, None, None, None] * along_x[None, :, None, None] + waves[:, 1, None, None, None] * along_y[None, None, :, None] + waves[:, 2, None, None, None] * along_z[None, None, None, :]) + phase[:, None, None, None]
    smooth = jnp.einsum('cm,mxyz->cxyz', amplitude, jnp.sin(angle))
    rough = 0.3 * jax.random.normal(keys[3], (3, NX, MY, MZ), jnp.float32)
    return (smooth + rough).astype(jnp.float32)


def draw_element_sample(key, part):
    total = NX * MY * MZ
    plane = MY * MZ
    chosen = jax.random.permutation(jax.random.fold_in(key, 11), total)[:RVES].astype(jnp.int32)
    seed_x = chosen // plane
    seed_y = chosen // MZ % MY
    seed_z = chosen % MZ
    labels = jnp.arange(RVES, dtype=jnp.int32)

    def nearest(layer):
        within = jnp.arange(plane, dtype=jnp.int32)
        offset_x = layer - seed_x[None, :]
        offset_y = (within // MZ)[:, None] - seed_y[None, :]
        offset_z = (within % MZ)[:, None] - seed_z[None, :]
        score = (offset_x * offset_x + offset_y * offset_y + offset_z * offset_z) * RVES + labels[None, :]
        return jnp.argmin(score, axis=1).astype(jnp.int32)
    return lax.map(nearest, jnp.arange(NX, dtype=jnp.int32)).reshape(NX, MY, MZ)


def plastic_table(key):
    keys = jax.random.split(jax.random.fold_in(key, 23), 3)
    index = jnp.arange(RVES, dtype=jnp.int32)
    zone_start = jax.random.randint(keys[0], (), 0, RVES)
    in_zone = (index - zone_start) % RVES < RVES // 4
    light = jax.random.randint(keys[1], (RVES,), 1, 3)
    heavy = jax.random.randint(keys[2], (RVES,), KMAX // 2, KMAX + 1)
    steps = jnp.where(in_zone, heavy, light)
    return jnp.where(index == zone_start, KMAX, steps).astype(jnp.int32)


def draw_plastic_steps(key, part):
    return plastic_table(key)


def draw_owner_slot(key, part):
    steps = plastic_table(key)
    blocks = steps.reshape(RVES // RVE_GRP, RVE_GRP)
    owners = RVE_GRP // RVE_DEV

    def assign(row):
        ranked = jnp.argsort(-row, stable=True).astype(jnp.int32)
        place = jnp.arange(RVE_GRP, dtype=jnp.int32)
        lap_number = place // owners
        column = place % owners
        owner = jnp.where(lap_number % 2 == 0, column, owners - 1 - column)
        slot_of_rank = owner * RVE_DEV + lap_number
        return jnp.zeros((RVE_GRP,), jnp.int32).at[ranked].set(slot_of_rank)
    return jax.vmap(assign)(blocks).reshape(RVES).astype(jnp.int32)


def level_of(rng, shape, cuts, least, top_value):
    factor_of = 1.0
    for position, shards_of in cuts:
        heights = jax.random.uniform(jax.random.fold_in(jax.random.fold_in(rng, 6), position), (shards_of,), jnp.float32, least / len(cuts), top_value / len(cuts))
        factor_of = factor_of * jnp.repeat(jnp.exp(heights), shape[position] // shards_of).reshape((-1,) + (1,) * (len(shape) - 1 - position))
    return factor_of


def gaussian(key, dims, scale, reach, shards=(), kind=jnp.bfloat16):
    values = scale * jax.random.normal(key, dims, jnp.float32)
    if shards:
        values = values * level_of(key, dims, shards, -0.22, 0.18)
    return jnp.clip(values, -reach, reach).astype(kind)


def setup_inputs(seed: int = 0) -> dict:
    key_of = jax.random.split(jax.random.key(seed), 8)
    displacement = draw_displacement(jax.random.fold_in(key_of[7], 71), 0)
    external_force = gaussian(key_of[1], (3, NX, MY, MZ), 1.0, 6.0, ((1, 32),), jnp.float32)
    element_sample = draw_element_sample(jax.random.fold_in(key_of[7], 71), 0)
    lame_field = jnp.clip(0.5 + 1.5 * jax.random.uniform(key_of[3], (RVES, VOX, VOX * VOX), jnp.float32) ** level_of(key_of[3], (RVES, VOX, VOX * VOX), ((0, 4), (1, 32)), -0.2, 0.2), 0.5, 2.0).astype(jnp.bfloat16)
    shear_field = jnp.clip(jnp.exp(math.log(3.0) - 2.306499 * jax.random.uniform(key_of[4], (RVES, VOX, VOX * VOX), jnp.float32) ** level_of(key_of[4], (RVES, VOX, VOX * VOX), ((0, 4), (1, 32)), -0.2, 0.2)), 0.29882812, 3.0).astype(jnp.bfloat16)
    plastic_steps = draw_plastic_steps(jax.random.fold_in(key_of[7], 71), 0)
    owner_slot = draw_owner_slot(jax.random.fold_in(key_of[7], 71), 0)
    return {"displacement": displacement, "external_force": external_force, "element_sample": element_sample, "lame_field": lame_field, "shear_field": shear_field, "plastic_steps": plastic_steps, "owner_slot": owner_slot}


shear_ref = 1.65
lame_ref = 1.25
green_ratio = (lame_ref + shear_ref) / (lame_ref + 2.0 * shear_ref)
relax_rate = 0.35
flow_scale = 4.0
spring_rate = 0.2


def wave_at(count, index):
    angle = (2.0 * jnp.pi / count) * index.astype(jnp.float32)
    return jnp.where(index % (count // 2) == 0, 0.0, jnp.sin(angle)).astype(jnp.float32)


def inverse_square(first, second, third):
    square = first * first + second * second + third * third
    live = square > 0.0
    return jnp.where(live, 1.0 / jnp.where(live, square, 1.0), 0.0)


def green_parts(parts, first, second, third, inverse):
    xx, yy, zz, yz, xz, xy = parts
    along_first = xx * first + xy * second + xz * third
    along_second = xy * first + yy * second + yz * third
    along_third = xz * first + yz * second + zz * third
    inner = first * along_first + second * along_second + third * along_third
    scaled = green_ratio * inner * inverse
    push_first = (along_first - scaled * first) * inverse / shear_ref
    push_second = (along_second - scaled * second) * inverse / shear_ref
    push_third = (along_third - scaled * third) * inverse / shear_ref
    return (first * push_first, second * push_second, third * push_third,
            0.5 * (second * push_third + third * push_second),
            0.5 * (first * push_third + third * push_first),
            0.5 * (first * push_second + second * push_first))


def measure(stress):
    return (stress[0] * stress[0] + stress[1] * stress[1] + stress[2] * stress[2]
            + 2.0 * (stress[3] * stress[3] + stress[4] * stress[4] + stress[5] * stress[5]))


def material(strain, lame, shear, steps, bound):
    trace = strain[0] + strain[1] + strain[2]
    third_trace = trace / 3.0
    deviator = jnp.concatenate([strain[:3] - third_trace, strain[3:]])

    def relax(count, plastic):
        ratio = measure(2.0 * shear * (deviator - plastic)) / flow_scale
        moved = plastic + relax_rate * (deviator - plastic) * (ratio / (1.0 + ratio))
        return jnp.where(count < steps, moved, plastic)

    plastic = lax.fori_loop(0, bound, relax, jnp.zeros_like(deviator))
    elastic = strain - plastic
    stress = jnp.concatenate([2.0 * shear * elastic[:3] + lame * trace, 2.0 * shear * elastic[3:]])
    ratio = measure(2.0 * shear * (deviator - plastic)) / flow_scale
    return stress, ratio


def green_real(stress, first, second, third, inverse):
    spectrum = jnp.fft.fftn(stress, axes=(1, 2, 3))
    parts = green_parts(tuple(spectrum[part] for part in range(6)), first, second, third, inverse)
    return jnp.real(jnp.fft.ifftn(jnp.stack(parts), axes=(1, 2, 3)))


def sample_solve(item, first, second, third, inverse):
    lame, shear, count, load = item
    lame = lame.astype(jnp.float32).reshape(VOX, VOX, VOX)
    shear = shear.astype(jnp.float32).reshape(VOX, VOX, VOX)
    strain = jnp.broadcast_to(load[:, None, None, None], (6, VOX, VOX, VOX))
    for sweep in range(ITERS):
        stress, ratio = material(strain, lame, shear, count, KMAX)
        strain = strain - green_real(stress, first, second, third, inverse)
    stress, ratio = material(strain, lame, shear, count, KMAX)
    response = jnp.concatenate([jnp.sum(stress, axis=(1, 2, 3)), jnp.sum(lame)[None],
                                jnp.sum(shear / (1.0 + ratio))[None]]) / (VOX ** 3)
    return strain, response


def shifted(field, axis, upward):
    extent = field.shape[axis]
    zero = jnp.zeros_like(lax.slice_in_dim(field, 0, 1, axis=axis))
    if upward:
        return jnp.concatenate([lax.slice_in_dim(field, 1, extent, axis=axis), zero], axis=axis)
    return jnp.concatenate([zero, lax.slice_in_dim(field, 0, extent - 1, axis=axis)], axis=axis)


def average_next(field, axis):
    return 0.5 * (field + shifted(field, axis, True))


def differ_next(field, axis):
    return shifted(field, axis, True) - field


def average_back(field, axis):
    return 0.5 * (field + shifted(field, axis, False))


def differ_back(field, axis):
    return shifted(field, axis, False) - field


def assemble(slope_x, slope_y, slope_z):
    return jnp.stack([slope_x[0], slope_y[1], slope_z[2], 0.5 * (slope_y[2] + slope_z[1]),
                      0.5 * (slope_x[2] + slope_z[0]), 0.5 * (slope_x[1] + slope_y[0])])


def strain_of(field):
    smooth_z = average_next(field, 3)
    slope_x = differ_next(average_next(smooth_z, 2), 1)
    slope_y = average_next(differ_next(smooth_z, 2), 1)
    slope_z = average_next(average_next(differ_next(field, 3), 2), 1)
    return assemble(slope_x, slope_y, slope_z)


def force_of(stress):
    xx, yy, zz, yz, xz, xy = stress
    along_x = jnp.stack([xx, xy, xz])
    along_y = jnp.stack([xy, yy, yz])
    along_z = jnp.stack([xz, yz, zz])
    first = average_back(average_back(along_x, 3), 2)
    rest = differ_back(average_back(along_y, 3), 2) + average_back(differ_back(along_z, 3), 2)
    return differ_back(first, 1) + average_back(rest, 1)


def stiffness(field, lame_cells, shear_cells):
    strain = strain_of(field)
    trace = strain[0] + strain[1] + strain[2]
    stress = jnp.concatenate([2.0 * shear_cells * strain[:3] + lame_cells * trace, 2.0 * shear_cells * strain[3:]])
    return force_of(stress) + spring_rate * field


def reference(displacement, external_force, element_sample, lame_field, shear_field, plastic_steps, owner_slot):
    element_strain = strain_of(displacement)
    flat_sample = element_sample.reshape(-1).astype(jnp.int32)
    sums = jax.ops.segment_sum(element_strain.reshape(6, -1).T, flat_sample, num_segments=RVES)
    counts = jax.ops.segment_sum(jnp.ones(flat_sample.shape, jnp.float32), flat_sample, num_segments=RVES)
    loads = sums / counts[:, None]
    index = jnp.arange(VOX, dtype=jnp.int32)
    waves = wave_at(VOX, index)
    first = waves[:, None, None]
    second = waves[None, :, None]
    third = waves[None, None, :]
    inverse = inverse_square(first, second, third)

    def solve_one(item):
        return sample_solve(item, first, second, third, inverse)

    strains, responses = lax.map(solve_one, (lame_field, shear_field, plastic_steps, loads))
    micro_strain = jnp.transpose(strains, (1, 0, 2, 3, 4)).reshape(6, RVES, VOX, VOX * VOX)
    rows = jnp.arange(RVES, dtype=jnp.int32)
    destination = (rows // RVE_GRP) * RVE_GRP + owner_slot.astype(jnp.int32)
    sample_response = jnp.zeros((RVES, 8), jnp.float32).at[destination].set(responses)
    element_table = jnp.take(responses, flat_sample, axis=0)
    fields = element_table.T.reshape((8,) + displacement.shape[1:])
    element_stress = fields[:6]
    lame_cells = fields[6]
    shear_cells = fields[7]
    residual = external_force - force_of(element_stress) - spring_rate * displacement
    update = jnp.zeros_like(displacement)
    remainder = residual
    direction = residual
    norm_now = jnp.sum(remainder * remainder)
    for turn in range(CG_STEPS):
        image = stiffness(direction, lame_cells, shear_cells)
        alpha = norm_now / jnp.sum(direction * image)
        update = update + alpha * direction
        remainder = remainder - alpha * image
        if turn + 1 < CG_STEPS:
            norm_next = jnp.sum(remainder * remainder)
            direction = remainder + (norm_next / norm_now) * direction
            norm_now = norm_next
    return displacement + update, sample_response, micro_strain
```

```python
import jax
import jax.numpy as jnp
import numpy as np
from jax import lax
from jax.experimental import pallas as pl
from jax.experimental.pallas import tpu as pltpu
from jax.sharding import PartitionSpec as P

VOX = 32
HALF = 512
KMAX = 4
MESH = pl.DeviceIdType.MESH
NEAR = (-2, -1, 1, 2)

shear_ref = 1.65
lame_ref = 1.25
green_ratio = (lame_ref + shear_ref) / (lame_ref + 2.0 * shear_ref)
relax_rate = 0.35
spring_rate = 0.2
wire = jnp.bfloat16
f32 = jnp.float32
bf16 = jnp.bfloat16


def tables():
    n = np.arange(VOX)
    theta = 2.0 * np.pi / VOX
    ky = np.repeat(n, 16)
    kz = np.tile(np.arange(16), VOX)
    yy = np.repeat(n, VOX)
    zz = np.tile(n, VOX)
    k16 = np.arange(16)

    def zeta(z, k):
        angle = theta * (z * k % VOX)
        return (
            np.where(k == 0, 1.0, np.cos(angle)),
            np.where(k == 0, (-1.0) ** z, -np.sin(angle)),
        )

    cy, sy = np.cos(theta * (np.outer(n, ky) % VOX)), np.sin(theta * (np.outer(n, ky) % VOX))
    zr, zi = zeta(n[:, None], kz[None, :])
    cv, sv = np.cos(theta * (np.outer(n, yy) % VOX)), np.sin(theta * (np.outer(n, yy) % VOX))
    vr, vi = zeta(zz[None, :], k16[:, None])
    c, s = np.cos(theta * (np.outer(n, n) % VOX)), np.sin(theta * (np.outer(n, n) % VOX))
    x = np.block([[c, s], [-s, c]])

    def wave(k):
        return np.where(k % 16 == 0, 0.0, np.sin(theta * k))

    one = np.ones((VOX, HALF))
    xx, xy, xz = wave(n)[:, None] * one, wave(ky)[None] * one, wave(kz)[None] * one
    square = xx * xx + xy * xy + xz * xz
    inverse = np.where(square > 0, 1.0 / np.where(square > 0, square, 1.0), 0.0)
    weight = np.where(kz == 0, 1.0, 2.0)[None] * one
    scaled = -(1.0 / shear_ref) * inverse * weight / VOX**3
    pairs = (xx * xx, xy * xy, xz * xz, 2 * xy * xz, 2 * xx * xz, 2 * xx * xy)
    spectral = np.stack([scaled] + [green_ratio * p * inverse for p in pairs])
    to = lambda a: np.asarray(a, np.float32)
    return (
        to(np.stack([cy, sy, zr, zi])),
        to(np.stack([cv, sv])),
        to(np.stack([vr, vi])),
        to(np.stack([x, x.T])),
        to(spectral),
    )


def split(a):
    high = a.astype(bf16)
    return high, (a - high.astype(f32)).astype(bf16)


def mm(a, b):
    return jnp.dot(a, b, preferred_element_type=f32)


def product(a, b):
    ah, al = split(a)
    bh, bl = split(b)
    return mm(ah, bh) + (mm(al, bh) + mm(ah, bl))


def lane_of(shape):
    return lax.broadcasted_iota(jnp.int32, shape, len(shape) - 1)


def row_of(shape):
    return lax.broadcasted_iota(jnp.int32, shape, len(shape) - 2)


def roll(a, shift, axis):
    return pltpu.roll(a, shift % a.shape[axis], axis)


def z_up(v):
    return jnp.where(lane_of(v.shape) % VOX == VOX - 1, 0.0, roll(v, -1, 2))


def z_down(v):
    return jnp.where(lane_of(v.shape) % VOX == 0, 0.0, roll(v, 1, 2))


def y_up(v):
    moved = roll(v, -VOX, 2)
    next_row = jnp.where(row_of(v.shape) == 7, 0.0, roll(moved, -1, 1))
    return jnp.where(lane_of(v.shape) < 96, moved, next_row)


def y_down(v):
    moved = roll(v, VOX, 2)
    last_row = jnp.where(row_of(v.shape) == 0, 0.0, roll(moved, 1, 1))
    return jnp.where(lane_of(v.shape) >= VOX, moved, last_row)


def zc(v):
    lane = lane_of(v.shape) % VOX
    up = jnp.where(lane == VOX - 1, roll(v, 31, 1), roll(v, -1, 1))
    down = jnp.where(lane == 0, roll(v, -31, 1), roll(v, 1, 1))
    return 0.5 * (up - down)


def yc(v):
    lane = lane_of(v.shape)
    up = roll(v, -VOX, 1)
    up = jnp.where(lane < 96, up, roll(up, -1, 0))
    down = roll(v, VOX, 1)
    down = jnp.where(lane >= VOX, down, roll(down, 1, 0))
    return 0.5 * (up - down)


def strain_of(fields):
    slopes = []
    for w in fields:
        up = z_up(w)
        mz, dz = 0.5 * (w + up), up - w
        moved = y_up(mz)
        a, b = 0.5 * (mz + moved), moved - mz
        c = 0.5 * (dz + y_up(dz))
        slopes.append((a[1:] - a[:-1], 0.5 * (b[1:] + b[:-1]), 0.5 * (c[1:] + c[:-1])))
    x, y, z = slopes
    return (
        x[0],
        y[1],
        z[2],
        0.5 * (z[1] + y[2]),
        0.5 * (z[0] + x[2]),
        0.5 * (y[0] + x[1]),
    )


def force_of(stress):
    xx, yy, zz, yz, xz, xy = stress
    result = []
    for along_x, along_y, along_z in ((xx, xy, xz), (xy, yy, yz), (xz, yz, zz)):
        smooth_x = 0.5 * (along_x + z_down(along_x))
        first = 0.5 * (smooth_x + y_down(smooth_x))
        smooth_y = 0.5 * (along_y + z_down(along_y))
        slope_z = z_down(along_z) - along_z
        rest = (y_down(smooth_y) - smooth_y) + 0.5 * (slope_z + y_down(slope_z))
        result.append((first[:-1] - first[1:]) + 0.5 * (rest[1:] + rest[:-1]))
    return result


def stress_of(strain, lame, shear):
    spread = lame * (strain[0] + strain[1] + strain[2])
    twice = 2.0 * shear
    return [twice * e + spread for e in strain[:3]] + [twice * e for e in strain[3:]]


def norm_of(d):
    return d[0] * d[0] + d[1] * d[1] + d[2] * d[2] + 2.0 * (d[3] * d[3] + d[4] * d[4] + d[5] * d[5])


def relaxed(mu, size, rates):
    base = mu * mu * size
    scale = jnp.ones_like(mu)
    for rate in rates:
        f = base * scale * scale
        scale = scale * (1.0 - rate * (f / (1.0 + f)))
    return scale, base * scale * scale


def kernel(
    steps_ref, slot_ref, disp_ref, force_ref, samp_ref, mod_ref,
    wt_ref, vt_ref, vz_ref, x_ref, spec_ref,
    disp_out, row_out, micro_out,
    nb_disp, nb_force, nb_samp, modbuf, part, partbuf, strainrow,
    wh, wl, vh, vl, field, pot, disp_u, flu, flubuf,
    rowbuf, joined, respbuf, moment, momentbuf,
    near_send, near_recv, mod_send, mod_recv, part_send, part_recv,
    y_send, y_recv, resp_send, resp_recv, flu_send, flu_recv, mom_send, mom_recv,
):
    me = lax.axis_index("dev")
    group = lax.axis_index("grp")
    count = disp_ref.shape[1]

    def peer_of(i):
        return lax.rem(me + i, 32)

    barrier = pltpu.get_barrier_semaphore()

    @pl.loop(1, 32)
    def _(i):
        pl.semaphore_signal(barrier, inc=1, device_id={"dev": peer_of(i)}, device_id_type=MESH)

    for i in range(1, 4):
        pl.semaphore_signal(
            barrier, inc=1, device_id={"grp": lax.rem(group + i, 4)}, device_id_type=MESH
        )

    part[...] = jnp.zeros_like(part)

    @pl.loop(0, 32)
    def _(y):
        c, s = wt_ref[0, pl.ds(y, 1), :], wt_ref[1, pl.ds(y, 1), :]
        zr, zi = wt_ref[2], wt_ref[3]
        rows = pl.ds(pl.multiple_of(y * 32, 32), 32)
        for k, block in enumerate((c * zr + s * zi, c * zi - s * zr)):
            high, low = split(block)
            wh[rows, pl.ds(k * HALF, HALF)] = high
            wl[rows, pl.ds(k * HALF, HALF)] = low

    pl.semaphore_wait(barrier, 34)

    def near_copies(source, target, k):
        out = []
        for o, offset in enumerate(NEAR):
            out.append(
                pltpu.make_async_remote_copy(
                    src_ref=source,
                    dst_ref=target.at[3 - o],
                    send_sem=near_send.at[k, o],
                    recv_sem=near_recv.at[k, 3 - o],
                    device_id={"dev": lax.rem(me + offset + 32, 32)},
                    device_id_type=MESH,
                )
            )
        return out

    near = [
        near_copies(disp_ref, nb_disp, 0),
        near_copies(force_ref, nb_force, 1),
        near_copies(samp_ref, nb_samp, 2),
    ]
    for o in (1, 2, 3, 0):
        near[0][o].start()

    def everyone(source, target, send, recv):
        @pl.loop(1, 32)
        def _(i):
            peer = peer_of(i)
            pltpu.make_async_remote_copy(
                src_ref=source(peer),
                dst_ref=target.at[me],
                send_sem=send,
                recv_sem=recv,
                device_id={"dev": peer},
                device_id_type=MESH,
            ).start()

    def all_arrived(target, recv):
        ref = target.at[pl.ds(0, 31)]
        pltpu.make_async_copy(ref, ref, recv).wait()

    everyone(lambda peer: mod_ref.at[peer], modbuf, mod_send, mod_recv)
    for k in (1, 2):
        for copy in near[k]:
            copy.start()
    modbuf[me] = mod_ref[me]

    pltpu.make_async_copy(disp_ref, nb_disp.at[2], near_recv.at[0, 2]).wait()
    inside_up = (me < 31).astype(f32)
    fields = [
        jnp.concatenate([disp_ref[c], nb_disp[2, c][:1] * inside_up], axis=0) for c in range(3)
    ]
    strain = strain_of(fields)
    one_hots, rows_high, rows_low = [], [], []
    for plane in range(count):
        for c in range(6):
            strainrow[plane, pl.ds(c * 8, 8), :] = strain[c][plane]
        strainrow[plane, pl.ds(48, 8), :] = jnp.ones((8, 128), f32)
        strainrow[plane, pl.ds(56, 8), :] = jnp.zeros((8, 128), f32)
    for plane in range(count):
        sample = samp_ref[plane]
        for s in range(8):
            rows = strainrow[plane, pl.ds(s, 8, stride=8), :]
            high, low = split(rows)
            rows_high.append(high)
            rows_low.append(low)
            hit = jnp.broadcast_to(sample[s : s + 1], (32, 128)) == (
                row_of((32, 128)) + group * 32
            )
            one_hots.append(jnp.where(hit, 1.0, 0.0).astype(bf16))
    one_hot = jnp.concatenate(one_hots, axis=1)

    def against(rows):
        return lax.dot_general(
            one_hot,
            jnp.concatenate(rows, axis=1),
            (((1,), (1,)), ((), ())),
            preferred_element_type=f32,
        )

    sums = against(rows_high) + against(rows_low)
    for r in range(32):
        part[r, :, pl.ds(0, 8)] = sums[r : r + 1]
    everyone(lambda peer: part.at[peer], partbuf, part_send, part_recv)
    partbuf[me] = part[me]

    @pl.loop(0, 32)
    def _(k):
        c, s = vt_ref[0, pl.ds(k, 1), :], vt_ref[1, pl.ds(k, 1), :]
        zr, zi = vz_ref[0], vz_ref[1]
        for p, block in enumerate((c * zr + s * zi, c * zi - s * zr)):
            rows = pl.ds(pl.multiple_of(p * HALF + k * 16, 16), 16)
            high, low = split(block)
            vh[rows, :] = high
            vl[rows, :] = low

    ref = modbuf.at[pl.ds(0, 31)]
    pltpu.make_async_copy(ref, ref, mod_recv).wait()

    def moduli(x):
        both = modbuf[x].astype(f32)
        return both[:8], both[8:]

    def forward(slot):
        rows = jnp.concatenate(
            [field[slot, pl.ds(s, 32, stride=8), :] for s in range(8)], axis=1
        )
        high, low = split(rows)
        both = mm(jnp.concatenate([high, low], axis=0), wh[...])
        plane = both[:32] + (both[32:] + mm(high, wl[...]))
        return product(x_ref[0], jnp.concatenate([plane[:, :HALF], plane[:, HALF:]], axis=0))

    @pl.loop(0, 32)
    def _(x):
        lame, shear = moduli(x)
        field[0, pl.ds(pl.multiple_of(x * 8, 8), 8), :] = lame + (2.0 / 3.0) * shear

    spectrum_a = forward(0)

    ref = partbuf.at[pl.ds(0, 31)]
    pltpu.make_async_copy(ref, ref, part_recv).wait()
    total = jnp.sum(partbuf[...], axis=0)
    lane1 = lane_of((1, 128))

    def pick(row, k):
        return jnp.sum(jnp.where(lane1 == k, row, 0.0), axis=1, keepdims=True)

    members = pick(total, 6)
    load = [pick(total, c) / members for c in range(6)]
    trace = load[0] + load[1] + load[2]
    d = [load[c] - trace / 3.0 if c < 3 else load[c] for c in range(6)]
    own_steps = steps_ref[group * 32 + me]
    rates = [jnp.where(k < own_steps, relax_rate, 0.0).astype(f32) for k in range(KMAX)]
    size = norm_of(d)

    @pl.loop(0, 32)
    def _(x):
        _, shear = moduli(x)
        scale, _ = relaxed(shear, size, rates)
        field[1, pl.ds(pl.multiple_of(x * 8, 8), 8), :] = 2.0 * shear * scale

    spectrum_b = forward(1)
    mix = d[0] * spec_ref[1]
    for c in range(1, 6):
        mix = mix + d[c] * spec_ref[1 + c]
    scaled = spec_ref[0]
    steady = (1.0 - green_ratio) * trace
    phi = [scaled * spectrum_b[:32], scaled * spectrum_b[32:]]
    pressure = [
        scaled * (steady * spectrum_a[:32]) - mix * phi[0],
        scaled * (steady * spectrum_a[32:]) - mix * phi[1],
    ]
    mixed = jnp.concatenate(
        [
            jnp.concatenate([pressure[0], phi[0]], axis=1),
            jnp.concatenate([pressure[1], phi[1]], axis=1),
        ],
        axis=0,
    )
    back = product(x_ref[1], mixed)
    lines = jnp.concatenate(
        [
            jnp.concatenate([back[:32, :HALF], back[32:, :HALF]], axis=1),
            jnp.concatenate([back[:32, HALF:], back[32:, HALF:]], axis=1),
        ],
        axis=0,
    )
    high, low = split(lines)
    both = mm(jnp.concatenate([high, low], axis=0), vh[...])
    space = both[:64] + (both[64:] + mm(high, vl[...]))
    for k in range(2):
        for s in range(8):
            pot[k, pl.ds(s, 32, stride=8), :] = space[k * 32 : k * 32 + 32, s * 128 : s * 128 + 128]

    def at(x):
        return pl.ds(pl.multiple_of(x * 8, 8), 8)

    @pl.loop(0, 32)
    def _(x):
        after, before = lax.rem(x + 1, 32), lax.rem(x + 31, 32)
        p, q = pot[0, at(x), :], pot[1, at(x), :]
        px = 0.5 * (pot[0, at(after), :] - pot[0, at(before), :])
        qx = 0.5 * (pot[1, at(after), :] - pot[1, at(before), :])
        py, pz, qy, qz = yc(p), zc(p), yc(q), zc(q)
        disp_u[0, at(x), :] = px + d[0] * qx + d[5] * qy + d[4] * qz
        disp_u[1, at(x), :] = py + d[5] * qx + d[1] * qy + d[3] * qz
        disp_u[2, at(x), :] = pz + d[4] * qx + d[3] * qy + d[2] * qz

    def voxel(x, sums):
        after, before = lax.rem(x + 1, 32), lax.rem(x + 31, 32)
        ux, uy, uz = (disp_u[c, at(x), :] for c in range(3))
        dx = [0.5 * (disp_u[c, at(after), :] - disp_u[c, at(before), :]) for c in range(3)]
        gamma = [
            dx[0],
            yc(uy),
            zc(uz),
            0.5 * (yc(uz) + zc(uy)),
            0.5 * (dx[2] + zc(ux)),
            0.5 * (dx[1] + yc(ux)),
        ]
        flu[x] = jnp.concatenate([-g for g in gamma], axis=0).astype(wire)
        lame, shear = moduli(x)
        e = [load[c] - gamma[c] for c in range(6)]
        tr = e[0] + e[1] + e[2]
        dv = [e[c] - tr / 3.0 if c < 3 else e[c] for c in range(6)]
        scale, f = relaxed(shear, norm_of(dv), rates)
        twice = 2.0 * shear * scale
        bulk = (lame + (2.0 / 3.0) * shear) * tr
        new = [bulk + twice * dv[c] if c < 3 else twice * dv[c] for c in range(6)]
        new += [lame, shear / (1.0 + f)]
        return tuple(a + b for a, b in zip(sums, new))

    sums = lax.fori_loop(0, 32, voxel, tuple(jnp.zeros((8, 128), f32) for _ in range(8)))
    column = jnp.concatenate([jnp.sum(a, axis=0, keepdims=True) for a in sums], axis=0)
    column = jnp.sum(column, axis=1, keepdims=True) * (1.0 / VOX**3)
    lane8, row8 = lane_of((8, 128)), row_of((8, 128))
    own_row = jnp.sum(
        jnp.where(lane8 == row8 + group * 16, column, 0.0), axis=0, keepdims=True
    )
    for c in range(6):
        own_row = own_row + jnp.where(lane1 == group * 16 + 8 + c, load[c], 0.0)

    rowbuf[3] = own_row
    rows_out = []
    for i in range(1, 4):
        rows_out.append(
            pltpu.make_async_remote_copy(
                src_ref=rowbuf.at[3],
                dst_ref=rowbuf.at[i - 1],
                send_sem=y_send.at[i - 1],
                recv_sem=y_recv.at[i - 1],
                device_id={"grp": lax.rem(group + i, 4)},
                device_id_type=MESH,
            )
        )
        rows_out[-1].start()
    for copy in rows_out:
        copy.wait_recv()
    joined[0] = rowbuf[0] + rowbuf[1] + rowbuf[2] + rowbuf[3]
    everyone(lambda peer: joined.at[0], respbuf, resp_send, resp_recv)
    respbuf[me] = joined[0]
    everyone(lambda peer: flu.at[peer], flubuf, flu_send, flu_recv)
    flubuf[me] = flu[me]

    for k in range(3):
        for o in range(4):
            if k == 0 and o == 2:
                continue
            ref = (nb_disp, nb_force, nb_samp)[k].at[o]
            pltpu.make_async_copy(ref, ref, near_recv.at[k, o]).wait()
    exists = [(me * count + j >= 3).astype(f32) * (me * count + j < 67).astype(f32) for j in range(8)]

    def extended(own, near_ref, c):
        def get(ref, p):
            return ref[c, pl.ds(p, 1)] if c is not None else ref[pl.ds(p, 1)]

        planes = [get(near_ref.at[0], 1), get(near_ref.at[1], 0), get(near_ref.at[1], 1)]
        planes += [get(own, 0), get(own, 1)]
        planes += [get(near_ref.at[2], 0), get(near_ref.at[2], 1), get(near_ref.at[3], 0)]
        return planes

    def masked(planes):
        return jnp.concatenate([p * m for p, m in zip(planes, exists)], axis=0)

    around = [masked(extended(disp_ref, nb_disp, c)) for c in range(3)]
    outside = [masked(extended(force_ref, nb_force, c)) for c in range(3)]
    samples = extended(samp_ref, nb_samp, None)

    all_arrived(respbuf, resp_recv)
    gathered = jnp.concatenate([respbuf[r] for r in range(32)], axis=0)
    gathered = jnp.concatenate([gathered, jnp.zeros((96, 128), f32)], axis=0).T
    cells = []
    for c in range(8):
        row = jnp.concatenate(
            [gathered[g * 16 + c : g * 16 + c + 1, :32] for g in range(4)], axis=1
        )
        source = jnp.broadcast_to(row, (8, 128))
        cells.append(
            masked(
                [
                    jnp.take_along_axis(source, s[0], axis=1, mode="promise_in_bounds")[None]
                    for s in samples
                ]
            )
        )
    lame, shear = cells[6], cells[7]
    pull = force_of(cells[:6])
    res = [
        (outside[c][1:] - pull[c] - spring_rate * around[c][1:])
        * jnp.concatenate([jnp.full((1, 8, 128), m) for m in exists[1:]], axis=0)
        for c in range(3)
    ]

    def stiff(w, low):
        n = w[0].shape[0]
        strain = strain_of(w)
        stress = stress_of(strain, lame[low : low + n - 1], shear[low : low + n - 1])
        pull = force_of(stress)
        mask = jnp.concatenate(
            [jnp.full((1, 8, 128), m) for m in exists[low + 1 : low + n - 1]], axis=0
        )
        return [(pull[c] + spring_rate * w[c][1:-1]) * mask for c in range(3)]

    k1 = stiff(res, 1)
    k2 = stiff(k1, 2)
    r_own = [a[2:4] for a in res]
    k1_own = [a[1:3] for a in k1]
    k2_own = [a[0:2] for a in k2]
    energy_strain = strain_of(k2)
    energy_stress = stress_of(energy_strain, lame[3:5], shear[3:5])

    def dotted(a, b):
        total = a[0] * b[0]
        for c in range(1, 3):
            total = total + a[c] * b[c]
        return jnp.sum(jnp.sum(total, axis=0), axis=0, keepdims=True)

    energy = energy_strain[0] * energy_stress[0]
    for c in range(1, 6):
        energy = energy + (1.0 if c < 3 else 2.0) * energy_strain[c] * energy_stress[c]
    energy = jnp.sum(jnp.sum(energy, axis=0), axis=0, keepdims=True) + spring_rate * dotted(
        k2_own, k2_own
    )
    rows = [
        dotted(r_own, r_own),
        dotted(r_own, k1_own),
        dotted(k1_own, k1_own),
        dotted(k1_own, k2_own),
        dotted(k2_own, k2_own),
        energy,
        jnp.zeros((2, 128), f32),
    ]
    column = jnp.sum(jnp.concatenate(rows, axis=0), axis=1, keepdims=True)
    moment[0] = jnp.sum(jnp.where(lane8 == row8, column, 0.0), axis=0, keepdims=True)
    everyone(lambda peer: moment.at[0], momentbuf, mom_send, mom_recv)
    momentbuf[me] = moment[0]

    def owner(r, acc):
        taken = jnp.where(slot_ref[group * 32 + r] == me, 1.0, 0.0).astype(f32)
        return acc + taken * respbuf[r]

    row = lax.fori_loop(0, 32, owner, jnp.zeros((1, 128), f32))
    shifted = jnp.zeros((1, 128), f32)
    for g in range(4):
        here = (group == g).astype(f32)
        shifted = shifted + here * roll(row, -16 * g, 1)
    row_out[...] = jnp.broadcast_to(shifted, row_out.shape)

    table = jnp.concatenate([respbuf[r] for r in range(32)], axis=0)
    lane32 = lane_of((32, 128))
    group_load = [
        jnp.sum(jnp.where(lane32 == group * 16 + 8 + c, table, 0.0), axis=1, keepdims=True)
        for c in range(6)
    ]
    all_arrived(flubuf, flu_recv)
    for r in range(32):
        block = flubuf[r].astype(f32)
        for c in range(6):
            micro_out[pl.ds((c * 32 + r) * 8, 8), :] = (
                group_load[c][r : r + 1] + block[c * 8 : c * 8 + 8]
            )

    all_arrived(momentbuf, mom_recv)
    total = jnp.sum(momentbuf[...], axis=0)
    m = [pick(total, k) for k in range(6)]

    def form(a, b, first):
        out = 0.0
        for i, p in enumerate(a):
            for j, q in enumerate(b):
                out = out + p * q * m[i + j + first]
        return out

    rr = m[0]
    alpha0 = rr / m[1]
    r1 = (jnp.ones_like(rr), -alpha0)
    rr1 = form(r1, r1, 0)
    beta0 = rr1 / rr
    p1 = (1.0 + beta0, -alpha0)
    alpha1 = rr1 / form(p1, p1, 1)
    r2 = (jnp.ones_like(rr), -alpha0 - alpha1 * p1[0], alpha1 * alpha0)
    rr2 = form(r2, r2, 0)
    beta1 = rr2 / rr1
    p2 = (r2[0] + beta1 * p1[0], r2[1] + beta1 * p1[1], r2[2])
    alpha2 = rr2 / form(p2, p2, 1)
    weight = (
        alpha0 + alpha1 * p1[0] + alpha2 * p2[0],
        alpha1 * p1[1] + alpha2 * p2[1],
        alpha2 * p2[2],
    )
    for c in range(3):
        disp_out[c] = disp_ref[c] + (
            weight[0] * r_own[c] + weight[1] * k1_own[c] + weight[2] * k2_own[c]
        )

    for k in range(3):
        for copy in near[k]:
            copy.wait_send()
    for copy in rows_out:
        copy.wait_send()
    for buffer, sem in (
        (modbuf, mod_send), (partbuf, part_send), (respbuf, resp_send),
        (flubuf, flu_send), (momentbuf, mom_send),
    ):
        ref = buffer.at[pl.ds(0, 31)]
        pltpu.make_async_copy(ref, ref, sem).wait()


def shards(
    displacement, external_force, element_sample, lame_field, shear_field, plastic_steps, owner_slot
):
    count = displacement.shape[1]
    disp = displacement.reshape(3, count, 8, 128)
    force = external_force.reshape(3, count, 8, 128)
    sample = element_sample.reshape(count, 8, 128)
    moduli = jnp.concatenate(
        [lame_field.reshape(32, 8, 128), shear_field.reshape(32, 8, 128)], axis=1
    )
    constants = [jnp.asarray(t) for t in tables()]
    vmem = pl.BlockSpec(memory_space=pltpu.VMEM)
    smem = pl.BlockSpec(memory_space=pltpu.SMEM)
    dma = pltpu.SemaphoreType.DMA
    disp_next, row, micro = pl.pallas_call(
        kernel,
        out_shape=(
            jax.ShapeDtypeStruct(disp.shape, f32),
            jax.ShapeDtypeStruct((8, 128), f32),
            jax.ShapeDtypeStruct((6 * 32 * 8, 128), f32),
        ),
        in_specs=[smem] * 2 + [vmem] * 9,
        out_specs=(vmem,) * 3,
        scratch_shapes=[
            pltpu.VMEM((4,) + disp.shape, f32),
            pltpu.VMEM((4,) + disp.shape, f32),
            pltpu.VMEM((4,) + sample.shape, jnp.int32),
            pltpu.VMEM((32, 16, 128), bf16),
            pltpu.VMEM((32, 1, 128), f32),
            pltpu.VMEM((32, 1, 128), f32),
            pltpu.VMEM((count, 64, 128), f32),
            pltpu.VMEM((1024, 1024), bf16),
            pltpu.VMEM((1024, 1024), bf16),
            pltpu.VMEM((1024, 1024), bf16),
            pltpu.VMEM((1024, 1024), bf16),
            pltpu.VMEM((2, 256, 128), f32),
            pltpu.VMEM((2, 256, 128), f32),
            pltpu.VMEM((3, 256, 128), f32),
            pltpu.VMEM((32, 48, 128), wire),
            pltpu.VMEM((32, 48, 128), wire),
            pltpu.VMEM((4, 1, 128), f32),
            pltpu.VMEM((1, 1, 128), f32),
            pltpu.VMEM((32, 1, 128), f32),
            pltpu.VMEM((1, 1, 128), f32),
            pltpu.VMEM((32, 1, 128), f32),
            dma((3, 4)), dma((3, 4)), dma, dma, dma, dma,
            dma((3,)), dma((3,)), dma, dma, dma, dma, dma, dma,
        ],
        compiler_params=pltpu.CompilerParams(collective_id=0, has_side_effects=True),
    )(plastic_steps, owner_slot, disp, force, sample, moduli, *constants)
    return (
        disp_next.reshape(displacement.shape),
        row[:1, :8],
        micro.reshape(6, 32, 1, 1024),
    )


def solution(mesh):
    in_specs = (
        P(None, "dev", None, None),
        P(None, "dev", None, None),
        P("dev", None, None),
        P("grp", "dev", None),
        P("grp", "dev", None),
        P(),
        P(),
    )
    out_specs = (P(None, "dev", None, None), P(("grp", "dev"), None), P(None, "grp", "dev", None))
    return jax.shard_map(shards, mesh=mesh, in_specs=in_specs, out_specs=out_specs, check_vma=False)
```

```python
import jax
import jax.numpy as jnp
import numpy as np
from jax import lax
from jax.experimental import pallas as pl
from jax.experimental.pallas import tpu as pltpu
from jax.sharding import PartitionSpec as P

VOX = 32
HALF = 512
KMAX = 4
MESH = pl.DeviceIdType.MESH
NEAR = (-2, -1, 1, 2)

shear_ref = 1.65
lame_ref = 1.25
green_ratio = (lame_ref + shear_ref) / (lame_ref + 2.0 * shear_ref)
relax_rate = 0.35
spring_rate = 0.2
wire = jnp.bfloat16
f32 = jnp.float32
bf16 = jnp.bfloat16


def tables():
    n = np.arange(VOX)
    theta = 2.0 * np.pi / VOX
    ky = np.repeat(n, 16)
    kz = np.tile(np.arange(16), VOX)
    yy = np.repeat(n, VOX)
    zz = np.tile(n, VOX)
    k16 = np.arange(16)

    def zeta(z, k):
        angle = theta * (z * k % VOX)
        return (
            np.where(k == 0, 1.0, np.cos(angle)),
            np.where(k == 0, (-1.0) ** z, -np.sin(angle)),
        )

    cy, sy = np.cos(theta * (np.outer(n, ky) % VOX)), np.sin(theta * (np.outer(n, ky) % VOX))
    zr, zi = zeta(n[:, None], kz[None, :])
    cv, sv = np.cos(theta * (np.outer(n, yy) % VOX)), np.sin(theta * (np.outer(n, yy) % VOX))
    vr, vi = zeta(zz[None, :], k16[:, None])
    c, s = np.cos(theta * (np.outer(n, n) % VOX)), np.sin(theta * (np.outer(n, n) % VOX))
    x = np.block([[c, s], [-s, c]])

    def wave(k):
        return np.where(k % 16 == 0, 0.0, np.sin(theta * k))

    one = np.ones((VOX, HALF))
    xx, xy, xz = wave(n)[:, None] * one, wave(ky)[None] * one, wave(kz)[None] * one
    square = xx * xx + xy * xy + xz * xz
    inverse = np.where(square > 0, 1.0 / np.where(square > 0, square, 1.0), 0.0)
    weight = np.where(kz == 0, 1.0, 2.0)[None] * one
    scaled = -(1.0 / shear_ref) * inverse * weight / VOX**3
    pairs = (xx * xx, xy * xy, xz * xz, 2 * xy * xz, 2 * xx * xz, 2 * xx * xy)
    spectral = np.stack([scaled] + [green_ratio * p * inverse for p in pairs])
    to = lambda a: np.asarray(a, np.float32)
    return (
        to(np.stack([cy, sy, zr, zi])),
        to(np.stack([cv, sv])),
        to(np.stack([vr, vi])),
        to(np.stack([x, x.T])),
        to(spectral),
    )


def split(a):
    high = a.astype(bf16)
    return high, (a - high.astype(f32)).astype(bf16)


def mm(a, b):
    return jnp.dot(a, b, preferred_element_type=f32)


def product(a, b):
    ah, al = split(a)
    bh, bl = split(b)
    return mm(ah, bh) + (mm(al, bh) + mm(ah, bl))


def lane_of(shape):
    return lax.broadcasted_iota(jnp.int32, shape, len(shape) - 1)


def row_of(shape):
    return lax.broadcasted_iota(jnp.int32, shape, len(shape) - 2)


def roll(a, shift, axis):
    return pltpu.roll(a, shift % a.shape[axis], axis)


def z_up(v):
    return jnp.where(lane_of(v.shape) % VOX == VOX - 1, 0.0, roll(v, -1, 2))


def z_down(v):
    return jnp.where(lane_of(v.shape) % VOX == 0, 0.0, roll(v, 1, 2))


def y_up(v):
    moved = roll(v, -VOX, 2)
    next_row = jnp.where(row_of(v.shape) == 7, 0.0, roll(moved, -1, 1))
    return jnp.where(lane_of(v.shape) < 96, moved, next_row)


def y_down(v):
    moved = roll(v, VOX, 2)
    last_row = jnp.where(row_of(v.shape) == 0, 0.0, roll(moved, 1, 1))
    return jnp.where(lane_of(v.shape) >= VOX, moved, last_row)


def zc(v):
    lane = lane_of(v.shape) % VOX
    up = jnp.where(lane == VOX - 1, roll(v, 31, 1), roll(v, -1, 1))
    down = jnp.where(lane == 0, roll(v, -31, 1), roll(v, 1, 1))
    return 0.5 * (up - down)


def yc(v):
    lane = lane_of(v.shape)
    up = roll(v, -VOX, 1)
    up = jnp.where(lane < 96, up, roll(up, -1, 0))
    down = roll(v, VOX, 1)
    down = jnp.where(lane >= VOX, down, roll(down, 1, 0))
    return 0.5 * (up - down)


def strain_of(fields):
    slopes = []
    for w in fields:
        up = z_up(w)
        mz, dz = 0.5 * (w + up), up - w
        moved = y_up(mz)
        a, b = 0.5 * (mz + moved), moved - mz
        c = 0.5 * (dz + y_up(dz))
        slopes.append((a[1:] - a[:-1], 0.5 * (b[1:] + b[:-1]), 0.5 * (c[1:] + c[:-1])))
    x, y, z = slopes
    return (
        x[0],
        y[1],
        z[2],
        0.5 * (z[1] + y[2]),
        0.5 * (z[0] + x[2]),
        0.5 * (y[0] + x[1]),
    )


def force_of(stress):
    xx, yy, zz, yz, xz, xy = stress
    result = []
    for along_x, along_y, along_z in ((xx, xy, xz), (xy, yy, yz), (xz, yz, zz)):
        smooth_x = 0.5 * (along_x + z_down(along_x))
        first = 0.5 * (smooth_x + y_down(smooth_x))
        smooth_y = 0.5 * (along_y + z_down(along_y))
        slope_z = z_down(along_z) - along_z
        rest = (y_down(smooth_y) - smooth_y) + 0.5 * (slope_z + y_down(slope_z))
        result.append((first[:-1] - first[1:]) + 0.5 * (rest[1:] + rest[:-1]))
    return result


def stress_of(strain, lame, shear):
    spread = lame * (strain[0] + strain[1] + strain[2])
    twice = 2.0 * shear
    return [twice * e + spread for e in strain[:3]] + [twice * e for e in strain[3:]]


def norm_of(d):
    return d[0] * d[0] + d[1] * d[1] + d[2] * d[2] + 2.0 * (d[3] * d[3] + d[4] * d[4] + d[5] * d[5])


def relaxed(mu, size, rates):
    base = mu * mu * size
    scale = jnp.ones_like(mu)
    for rate in rates:
        f = base * scale * scale
        scale = scale * (1.0 - rate * (f / (1.0 + f)))
    return scale, base * scale * scale


def kernel(
    disp_in, wt_in, lame_in, shear_in, force_in, samp_in, vt_in, vz_in, x_in, spec_in, steps_in, slot_in,
    disp_out, row_out, micro_out,
    disp_raw, wt_ref, lame_raw, shear_raw, force_raw, samp_raw, vt_ref, vz_ref, x_ref, spec_ref,
    steps_ref, slot_ref, in_sem,
    disp_ref, force_ref, samp_ref, mod_ref, modwide,
    nb_disp, nb_force, nb_samp, modbuf, part, partbuf, strainrow,
    wh, wl, vh, vl, field, pot, disp_u, flu, flubuf,
    rowbuf, joined, respbuf, moment, momentbuf,
    near_send, near_recv, mod_send, mod_recv, part_send, part_recv,
    y_send, y_recv, resp_send, resp_recv, flu_send, flu_recv, mom_send, mom_recv,
):
    me = lax.axis_index("dev")
    group = lax.axis_index("grp")
    count = disp_raw.shape[1]

    def peer_of(i):
        return lax.rem(me + i, 32)

    loads = [
        pltpu.make_async_copy(source, target, in_sem.at[k])
        for k, (source, target) in enumerate(
            (
                (disp_in, disp_raw), (wt_in, wt_ref), (lame_in, lame_raw), (shear_in, shear_raw),
                (force_in, force_raw), (samp_in, samp_raw), (vt_in, vt_ref), (vz_in, vz_ref),
                (x_in, x_ref), (spec_in, spec_ref), (steps_in, steps_ref), (slot_in, slot_ref),
            )
        )
    ]
    for copy in loads:
        copy.start()

    barrier = pltpu.get_barrier_semaphore()

    @pl.loop(1, 32)
    def _(i):
        pl.semaphore_signal(barrier, inc=1, device_id={"dev": peer_of(i)}, device_id_type=MESH)

    for i in range(1, 4):
        pl.semaphore_signal(
            barrier, inc=1, device_id={"grp": lax.rem(group + i, 4)}, device_id_type=MESH
        )

    for k in (0, 2, 3, 4, 5):
        loads[k].wait()
    for raw, dense in ((disp_raw, disp_ref), (force_raw, force_ref), (samp_raw, samp_ref)):
        for index in np.ndindex(raw.shape[:-2]):
            dense[index] = jnp.concatenate(
                [raw[(*index, pl.ds(q, 8, stride=4), slice(None))] for q in range(4)], axis=1
            )
    for k, raw in enumerate((lame_raw, shear_raw)):
        wide = raw[...].astype(f32)
        for t in range(8):
            modwide[pl.ds(k * 8 + t, 32, stride=16), :] = wide[:, t * 128 : t * 128 + 128]
    for r in range(32):
        mod_ref[r] = modwide[pl.ds(r * 16, 16), :].astype(bf16)

    loads[1].wait()
    part[...] = jnp.zeros_like(part)

    @pl.loop(0, 32)
    def _(y):
        c, s = wt_ref[0, pl.ds(y, 1), :], wt_ref[1, pl.ds(y, 1), :]
        zr, zi = wt_ref[2], wt_ref[3]
        rows = pl.ds(pl.multiple_of(y * 32, 32), 32)
        for k, block in enumerate((c * zr + s * zi, c * zi - s * zr)):
            high, low = split(block)
            wh[rows, pl.ds(k * HALF, HALF)] = high
            wl[rows, pl.ds(k * HALF, HALF)] = low

    pl.semaphore_wait(barrier, 34)

    def near_copies(source, target, k):
        out = []
        for o, offset in enumerate(NEAR):
            out.append(
                pltpu.make_async_remote_copy(
                    src_ref=source,
                    dst_ref=target.at[3 - o],
                    send_sem=near_send.at[k, o],
                    recv_sem=near_recv.at[k, 3 - o],
                    device_id={"dev": lax.rem(me + offset + 32, 32)},
                    device_id_type=MESH,
                )
            )
        return out

    near = [
        near_copies(disp_ref, nb_disp, 0),
        near_copies(force_ref, nb_force, 1),
        near_copies(samp_ref, nb_samp, 2),
    ]
    for o in (1, 2, 3, 0):
        near[0][o].start()

    def everyone(source, target, send, recv):
        @pl.loop(1, 32)
        def _(i):
            peer = peer_of(i)
            pltpu.make_async_remote_copy(
                src_ref=source(peer),
                dst_ref=target.at[me],
                send_sem=send,
                recv_sem=recv,
                device_id={"dev": peer},
                device_id_type=MESH,
            ).start()

    def all_arrived(target, recv):
        ref = target.at[pl.ds(0, 31)]
        pltpu.make_async_copy(ref, ref, recv).wait()

    everyone(lambda peer: mod_ref.at[peer], modbuf, mod_send, mod_recv)
    for k in (1, 2):
        for copy in near[k]:
            copy.start()
    modbuf[me] = mod_ref[me]

    pltpu.make_async_copy(disp_ref, nb_disp.at[2], near_recv.at[0, 2]).wait()
    inside_up = (me < 31).astype(f32)
    fields = [
        jnp.concatenate([disp_ref[c], nb_disp[2, c][:1] * inside_up], axis=0) for c in range(3)
    ]
    strain = strain_of(fields)
    one_hots, rows_high, rows_low = [], [], []
    for plane in range(count):
        for c in range(6):
            strainrow[plane, pl.ds(c * 8, 8), :] = strain[c][plane]
        strainrow[plane, pl.ds(48, 8), :] = jnp.ones((8, 128), f32)
        strainrow[plane, pl.ds(56, 8), :] = jnp.zeros((8, 128), f32)
    for plane in range(count):
        sample = samp_ref[plane]
        for s in range(8):
            rows = strainrow[plane, pl.ds(s, 8, stride=8), :]
            high, low = split(rows)
            rows_high.append(high)
            rows_low.append(low)
            hit = jnp.broadcast_to(sample[s : s + 1], (32, 128)) == (
                row_of((32, 128)) + group * 32
            )
            one_hots.append(jnp.where(hit, 1.0, 0.0).astype(bf16))
    one_hot = jnp.concatenate(one_hots, axis=1)

    def against(rows):
        return lax.dot_general(
            one_hot,
            jnp.concatenate(rows, axis=1),
            (((1,), (1,)), ((), ())),
            preferred_element_type=f32,
        )

    sums = against(rows_high) + against(rows_low)
    for r in range(32):
        part[r, :, pl.ds(0, 8)] = sums[r : r + 1]
    everyone(lambda peer: part.at[peer], partbuf, part_send, part_recv)
    partbuf[me] = part[me]
    for k in range(6, 12):
        loads[k].wait()

    @pl.loop(0, 32)
    def _(k):
        c, s = vt_ref[0, pl.ds(k, 1), :], vt_ref[1, pl.ds(k, 1), :]
        zr, zi = vz_ref[0], vz_ref[1]
        for p, block in enumerate((c * zr + s * zi, c * zi - s * zr)):
            rows = pl.ds(pl.multiple_of(p * HALF + k * 16, 16), 16)
            high, low = split(block)
            vh[rows, :] = high
            vl[rows, :] = low

    ref = modbuf.at[pl.ds(0, 31)]
    pltpu.make_async_copy(ref, ref, mod_recv).wait()

    def moduli(x):
        both = modbuf[x].astype(f32)
        return both[:8], both[8:]

    def forward(slot):
        rows = jnp.concatenate(
            [field[slot, pl.ds(s, 32, stride=8), :] for s in range(8)], axis=1
        )
        high, low = split(rows)
        both = mm(jnp.concatenate([high, low], axis=0), wh[...])
        plane = both[:32] + (both[32:] + mm(high, wl[...]))
        return product(x_ref[0], jnp.concatenate([plane[:, :HALF], plane[:, HALF:]], axis=0))

    @pl.loop(0, 32)
    def _(x):
        lame, shear = moduli(x)
        field[0, pl.ds(pl.multiple_of(x * 8, 8), 8), :] = lame + (2.0 / 3.0) * shear

    spectrum_a = forward(0)

    ref = partbuf.at[pl.ds(0, 31)]
    pltpu.make_async_copy(ref, ref, part_recv).wait()
    total = jnp.sum(partbuf[...], axis=0)
    lane1 = lane_of((1, 128))

    def pick(row, k):
        return jnp.sum(jnp.where(lane1 == k, row, 0.0), axis=1, keepdims=True)

    members = pick(total, 6)
    load = [pick(total, c) / members for c in range(6)]
    trace = load[0] + load[1] + load[2]
    d = [load[c] - trace / 3.0 if c < 3 else load[c] for c in range(6)]
    own_steps = steps_ref[group * 32 + me]
    rates = [jnp.where(k < own_steps, relax_rate, 0.0).astype(f32) for k in range(KMAX)]
    size = norm_of(d)

    @pl.loop(0, 32)
    def _(x):
        _, shear = moduli(x)
        scale, _ = relaxed(shear, size, rates)
        field[1, pl.ds(pl.multiple_of(x * 8, 8), 8), :] = 2.0 * shear * scale

    spectrum_b = forward(1)
    mix = d[0] * spec_ref[1]
    for c in range(1, 6):
        mix = mix + d[c] * spec_ref[1 + c]
    scaled = spec_ref[0]
    steady = (1.0 - green_ratio) * trace
    phi = [scaled * spectrum_b[:32], scaled * spectrum_b[32:]]
    pressure = [
        scaled * (steady * spectrum_a[:32]) - mix * phi[0],
        scaled * (steady * spectrum_a[32:]) - mix * phi[1],
    ]
    mixed = jnp.concatenate(
        [
            jnp.concatenate([pressure[0], phi[0]], axis=1),
            jnp.concatenate([pressure[1], phi[1]], axis=1),
        ],
        axis=0,
    )
    back = product(x_ref[1], mixed)
    lines = jnp.concatenate(
        [
            jnp.concatenate([back[:32, :HALF], back[32:, :HALF]], axis=1),
            jnp.concatenate([back[:32, HALF:], back[32:, HALF:]], axis=1),
        ],
        axis=0,
    )
    high, low = split(lines)
    both = mm(jnp.concatenate([high, low], axis=0), vh[...])
    space = both[:64] + (both[64:] + mm(high, vl[...]))
    for k in range(2):
        for s in range(8):
            pot[k, pl.ds(s, 32, stride=8), :] = space[k * 32 : k * 32 + 32, s * 128 : s * 128 + 128]

    def at(x):
        return pl.ds(pl.multiple_of(x * 8, 8), 8)

    @pl.loop(0, 32)
    def _(x):
        after, before = lax.rem(x + 1, 32), lax.rem(x + 31, 32)
        p, q = pot[0, at(x), :], pot[1, at(x), :]
        px = 0.5 * (pot[0, at(after), :] - pot[0, at(before), :])
        qx = 0.5 * (pot[1, at(after), :] - pot[1, at(before), :])
        py, pz, qy, qz = yc(p), zc(p), yc(q), zc(q)
        disp_u[0, at(x), :] = px + d[0] * qx + d[5] * qy + d[4] * qz
        disp_u[1, at(x), :] = py + d[5] * qx + d[1] * qy + d[3] * qz
        disp_u[2, at(x), :] = pz + d[4] * qx + d[3] * qy + d[2] * qz

    def voxel(x, sums):
        after, before = lax.rem(x + 1, 32), lax.rem(x + 31, 32)
        ux, uy, uz = (disp_u[c, at(x), :] for c in range(3))
        dx = [0.5 * (disp_u[c, at(after), :] - disp_u[c, at(before), :]) for c in range(3)]
        gamma = [
            dx[0],
            yc(uy),
            zc(uz),
            0.5 * (yc(uz) + zc(uy)),
            0.5 * (dx[2] + zc(ux)),
            0.5 * (dx[1] + yc(ux)),
        ]
        flu[x] = jnp.concatenate([-g for g in gamma], axis=0).astype(wire)
        lame, shear = moduli(x)
        e = [load[c] - gamma[c] for c in range(6)]
        tr = e[0] + e[1] + e[2]
        dv = [e[c] - tr / 3.0 if c < 3 else e[c] for c in range(6)]
        scale, f = relaxed(shear, norm_of(dv), rates)
        twice = 2.0 * shear * scale
        bulk = (lame + (2.0 / 3.0) * shear) * tr
        new = [bulk + twice * dv[c] if c < 3 else twice * dv[c] for c in range(6)]
        new += [lame, shear / (1.0 + f)]
        return tuple(a + b for a, b in zip(sums, new))

    sums = lax.fori_loop(0, 32, voxel, tuple(jnp.zeros((8, 128), f32) for _ in range(8)))
    column = jnp.concatenate([jnp.sum(a, axis=0, keepdims=True) for a in sums], axis=0)
    column = jnp.sum(column, axis=1, keepdims=True) * (1.0 / VOX**3)
    lane8, row8 = lane_of((8, 128)), row_of((8, 128))
    own_row = jnp.sum(
        jnp.where(lane8 == row8 + group * 16, column, 0.0), axis=0, keepdims=True
    )
    for c in range(6):
        own_row = own_row + jnp.where(lane1 == group * 16 + 8 + c, load[c], 0.0)

    rowbuf[3] = own_row
    rows_out = []
    for i in range(1, 4):
        rows_out.append(
            pltpu.make_async_remote_copy(
                src_ref=rowbuf.at[3],
                dst_ref=rowbuf.at[i - 1],
                send_sem=y_send.at[i - 1],
                recv_sem=y_recv.at[i - 1],
                device_id={"grp": lax.rem(group + i, 4)},
                device_id_type=MESH,
            )
        )
        rows_out[-1].start()
    for copy in rows_out:
        copy.wait_recv()
    joined[0] = rowbuf[0] + rowbuf[1] + rowbuf[2] + rowbuf[3]
    everyone(lambda peer: joined.at[0], respbuf, resp_send, resp_recv)
    respbuf[me] = joined[0]
    everyone(lambda peer: flu.at[peer], flubuf, flu_send, flu_recv)
    flubuf[me] = flu[me]

    for k in range(3):
        for o in range(4):
            if k == 0 and o == 2:
                continue
            ref = (nb_disp, nb_force, nb_samp)[k].at[o]
            pltpu.make_async_copy(ref, ref, near_recv.at[k, o]).wait()
    exists = [(me * count + j >= 3).astype(f32) * (me * count + j < 67).astype(f32) for j in range(8)]

    def extended(own, near_ref, c):
        def get(ref, p):
            return ref[c, pl.ds(p, 1)] if c is not None else ref[pl.ds(p, 1)]

        planes = [get(near_ref.at[0], 1), get(near_ref.at[1], 0), get(near_ref.at[1], 1)]
        planes += [get(own, 0), get(own, 1)]
        planes += [get(near_ref.at[2], 0), get(near_ref.at[2], 1), get(near_ref.at[3], 0)]
        return planes

    def masked(planes):
        return jnp.concatenate([p * m for p, m in zip(planes, exists)], axis=0)

    around = [masked(extended(disp_ref, nb_disp, c)) for c in range(3)]
    outside = [masked(extended(force_ref, nb_force, c)) for c in range(3)]
    samples = extended(samp_ref, nb_samp, None)

    all_arrived(respbuf, resp_recv)
    gathered = jnp.concatenate([respbuf[r] for r in range(32)], axis=0)
    gathered = jnp.concatenate([gathered, jnp.zeros((96, 128), f32)], axis=0).T
    cells = []
    for c in range(8):
        row = jnp.concatenate(
            [gathered[g * 16 + c : g * 16 + c + 1, :32] for g in range(4)], axis=1
        )
        source = jnp.broadcast_to(row, (8, 128))
        cells.append(
            masked(
                [
                    jnp.take_along_axis(source, s[0], axis=1, mode="promise_in_bounds")[None]
                    for s in samples
                ]
            )
        )
    lame, shear = cells[6], cells[7]
    pull = force_of(cells[:6])
    res = [
        (outside[c][1:] - pull[c] - spring_rate * around[c][1:])
        * jnp.concatenate([jnp.full((1, 8, 128), m) for m in exists[1:]], axis=0)
        for c in range(3)
    ]

    def stiff(w, low):
        n = w[0].shape[0]
        strain = strain_of(w)
        stress = stress_of(strain, lame[low : low + n - 1], shear[low : low + n - 1])
        pull = force_of(stress)
        mask = jnp.concatenate(
            [jnp.full((1, 8, 128), m) for m in exists[low + 1 : low + n - 1]], axis=0
        )
        return [(pull[c] + spring_rate * w[c][1:-1]) * mask for c in range(3)]

    k1 = stiff(res, 1)
    k2 = stiff(k1, 2)
    r_own = [a[2:4] for a in res]
    k1_own = [a[1:3] for a in k1]
    k2_own = [a[0:2] for a in k2]
    energy_strain = strain_of(k2)
    energy_stress = stress_of(energy_strain, lame[3:5], shear[3:5])

    def dotted(a, b):
        total = a[0] * b[0]
        for c in range(1, 3):
            total = total + a[c] * b[c]
        return jnp.sum(jnp.sum(total, axis=0), axis=0, keepdims=True)

    energy = energy_strain[0] * energy_stress[0]
    for c in range(1, 6):
        energy = energy + (1.0 if c < 3 else 2.0) * energy_strain[c] * energy_stress[c]
    energy = jnp.sum(jnp.sum(energy, axis=0), axis=0, keepdims=True) + spring_rate * dotted(
        k2_own, k2_own
    )
    rows = [
        dotted(r_own, r_own),
        dotted(r_own, k1_own),
        dotted(k1_own, k1_own),
        dotted(k1_own, k2_own),
        dotted(k2_own, k2_own),
        energy,
        jnp.zeros((2, 128), f32),
    ]
    column = jnp.sum(jnp.concatenate(rows, axis=0), axis=1, keepdims=True)
    moment[0] = jnp.sum(jnp.where(lane8 == row8, column, 0.0), axis=0, keepdims=True)
    everyone(lambda peer: moment.at[0], momentbuf, mom_send, mom_recv)
    momentbuf[me] = moment[0]

    def owner(r, acc):
        taken = jnp.where(slot_ref[group * 32 + r] == me, 1.0, 0.0).astype(f32)
        return acc + taken * respbuf[r]

    row = lax.fori_loop(0, 32, owner, jnp.zeros((1, 128), f32))
    shifted = jnp.zeros((1, 128), f32)
    for g in range(4):
        here = (group == g).astype(f32)
        shifted = shifted + here * roll(row, -16 * g, 1)
    row_out[...] = shifted[:, :8]

    table = jnp.concatenate([respbuf[r] for r in range(32)], axis=0)
    lane32 = lane_of((32, 128))
    group_load = [
        jnp.sum(jnp.where(lane32 == group * 16 + 8 + c, table, 0.0), axis=1, keepdims=True)
        for c in range(6)
    ]
    all_arrived(flubuf, flu_recv)
    for r in range(32):
        block = flubuf[r].astype(f32)
        for c in range(6):
            micro_out[pl.ds((c * 32 + r) * 8, 8), :] = (
                group_load[c][r : r + 1] + block[c * 8 : c * 8 + 8]
            )

    all_arrived(momentbuf, mom_recv)
    total = jnp.sum(momentbuf[...], axis=0)
    m = [pick(total, k) for k in range(6)]

    def form(a, b, first):
        out = 0.0
        for i, p in enumerate(a):
            for j, q in enumerate(b):
                out = out + p * q * m[i + j + first]
        return out

    rr = m[0]
    alpha0 = rr / m[1]
    r1 = (jnp.ones_like(rr), -alpha0)
    rr1 = form(r1, r1, 0)
    beta0 = rr1 / rr
    p1 = (1.0 + beta0, -alpha0)
    alpha1 = rr1 / form(p1, p1, 1)
    r2 = (jnp.ones_like(rr), -alpha0 - alpha1 * p1[0], alpha1 * alpha0)
    rr2 = form(r2, r2, 0)
    beta1 = rr2 / rr1
    p2 = (r2[0] + beta1 * p1[0], r2[1] + beta1 * p1[1], r2[2])
    alpha2 = rr2 / form(p2, p2, 1)
    weight = (
        alpha0 + alpha1 * p1[0] + alpha2 * p2[0],
        alpha1 * p1[1] + alpha2 * p2[1],
        alpha2 * p2[2],
    )
    for c in range(3):
        new = disp_ref[c] + (
            weight[0] * r_own[c] + weight[1] * k1_own[c] + weight[2] * k2_own[c]
        )
        for p in range(count):
            for q in range(4):
                disp_out[c, p, pl.ds(q, 8, stride=4), :] = new[p][:, q * 32 : q * 32 + 32]

    for k in range(3):
        for copy in near[k]:
            copy.wait_send()
    for copy in rows_out:
        copy.wait_send()
    for buffer, sem in (
        (modbuf, mod_send), (partbuf, part_send), (respbuf, resp_send),
        (flubuf, flu_send), (momentbuf, mom_send),
    ):
        ref = buffer.at[pl.ds(0, 31)]
        pltpu.make_async_copy(ref, ref, sem).wait()


def shards(
    displacement, external_force, element_sample, lame_field, shear_field, plastic_steps, owner_slot
):
    count = displacement.shape[1]
    disp, sample = (3, count, 8, 128), (count, 8, 128)
    wt, vt, vz, x, spec = (jnp.asarray(t) for t in tables())
    operands = (
        displacement,
        wt,
        lame_field.reshape(32, 1024),
        shear_field.reshape(32, 1024),
        external_force,
        element_sample,
        vt,
        vz,
        x,
        spec,
    )
    scalars = (plastic_steps, owner_slot)
    vmem = pl.BlockSpec(memory_space=pltpu.VMEM)
    hbm = pl.BlockSpec(memory_space=pltpu.HBM)
    dma = pltpu.SemaphoreType.DMA
    disp_next, row, micro = pl.pallas_call(
        kernel,
        out_shape=(
            jax.ShapeDtypeStruct(displacement.shape, f32),
            jax.ShapeDtypeStruct((1, 8), f32),
            jax.ShapeDtypeStruct((6 * 32 * 8, 128), f32),
        ),
        in_specs=[hbm] * 12,
        out_specs=(vmem,) * 3,
        scratch_shapes=[
            *(pltpu.VMEM(a.shape, a.dtype) for a in operands),
            *(pltpu.SMEM(a.shape, a.dtype) for a in scalars),
            dma((12,)),
            pltpu.VMEM(disp, f32),
            pltpu.VMEM(disp, f32),
            pltpu.VMEM(sample, jnp.int32),
            pltpu.VMEM((32, 16, 128), bf16),
            pltpu.VMEM((512, 128), f32),
            pltpu.VMEM((4,) + disp, f32),
            pltpu.VMEM((4,) + disp, f32),
            pltpu.VMEM((4,) + sample, jnp.int32),
            pltpu.VMEM((32, 16, 128), bf16),
            pltpu.VMEM((32, 1, 128), f32),
            pltpu.VMEM((32, 1, 128), f32),
            pltpu.VMEM((count, 64, 128), f32),
            pltpu.VMEM((1024, 1024), bf16),
            pltpu.VMEM((1024, 1024), bf16),
            pltpu.VMEM((1024, 1024), bf16),
            pltpu.VMEM((1024, 1024), bf16),
            pltpu.VMEM((2, 256, 128), f32),
            pltpu.VMEM((2, 256, 128), f32),
            pltpu.VMEM((3, 256, 128), f32),
            pltpu.VMEM((32, 48, 128), wire),
            pltpu.VMEM((32, 48, 128), wire),
            pltpu.VMEM((4, 1, 128), f32),
            pltpu.VMEM((1, 1, 128), f32),
            pltpu.VMEM((32, 1, 128), f32),
            pltpu.VMEM((1, 1, 128), f32),
            pltpu.VMEM((32, 1, 128), f32),
            dma((3, 4)), dma((3, 4)), dma, dma, dma, dma,
            dma((3,)), dma((3,)), dma, dma, dma, dma, dma, dma,
        ],
        compiler_params=pltpu.CompilerParams(collective_id=0, has_side_effects=True, vmem_limit_bytes=24 << 20),
    )(*[pltpu.with_memory_space_constraint(a, pltpu.HBM) for a in operands + scalars])
    return disp_next, row, micro.reshape(6, 32, 1, 1024)


def solution(mesh):
    in_specs = (
        P(None, "dev", None, None),
        P(None, "dev", None, None),
        P("dev", None, None),
        P("grp", "dev", None),
        P("grp", "dev", None),
        P(),
        P(),
    )
    out_specs = (P(None, "dev", None, None), P(("grp", "dev"), None), P(None, "grp", "dev", None))
    return jax.shard_map(shards, mesh=mesh, in_specs=in_specs, out_specs=out_specs, check_vma=False)
```

```python
import jax
import jax.numpy as jnp
import numpy as np
from jax import lax
from jax.experimental import pallas as pl
from jax.experimental.pallas import tpu as pltpu
from jax.sharding import PartitionSpec as P

VOX = 32
HALF = 512
KMAX = 4
MESH = pl.DeviceIdType.MESH
NEAR = (-2, -1, 1, 2)

shear_ref = 1.65
lame_ref = 1.25
green_ratio = (lame_ref + shear_ref) / (lame_ref + 2.0 * shear_ref)
relax_rate = 0.35
spring_rate = 0.2
wire = jnp.bfloat16
f32 = jnp.float32
bf16 = jnp.bfloat16


def tables():
    n = np.arange(VOX)
    theta = 2.0 * np.pi / VOX
    ky = np.repeat(n, 16)
    kz = np.tile(np.arange(16), VOX)
    yy = np.repeat(n, VOX)
    zz = np.tile(n, VOX)
    k16 = np.arange(16)

    def zeta(z, k):
        angle = theta * (z * k % VOX)
        return (
            np.where(k == 0, 1.0, np.cos(angle)),
            np.where(k == 0, (-1.0) ** z, -np.sin(angle)),
        )

    cy, sy = np.cos(theta * (np.outer(n, ky) % VOX)), np.sin(theta * (np.outer(n, ky) % VOX))
    zr, zi = zeta(n[:, None], kz[None, :])
    cv, sv = np.cos(theta * (np.outer(n, yy) % VOX)), np.sin(theta * (np.outer(n, yy) % VOX))
    vr, vi = zeta(zz[None, :], k16[:, None])
    c, s = np.cos(theta * (np.outer(n, n) % VOX)), np.sin(theta * (np.outer(n, n) % VOX))
    x = np.block([[c, s], [-s, c]])

    def wave(k):
        return np.where(k % 16 == 0, 0.0, np.sin(theta * k))

    one = np.ones((VOX, HALF))
    xx, xy, xz = wave(n)[:, None] * one, wave(ky)[None] * one, wave(kz)[None] * one
    square = xx * xx + xy * xy + xz * xz
    inverse = np.where(square > 0, 1.0 / np.where(square > 0, square, 1.0), 0.0)
    weight = np.where(kz == 0, 1.0, 2.0)[None] * one
    scaled = -(1.0 / shear_ref) * inverse * weight / VOX**3
    pairs = (xx * xx, xy * xy, xz * xz, 2 * xy * xz, 2 * xx * xz, 2 * xx * xy)
    spectral = np.stack([scaled] + [green_ratio * p * inverse for p in pairs])
    to = lambda a: np.asarray(a, np.float32)
    return (
        to(np.stack([cy, sy, zr, zi])),
        to(np.stack([cv, sv])),
        to(np.stack([vr, vi])),
        to(np.stack([x, x.T])),
        to(spectral),
    )


def split(a):
    high = a.astype(bf16)
    return high, (a - high.astype(f32)).astype(bf16)


def mm(a, b):
    return jnp.dot(a, b, preferred_element_type=f32)


def product(a, b):
    ah, al = split(a)
    bh, bl = split(b)
    return mm(ah, bh) + (mm(al, bh) + mm(ah, bl))


def lane_of(shape):
    return lax.broadcasted_iota(jnp.int32, shape, len(shape) - 1)


def row_of(shape):
    return lax.broadcasted_iota(jnp.int32, shape, len(shape) - 2)


def roll(a, shift, axis):
    return pltpu.roll(a, shift % a.shape[axis], axis)


def z_up(v):
    return jnp.where(lane_of(v.shape) % VOX == VOX - 1, 0.0, roll(v, -1, 2))


def z_down(v):
    return jnp.where(lane_of(v.shape) % VOX == 0, 0.0, roll(v, 1, 2))


def y_up(v):
    moved = roll(v, -VOX, 2)
    next_row = jnp.where(row_of(v.shape) == 7, 0.0, roll(moved, -1, 1))
    return jnp.where(lane_of(v.shape) < 96, moved, next_row)


def y_down(v):
    moved = roll(v, VOX, 2)
    last_row = jnp.where(row_of(v.shape) == 0, 0.0, roll(moved, 1, 1))
    return jnp.where(lane_of(v.shape) >= VOX, moved, last_row)


def zc(v):
    lane = lane_of(v.shape) % VOX
    up = jnp.where(lane == VOX - 1, roll(v, 31, 2), roll(v, -1, 2))
    down = jnp.where(lane == 0, roll(v, -31, 2), roll(v, 1, 2))
    return 0.5 * (up - down)


def yc(v):
    lane = lane_of(v.shape)
    up = roll(v, -VOX, 2)
    up = jnp.where(lane < 96, up, roll(up, -1, 1))
    down = roll(v, VOX, 2)
    down = jnp.where(lane >= VOX, down, roll(down, 1, 1))
    return 0.5 * (up - down)


def spans(distance):
    return min(distance, 4 - distance)


OTHERS = sorted(
    ((a, b, c) for a in range(4) for b in range(4) for c in range(2) if (a, b, c) != (0, 0, 0)),
    key=lambda p: (-spans(p[0]) - spans(p[1]), -p[2], p),
)


def strain_of(fields):
    slopes = []
    for w in fields:
        up = z_up(w)
        mz, dz = 0.5 * (w + up), up - w
        moved = y_up(mz)
        a, b = 0.5 * (mz + moved), moved - mz
        c = 0.5 * (dz + y_up(dz))
        slopes.append((a[1:] - a[:-1], 0.5 * (b[1:] + b[:-1]), 0.5 * (c[1:] + c[:-1])))
    x, y, z = slopes
    return (
        x[0],
        y[1],
        z[2],
        0.5 * (z[1] + y[2]),
        0.5 * (z[0] + x[2]),
        0.5 * (y[0] + x[1]),
    )


def force_of(stress):
    xx, yy, zz, yz, xz, xy = stress
    result = []
    for along_x, along_y, along_z in ((xx, xy, xz), (xy, yy, yz), (xz, yz, zz)):
        smooth_x = 0.5 * (along_x + z_down(along_x))
        first = 0.5 * (smooth_x + y_down(smooth_x))
        smooth_y = 0.5 * (along_y + z_down(along_y))
        slope_z = z_down(along_z) - along_z
        rest = (y_down(smooth_y) - smooth_y) + 0.5 * (slope_z + y_down(slope_z))
        result.append((first[:-1] - first[1:]) + 0.5 * (rest[1:] + rest[:-1]))
    return result


def stress_of(strain, lame, shear):
    spread = lame * (strain[0] + strain[1] + strain[2])
    twice = 2.0 * shear
    return [twice * e + spread for e in strain[:3]] + [twice * e for e in strain[3:]]


def norm_of(d):
    return d[0] * d[0] + d[1] * d[1] + d[2] * d[2] + 2.0 * (d[3] * d[3] + d[4] * d[4] + d[5] * d[5])


def relaxed(mu, size, rates):
    base = mu * mu * size
    scale = jnp.ones_like(mu)
    for rate in rates:
        f = base * scale * scale
        scale = scale * (1.0 - rate * (f / (1.0 + f)))
    return scale, base * scale * scale


def kernel(
    disp_in, wt_in, lame_in, shear_in, force_in, samp_in, vt_in, vz_in, x_in, spec_in, steps_in, slot_in,
    disp_out, row_out, micro_out,
    disp_raw, wt_ref, lame_raw, shear_raw, force_raw, samp_raw, vt_ref, vz_ref, x_ref, spec_ref,
    steps_ref, slot_ref, in_sem,
    disp_ref, force_ref, samp_ref, mod_ref, modwide,
    nb_first, nb_disp, nb_force, nb_samp, modbuf, part, partbuf, strainrow,
    wh, wl, vh, vl, field, pot, disp_u, gam, flu, flubuf,
    rowbuf, joined, respbuf, moment, momentbuf,
    first_sem, near_send, near_recv, mod_send, mod_recv, part_send, part_recv,
    y_send, y_recv, resp_send, resp_recv, flu_send, flu_recv, mom_send, mom_recv,
):
    me = lax.axis_index("dev")
    group = lax.axis_index("grp")
    count = disp_raw.shape[1]

    me_x, me_z, me_c = me // 8, lax.rem(me // 2, 4), lax.rem(me, 2)
    at_x = [lax.rem(me_x + k, 4) * 8 for k in range(4)]
    at_z = [lax.rem(me_z + k, 4) * 2 for k in range(4)]
    at_c = [me_c, 1 - me_c]
    peers = [at_x[a] + at_z[b] + at_c[c] for a, b, c in OTHERS]

    loads = [
        pltpu.make_async_copy(source, target, in_sem.at[k])
        for k, (source, target) in enumerate(
            (
                (disp_in, disp_raw), (wt_in, wt_ref), (lame_in, lame_raw), (shear_in, shear_raw),
                (force_in, force_raw), (samp_in, samp_raw), (vt_in, vt_ref), (vz_in, vz_ref),
                (x_in, x_ref), (spec_in, spec_ref), (steps_in, steps_ref), (slot_in, slot_ref),
            )
        )
    ]
    for copy in loads:
        copy.start()

    barrier = pltpu.get_barrier_semaphore()

    for peer in peers:
        pl.semaphore_signal(barrier, inc=1, device_id={"dev": peer}, device_id_type=MESH)
    for i in range(1, 4):
        pl.semaphore_signal(
            barrier, inc=1, device_id={"grp": lax.rem(group + i, 4)}, device_id_type=MESH
        )

    for k in (0, 2, 3, 4, 5):
        loads[k].wait()
    for raw, dense in ((disp_raw, disp_ref), (force_raw, force_ref), (samp_raw, samp_ref)):
        for index in np.ndindex(raw.shape[:-2]):
            dense[index] = jnp.concatenate(
                [raw[(*index, pl.ds(q, 8, stride=4), slice(None))] for q in range(4)], axis=1
            )
    for k, raw in enumerate((lame_raw, shear_raw)):
        wide = raw[...].astype(f32)
        for t in range(8):
            modwide[pl.ds(k * 8 + t, 32, stride=16), :] = wide[:, t * 128 : t * 128 + 128]
    for r in range(32):
        mod_ref[r] = modwide[pl.ds(r * 16, 16), :].astype(bf16)

    part[...] = jnp.zeros_like(part)
    pl.semaphore_wait(barrier, 34)

    def near_copies(source, target, k):
        out = []
        for o, offset in enumerate(NEAR):
            out.append(
                pltpu.make_async_remote_copy(
                    src_ref=source,
                    dst_ref=target.at[3 - o],
                    send_sem=near_send.at[k, o],
                    recv_sem=near_recv.at[k, 3 - o],
                    device_id={"dev": lax.rem(me + offset + 32, 32)},
                    device_id_type=MESH,
                )
            )
        return out

    near = [
        near_copies(disp_ref, nb_disp, 0),
        near_copies(force_ref, nb_force, 1),
        near_copies(samp_ref, nb_samp, 2),
    ]
    first_plane = pltpu.make_async_remote_copy(
        src_ref=disp_ref.at[:, 0],
        dst_ref=nb_first,
        send_sem=first_sem.at[0],
        recv_sem=first_sem.at[1],
        device_id={"dev": lax.rem(me + 31, 32)},
        device_id_type=MESH,
    )
    first_plane.start()

    def everyone(source, target, send, recv):
        for peer in peers:
            pltpu.make_async_remote_copy(
                src_ref=source(peer),
                dst_ref=target.at[me],
                send_sem=send,
                recv_sem=recv,
                device_id={"dev": peer},
                device_id_type=MESH,
            ).start()

    def all_arrived(target, recv):
        ref = target.at[pl.ds(0, 31)]
        pltpu.make_async_copy(ref, ref, recv).wait()

    everyone(lambda peer: mod_ref.at[peer], modbuf, mod_send, mod_recv)
    modbuf[me] = mod_ref[me]

    loads[1].wait()

    @pl.loop(0, 32)
    def _(y):
        c, s = wt_ref[0, pl.ds(y, 1), :], wt_ref[1, pl.ds(y, 1), :]
        zr, zi = wt_ref[2], wt_ref[3]
        rows = pl.ds(pl.multiple_of(y * 32, 32), 32)
        for k, block in enumerate((c * zr + s * zi, c * zi - s * zr)):
            high, low = split(block)
            wh[rows, pl.ds(k * HALF, HALF)] = high
            wl[rows, pl.ds(k * HALF, HALF)] = low

    first_plane.wait_recv()
    inside_up = (me < 31).astype(f32)
    fields = [
        jnp.concatenate([disp_ref[c], nb_first[pl.ds(c, 1)] * inside_up], axis=0) for c in range(3)
    ]
    strain = strain_of(fields)
    one_hots, rows_high, rows_low = [], [], []
    for plane in range(count):
        for c in range(6):
            strainrow[plane, pl.ds(c * 8, 8), :] = strain[c][plane]
        strainrow[plane, pl.ds(48, 8), :] = jnp.ones((8, 128), f32)
        strainrow[plane, pl.ds(56, 8), :] = jnp.zeros((8, 128), f32)
    for plane in range(count):
        sample = samp_ref[plane]
        for s in range(8):
            rows = strainrow[plane, pl.ds(s, 8, stride=8), :]
            high, low = split(rows)
            rows_high.append(high)
            rows_low.append(low)
            hit = jnp.broadcast_to(sample[s : s + 1], (32, 128)) == (
                row_of((32, 128)) + group * 32
            )
            one_hots.append(jnp.where(hit, 1.0, 0.0).astype(bf16))
    one_hot = jnp.concatenate(one_hots, axis=1)

    def against(rows):
        return lax.dot_general(
            one_hot,
            jnp.concatenate(rows, axis=1),
            (((1,), (1,)), ((), ())),
            preferred_element_type=f32,
        )

    sums = against(rows_high) + against(rows_low)
    for r in range(32):
        part[r, :, pl.ds(0, 8)] = sums[r : r + 1]
    everyone(lambda peer: part.at[peer], partbuf, part_send, part_recv)
    partbuf[me] = part[me]
    for k in range(3):
        for copy in near[k]:
            copy.start()
    for k in range(6, 12):
        loads[k].wait()

    @pl.loop(0, 32)
    def _(k):
        c, s = vt_ref[0, pl.ds(k, 1), :], vt_ref[1, pl.ds(k, 1), :]
        zr, zi = vz_ref[0], vz_ref[1]
        for p, block in enumerate((c * zr + s * zi, c * zi - s * zr)):
            rows = pl.ds(pl.multiple_of(p * HALF + k * 16, 16), 16)
            high, low = split(block)
            vh[rows, :] = high
            vl[rows, :] = low

    ref = modbuf.at[pl.ds(0, 31)]
    pltpu.make_async_copy(ref, ref, mod_recv).wait()

    def moduli(x, n):
        both = modbuf[pl.ds(x, n)].astype(f32)
        return both[:, :8], both[:, 8:]

    def at(x, n):
        return pl.ds(pl.multiple_of(x * 8, 8), n * 8)

    def planes(ref, k, x, n):
        return ref[k, at(x, n), :].reshape(n, 8, 128)

    def x_slope(ref, k, x, n, v):
        after = planes(ref, k, lax.rem(x + n, 32), 1)
        before = planes(ref, k, lax.rem(x + 31, 32), 1)
        up = jnp.concatenate([v[1:], after], axis=0)
        down = jnp.concatenate([before, v[:-1]], axis=0)
        return 0.5 * (up - down)

    def forward(slot):
        rows = jnp.concatenate(
            [field[slot, pl.ds(s, 32, stride=8), :] for s in range(8)], axis=1
        )
        high, low = split(rows)
        both = mm(jnp.concatenate([high, low], axis=0), wh[...])
        plane = both[:32] + (both[32:] + mm(high, wl[...]))
        return product(x_ref[0], jnp.concatenate([plane[:, :HALF], plane[:, HALF:]], axis=0))

    @pl.loop(0, 4)
    def _(t):
        lame, shear = moduli(t * 8, 8)
        field[0, at(t * 8, 8), :] = (lame + (2.0 / 3.0) * shear).reshape(64, 128)

    spectrum_a = forward(0)

    ref = partbuf.at[pl.ds(0, 31)]
    pltpu.make_async_copy(ref, ref, part_recv).wait()
    total = jnp.sum(partbuf[...], axis=0)
    lane1 = lane_of((1, 128))

    def pick(row, k):
        return jnp.sum(jnp.where(lane1 == k, row, 0.0), axis=1, keepdims=True)

    members = pick(total, 6)
    load = [pick(total, c) / members for c in range(6)]
    trace = load[0] + load[1] + load[2]
    d = [load[c] - trace / 3.0 if c < 3 else load[c] for c in range(6)]
    own_steps = steps_ref[group * 32 + me]
    rates = [jnp.where(k < own_steps, relax_rate, 0.0).astype(f32) for k in range(KMAX)]
    size = norm_of(d)

    @pl.loop(0, 4)
    def _(t):
        _, shear = moduli(t * 8, 8)
        scale, _ = relaxed(shear, size, rates)
        field[1, at(t * 8, 8), :] = (2.0 * shear * scale).reshape(64, 128)

    spectrum_b = forward(1)
    mix = d[0] * spec_ref[1]
    for c in range(1, 6):
        mix = mix + d[c] * spec_ref[1 + c]
    scaled = spec_ref[0]
    steady = (1.0 - green_ratio) * trace
    phi = [scaled * spectrum_b[:32], scaled * spectrum_b[32:]]
    pressure = [
        scaled * (steady * spectrum_a[:32]) - mix * phi[0],
        scaled * (steady * spectrum_a[32:]) - mix * phi[1],
    ]
    mixed = jnp.concatenate(
        [
            jnp.concatenate([pressure[0], phi[0]], axis=1),
            jnp.concatenate([pressure[1], phi[1]], axis=1),
        ],
        axis=0,
    )
    back = product(x_ref[1], mixed)
    lines = jnp.concatenate(
        [
            jnp.concatenate([back[:32, :HALF], back[32:, :HALF]], axis=1),
            jnp.concatenate([back[:32, HALF:], back[32:, HALF:]], axis=1),
        ],
        axis=0,
    )
    high, low = split(lines)
    both = mm(jnp.concatenate([high, low], axis=0), vh[...])
    space = both[:64] + (both[64:] + mm(high, vl[...]))
    for k in range(2):
        for s in range(8):
            pot[k, pl.ds(s, 32, stride=8), :] = space[k * 32 : k * 32 + 32, s * 128 : s * 128 + 128]

    @pl.loop(0, 8)
    def _(t):
        x = t * 4
        p, q = planes(pot, 0, x, 4), planes(pot, 1, x, 4)
        px, qx = x_slope(pot, 0, x, 4, p), x_slope(pot, 1, x, 4, q)
        py, pz, qy, qz = yc(p), zc(p), yc(q), zc(q)
        ux = px + d[0] * qx + d[5] * qy + d[4] * qz
        uy = py + d[5] * qx + d[1] * qy + d[3] * qz
        uz = pz + d[4] * qx + d[3] * qy + d[2] * qz
        for c, u in enumerate((ux, uy, uz)):
            disp_u[c, at(x, 4), :] = u.reshape(32, 128)

    def send_planes(t):
        for b, c in sorted(((b, c) for b in range(4) for c in range(2)), key=lambda p: -spans(p[0])):
            peer = lax.rem(me_x + 2 + t, 4) * 8 + at_z[b] + at_c[c]

            def start(peer=peer):
                pltpu.make_async_remote_copy(
                    src_ref=flu.at[peer],
                    dst_ref=flubuf.at[me],
                    send_sem=flu_send,
                    recv_sem=flu_recv,
                    device_id={"dev": peer},
                    device_id_type=MESH,
                ).start()

            if (b, c) == (0, 0):
                pl.when(t != 2)(start)
            else:
                start()

    @pl.loop(0, 4)
    def _(t):
        x = lax.rem(me_x + 2 + t, 4) * 8
        ux, uy, uz = (planes(disp_u, c, x, 8) for c in range(3))
        dx = [x_slope(disp_u, c, x, 8, u) for c, u in enumerate((ux, uy, uz))]
        change = [
            -dx[0],
            -yc(uy),
            -zc(uz),
            -0.5 * (yc(uz) + zc(uy)),
            -0.5 * (dx[2] + zc(ux)),
            -0.5 * (dx[1] + yc(ux)),
        ]
        for c in range(6):
            gam[c, at(x, 8), :] = change[c].reshape(64, 128)
        for k in range(3):
            pair = jnp.concatenate(change[2 * k : 2 * k + 2], axis=1)
            flu[pl.ds(x, 8), pl.ds(k * 16, 16), :] = pair.astype(wire)
        send_planes(t)

    flubuf[me] = flu[me]

    def voxel(t, sums):
        x = t * 4
        lame, shear = moduli(x, 4)
        e = [load[c] + planes(gam, c, x, 4) for c in range(6)]
        tr = e[0] + e[1] + e[2]
        dv = [e[c] - tr / 3.0 if c < 3 else e[c] for c in range(6)]
        scale, f = relaxed(shear, norm_of(dv), rates)
        twice = 2.0 * shear * scale
        bulk = (lame + (2.0 / 3.0) * shear) * tr
        new = [bulk + twice * dv[c] if c < 3 else twice * dv[c] for c in range(6)]
        new += [lame, shear / (1.0 + f)]
        return tuple(a + jnp.sum(b, axis=0) for a, b in zip(sums, new))

    sums = lax.fori_loop(0, 8, voxel, tuple(jnp.zeros((8, 128), f32) for _ in range(8)))
    column = jnp.concatenate([jnp.sum(a, axis=0, keepdims=True) for a in sums], axis=0)
    column = jnp.sum(column, axis=1, keepdims=True) * (1.0 / VOX**3)
    lane8, row8 = lane_of((8, 128)), row_of((8, 128))
    own_row = jnp.sum(
        jnp.where(lane8 == row8 + group * 16, column, 0.0), axis=0, keepdims=True
    )
    for c in range(6):
        own_row = own_row + jnp.where(lane1 == group * 16 + 8 + c, load[c], 0.0)

    rowbuf[3] = own_row
    rows_out = []
    for i in range(1, 4):
        rows_out.append(
            pltpu.make_async_remote_copy(
                src_ref=rowbuf.at[3],
                dst_ref=rowbuf.at[i - 1],
                send_sem=y_send.at[i - 1],
                recv_sem=y_recv.at[i - 1],
                device_id={"grp": lax.rem(group + i, 4)},
                device_id_type=MESH,
            )
        )
        rows_out[-1].start()
    for copy in rows_out:
        copy.wait_recv()
    joined[0] = rowbuf[0] + rowbuf[1] + rowbuf[2] + rowbuf[3]
    everyone(lambda peer: joined.at[0], respbuf, resp_send, resp_recv)
    respbuf[me] = joined[0]

    for k in range(3):
        for o in range(4):
            ref = (nb_disp, nb_force, nb_samp)[k].at[o]
            pltpu.make_async_copy(ref, ref, near_recv.at[k, o]).wait()
    exists = [(me * count + j >= 3).astype(f32) * (me * count + j < 67).astype(f32) for j in range(8)]

    def extended(own, near_ref, c):
        def get(ref, p):
            return ref[c, pl.ds(p, 1)] if c is not None else ref[pl.ds(p, 1)]

        planes = [get(near_ref.at[0], 1), get(near_ref.at[1], 0), get(near_ref.at[1], 1)]
        planes += [get(own, 0), get(own, 1)]
        planes += [get(near_ref.at[2], 0), get(near_ref.at[2], 1), get(near_ref.at[3], 0)]
        return planes

    def masked(planes):
        return jnp.concatenate([p * m for p, m in zip(planes, exists)], axis=0)

    around = [masked(extended(disp_ref, nb_disp, c)) for c in range(3)]
    outside = [masked(extended(force_ref, nb_force, c)) for c in range(3)]
    samples = extended(samp_ref, nb_samp, None)

    all_arrived(respbuf, resp_recv)
    gathered = jnp.concatenate([respbuf[r] for r in range(32)], axis=0)
    gathered = jnp.concatenate([gathered, jnp.zeros((96, 128), f32)], axis=0).T
    cells = []
    for c in range(8):
        row = jnp.concatenate(
            [gathered[g * 16 + c : g * 16 + c + 1, :32] for g in range(4)], axis=1
        )
        source = jnp.broadcast_to(row, (8, 128))
        cells.append(
            masked(
                [
                    jnp.take_along_axis(source, s[0], axis=1, mode="promise_in_bounds")[None]
                    for s in samples
                ]
            )
        )
    lame, shear = cells[6], cells[7]
    pull = force_of(cells[:6])
    res = [
        (outside[c][1:] - pull[c] - spring_rate * around[c][1:])
        * jnp.concatenate([jnp.full((1, 8, 128), m) for m in exists[1:]], axis=0)
        for c in range(3)
    ]

    def stiff(w, low):
        n = w[0].shape[0]
        strain = strain_of(w)
        stress = stress_of(strain, lame[low : low + n - 1], shear[low : low + n - 1])
        pull = force_of(stress)
        mask = jnp.concatenate(
            [jnp.full((1, 8, 128), m) for m in exists[low + 1 : low + n - 1]], axis=0
        )
        return [(pull[c] + spring_rate * w[c][1:-1]) * mask for c in range(3)]

    k1 = stiff(res, 1)
    k2 = stiff(k1, 2)
    r_own = [a[2:4] for a in res]
    k1_own = [a[1:3] for a in k1]
    k2_own = [a[0:2] for a in k2]
    energy_strain = strain_of(k2)
    energy_stress = stress_of(energy_strain, lame[3:5], shear[3:5])

    def dotted(a, b):
        total = a[0] * b[0]
        for c in range(1, 3):
            total = total + a[c] * b[c]
        return jnp.sum(jnp.sum(total, axis=0), axis=0, keepdims=True)

    energy = energy_strain[0] * energy_stress[0]
    for c in range(1, 6):
        energy = energy + (1.0 if c < 3 else 2.0) * energy_strain[c] * energy_stress[c]
    energy = jnp.sum(jnp.sum(energy, axis=0), axis=0, keepdims=True) + spring_rate * dotted(
        k2_own, k2_own
    )
    rows = [
        dotted(r_own, r_own),
        dotted(r_own, k1_own),
        dotted(k1_own, k1_own),
        dotted(k1_own, k2_own),
        dotted(k2_own, k2_own),
        energy,
        jnp.zeros((2, 128), f32),
    ]
    column = jnp.sum(jnp.concatenate(rows, axis=0), axis=1, keepdims=True)
    moment[0] = jnp.sum(jnp.where(lane8 == row8, column, 0.0), axis=0, keepdims=True)
    everyone(lambda peer: moment.at[0], momentbuf, mom_send, mom_recv)
    momentbuf[me] = moment[0]

    def owner(r, acc):
        taken = jnp.where(slot_ref[group * 32 + r] == me, 1.0, 0.0).astype(f32)
        return acc + taken * respbuf[r]

    row = lax.fori_loop(0, 32, owner, jnp.zeros((1, 128), f32))
    shifted = jnp.zeros((1, 128), f32)
    for g in range(4):
        here = (group == g).astype(f32)
        shifted = shifted + here * roll(row, -16 * g, 1)
    row_out[...] = shifted[:, :8]

    table = jnp.concatenate([respbuf[r] for r in range(32)], axis=0)
    lane32 = lane_of((32, 128))
    group_load = [
        jnp.sum(jnp.where(lane32 == group * 16 + 8 + c, table, 0.0), axis=1, keepdims=True)
        for c in range(6)
    ]
    all_arrived(flubuf, flu_recv)
    for r in range(32):
        block = flubuf[r].astype(f32)
        for c in range(6):
            micro_out[pl.ds((c * 32 + r) * 8, 8), :] = (
                group_load[c][r : r + 1] + block[c * 8 : c * 8 + 8]
            )

    all_arrived(momentbuf, mom_recv)
    total = jnp.sum(momentbuf[...], axis=0)
    m = [pick(total, k) for k in range(6)]

    def form(a, b, first):
        out = 0.0
        for i, p in enumerate(a):
            for j, q in enumerate(b):
                out = out + p * q * m[i + j + first]
        return out

    rr = m[0]
    alpha0 = rr / m[1]
    r1 = (jnp.ones_like(rr), -alpha0)
    rr1 = form(r1, r1, 0)
    beta0 = rr1 / rr
    p1 = (1.0 + beta0, -alpha0)
    alpha1 = rr1 / form(p1, p1, 1)
    r2 = (jnp.ones_like(rr), -alpha0 - alpha1 * p1[0], alpha1 * alpha0)
    rr2 = form(r2, r2, 0)
    beta1 = rr2 / rr1
    p2 = (r2[0] + beta1 * p1[0], r2[1] + beta1 * p1[1], r2[2])
    alpha2 = rr2 / form(p2, p2, 1)
    weight = (
        alpha0 + alpha1 * p1[0] + alpha2 * p2[0],
        alpha1 * p1[1] + alpha2 * p2[1],
        alpha2 * p2[2],
    )
    for c in range(3):
        new = disp_ref[c] + (
            weight[0] * r_own[c] + weight[1] * k1_own[c] + weight[2] * k2_own[c]
        )
        for p in range(count):
            for q in range(4):
                disp_out[c, p, pl.ds(q, 8, stride=4), :] = new[p][:, q * 32 : q * 32 + 32]

    first_plane.wait_send()
    for k in range(3):
        for copy in near[k]:
            copy.wait_send()
    for copy in rows_out:
        copy.wait_send()
    for buffer, sem in (
        (modbuf, mod_send), (partbuf, part_send), (respbuf, resp_send),
        (flubuf, flu_send), (momentbuf, mom_send),
    ):
        ref = buffer.at[pl.ds(0, 31)]
        pltpu.make_async_copy(ref, ref, sem).wait()


def leave(a, b, c, a_out, b_out, c_out, sem):
    copies = [
        pltpu.make_async_copy(source, target, sem.at[k])
        for k, (source, target) in enumerate(((c, c_out), (a, a_out), (b, b_out)))
    ]
    for copy in copies:
        copy.start()
    for copy in copies:
        copy.wait()


def shards(
    displacement, external_force, element_sample, lame_field, shear_field, plastic_steps, owner_slot
):
    count = displacement.shape[1]
    disp, sample = (3, count, 8, 128), (count, 8, 128)
    wt, vt, vz, x, spec = (jnp.asarray(t) for t in tables())
    operands = (
        displacement,
        wt,
        lame_field.reshape(32, 1024),
        shear_field.reshape(32, 1024),
        external_force,
        element_sample,
        vt,
        vz,
        x,
        spec,
    )
    scalars = (plastic_steps, owner_slot)
    vmem = pl.BlockSpec(memory_space=pltpu.VMEM)
    hbm = pl.BlockSpec(memory_space=pltpu.HBM)
    dma = pltpu.SemaphoreType.DMA
    disp_next, row, micro = pl.pallas_call(
        kernel,
        out_shape=(
            jax.ShapeDtypeStruct(displacement.shape, f32),
            jax.ShapeDtypeStruct((1, 8), f32),
            jax.ShapeDtypeStruct((6 * 32 * 8, 128), f32),
        ),
        in_specs=[hbm] * 12,
        out_specs=(vmem,) * 3,
        scratch_shapes=[
            *(pltpu.VMEM(a.shape, a.dtype) for a in operands),
            *(pltpu.SMEM(a.shape, a.dtype) for a in scalars),
            dma((12,)),
            pltpu.VMEM(disp, f32),
            pltpu.VMEM(disp, f32),
            pltpu.VMEM(sample, jnp.int32),
            pltpu.VMEM((32, 16, 128), bf16),
            pltpu.VMEM((512, 128), f32),
            pltpu.VMEM((3, 8, 128), f32),
            pltpu.VMEM((4,) + disp, f32),
            pltpu.VMEM((4,) + disp, f32),
            pltpu.VMEM((4,) + sample, jnp.int32),
            pltpu.VMEM((32, 16, 128), bf16),
            pltpu.VMEM((32, 1, 128), f32),
            pltpu.VMEM((32, 1, 128), f32),
            pltpu.VMEM((count, 64, 128), f32),
            pltpu.VMEM((1024, 1024), bf16),
            pltpu.VMEM((1024, 1024), bf16),
            pltpu.VMEM((1024, 1024), bf16),
            pltpu.VMEM((1024, 1024), bf16),
            pltpu.VMEM((2, 256, 128), f32),
            pltpu.VMEM((2, 256, 128), f32),
            pltpu.VMEM((3, 256, 128), f32),
            pltpu.VMEM((6, 256, 128), f32),
            pltpu.VMEM((32, 48, 128), wire),
            pltpu.VMEM((32, 48, 128), wire),
            pltpu.VMEM((4, 1, 128), f32),
            pltpu.VMEM((1, 1, 128), f32),
            pltpu.VMEM((32, 1, 128), f32),
            pltpu.VMEM((1, 1, 128), f32),
            pltpu.VMEM((32, 1, 128), f32),
            dma((2,)), dma((3, 4)), dma((3, 4)), dma, dma, dma, dma,
            dma((3,)), dma((3,)), dma, dma, dma, dma, dma, dma,
        ],
        compiler_params=pltpu.CompilerParams(collective_id=0, has_side_effects=True, vmem_limit_bytes=24 << 20),
    )(*[pltpu.with_memory_space_constraint(a, pltpu.HBM) for a in operands + scalars])
    results = (disp_next, row, micro)
    disp_next, row, micro = pl.pallas_call(
        leave,
        out_shape=tuple(jax.ShapeDtypeStruct(a.shape, a.dtype) for a in results),
        in_specs=[pl.BlockSpec(memory_space=pl.ANY)] * 3,
        out_specs=(pl.BlockSpec(memory_space=pltpu.HBM),) * 3,
        scratch_shapes=[dma((3,))],
        compiler_params=pltpu.CompilerParams(vmem_limit_bytes=1 << 20),
    )(*results)
    return disp_next, row, micro.reshape(6, 32, 1, 1024)


def solution(mesh):
    in_specs = (
        P(None, "dev", None, None),
        P(None, "dev", None, None),
        P("dev", None, None),
        P("grp", "dev", None),
        P("grp", "dev", None),
        P(),
        P(),
    )
    out_specs = (P(None, "dev", None, None), P(("grp", "dev"), None), P(None, "grp", "dev", None))
    return jax.shard_map(shards, mesh=mesh, in_specs=in_specs, out_specs=out_specs, check_vma=False)
```

```python
import jax
import jax.numpy as jnp
import numpy as np
from jax import lax
from jax.experimental import pallas as pl
from jax.experimental.pallas import tpu as pltpu
from jax.sharding import PartitionSpec as P

VOX = 32
HALF = 512
PIECES = 2
KMAX = 4
MESH = pl.DeviceIdType.MESH
NEAR = (-2, -1, 1, 2)

shear_ref = 1.65
lame_ref = 1.25
green_ratio = (lame_ref + shear_ref) / (lame_ref + 2.0 * shear_ref)
relax_rate = 0.35
spring_rate = 0.2
wire = jnp.bfloat16
f32 = jnp.float32
bf16 = jnp.bfloat16


def tables():
    n = np.arange(VOX)
    theta = 2.0 * np.pi / VOX
    ky = np.repeat(n, 16)
    kz = np.tile(np.arange(16), VOX)
    yy = np.repeat(n, VOX)
    zz = np.tile(n, VOX)
    k16 = np.arange(16)

    def zeta(z, k):
        angle = theta * (z * k % VOX)
        return (
            np.where(k == 0, 1.0, np.cos(angle)),
            np.where(k == 0, (-1.0) ** z, -np.sin(angle)),
        )

    cy, sy = np.cos(theta * (np.outer(n, ky) % VOX)), np.sin(theta * (np.outer(n, ky) % VOX))
    zr, zi = zeta(n[:, None], kz[None, :])
    cv, sv = np.cos(theta * (np.outer(n, yy) % VOX)), np.sin(theta * (np.outer(n, yy) % VOX))
    vr, vi = zeta(zz[None, :], k16[:, None])
    c, s = np.cos(theta * (np.outer(n, n) % VOX)), np.sin(theta * (np.outer(n, n) % VOX))
    x = np.block([[c, s], [-s, c]])

    def wave(k):
        return np.where(k % 16 == 0, 0.0, np.sin(theta * k))

    one = np.ones((VOX, HALF))
    xx, xy, xz = wave(n)[:, None] * one, wave(ky)[None] * one, wave(kz)[None] * one
    square = xx * xx + xy * xy + xz * xz
    inverse = np.where(square > 0, 1.0 / np.where(square > 0, square, 1.0), 0.0)
    weight = np.where(kz == 0, 1.0, 2.0)[None] * one
    scaled = -(1.0 / shear_ref) * inverse * weight / VOX**3
    pairs = (xx * xx, xy * xy, xz * xz, 2 * xy * xz, 2 * xx * xz, 2 * xx * xy)
    spectral = np.stack([scaled] + [green_ratio * p * inverse for p in pairs] + [xx, xy, xz])
    to = lambda a: np.asarray(a, np.float32)
    return (
        to(np.stack([cy, sy, zr, zi])),
        to(np.stack([cv, sv])),
        to(np.stack([vr, vi])),
        to(np.stack([x, x.T])),
        to(spectral),
    )


def split(a):
    high = a.astype(bf16)
    return high, (a - high.astype(f32)).astype(bf16)


def mm(a, b):
    return jnp.dot(a, b, preferred_element_type=f32)


def product(a, b):
    ah, al = split(a)
    bh, bl = split(b)
    return mm(ah, bh) + (mm(al, bh) + mm(ah, bl))


def lane_of(shape):
    return lax.broadcasted_iota(jnp.int32, shape, len(shape) - 1)


def row_of(shape):
    return lax.broadcasted_iota(jnp.int32, shape, len(shape) - 2)


def roll(a, shift, axis):
    return pltpu.roll(a, shift % a.shape[axis], axis)


def z_up(v):
    return jnp.where(lane_of(v.shape) % VOX == VOX - 1, 0.0, roll(v, -1, 2))


def z_down(v):
    return jnp.where(lane_of(v.shape) % VOX == 0, 0.0, roll(v, 1, 2))


def y_up(v):
    moved = roll(v, -VOX, 2)
    next_row = jnp.where(row_of(v.shape) == 7, 0.0, roll(moved, -1, 1))
    return jnp.where(lane_of(v.shape) < 96, moved, next_row)


def y_down(v):
    moved = roll(v, VOX, 2)
    last_row = jnp.where(row_of(v.shape) == 0, 0.0, roll(moved, 1, 1))
    return jnp.where(lane_of(v.shape) >= VOX, moved, last_row)


def yc(v):
    lane = lane_of(v.shape)
    up = roll(v, -VOX, 2)
    up = jnp.where(lane < 96, up, roll(up, -1, 1))
    down = roll(v, VOX, 2)
    down = jnp.where(lane >= VOX, down, roll(down, 1, 1))
    return 0.5 * (up - down)


def spans(distance):
    return min(distance, 4 - distance)


OTHERS = sorted(
    ((a, b, c) for a in range(4) for b in range(4) for c in range(2) if (a, b, c) != (0, 0, 0)),
    key=lambda p: (-spans(p[0]) - spans(p[1]), -p[2], p),
)


def strain_of(fields):
    slopes = []
    for w in fields:
        up = z_up(w)
        mz, dz = 0.5 * (w + up), up - w
        moved = y_up(mz)
        a, b = 0.5 * (mz + moved), moved - mz
        c = 0.5 * (dz + y_up(dz))
        slopes.append((a[1:] - a[:-1], 0.5 * (b[1:] + b[:-1]), 0.5 * (c[1:] + c[:-1])))
    x, y, z = slopes
    return (
        x[0],
        y[1],
        z[2],
        0.5 * (z[1] + y[2]),
        0.5 * (z[0] + x[2]),
        0.5 * (y[0] + x[1]),
    )


def force_of(stress):
    xx, yy, zz, yz, xz, xy = stress
    result = []
    for along_x, along_y, along_z in ((xx, xy, xz), (xy, yy, yz), (xz, yz, zz)):
        smooth = along_x + z_down(along_x)
        first = 0.25 * (smooth + y_down(smooth))
        both = along_y + along_z
        less = along_z - along_y
        rest = y_down(0.5 * (z_down(both) - less)) + 0.5 * (z_down(less) - both)
        result.append((first[:-1] - first[1:]) + 0.5 * (rest[1:] + rest[:-1]))
    return result


def stress_of(strain, lame, shear):
    spread = lame * (strain[0] + strain[1] + strain[2])
    twice = 2.0 * shear
    return [twice * e + spread for e in strain[:3]] + [twice * e for e in strain[3:]]


def norm_of(d):
    return d[0] * d[0] + d[1] * d[1] + d[2] * d[2] + 2.0 * (d[3] * d[3] + d[4] * d[4] + d[5] * d[5])


def relaxed(mu, size, rates):
    base = mu * mu * size
    scale = jnp.ones_like(mu)
    for rate in rates:
        f = base * scale * scale
        scale = scale * (1.0 - rate * (f / (1.0 + f)))
    return scale, base * scale * scale


def kernel(
    disp_in, wt_in, lame_in, shear_in, force_in, samp_in, vt_in, vz_in, x_in, spec_in, steps_in, slot_in,
    disp_out, row_out, micro_out,
    disp_raw, wt_ref, lame_raw, shear_raw, force_raw, samp_raw, vt_ref, vz_ref, x_ref, spec_ref,
    steps_ref, slot_ref, in_sem,
    disp_ref, force_ref, samp_ref, mod_ref, modwide,
    nb_first, nb_disp, nb_force, nb_samp, modbuf, part, partbuf, strainrow, one_hot_ref,
    wh, wl, vh, vl, field, disp_u, gam, flu, flubuf,
    rowbuf, joined, respbuf, moment, momentbuf,
    ready, first_sem, near_send, near_recv, mod_send, mod_recv, part_send, part_recv,
    y_send, y_recv, resp_send, resp_recv, flu_send, flu_recv, mom_send, mom_recv,
):
    me = lax.axis_index("dev")
    group = lax.axis_index("grp")
    count = disp_raw.shape[1]

    me_x, me_z, me_c = me // 8, lax.rem(me // 2, 4), lax.rem(me, 2)
    at_x = [lax.rem(me_x + k, 4) * 8 for k in range(4)]
    at_z = [lax.rem(me_z + k, 4) * 2 for k in range(4)]
    at_c = [me_c, 1 - me_c]
    peers = [at_x[a] + at_z[b] + at_c[c] for a, b, c in OTHERS]

    loads = [
        pltpu.make_async_copy(source, target, in_sem.at[k])
        for k, (source, target) in enumerate(
            (
                (disp_in, disp_raw), (wt_in, wt_ref), (lame_in, lame_raw), (shear_in, shear_raw),
                (force_in, force_raw), (samp_in, samp_raw), (vt_in, vt_ref), (vz_in, vz_ref),
                (x_in, x_ref), (spec_in, spec_ref), (steps_in, steps_ref), (slot_in, slot_ref),
            )
        )
    ]
    loads[0].start()

    barrier = pltpu.get_barrier_semaphore()
    layer = [peer for peer, (a, _, _) in zip(peers, OTHERS) if a == 0]
    entry = [peer for peer, (_, b, c) in zip(peers, OTHERS) if (b, c) == (0, 0)] + layer
    entry.append(lax.rem(me + 1, 32))
    for peer in entry:
        pl.semaphore_signal(barrier, inc=1, device_id={"dev": peer}, device_id_type=MESH)
    for i in range(1, 4):
        pl.semaphore_signal(
            barrier, inc=1, device_id={"grp": lax.rem(group + i, 4)}, device_id_type=MESH
        )
    for copy in loads[1:]:
        copy.start()

    def dense(raw, out):
        for index in np.ndindex(raw.shape[:-2]):
            out[index] = jnp.concatenate(
                [raw[(*index, pl.ds(q, 8, stride=4), slice(None))] for q in range(4)], axis=1
            )

    loads[0].wait()
    dense(disp_raw, disp_ref)
    pl.semaphore_wait(barrier, len(entry) + 3)
    first_plane = pltpu.make_async_remote_copy(
        src_ref=disp_ref.at[:, 0],
        dst_ref=nb_first,
        send_sem=first_sem.at[0],
        recv_sem=first_sem.at[1],
        device_id={"dev": lax.rem(me + 31, 32)},
        device_id_type=MESH,
    )
    first_plane.start()
    for peer in layer:
        pl.semaphore_signal(ready, inc=1, device_id={"dev": peer}, device_id_type=MESH)
    for k in range(2, 6):
        loads[k].wait()
    dense(force_raw, force_ref)
    dense(samp_raw, samp_ref)
    for k, raw in enumerate((lame_raw, shear_raw)):
        wide = raw[...].astype(f32)
        for t in range(8):
            modwide[pl.ds(k * 8 + t, 32, stride=16), :] = wide[:, t * 128 : t * 128 + 128]
    for r in range(32):
        mod_ref[r] = modwide[pl.ds(r * 16, 16), :].astype(bf16)

    part[...] = jnp.zeros_like(part)
    for plane in range(count):
        strainrow[plane, pl.ds(48, 8), :] = jnp.ones((8, 128), f32)
        strainrow[plane, pl.ds(56, 8), :] = jnp.zeros((8, 128), f32)

    def near_copies(source, target, k):
        out = []
        for o, offset in enumerate(NEAR):
            out.append(
                pltpu.make_async_remote_copy(
                    src_ref=source,
                    dst_ref=target.at[3 - o],
                    send_sem=near_send.at[k, o],
                    recv_sem=near_recv.at[k, 3 - o],
                    device_id={"dev": lax.rem(me + offset + 32, 32)},
                    device_id_type=MESH,
                )
            )
        return out

    near = [
        near_copies(disp_ref, nb_disp, 0),
        near_copies(force_ref, nb_force, 1),
        near_copies(samp_ref, nb_samp, 2),
    ]

    def everyone(source, target, send, recv):
        for peer in peers:
            pltpu.make_async_remote_copy(
                src_ref=source(peer),
                dst_ref=target.at[me],
                send_sem=send,
                recv_sem=recv,
                device_id={"dev": peer},
                device_id_type=MESH,
            ).start()

    def all_arrived(target, recv):
        ref = target.at[pl.ds(0, 31)]
        pltpu.make_async_copy(ref, ref, recv).wait()

    loads[1].wait()

    @pl.loop(0, 32)
    def _(y):
        c, s = wt_ref[0, pl.ds(y, 1), :], wt_ref[1, pl.ds(y, 1), :]
        zr, zi = wt_ref[2], wt_ref[3]
        rows = pl.ds(pl.multiple_of(y * 32, 32), 32)
        for k, block in enumerate((c * zr + s * zi, c * zi - s * zr)):
            high, low = split(block)
            wh[rows, pl.ds(k * HALF, HALF)] = high
            wl[rows, pl.ds(k * HALF, HALF)] = low

    one_hots, rows_high, rows_low = [], [], []
    for plane in range(count):
        sample = samp_ref[plane]
        for s in range(8):
            hit = jnp.broadcast_to(sample[s : s + 1], (32, 128)) == (
                row_of((32, 128)) + group * 32
            )
            one_hots.append(jnp.where(hit, 1.0, 0.0).astype(bf16))
    one_hot_ref[...] = jnp.concatenate(one_hots, axis=1)
    pl.semaphore_wait(ready, len(layer))
    everyone(lambda peer: mod_ref.at[peer], modbuf, mod_send, mod_recv)
    modbuf[me] = mod_ref[me]

    first_plane.wait_recv()
    inside_up = (me < 31).astype(f32)
    fields = [
        jnp.concatenate([disp_ref[c], nb_first[pl.ds(c, 1)] * inside_up], axis=0) for c in range(3)
    ]
    strain = strain_of(fields)
    for plane in range(count):
        for c in range(6):
            strainrow[plane, pl.ds(c * 8, 8), :] = strain[c][plane]
    for plane in range(count):
        for s in range(8):
            rows = strainrow[plane, pl.ds(s, 8, stride=8), :]
            high, low = split(rows)
            rows_high.append(high)
            rows_low.append(low)
    one_hot = one_hot_ref[...]

    def against(rows):
        return lax.dot_general(
            one_hot,
            jnp.concatenate(rows, axis=1),
            (((1,), (1,)), ((), ())),
            preferred_element_type=f32,
        )

    sums = against(rows_high) + against(rows_low)
    for r in range(32):
        part[r, :, pl.ds(0, 8)] = sums[r : r + 1]
    everyone(lambda peer: part.at[peer], partbuf, part_send, part_recv)
    partbuf[me] = part[me]
    for k in range(3):
        for copy in near[k]:
            copy.start()
    for k in range(6, 12):
        loads[k].wait()

    @pl.loop(0, 32)
    def _(k):
        c, s = vt_ref[0, pl.ds(k, 1), :], vt_ref[1, pl.ds(k, 1), :]
        zr, zi = vz_ref[0], vz_ref[1]
        for p, block in enumerate((c * zr + s * zi, c * zi - s * zr)):
            rows = pl.ds(pl.multiple_of(p * HALF + k * 16, 16), 16)
            high, low = split(block)
            vh[rows, :] = high
            vl[rows, :] = low

    ref = modbuf.at[pl.ds(0, 31)]
    pltpu.make_async_copy(ref, ref, mod_recv).wait()

    def moduli(x, n):
        both = modbuf[pl.ds(x, n)].astype(f32)
        return both[:, :8], both[:, 8:]

    def at(x, n):
        return pl.ds(pl.multiple_of(x * 8, 8), n * 8)

    def planes(ref, k, x, n):
        return ref[k, at(x, n), :].reshape(n, 8, 128)

    def x_slope(ref, k, x, n, v):
        after = planes(ref, k, lax.rem(x + n, 32), 1)
        before = planes(ref, k, lax.rem(x + 31, 32), 1)
        up = jnp.concatenate([v[1:], after], axis=0)
        down = jnp.concatenate([before, v[:-1]], axis=0)
        return 0.5 * (up - down)

    def forward():
        rows = jnp.concatenate(
            [
                jnp.concatenate([field[k, pl.ds(s, 32, stride=8), :] for k in range(2)], axis=0)
                for s in range(8)
            ],
            axis=1,
        )
        high, low = split(rows)
        both = mm(jnp.concatenate([high, low], axis=0), wh[...])
        plane = both[:64] + (both[64:] + mm(high, wl[...]))
        stacked = jnp.concatenate(
            [
                jnp.concatenate([plane[:32, :HALF], plane[32:, :HALF]], axis=1),
                jnp.concatenate([plane[:32, HALF:], plane[32:, HALF:]], axis=1),
            ],
            axis=0,
        )
        return product(x_ref[0], stacked)

    ref = partbuf.at[pl.ds(0, 31)]
    pltpu.make_async_copy(ref, ref, part_recv).wait()
    total = jnp.sum(partbuf[...], axis=0)
    lane1 = lane_of((1, 128))

    def pick(row, k):
        return jnp.sum(jnp.where(lane1 == k, row, 0.0), axis=1, keepdims=True)

    members = pick(total, 6)
    load = [pick(total, c) / members for c in range(6)]
    trace = load[0] + load[1] + load[2]
    d = [load[c] - trace / 3.0 if c < 3 else load[c] for c in range(6)]
    own_steps = steps_ref[group * 32 + me]
    rates = [jnp.where(k < own_steps, relax_rate, 0.0).astype(f32) for k in range(KMAX)]
    size = norm_of(d)

    @pl.loop(0, 4)
    def _(t):
        lame, shear = moduli(t * 8, 8)
        field[0, at(t * 8, 8), :] = (lame + (2.0 / 3.0) * shear).reshape(64, 128)
        scale, _ = relaxed(shear, size, rates)
        field[1, at(t * 8, 8), :] = (2.0 * shear * scale).reshape(64, 128)

    spectrum = forward()
    spectrum_a, spectrum_b = spectrum[:, :HALF], spectrum[:, HALF:]
    mix = d[0] * spec_ref[1]
    for c in range(1, 6):
        mix = mix + d[c] * spec_ref[1 + c]
    scaled = spec_ref[0]
    steady = (1.0 - green_ratio) * trace
    phi = [scaled * spectrum_b[:32], scaled * spectrum_b[32:]]
    pressure = [
        scaled * (steady * spectrum_a[:32]) - mix * phi[0],
        scaled * (steady * spectrum_a[32:]) - mix * phi[1],
    ]
    waves = [spec_ref[7 + c] for c in range(3)]
    turned = [
        d[0] * waves[0] + d[5] * waves[1] + d[4] * waves[2],
        d[5] * waves[0] + d[1] * waves[1] + d[3] * waves[2],
        d[4] * waves[0] + d[3] * waves[1] + d[2] * waves[2],
    ]
    slopes = [
        [waves[c] * pressure[k] + turned[c] * phi[k] for k in range(2)] for c in range(3)
    ]
    mixed = jnp.concatenate(
        [
            jnp.concatenate([-slopes[c][1] for c in range(3)], axis=1),
            jnp.concatenate([slopes[c][0] for c in range(3)], axis=1),
        ],
        axis=0,
    )
    back = product(x_ref[1], mixed)
    lines = jnp.concatenate(
        [
            jnp.concatenate([back[:32, c * HALF :][:, :HALF], back[32:, c * HALF :][:, :HALF]], axis=1)
            for c in range(3)
        ],
        axis=0,
    )
    high, low = split(lines)
    both = mm(jnp.concatenate([high, low], axis=0), vh[...])
    space = both[:96] + (both[96:] + mm(high, vl[...]))
    for c in range(3):
        for s in range(8):
            disp_u[c, pl.ds(s, 32, stride=8), :] = space[
                c * 32 : c * 32 + 32, s * 128 : s * 128 + 128
            ]

    source, target = row_of((128, 128)), lane_of((128, 128))
    line = source // VOX == target // VOX
    ahead = line & ((target + 1) % VOX == source % VOX)
    behind = line & ((target + VOX - 1) % VOX == source % VOX)
    z_matrix = (jnp.where(ahead, 0.5, 0.0) - jnp.where(behind, 0.5, 0.0)).astype(bf16)

    def send_planes(t):
        for b, c in sorted(((b, c) for b in range(4) for c in range(2)), key=lambda p: -spans(p[0])):
            peer = lax.rem(me_x + 2 + t, 4) * 8 + at_z[b] + at_c[c]

            def start(peer=peer):
                pltpu.make_async_remote_copy(
                    src_ref=flu.at[peer],
                    dst_ref=flubuf.at[me],
                    send_sem=flu_send,
                    recv_sem=flu_recv,
                    device_id={"dev": peer},
                    device_id_type=MESH,
                ).start()

            if (b, c) == (0, 0):
                pl.when(t != 2)(start)
            else:
                start()

    @pl.loop(0, 4)
    def _(t):
        x = lax.rem(me_x + 2 + t, 4) * 8
        ux, uy, uz = (planes(disp_u, c, x, 8) for c in range(3))
        dx = [x_slope(disp_u, c, x, 8, u) for c, u in enumerate((ux, uy, uz))]
        high, low = split(jnp.concatenate([ux, uy, uz], axis=0).reshape(192, 128))
        dz = (mm(high, z_matrix) + mm(low, z_matrix)).reshape(3, 8, 8, 128)
        change = [
            -dx[0],
            -yc(uy),
            -dz[2],
            -0.5 * (yc(uz) + dz[1]),
            -0.5 * (dx[2] + dz[0]),
            -0.5 * (dx[1] + yc(ux)),
        ]
        for c in range(6):
            gam[c, at(x, 8), :] = change[c].reshape(64, 128)
        for k in range(3):
            pair = jnp.concatenate(change[2 * k : 2 * k + 2], axis=1)
            flu[pl.ds(x, 8), pl.ds(k * 16, 16), :] = pair.astype(wire)
        send_planes(t)

    flubuf[me] = flu[me]

    def voxel(t, sums):
        x = t * 4
        lame, shear = moduli(x, 4)
        e = [load[c] + planes(gam, c, x, 4) for c in range(6)]
        tr = e[0] + e[1] + e[2]
        dv = [e[c] - tr / 3.0 if c < 3 else e[c] for c in range(6)]
        scale, f = relaxed(shear, norm_of(dv), rates)
        twice = 2.0 * shear * scale
        bulk = (lame + (2.0 / 3.0) * shear) * tr
        new = [bulk + twice * dv[c] if c < 3 else twice * dv[c] for c in range(6)]
        new += [lame, shear / (1.0 + f)]
        return tuple(a + jnp.sum(b, axis=0) for a, b in zip(sums, new))

    sums = lax.fori_loop(0, 8, voxel, tuple(jnp.zeros((8, 128), f32) for _ in range(8)))
    column = jnp.concatenate([jnp.sum(a, axis=0, keepdims=True) for a in sums], axis=0)
    column = jnp.sum(column, axis=1, keepdims=True) * (1.0 / VOX**3)
    lane8, row8 = lane_of((8, 128)), row_of((8, 128))
    own_row = jnp.sum(
        jnp.where(lane8 == row8 + group * 16, column, 0.0), axis=0, keepdims=True
    )
    for c in range(6):
        own_row = own_row + jnp.where(lane1 == group * 16 + 8 + c, load[c], 0.0)

    rowbuf[3] = own_row
    rows_out = []
    for i in range(1, 4):
        rows_out.append(
            pltpu.make_async_remote_copy(
                src_ref=rowbuf.at[3],
                dst_ref=rowbuf.at[i - 1],
                send_sem=y_send.at[i - 1],
                recv_sem=y_recv.at[i - 1],
                device_id={"grp": lax.rem(group + i, 4)},
                device_id_type=MESH,
            )
        )
        rows_out[-1].start()
    for copy in rows_out:
        copy.wait_recv()
    joined[0] = rowbuf[0] + rowbuf[1] + rowbuf[2] + rowbuf[3]
    everyone(lambda peer: joined.at[0], respbuf, resp_send, resp_recv)
    respbuf[me] = joined[0]

    for k in range(3):
        for o in range(4):
            ref = (nb_disp, nb_force, nb_samp)[k].at[o]
            pltpu.make_async_copy(ref, ref, near_recv.at[k, o]).wait()
    exists = [(me * count + j >= 3).astype(f32) * (me * count + j < 67).astype(f32) for j in range(8)]

    def extended(own, near_ref, c):
        def get(ref, p):
            return ref[c, pl.ds(p, 1)] if c is not None else ref[pl.ds(p, 1)]

        planes = [get(near_ref.at[0], 1), get(near_ref.at[1], 0), get(near_ref.at[1], 1)]
        planes += [get(own, 0), get(own, 1)]
        planes += [get(near_ref.at[2], 0), get(near_ref.at[2], 1), get(near_ref.at[3], 0)]
        return planes

    def masked(planes):
        return jnp.concatenate([p * m for p, m in zip(planes, exists)], axis=0)

    around = [masked(extended(disp_ref, nb_disp, c)) for c in range(3)]
    outside = [masked(extended(force_ref, nb_force, c)) for c in range(3)]
    samples = extended(samp_ref, nb_samp, None)

    all_arrived(respbuf, resp_recv)
    gathered = jnp.concatenate([respbuf[r] for r in range(32)], axis=0)
    gathered = jnp.concatenate([gathered, jnp.zeros((96, 128), f32)], axis=0).T
    cells = []
    for c in range(8):
        row = jnp.concatenate(
            [gathered[g * 16 + c : g * 16 + c + 1, :32] for g in range(4)], axis=1
        )
        source = jnp.broadcast_to(row, (8, 128))
        cells.append(
            masked(
                [
                    jnp.take_along_axis(source, s[0], axis=1, mode="promise_in_bounds")[None]
                    for s in samples
                ]
            )
        )
    lame, shear = cells[6], cells[7]
    pull = force_of(cells[:6])
    res = [
        (outside[c][1:] - pull[c] - spring_rate * around[c][1:])
        * jnp.concatenate([jnp.full((1, 8, 128), m) for m in exists[1:]], axis=0)
        for c in range(3)
    ]

    def stiff(w, low):
        n = w[0].shape[0]
        strain = strain_of(w)
        stress = stress_of(strain, lame[low : low + n - 1], shear[low : low + n - 1])
        pull = force_of(stress)
        mask = jnp.concatenate(
            [jnp.full((1, 8, 128), m) for m in exists[low + 1 : low + n - 1]], axis=0
        )
        return [(pull[c] + spring_rate * w[c][1:-1]) * mask for c in range(3)]

    k1 = stiff(res, 1)
    k2 = stiff(k1, 2)
    r_own = [a[2:4] for a in res]
    k1_own = [a[1:3] for a in k1]
    k2_own = [a[0:2] for a in k2]
    energy_strain = strain_of(k2)
    energy_stress = stress_of(energy_strain, lame[3:5], shear[3:5])

    def dotted(a, b):
        total = a[0] * b[0]
        for c in range(1, 3):
            total = total + a[c] * b[c]
        return jnp.sum(jnp.sum(total, axis=0), axis=0, keepdims=True)

    energy = energy_strain[0] * energy_stress[0]
    for c in range(1, 6):
        energy = energy + (1.0 if c < 3 else 2.0) * energy_strain[c] * energy_stress[c]
    energy = jnp.sum(jnp.sum(energy, axis=0), axis=0, keepdims=True) + spring_rate * dotted(
        k2_own, k2_own
    )
    rows = [
        dotted(r_own, r_own),
        dotted(r_own, k1_own),
        dotted(k1_own, k1_own),
        dotted(k1_own, k2_own),
        dotted(k2_own, k2_own),
        energy,
        jnp.zeros((2, 128), f32),
    ]
    column = jnp.sum(jnp.concatenate(rows, axis=0), axis=1, keepdims=True)
    moment[0] = jnp.sum(jnp.where(lane8 == row8, column, 0.0), axis=0, keepdims=True)
    everyone(lambda peer: moment.at[0], momentbuf, mom_send, mom_recv)
    momentbuf[me] = moment[0]

    def owner(r, acc):
        taken = jnp.where(slot_ref[group * 32 + r] == me, 1.0, 0.0).astype(f32)
        return acc + taken * respbuf[r]

    row = lax.fori_loop(0, 32, owner, jnp.zeros((1, 128), f32))
    shifted = jnp.zeros((1, 128), f32)
    for g in range(4):
        here = (group == g).astype(f32)
        shifted = shifted + here * roll(row, -16 * g, 1)
    row_out[...] = shifted[:, :8]

    table = jnp.concatenate([respbuf[r] for r in range(32)], axis=0)
    lane32 = lane_of((32, 128))
    group_load = [
        jnp.sum(jnp.where(lane32 == group * 16 + 8 + c, table, 0.0), axis=1, keepdims=True)
        for c in range(6)
    ]
    all_arrived(flubuf, flu_recv)
    for r in range(32):
        block = flubuf[r].astype(f32)
        for c in range(6):
            micro_out[pl.ds((c * 32 + r) * 8, 8), :] = (
                group_load[c][r : r + 1] + block[c * 8 : c * 8 + 8]
            )

    all_arrived(momentbuf, mom_recv)
    total = jnp.sum(momentbuf[...], axis=0)
    m = [pick(total, k) for k in range(6)]

    def form(a, b, first):
        out = 0.0
        for i, p in enumerate(a):
            for j, q in enumerate(b):
                out = out + p * q * m[i + j + first]
        return out

    rr = m[0]
    alpha0 = rr / m[1]
    r1 = (jnp.ones_like(rr), -alpha0)
    rr1 = form(r1, r1, 0)
    beta0 = rr1 / rr
    p1 = (1.0 + beta0, -alpha0)
    alpha1 = rr1 / form(p1, p1, 1)
    r2 = (jnp.ones_like(rr), -alpha0 - alpha1 * p1[0], alpha1 * alpha0)
    rr2 = form(r2, r2, 0)
    beta1 = rr2 / rr1
    p2 = (r2[0] + beta1 * p1[0], r2[1] + beta1 * p1[1], r2[2])
    alpha2 = rr2 / form(p2, p2, 1)
    weight = (
        alpha0 + alpha1 * p1[0] + alpha2 * p2[0],
        alpha1 * p1[1] + alpha2 * p2[1],
        alpha2 * p2[2],
    )
    for c in range(3):
        new = disp_ref[c] + (
            weight[0] * r_own[c] + weight[1] * k1_own[c] + weight[2] * k2_own[c]
        )
        for p in range(count):
            for q in range(4):
                disp_out[c, p, pl.ds(q, 8, stride=4), :] = new[p][:, q * 32 : q * 32 + 32]

    first_plane.wait_send()
    for k in range(3):
        for copy in near[k]:
            copy.wait_send()
    for copy in rows_out:
        copy.wait_send()
    for buffer, sem in (
        (modbuf, mod_send), (partbuf, part_send), (respbuf, resp_send),
        (flubuf, flu_send), (momentbuf, mom_send),
    ):
        ref = buffer.at[pl.ds(0, 31)]
        pltpu.make_async_copy(ref, ref, sem).wait()


def leave(a, b, c, a_out, b_out, c_out, sem):
    step = c.shape[0] // PIECES
    pairs = [(a, a_out), (b, b_out)]
    pairs += [(c.at[pl.ds(k * step, step)], c_out.at[pl.ds(k * step, step)]) for k in range(PIECES)]
    copies = [pltpu.make_async_copy(*pair, sem.at[k]) for k, pair in enumerate(pairs)]
    for copy in copies:
        copy.start()
    for copy in copies:
        copy.wait()


def shards(
    displacement, external_force, element_sample, lame_field, shear_field, plastic_steps, owner_slot
):
    count = displacement.shape[1]
    disp, sample = (3, count, 8, 128), (count, 8, 128)
    wt, vt, vz, x, spec = (jnp.asarray(t) for t in tables())
    operands = (
        displacement,
        wt,
        lame_field.reshape(32, 1024),
        shear_field.reshape(32, 1024),
        external_force,
        element_sample,
        vt,
        vz,
        x,
        spec,
    )
    scalars = (plastic_steps, owner_slot)
    vmem = pl.BlockSpec(memory_space=pltpu.VMEM)
    hbm = pl.BlockSpec(memory_space=pltpu.HBM)
    dma = pltpu.SemaphoreType.DMA
    disp_next, row, micro = pl.pallas_call(
        kernel,
        out_shape=(
            jax.ShapeDtypeStruct(displacement.shape, f32),
            jax.ShapeDtypeStruct((1, 8), f32),
            jax.ShapeDtypeStruct((6 * 32 * 8, 128), f32),
        ),
        in_specs=[hbm] * 12,
        out_specs=(vmem,) * 3,
        scratch_shapes=[
            *(pltpu.VMEM(a.shape, a.dtype) for a in operands),
            *(pltpu.SMEM(a.shape, a.dtype) for a in scalars),
            dma((12,)),
            pltpu.VMEM(disp, f32),
            pltpu.VMEM(disp, f32),
            pltpu.VMEM(sample, jnp.int32),
            pltpu.VMEM((32, 16, 128), bf16),
            pltpu.VMEM((512, 128), f32),
            pltpu.VMEM((3, 8, 128), f32),
            pltpu.VMEM((4,) + disp, f32),
            pltpu.VMEM((4,) + disp, f32),
            pltpu.VMEM((4,) + sample, jnp.int32),
            pltpu.VMEM((32, 16, 128), bf16),
            pltpu.VMEM((32, 1, 128), f32),
            pltpu.VMEM((32, 1, 128), f32),
            pltpu.VMEM((count, 64, 128), f32),
            pltpu.VMEM((32, count * 1024), bf16),
            pltpu.VMEM((1024, 1024), bf16),
            pltpu.VMEM((1024, 1024), bf16),
            pltpu.VMEM((1024, 1024), bf16),
            pltpu.VMEM((1024, 1024), bf16),
            pltpu.VMEM((2, 256, 128), f32),
            pltpu.VMEM((3, 256, 128), f32),
            pltpu.VMEM((6, 256, 128), f32),
            pltpu.VMEM((32, 48, 128), wire),
            pltpu.VMEM((32, 48, 128), wire),
            pltpu.VMEM((4, 1, 128), f32),
            pltpu.VMEM((1, 1, 128), f32),
            pltpu.VMEM((32, 1, 128), f32),
            pltpu.VMEM((1, 1, 128), f32),
            pltpu.VMEM((32, 1, 128), f32),
            pltpu.SemaphoreType.REGULAR, dma((2,)), dma((3, 4)), dma((3, 4)), dma, dma, dma, dma,
            dma((3,)), dma((3,)), dma, dma, dma, dma, dma, dma,
        ],
        compiler_params=pltpu.CompilerParams(collective_id=0, has_side_effects=True, vmem_limit_bytes=24 << 20),
    )(*[pltpu.with_memory_space_constraint(a, pltpu.HBM) for a in operands + scalars])
    results = (disp_next, row, micro)
    disp_next, row, micro = pl.pallas_call(
        leave,
        out_shape=tuple(jax.ShapeDtypeStruct(a.shape, a.dtype) for a in results),
        in_specs=[pl.BlockSpec(memory_space=pl.ANY)] * 3,
        out_specs=(pl.BlockSpec(memory_space=pltpu.HBM),) * 3,
        scratch_shapes=[dma((PIECES + 2,))],
        compiler_params=pltpu.CompilerParams(vmem_limit_bytes=1 << 20),
    )(*results)
    return disp_next, row, micro.reshape(6, 32, 1, 1024)


def solution(mesh):
    in_specs = (
        P(None, "dev", None, None),
        P(None, "dev", None, None),
        P("dev", None, None),
        P("grp", "dev", None),
        P("grp", "dev", None),
        P(),
        P(),
    )
    out_specs = (P(None, "dev", None, None), P(("grp", "dev"), None), P(None, "grp", "dev", None))
    return jax.shard_map(shards, mesh=mesh, in_specs=in_specs, out_specs=out_specs, check_vma=False)
```

```python
import jax
import jax.numpy as jnp
import numpy as np
from jax import lax
from jax.experimental import pallas as pl
from jax.experimental.pallas import tpu as pltpu
from jax.sharding import PartitionSpec as P

VOX = 32
HALF = 512
PIECES = 2
KMAX = 4
MESH = pl.DeviceIdType.MESH
NEAR = (-2, -1, 1, 2)

shear_ref = 1.65
lame_ref = 1.25
green_ratio = (lame_ref + shear_ref) / (lame_ref + 2.0 * shear_ref)
relax_rate = 0.35
spring_rate = 0.2
wire = jnp.bfloat16
f32 = jnp.float32
bf16 = jnp.bfloat16


def tables():
    n = np.arange(VOX)
    theta = 2.0 * np.pi / VOX
    ky = np.repeat(n, 16)
    kz = np.tile(np.arange(16), VOX)
    yy = np.repeat(n, VOX)
    zz = np.tile(n, VOX)
    k16 = np.arange(16)

    def zeta(z, k):
        angle = theta * (z * k % VOX)
        return (
            np.where(k == 0, 1.0, np.cos(angle)),
            np.where(k == 0, (-1.0) ** z, -np.sin(angle)),
        )

    cy, sy = np.cos(theta * (np.outer(n, ky) % VOX)), np.sin(theta * (np.outer(n, ky) % VOX))
    zr, zi = zeta(n[:, None], kz[None, :])
    cv, sv = np.cos(theta * (np.outer(n, yy) % VOX)), np.sin(theta * (np.outer(n, yy) % VOX))
    vr, vi = zeta(zz[None, :], k16[:, None])
    c, s = np.cos(theta * (np.outer(n, n) % VOX)), np.sin(theta * (np.outer(n, n) % VOX))
    x = np.block([[c, s], [-s, c]])

    def wave(k):
        return np.where(k % 16 == 0, 0.0, np.sin(theta * k))

    one = np.ones((VOX, HALF))
    xx, xy, xz = wave(n)[:, None] * one, wave(ky)[None] * one, wave(kz)[None] * one
    square = xx * xx + xy * xy + xz * xz
    inverse = np.where(square > 0, 1.0 / np.where(square > 0, square, 1.0), 0.0)
    weight = np.where(kz == 0, 1.0, 2.0)[None] * one
    scaled = -(1.0 / shear_ref) * inverse * weight / VOX**3
    pairs = (xx * xx, xy * xy, xz * xz, 2 * xy * xz, 2 * xx * xz, 2 * xx * xy)
    spectral = np.stack([scaled] + [green_ratio * p * inverse for p in pairs] + [xx, xy, xz])
    to = lambda a: np.asarray(a, np.float32)
    return (
        to(np.stack([cy, sy, zr, zi])),
        to(np.stack([cv, sv])),
        to(np.stack([vr, vi])),
        to(np.stack([x, x.T])),
        to(spectral),
    )


def split(a):
    high = a.astype(bf16)
    return high, (a - high.astype(f32)).astype(bf16)


def mm(a, b):
    return jnp.dot(a, b, preferred_element_type=f32)


def product(a, b):
    ah, al = split(a)
    bh, bl = split(b)
    return mm(ah, bh) + (mm(al, bh) + mm(ah, bl))


def lane_of(shape):
    return lax.broadcasted_iota(jnp.int32, shape, len(shape) - 1)


def row_of(shape):
    return lax.broadcasted_iota(jnp.int32, shape, len(shape) - 2)


def roll(a, shift, axis):
    return pltpu.roll(a, shift % a.shape[axis], axis)


def z_up(v):
    return jnp.where(lane_of(v.shape) % VOX == VOX - 1, 0.0, roll(v, -1, 2))


def z_down(v):
    return jnp.where(lane_of(v.shape) % VOX == 0, 0.0, roll(v, 1, 2))


def y_up(v):
    moved = roll(v, -VOX, 2)
    next_row = jnp.where(row_of(v.shape) == 7, 0.0, roll(moved, -1, 1))
    return jnp.where(lane_of(v.shape) < 96, moved, next_row)


def y_down(v):
    moved = roll(v, VOX, 2)
    last_row = jnp.where(row_of(v.shape) == 0, 0.0, roll(moved, 1, 1))
    return jnp.where(lane_of(v.shape) >= VOX, moved, last_row)


def yc(v):
    lane = lane_of(v.shape)
    up = roll(v, -VOX, 2)
    up = jnp.where(lane < 96, up, roll(up, -1, 1))
    down = roll(v, VOX, 2)
    down = jnp.where(lane >= VOX, down, roll(down, 1, 1))
    return 0.5 * (up - down)


def spans(distance):
    return min(distance, 4 - distance)


OTHERS = sorted(
    ((a, b, c) for a in range(4) for b in range(4) for c in range(2) if (a, b, c) != (0, 0, 0)),
    key=lambda p: (-spans(p[0]) - spans(p[1]), -p[2], p),
)


def strain_of(fields):
    slopes = []
    for w in fields:
        up = z_up(w)
        mz, dz = 0.5 * (w + up), up - w
        moved = y_up(mz)
        a, b = 0.5 * (mz + moved), moved - mz
        c = 0.5 * (dz + y_up(dz))
        slopes.append((a[1:] - a[:-1], 0.5 * (b[1:] + b[:-1]), 0.5 * (c[1:] + c[:-1])))
    x, y, z = slopes
    return (
        x[0],
        y[1],
        z[2],
        0.5 * (z[1] + y[2]),
        0.5 * (z[0] + x[2]),
        0.5 * (y[0] + x[1]),
    )


def force_of(stress):
    xx, yy, zz, yz, xz, xy = stress
    result = []
    for along_x, along_y, along_z in ((xx, xy, xz), (xy, yy, yz), (xz, yz, zz)):
        smooth = along_x + z_down(along_x)
        first = 0.25 * (smooth + y_down(smooth))
        both = along_y + along_z
        less = along_z - along_y
        rest = y_down(0.5 * (z_down(both) - less)) + 0.5 * (z_down(less) - both)
        result.append((first[:-1] - first[1:]) + 0.5 * (rest[1:] + rest[:-1]))
    return result


def stress_of(strain, lame, shear):
    spread = lame * (strain[0] + strain[1] + strain[2])
    twice = 2.0 * shear
    return [twice * e + spread for e in strain[:3]] + [twice * e for e in strain[3:]]


def norm_of(d):
    return d[0] * d[0] + d[1] * d[1] + d[2] * d[2] + 2.0 * (d[3] * d[3] + d[4] * d[4] + d[5] * d[5])


def relaxed(mu, size, rates):
    base = mu * mu * size
    scale = jnp.ones_like(mu)
    for rate in rates:
        f = base * scale * scale
        scale = scale * (1.0 - rate * (f / (1.0 + f)))
    return scale, base * scale * scale


def kernel(
    disp_in, wt_in, lame_in, shear_in, force_in, samp_in, vt_in, vz_in, x_in, spec_in, steps_in, slot_in,
    disp_out, row_out, micro_out,
    disp_raw, wt_ref, lame_raw, shear_raw, force_raw, samp_raw, vt_ref, vz_ref, x_ref, spec_ref,
    steps_ref, slot_ref, in_sem,
    disp_ref, force_ref, samp_ref, mod_ref, modwide,
    nb_first, nb_disp, nb_force, nb_samp, modbuf, part, partbuf, strainrow, one_hot_ref,
    wh, wl, vh, vl, field, disp_u, gam, flu, flubuf,
    rowbuf, joined, respbuf, moment, momentbuf,
    ready, first_sem, near_send, near_recv, mod_send, mod_recv, part_send, part_recv,
    y_send, y_recv, resp_send, resp_recv, flu_send, flu_recv, mom_send, mom_recv,
):
    me = lax.axis_index("dev")
    group = lax.axis_index("grp")
    count = disp_raw.shape[1]

    me_x, me_z, me_c = me // 8, lax.rem(me // 2, 4), lax.rem(me, 2)
    at_x = [lax.rem(me_x + k, 4) * 8 for k in range(4)]
    at_z = [lax.rem(me_z + k, 4) * 2 for k in range(4)]
    at_c = [me_c, 1 - me_c]
    peers = [at_x[a] + at_z[b] + at_c[c] for a, b, c in OTHERS]

    loads = [
        pltpu.make_async_copy(source, target, in_sem.at[k])
        for k, (source, target) in enumerate(
            (
                (disp_in, disp_raw), (wt_in, wt_ref), (lame_in, lame_raw), (shear_in, shear_raw),
                (force_in, force_raw), (samp_in, samp_raw), (vt_in, vt_ref), (vz_in, vz_ref),
                (x_in, x_ref), (spec_in, spec_ref), (steps_in, steps_ref), (slot_in, slot_ref),
            )
        )
    ]
    loads[0].start()

    barrier = pltpu.get_barrier_semaphore()
    layer = [peer for peer, (a, _, _) in zip(peers, OTHERS) if a == 0]
    entry = [peer for peer, (_, b, c) in zip(peers, OTHERS) if (b, c) == (0, 0)] + layer
    entry.append(lax.rem(me + 1, 32))
    for peer in entry:
        pl.semaphore_signal(barrier, inc=1, device_id={"dev": peer}, device_id_type=MESH)
    for i in range(1, 4):
        pl.semaphore_signal(
            barrier, inc=1, device_id={"grp": lax.rem(group + i, 4)}, device_id_type=MESH
        )
    for copy in loads[1:]:
        copy.start()

    def dense(raw, out):
        for index in np.ndindex(raw.shape[:-2]):
            out[index] = jnp.concatenate(
                [raw[(*index, pl.ds(q, 8, stride=4), slice(None))] for q in range(4)], axis=1
            )

    loads[0].wait()
    dense(disp_raw, disp_ref)
    pl.semaphore_wait(barrier, len(entry) + 3)
    first_plane = pltpu.make_async_remote_copy(
        src_ref=disp_ref.at[:, 0],
        dst_ref=nb_first,
        send_sem=first_sem.at[0],
        recv_sem=first_sem.at[1],
        device_id={"dev": lax.rem(me + 31, 32)},
        device_id_type=MESH,
    )
    pl.when(me > 0)(first_plane.start)
    for peer in layer:
        pl.semaphore_signal(ready, inc=1, device_id={"dev": peer}, device_id_type=MESH)
    for k in range(2, 6):
        loads[k].wait()
    dense(force_raw, force_ref)
    dense(samp_raw, samp_ref)
    for k, raw in enumerate((lame_raw, shear_raw)):
        wide = raw[...].astype(f32)
        for t in range(8):
            modwide[pl.ds(k * 8 + t, 32, stride=16), :] = wide[:, t * 128 : t * 128 + 128]
    for r in range(32):
        mod_ref[r] = modwide[pl.ds(r * 16, 16), :].astype(bf16)

    part[...] = jnp.zeros_like(part)
    for plane in range(count):
        strainrow[plane, pl.ds(48, 8), :] = jnp.ones((8, 128), f32)
        strainrow[plane, pl.ds(56, 8), :] = jnp.zeros((8, 128), f32)

    near = []
    for k, (source, target) in enumerate(
        ((disp_ref, nb_disp), (force_ref, nb_force), (samp_ref, nb_samp))
    ):
        for o, offset in enumerate(NEAR):
            if offset == 2 and k < 2:
                continue
            part_of = pl.ds(0 if offset == -2 else count - 1, 1) if abs(offset) == 2 else pl.ds(0, count)
            index = (part_of,) if k == 2 else (slice(None), part_of)
            near.append(
                pltpu.make_async_remote_copy(
                    src_ref=source.at[index],
                    dst_ref=target.at[(3 - o, *index)],
                    send_sem=near_send.at[k, o],
                    recv_sem=near_recv.at[k, 3 - o],
                    device_id={"dev": lax.rem(me + offset + 32, 32)},
                    device_id_type=MESH,
                )
            )

    def everyone(source, target, send, recv):
        for peer in peers:
            pltpu.make_async_remote_copy(
                src_ref=source(peer),
                dst_ref=target.at[me],
                send_sem=send,
                recv_sem=recv,
                device_id={"dev": peer},
                device_id_type=MESH,
            ).start()

    def all_arrived(target, recv):
        ref = target.at[pl.ds(0, 31)]
        pltpu.make_async_copy(ref, ref, recv).wait()

    loads[1].wait()

    @pl.loop(0, 32)
    def _(y):
        c, s = wt_ref[0, pl.ds(y, 1), :], wt_ref[1, pl.ds(y, 1), :]
        zr, zi = wt_ref[2], wt_ref[3]
        rows = pl.ds(pl.multiple_of(y * 32, 32), 32)
        for k, block in enumerate((c * zr + s * zi, c * zi - s * zr)):
            high, low = split(block)
            wh[rows, pl.ds(k * HALF, HALF)] = high
            wl[rows, pl.ds(k * HALF, HALF)] = low

    one_hots, rows_high, rows_low = [], [], []
    for plane in range(count):
        sample = samp_ref[plane]
        for s in range(8):
            hit = jnp.broadcast_to(sample[s : s + 1], (32, 128)) == (
                row_of((32, 128)) + group * 32
            )
            one_hots.append(jnp.where(hit, 1.0, 0.0).astype(bf16))
    one_hot_ref[...] = jnp.concatenate(one_hots, axis=1)
    pl.semaphore_wait(ready, len(layer))
    everyone(lambda peer: mod_ref.at[peer], modbuf, mod_send, mod_recv)
    modbuf[me] = mod_ref[me]

    pl.when(me < 31)(first_plane.wait_recv)
    fields = [
        jnp.concatenate([disp_ref[c], jnp.where(me < 31, nb_first[pl.ds(c, 1)], 0.0)], axis=0) for c in range(3)
    ]
    strain = strain_of(fields)
    for plane in range(count):
        for c in range(6):
            strainrow[plane, pl.ds(c * 8, 8), :] = strain[c][plane]
    for plane in range(count):
        for s in range(8):
            rows = strainrow[plane, pl.ds(s, 8, stride=8), :]
            high, low = split(rows)
            rows_high.append(high)
            rows_low.append(low)
    one_hot = one_hot_ref[...]

    def against(rows):
        return lax.dot_general(
            one_hot,
            jnp.concatenate(rows, axis=1),
            (((1,), (1,)), ((), ())),
            preferred_element_type=f32,
        )

    sums = against(rows_high) + against(rows_low)
    for r in range(32):
        part[r, :, pl.ds(0, 8)] = sums[r : r + 1]
    everyone(lambda peer: part.at[peer], partbuf, part_send, part_recv)
    partbuf[me] = part[me]
    for k in range(6, 12):
        loads[k].wait()

    @pl.loop(0, 32)
    def _(k):
        c, s = vt_ref[0, pl.ds(k, 1), :], vt_ref[1, pl.ds(k, 1), :]
        zr, zi = vz_ref[0], vz_ref[1]
        for p, block in enumerate((c * zr + s * zi, c * zi - s * zr)):
            rows = pl.ds(pl.multiple_of(p * HALF + k * 16, 16), 16)
            high, low = split(block)
            vh[rows, :] = high
            vl[rows, :] = low

    ref = modbuf.at[pl.ds(0, 31)]
    pltpu.make_async_copy(ref, ref, mod_recv).wait()

    def moduli(x, n):
        both = modbuf[pl.ds(x, n)].astype(f32)
        return both[:, :8], both[:, 8:]

    def at(x, n):
        return pl.ds(pl.multiple_of(x * 8, 8), n * 8)

    def planes(ref, k, x, n):
        return ref[k, at(x, n), :].reshape(n, 8, 128)

    def x_slope(ref, k, x, n, v):
        after = planes(ref, k, lax.rem(x + n, 32), 1)
        before = planes(ref, k, lax.rem(x + 31, 32), 1)
        up = jnp.concatenate([v[1:], after], axis=0)
        down = jnp.concatenate([before, v[:-1]], axis=0)
        return 0.5 * (up - down)

    def forward():
        rows = jnp.concatenate(
            [
                jnp.concatenate([field[k, pl.ds(s, 32, stride=8), :] for k in range(2)], axis=0)
                for s in range(8)
            ],
            axis=1,
        )
        high, low = split(rows)
        both = mm(jnp.concatenate([high, low], axis=0), wh[...])
        plane = both[:64] + (both[64:] + mm(high, wl[...]))
        stacked = jnp.concatenate(
            [
                jnp.concatenate([plane[:32, :HALF], plane[32:, :HALF]], axis=1),
                jnp.concatenate([plane[:32, HALF:], plane[32:, HALF:]], axis=1),
            ],
            axis=0,
        )
        return product(x_ref[0], stacked)

    ref = partbuf.at[pl.ds(0, 31)]
    pltpu.make_async_copy(ref, ref, part_recv).wait()
    for copy in near:
        copy.start()
    total = jnp.sum(partbuf[...], axis=0)
    lane1 = lane_of((1, 128))

    def pick(row, k):
        return jnp.sum(jnp.where(lane1 == k, row, 0.0), axis=1, keepdims=True)

    members = pick(total, 6)
    load = [pick(total, c) / members for c in range(6)]
    trace = load[0] + load[1] + load[2]
    d = [load[c] - trace / 3.0 if c < 3 else load[c] for c in range(6)]
    own_steps = steps_ref[group * 32 + me]
    rates = [jnp.where(k < own_steps, relax_rate, 0.0).astype(f32) for k in range(KMAX)]
    size = norm_of(d)

    @pl.loop(0, 4)
    def _(t):
        lame, shear = moduli(t * 8, 8)
        field[0, at(t * 8, 8), :] = (lame + (2.0 / 3.0) * shear).reshape(64, 128)
        scale, _ = relaxed(shear, size, rates)
        field[1, at(t * 8, 8), :] = (2.0 * shear * scale).reshape(64, 128)

    spectrum = forward()
    spectrum_a, spectrum_b = spectrum[:, :HALF], spectrum[:, HALF:]
    mix = d[0] * spec_ref[1]
    for c in range(1, 6):
        mix = mix + d[c] * spec_ref[1 + c]
    scaled = spec_ref[0]
    steady = (1.0 - green_ratio) * trace
    phi = [scaled * spectrum_b[:32], scaled * spectrum_b[32:]]
    pressure = [
        scaled * (steady * spectrum_a[:32]) - mix * phi[0],
        scaled * (steady * spectrum_a[32:]) - mix * phi[1],
    ]
    waves = [spec_ref[7 + c] for c in range(3)]
    turned = [
        d[0] * waves[0] + d[5] * waves[1] + d[4] * waves[2],
        d[5] * waves[0] + d[1] * waves[1] + d[3] * waves[2],
        d[4] * waves[0] + d[3] * waves[1] + d[2] * waves[2],
    ]
    slopes = [
        [waves[c] * pressure[k] + turned[c] * phi[k] for k in range(2)] for c in range(3)
    ]
    mixed = jnp.concatenate(
        [
            jnp.concatenate([-slopes[c][1] for c in range(3)], axis=1),
            jnp.concatenate([slopes[c][0] for c in range(3)], axis=1),
        ],
        axis=0,
    )
    back = product(x_ref[1], mixed)
    lines = jnp.concatenate(
        [
            jnp.concatenate([back[:32, c * HALF :][:, :HALF], back[32:, c * HALF :][:, :HALF]], axis=1)
            for c in range(3)
        ],
        axis=0,
    )
    high, low = split(lines)
    both = mm(jnp.concatenate([high, low], axis=0), vh[...])
    space = both[:96] + (both[96:] + mm(high, vl[...]))
    for c in range(3):
        for s in range(8):
            disp_u[c, pl.ds(s, 32, stride=8), :] = space[
                c * 32 : c * 32 + 32, s * 128 : s * 128 + 128
            ]

    source, target = row_of((128, 128)), lane_of((128, 128))
    line = source // VOX == target // VOX
    ahead = line & ((target + 1) % VOX == source % VOX)
    behind = line & ((target + VOX - 1) % VOX == source % VOX)
    z_matrix = (jnp.where(ahead, 0.5, 0.0) - jnp.where(behind, 0.5, 0.0)).astype(bf16)

    def send_planes(t):
        for b, c in sorted(((b, c) for b in range(4) for c in range(2)), key=lambda p: -spans(p[0])):
            peer = lax.rem(me_x + 2 + t, 4) * 8 + at_z[b] + at_c[c]

            def start(peer=peer):
                pltpu.make_async_remote_copy(
                    src_ref=flu.at[peer],
                    dst_ref=flubuf.at[me],
                    send_sem=flu_send,
                    recv_sem=flu_recv,
                    device_id={"dev": peer},
                    device_id_type=MESH,
                ).start()

            if (b, c) == (0, 0):
                pl.when(t != 2)(start)
            else:
                start()

    @pl.loop(0, 4)
    def _(t):
        x = lax.rem(me_x + 2 + t, 4) * 8
        ux, uy, uz = (planes(disp_u, c, x, 8) for c in range(3))
        dx = [x_slope(disp_u, c, x, 8, u) for c, u in enumerate((ux, uy, uz))]
        high, low = split(jnp.concatenate([ux, uy, uz], axis=0).reshape(192, 128))
        dz = (mm(high, z_matrix) + mm(low, z_matrix)).reshape(3, 8, 8, 128)
        change = [
            -dx[0],
            -yc(uy),
            -dz[2],
            -0.5 * (yc(uz) + dz[1]),
            -0.5 * (dx[2] + dz[0]),
            -0.5 * (dx[1] + yc(ux)),
        ]
        for c in range(6):
            gam[c, at(x, 8), :] = change[c].reshape(64, 128)
        for k in range(3):
            pair = jnp.concatenate(change[2 * k : 2 * k + 2], axis=1)
            flu[pl.ds(x, 8), pl.ds(k * 16, 16), :] = pair.astype(wire)
        send_planes(t)

    flubuf[me] = flu[me]

    def voxel(t, sums):
        x = t * 4
        lame, shear = moduli(x, 4)
        e = [load[c] + planes(gam, c, x, 4) for c in range(6)]
        tr = e[0] + e[1] + e[2]
        dv = [e[c] - tr / 3.0 if c < 3 else e[c] for c in range(6)]
        scale, f = relaxed(shear, norm_of(dv), rates)
        twice = 2.0 * shear * scale
        bulk = (lame + (2.0 / 3.0) * shear) * tr
        new = [bulk + twice * dv[c] if c < 3 else twice * dv[c] for c in range(6)]
        new += [lame, shear / (1.0 + f)]
        return tuple(a + jnp.sum(b, axis=0) for a, b in zip(sums, new))

    sums = lax.fori_loop(0, 8, voxel, tuple(jnp.zeros((8, 128), f32) for _ in range(8)))
    column = jnp.concatenate([jnp.sum(a, axis=0, keepdims=True) for a in sums], axis=0)
    column = jnp.sum(column, axis=1, keepdims=True) * (1.0 / VOX**3)
    lane8, row8 = lane_of((8, 128)), row_of((8, 128))
    own_row = jnp.sum(
        jnp.where(lane8 == row8 + group * 16, column, 0.0), axis=0, keepdims=True
    )
    for c in range(6):
        own_row = own_row + jnp.where(lane1 == group * 16 + 8 + c, load[c], 0.0)

    rowbuf[3] = own_row
    rows_out = []
    for i in range(1, 4):
        rows_out.append(
            pltpu.make_async_remote_copy(
                src_ref=rowbuf.at[3],
                dst_ref=rowbuf.at[i - 1],
                send_sem=y_send.at[i - 1],
                recv_sem=y_recv.at[i - 1],
                device_id={"grp": lax.rem(group + i, 4)},
                device_id_type=MESH,
            )
        )
        rows_out[-1].start()
    for copy in rows_out:
        copy.wait_recv()
    joined[0] = rowbuf[0] + rowbuf[1] + rowbuf[2] + rowbuf[3]
    everyone(lambda peer: joined.at[0], respbuf, resp_send, resp_recv)
    respbuf[me] = joined[0]

    for copy in near:
        copy.wait_recv()
    exists = [(me * count + j >= 3).astype(f32) * (me * count + j < 67).astype(f32) for j in range(8)]

    def extended(own, near_ref, c):
        def get(ref, p):
            return ref[c, pl.ds(p, 1)] if c is not None else ref[pl.ds(p, 1)]

        lowest = get(near_ref.at[0], 1) if c is None else get(near_ref.at[1], 0)
        planes = [lowest, get(near_ref.at[1], 0), get(near_ref.at[1], 1)]
        planes += [get(own, 0), get(own, 1)]
        planes += [get(near_ref.at[2], 0), get(near_ref.at[2], 1), get(near_ref.at[3], 0)]
        return planes

    def masked(planes):
        return jnp.concatenate([p * m for p, m in zip(planes, exists)], axis=0)

    around = [masked(extended(disp_ref, nb_disp, c)) for c in range(3)]
    outside = [masked(extended(force_ref, nb_force, c)) for c in range(3)]
    samples = extended(samp_ref, nb_samp, None)

    all_arrived(respbuf, resp_recv)
    gathered = jnp.concatenate([respbuf[r] for r in range(32)], axis=0)
    gathered = jnp.concatenate([gathered, jnp.zeros((96, 128), f32)], axis=0).T
    cells = []
    for c in range(8):
        row = jnp.concatenate(
            [gathered[g * 16 + c : g * 16 + c + 1, :32] for g in range(4)], axis=1
        )
        source = jnp.broadcast_to(row, (8, 128))
        cells.append(
            masked(
                [
                    jnp.take_along_axis(source, s[0], axis=1, mode="promise_in_bounds")[None]
                    for s in samples
                ]
            )
        )
    lame, shear = cells[6], cells[7]
    pull = force_of(cells[:6])
    res = [
        (outside[c][1:] - pull[c] - spring_rate * around[c][1:])
        * jnp.concatenate([jnp.full((1, 8, 128), m) for m in exists[1:]], axis=0)
        for c in range(3)
    ]

    def stiff(w, low):
        n = w[0].shape[0]
        strain = strain_of(w)
        stress = stress_of(strain, lame[low : low + n - 1], shear[low : low + n - 1])
        pull = force_of(stress)
        mask = jnp.concatenate(
            [jnp.full((1, 8, 128), m) for m in exists[low + 1 : low + n - 1]], axis=0
        )
        return [(pull[c] + spring_rate * w[c][1:-1]) * mask for c in range(3)]

    k1 = stiff(res, 1)
    k2 = stiff(k1, 2)
    r_own = [a[2:4] for a in res]
    k1_own = [a[1:3] for a in k1]
    k2_own = [a[0:2] for a in k2]
    energy_strain = strain_of(k2)
    energy_stress = stress_of(energy_strain, lame[3:5], shear[3:5])

    def dotted(a, b):
        total = a[0] * b[0]
        for c in range(1, 3):
            total = total + a[c] * b[c]
        return jnp.sum(jnp.sum(total, axis=0), axis=0, keepdims=True)

    energy = energy_strain[0] * energy_stress[0]
    for c in range(1, 6):
        energy = energy + (1.0 if c < 3 else 2.0) * energy_strain[c] * energy_stress[c]
    energy = jnp.sum(jnp.sum(energy, axis=0), axis=0, keepdims=True) + spring_rate * dotted(
        k2_own, k2_own
    )
    rows = [
        dotted(r_own, r_own),
        dotted(r_own, k1_own),
        dotted(k1_own, k1_own),
        dotted(k1_own, k2_own),
        dotted(k2_own, k2_own),
        energy,
        jnp.zeros((2, 128), f32),
    ]
    column = jnp.sum(jnp.concatenate(rows, axis=0), axis=1, keepdims=True)
    moment[0] = jnp.sum(jnp.where(lane8 == row8, column, 0.0), axis=0, keepdims=True)
    everyone(lambda peer: moment.at[0], momentbuf, mom_send, mom_recv)
    momentbuf[me] = moment[0]

    def owner(r, acc):
        taken = jnp.where(slot_ref[group * 32 + r] == me, 1.0, 0.0).astype(f32)
        return acc + taken * respbuf[r]

    row = lax.fori_loop(0, 32, owner, jnp.zeros((1, 128), f32))
    shifted = jnp.zeros((1, 128), f32)
    for g in range(4):
        here = (group == g).astype(f32)
        shifted = shifted + here * roll(row, -16 * g, 1)
    row_out[...] = shifted[:, :8]

    table = jnp.concatenate([respbuf[r] for r in range(32)], axis=0)
    lane32 = lane_of((32, 128))
    group_load = [
        jnp.sum(jnp.where(lane32 == group * 16 + 8 + c, table, 0.0), axis=1, keepdims=True)
        for c in range(6)
    ]
    all_arrived(flubuf, flu_recv)
    for r in range(32):
        block = flubuf[r].astype(f32)
        for c in range(6):
            micro_out[pl.ds((c * 32 + r) * 8, 8), :] = (
                group_load[c][r : r + 1] + block[c * 8 : c * 8 + 8]
            )

    all_arrived(momentbuf, mom_recv)
    total = jnp.sum(momentbuf[...], axis=0)
    m = [pick(total, k) for k in range(6)]

    def form(a, b, first):
        out = 0.0
        for i, p in enumerate(a):
            for j, q in enumerate(b):
                out = out + p * q * m[i + j + first]
        return out

    rr = m[0]
    alpha0 = rr / m[1]
    r1 = (jnp.ones_like(rr), -alpha0)
    rr1 = form(r1, r1, 0)
    beta0 = rr1 / rr
    p1 = (1.0 + beta0, -alpha0)
    alpha1 = rr1 / form(p1, p1, 1)
    r2 = (jnp.ones_like(rr), -alpha0 - alpha1 * p1[0], alpha1 * alpha0)
    rr2 = form(r2, r2, 0)
    beta1 = rr2 / rr1
    p2 = (r2[0] + beta1 * p1[0], r2[1] + beta1 * p1[1], r2[2])
    alpha2 = rr2 / form(p2, p2, 1)
    weight = (
        alpha0 + alpha1 * p1[0] + alpha2 * p2[0],
        alpha1 * p1[1] + alpha2 * p2[1],
        alpha2 * p2[2],
    )
    for c in range(3):
        new = disp_ref[c] + (
            weight[0] * r_own[c] + weight[1] * k1_own[c] + weight[2] * k2_own[c]
        )
        for p in range(count):
            for q in range(4):
                disp_out[c, p, pl.ds(q, 8, stride=4), :] = new[p][:, q * 32 : q * 32 + 32]

    pl.when(me > 0)(first_plane.wait_send)
    for copy in near:
        copy.wait_send()
    for copy in rows_out:
        copy.wait_send()
    for buffer, sem in (
        (modbuf, mod_send), (partbuf, part_send), (respbuf, resp_send),
        (flubuf, flu_send), (momentbuf, mom_send),
    ):
        ref = buffer.at[pl.ds(0, 31)]
        pltpu.make_async_copy(ref, ref, sem).wait()


def leave(a, b, c, a_out, b_out, c_out, sem):
    step = c.shape[0] // PIECES
    pairs = [(a, a_out), (b, b_out)]
    pairs += [(c.at[pl.ds(k * step, step)], c_out.at[pl.ds(k * step, step)]) for k in range(PIECES)]
    copies = [pltpu.make_async_copy(*pair, sem.at[k]) for k, pair in enumerate(pairs)]
    for copy in copies:
        copy.start()
    for copy in copies:
        copy.wait()


def shards(
    displacement, external_force, element_sample, lame_field, shear_field, plastic_steps, owner_slot
):
    count = displacement.shape[1]
    disp, sample = (3, count, 8, 128), (count, 8, 128)
    wt, vt, vz, x, spec = (jnp.asarray(t) for t in tables())
    operands = (
        displacement,
        wt,
        lame_field.reshape(32, 1024),
        shear_field.reshape(32, 1024),
        external_force,
        element_sample,
        vt,
        vz,
        x,
        spec,
    )
    scalars = (plastic_steps, owner_slot)
    vmem = pl.BlockSpec(memory_space=pltpu.VMEM)
    hbm = pl.BlockSpec(memory_space=pltpu.HBM)
    dma = pltpu.SemaphoreType.DMA
    disp_next, row, micro = pl.pallas_call(
        kernel,
        out_shape=(
            jax.ShapeDtypeStruct(displacement.shape, f32),
            jax.ShapeDtypeStruct((1, 8), f32),
            jax.ShapeDtypeStruct((6 * 32 * 8, 128), f32),
        ),
        in_specs=[hbm] * 12,
        out_specs=(vmem,) * 3,
        scratch_shapes=[
            *(pltpu.VMEM(a.shape, a.dtype) for a in operands),
            *(pltpu.SMEM(a.shape, a.dtype) for a in scalars),
            dma((12,)),
            pltpu.VMEM(disp, f32),
            pltpu.VMEM(disp, f32),
            pltpu.VMEM(sample, jnp.int32),
            pltpu.VMEM((32, 16, 128), bf16),
            pltpu.VMEM((512, 128), f32),
            pltpu.VMEM((3, 8, 128), f32),
            pltpu.VMEM((4,) + disp, f32),
            pltpu.VMEM((4,) + disp, f32),
            pltpu.VMEM((4,) + sample, jnp.int32),
            pltpu.VMEM((32, 16, 128), bf16),
            pltpu.VMEM((32, 1, 128), f32),
            pltpu.VMEM((32, 1, 128), f32),
            pltpu.VMEM((count, 64, 128), f32),
            pltpu.VMEM((32, count * 1024), bf16),
            pltpu.VMEM((1024, 1024), bf16),
            pltpu.VMEM((1024, 1024), bf16),
            pltpu.VMEM((1024, 1024), bf16),
            pltpu.VMEM((1024, 1024), bf16),
            pltpu.VMEM((2, 256, 128), f32),
            pltpu.VMEM((3, 256, 128), f32),
            pltpu.VMEM((6, 256, 128), f32),
            pltpu.VMEM((32, 48, 128), wire),
            pltpu.VMEM((32, 48, 128), wire),
            pltpu.VMEM((4, 1, 128), f32),
            pltpu.VMEM((1, 1, 128), f32),
            pltpu.VMEM((32, 1, 128), f32),
            pltpu.VMEM((1, 1, 128), f32),
            pltpu.VMEM((32, 1, 128), f32),
            pltpu.SemaphoreType.REGULAR, dma((2,)), dma((3, 4)), dma((3, 4)), dma, dma, dma, dma,
            dma((3,)), dma((3,)), dma, dma, dma, dma, dma, dma,
        ],
        compiler_params=pltpu.CompilerParams(collective_id=0, has_side_effects=True, vmem_limit_bytes=24 << 20),
    )(*[pltpu.with_memory_space_constraint(a, pltpu.HBM) for a in operands + scalars])
    results = (disp_next, row, micro)
    disp_next, row, micro = pl.pallas_call(
        leave,
        out_shape=tuple(jax.ShapeDtypeStruct(a.shape, a.dtype) for a in results),
        in_specs=[pl.BlockSpec(memory_space=pl.ANY)] * 3,
        out_specs=(pl.BlockSpec(memory_space=pltpu.HBM),) * 3,
        scratch_shapes=[dma((PIECES + 2,))],
        compiler_params=pltpu.CompilerParams(vmem_limit_bytes=1 << 20),
    )(*results)
    return disp_next, row, micro.reshape(6, 32, 1, 1024)


def solution(mesh):
    in_specs = (
        P(None, "dev", None, None),
        P(None, "dev", None, None),
        P("dev", None, None),
        P("grp", "dev", None),
        P("grp", "dev", None),
        P(),
        P(),
    )
    out_specs = (P(None, "dev", None, None), P(("grp", "dev"), None), P(None, "grp", "dev", None))
    return jax.shard_map(shards, mesh=mesh, in_specs=in_specs, out_specs=out_specs, check_vma=False)
```

```python
import jax
import jax.numpy as jnp
import numpy as np
from jax import lax
from jax.experimental import pallas as pl
from jax.experimental.pallas import tpu as pltpu
from jax.sharding import PartitionSpec as P

VOX = 32
HALF = 512
BLOCK = 32
PIECES = 1
KMAX = 4
MESH = pl.DeviceIdType.MESH
NEAR = (-2, -1, 1, 2)

shear_ref = 1.65
lame_ref = 1.25
green_ratio = (lame_ref + shear_ref) / (lame_ref + 2.0 * shear_ref)
relax_rate = 0.35
spring_rate = 0.2
wire = jnp.bfloat16
f32 = jnp.float32
bf16 = jnp.bfloat16


def tables():
    n = np.arange(VOX)
    theta = 2.0 * np.pi / VOX
    order = np.concatenate([n[::2], n[1::2]])
    ky = np.repeat(order, 16)
    kz = np.tile(np.arange(16), VOX)
    yy = np.repeat(n[:16], VOX)
    zz = np.tile(n, 16)
    k16 = np.arange(16)

    def zeta(z, k):
        angle = theta * (z * k % VOX)
        return (
            np.where(k == 0, 1.0, np.cos(angle)),
            np.where(k == 0, (-1.0) ** z, -np.sin(angle)),
        )

    cy, sy = np.cos(theta * (np.outer(n, ky) % VOX)), np.sin(theta * (np.outer(n, ky) % VOX))
    zr, zi = zeta(n[:, None], kz[None, :])
    cv, sv = np.cos(theta * (np.outer(order, yy) % VOX)), np.sin(theta * (np.outer(order, yy) % VOX))
    vr, vi = zeta(zz[None, :], k16[:, None])
    c, s = np.cos(theta * (np.outer(n, n) % VOX)), np.sin(theta * (np.outer(n, n) % VOX))
    x = np.block([[c, s], [-s, c]])

    def wave(k):
        return np.where(k % 16 == 0, 0.0, np.sin(theta * k))

    one = np.ones((VOX, HALF))
    xx, xy, xz = wave(n)[:, None] * one, wave(ky)[None] * one, wave(kz)[None] * one
    square = xx * xx + xy * xy + xz * xz
    inverse = np.where(square > 0, 1.0 / np.where(square > 0, square, 1.0), 0.0)
    weight = np.where(kz == 0, 1.0, 2.0)[None] * one
    scaled = -(1.0 / shear_ref) * inverse * weight / VOX**3
    pairs = (xx * xx, xy * xy, xz * xz, 2 * xy * xz, 2 * xx * xz, 2 * xx * xy)
    spectral = np.stack([scaled] + [green_ratio * p * inverse for p in pairs] + [xx, xy, xz])
    to = lambda a: np.asarray(a, np.float32)
    return (
        to(np.stack([cy, sy, zr, zi])),
        to(np.stack([cv, sv])),
        to(np.stack([vr, vi])),
        to(np.stack([x, x.T])),
        to(spectral),
    )


def split(a):
    high = a.astype(bf16)
    return high, (a - high.astype(f32)).astype(bf16)


def mm(a, b):
    return jnp.dot(a, b, preferred_element_type=f32)


def product(a, b):
    ah, al = split(a)
    bh, bl = split(b)
    return mm(jnp.concatenate([ah, al, ah], axis=1), jnp.concatenate([bh, bh, bl], axis=0))


def lane_of(shape):
    return lax.broadcasted_iota(jnp.int32, shape, len(shape) - 1)


def row_of(shape):
    return lax.broadcasted_iota(jnp.int32, shape, len(shape) - 2)


def roll(a, shift, axis):
    return pltpu.roll(a, shift % a.shape[axis], axis)


def shifts(v, sign):
    lane, row = lane_of(v.shape), row_of(v.shape)
    edge = lane % VOX == (VOX - 1 if sign > 0 else 0)
    inner = lane < 96 if sign > 0 else lane >= VOX
    last = row == (7 if sign > 0 else 0)

    def along_y(moved):
        return jnp.where(inner, moved, jnp.where(last, 0.0, roll(moved, -sign, 1)))

    z = jnp.where(edge, 0.0, roll(v, -sign, 2))
    y = along_y(roll(v, -sign * VOX, 2))
    both = jnp.where(edge, 0.0, along_y(roll(v, -sign * (VOX + 1), 2)))
    return z, y, both


def yc(v):
    lane = lane_of(v.shape)
    up = roll(v, -VOX, 2)
    up = jnp.where(lane < 96, up, roll(up, -1, 1))
    down = roll(v, VOX, 2)
    down = jnp.where(lane >= VOX, down, roll(down, 1, 1))
    return 0.5 * (up - down)


def spans(distance):
    return min(distance, 4 - distance)


OTHERS = sorted(
    ((a, b, c) for a in range(4) for b in range(4) for c in range(2) if (a, b, c) != (0, 0, 0)),
    key=lambda p: (-spans(p[0]) - spans(p[1]), -p[2], p),
)


def strain_of(fields):
    slopes = []
    for w in fields:
        z, y, yz = shifts(w, 1)
        near, far = w + z, y + yz
        a, b = 0.25 * (near + far), 0.5 * (far - near)
        c = 0.5 * ((z + yz) - (w + y))
        slopes.append((a[1:] - a[:-1], 0.5 * (b[1:] + b[:-1]), 0.5 * (c[1:] + c[:-1])))
    x, y, z = slopes
    return (
        x[0],
        y[1],
        z[2],
        0.5 * (z[1] + y[2]),
        0.5 * (z[0] + x[2]),
        0.5 * (y[0] + x[1]),
    )


def force_of(stress):
    xx, yy, zz, yz, xz, xy = stress
    result = []
    for along_x, along_y, along_z in ((xx, xy, xz), (xy, yy, yz), (xz, yz, zz)):
        z, y, yz = shifts(along_x, -1)
        first = 0.25 * ((along_x + z) + (y + yz))
        both = along_y + along_z
        less = along_z - along_y
        z, y, _ = shifts(less, -1)
        _, _, yz = shifts(both, -1)
        rest = 0.5 * ((yz - y) + (z - both))
        result.append((first[:-1] - first[1:]) + 0.5 * (rest[1:] + rest[:-1]))
    return result


def stress_of(strain, lame, shear):
    spread = lame * (strain[0] + strain[1] + strain[2])
    twice = 2.0 * shear
    return [twice * e + spread for e in strain[:3]] + [twice * e for e in strain[3:]]


def norm_of(d):
    return d[0] * d[0] + d[1] * d[1] + d[2] * d[2] + 2.0 * (d[3] * d[3] + d[4] * d[4] + d[5] * d[5])


def relaxed(mu, size, rates):
    base = mu * mu * size
    scale = jnp.ones_like(mu)
    for rate in rates:
        f = base * scale * scale
        scale = scale * (1.0 - rate * (f / (1.0 + f)))
    return scale, base * scale * scale


def kernel(
    disp_in, wt_in, lame_in, shear_in, force_in, samp_in, vt_in, vz_in, x_in, spec_in, steps_in, slot_in,
    disp_out, row_out, micro_out,
    disp_raw, wt_ref, lame_raw, shear_raw, force_raw, samp_raw, vt_ref, vz_ref, x_ref, spec_ref,
    steps_ref, slot_ref, in_sem,
    disp_ref, force_ref, samp_ref, mod_ref, modwide,
    nb_first, nb_disp, nb_force, nb_samp, modbuf, part, partbuf, strainrow, one_hot_ref,
    wh, wl, vh, vl, field, disp_u, flu, flubuf,
    rowbuf, joined, respbuf, moment, momentbuf,
    ready, first_sem, near_send, near_recv, mod_send, mod_recv, part_send, part_recv,
    y_send, y_recv, resp_send, resp_recv, flu_send, flu_recv, mom_send, mom_recv,
):
    me = lax.axis_index("dev")
    group = lax.axis_index("grp")
    count = disp_raw.shape[1]

    me_x, me_z, me_c = me // 8, lax.rem(me // 2, 4), lax.rem(me, 2)
    at_x = [lax.rem(me_x + k, 4) * 8 for k in range(4)]
    at_z = [lax.rem(me_z + k, 4) * 2 for k in range(4)]
    at_c = [me_c, 1 - me_c]
    peers = [at_x[a] + at_z[b] + at_c[c] for a, b, c in OTHERS]

    loads = [
        pltpu.make_async_copy(source, target, in_sem.at[k])
        for k, (source, target) in enumerate(
            (
                (disp_in, disp_raw), (wt_in, wt_ref), (lame_in, lame_raw), (shear_in, shear_raw),
                (force_in, force_raw), (samp_in, samp_raw), (vt_in, vt_ref), (vz_in, vz_ref),
                (x_in, x_ref), (spec_in, spec_ref), (steps_in, steps_ref), (slot_in, slot_ref),
            )
        )
    ]
    loads[0].start()

    barrier = pltpu.get_barrier_semaphore()
    layer = [peer for peer, (a, _, _) in zip(peers, OTHERS) if a == 0]
    entry = [peer for peer, (_, b, c) in zip(peers, OTHERS) if (b, c) == (0, 0)] + layer
    entry.append(lax.rem(me + 1, 32))
    for peer in entry:
        pl.semaphore_signal(barrier, inc=1, device_id={"dev": peer}, device_id_type=MESH)
    for i in range(1, 4):
        pl.semaphore_signal(
            barrier, inc=1, device_id={"grp": lax.rem(group + i, 4)}, device_id_type=MESH
        )
    for copy in loads[1:]:
        copy.start()

    def dense(raw, out):
        for index in np.ndindex(raw.shape[:-2]):
            out[index] = jnp.concatenate(
                [raw[(*index, pl.ds(q, 8, stride=4), slice(None))] for q in range(4)], axis=1
            )

    loads[0].wait()
    dense(disp_raw, disp_ref)
    pl.semaphore_wait(barrier, len(entry) + 3)
    first_plane = pltpu.make_async_remote_copy(
        src_ref=disp_ref.at[:, 0],
        dst_ref=nb_first,
        send_sem=first_sem.at[0],
        recv_sem=first_sem.at[1],
        device_id={"dev": lax.rem(me + 31, 32)},
        device_id_type=MESH,
    )
    pl.when(me > 0)(first_plane.start)
    for peer in layer:
        pl.semaphore_signal(ready, inc=1, device_id={"dev": peer}, device_id_type=MESH)
    for k in range(2, 6):
        loads[k].wait()
    dense(force_raw, force_ref)
    dense(samp_raw, samp_ref)
    for k, raw in enumerate((lame_raw, shear_raw)):
        wide = raw[...].astype(f32)
        for t in range(8):
            modwide[pl.ds(k * 8 + t, 32, stride=16), :] = wide[:, t * 128 : t * 128 + 128]
    for r in range(32):
        mod_ref[r] = modwide[pl.ds(r * 16, 16), :].astype(bf16)

    part[...] = jnp.zeros_like(part)
    for plane in range(count):
        strainrow[plane, pl.ds(48, 8), :] = jnp.ones((8, 128), f32)
        strainrow[plane, pl.ds(56, 8), :] = jnp.zeros((8, 128), f32)

    near = []
    for k, (source, target) in enumerate(
        ((disp_ref, nb_disp), (force_ref, nb_force), (samp_ref, nb_samp))
    ):
        for o, offset in enumerate(NEAR):
            if offset == 2 and k < 2:
                continue
            part_of = pl.ds(0 if offset == -2 else count - 1, 1) if abs(offset) == 2 else pl.ds(0, count)
            index = (part_of,) if k == 2 else (slice(None), part_of)
            near.append(
                pltpu.make_async_remote_copy(
                    src_ref=source.at[index],
                    dst_ref=target.at[(3 - o, *index)],
                    send_sem=near_send.at[k, o],
                    recv_sem=near_recv.at[k, 3 - o],
                    device_id={"dev": lax.rem(me + offset + 32, 32)},
                    device_id_type=MESH,
                )
            )

    def everyone(source, target, send, recv):
        for peer in peers:
            pltpu.make_async_remote_copy(
                src_ref=source(peer),
                dst_ref=target.at[me],
                send_sem=send,
                recv_sem=recv,
                device_id={"dev": peer},
                device_id_type=MESH,
            ).start()

    def all_arrived(target, recv):
        ref = target.at[pl.ds(0, 31)]
        pltpu.make_async_copy(ref, ref, recv).wait()

    loads[1].wait()

    @pl.loop(0, 16)
    def _(y):
        c, s = wt_ref[0, pl.ds(y, 1), :], wt_ref[1, pl.ds(y, 1), :]
        zr, zi = wt_ref[2], wt_ref[3]
        rows = pl.ds(pl.multiple_of(y * 32, 32), 32)
        for k, block in enumerate((c * zr + s * zi, c * zi - s * zr)):
            high, low = split(block)
            for odd in range(2):
                lanes = slice(odd * 256, odd * 256 + 256)
                wh[odd, rows, pl.ds(k * 256, 256)] = high[:, lanes]
                wl[odd, rows, pl.ds(k * 256, 256)] = low[:, lanes]

    one_hots, rows_high, rows_low = [], [], []
    for plane in range(count):
        sample = samp_ref[plane]
        for s in range(8):
            hit = jnp.broadcast_to(sample[s : s + 1], (32, 128)) == (
                row_of((32, 128)) + group * 32
            )
            one_hots.append(jnp.where(hit, 1.0, 0.0).astype(bf16))
    one_hot_ref[...] = jnp.concatenate(one_hots, axis=1)
    pl.semaphore_wait(ready, len(layer))
    everyone(lambda peer: mod_ref.at[peer], modbuf, mod_send, mod_recv)
    modbuf[me] = mod_ref[me]

    pl.when(me < 31)(first_plane.wait_recv)
    fields = [
        jnp.concatenate([disp_ref[c], jnp.where(me < 31, nb_first[pl.ds(c, 1)], 0.0)], axis=0) for c in range(3)
    ]
    strain = strain_of(fields)
    for plane in range(count):
        for c in range(6):
            strainrow[plane, pl.ds(c * 8, 8), :] = strain[c][plane]
    for plane in range(count):
        for s in range(8):
            rows = strainrow[plane, pl.ds(s, 8, stride=8), :]
            high, low = split(rows)
            rows_high.append(high)
            rows_low.append(low)
    one_hot = one_hot_ref[...]

    def against(rows):
        return lax.dot_general(
            one_hot,
            jnp.concatenate(rows, axis=1),
            (((1,), (1,)), ((), ())),
            preferred_element_type=f32,
        )

    sums = against(rows_high) + against(rows_low)
    for r in range(32):
        part[r, :, pl.ds(0, 8)] = sums[r : r + 1]
    everyone(lambda peer: part.at[peer], partbuf, part_send, part_recv)
    partbuf[me] = part[me]
    for k in range(6, 12):
        loads[k].wait()

    for odd in range(2):

        @pl.loop(0, 16)
        def _(k):
            row = pl.ds(odd * 16 + k, 1)
            c, s = vt_ref[0, row, :], vt_ref[1, row, :]
            zr, zi = vz_ref[0], vz_ref[1]
            for p, block in enumerate((c * zr + s * zi, c * zi - s * zr)):
                rows = pl.ds(pl.multiple_of(p * 256 + k * 16, 16), 16)
                high, low = split(block)
                vh[odd, rows, :] = high
                vl[odd, rows, :] = low

    ref = modbuf.at[pl.ds(0, 31)]
    pltpu.make_async_copy(ref, ref, mod_recv).wait()

    def moduli(x, n):
        both = modbuf[pl.ds(x, n)].astype(f32)
        return both[:, :8], both[:, 8:]

    def at(x, n):
        return pl.ds(pl.multiple_of(x * 8, 8), n * 8)

    def planes(ref, k, x, n):
        return ref[k, at(x, n), :].reshape(n, 8, 128)

    def x_slope(ref, k, x, n, v):
        after = planes(ref, k, lax.rem(x + n, 32), 1)
        before = planes(ref, k, lax.rem(x + 31, 32), 1)
        up = jnp.concatenate([v[1:], after], axis=0)
        down = jnp.concatenate([before, v[:-1]], axis=0)
        return 0.5 * (up - down)

    def forward():
        rows = jnp.concatenate(
            [
                jnp.concatenate([field[k, pl.ds(s, 32, stride=8), :] for k in range(2)], axis=0)
                for s in range(8)
            ],
            axis=1,
        )
        halves = [rows[:, :HALF] + rows[:, HALF:], rows[:, :HALF] - rows[:, HALF:]]
        sides = []
        for odd, half in enumerate(halves):
            high, low = split(half)
            both = mm(jnp.concatenate([high, low], axis=0), wh[odd])
            sides.append(both[:64] + (both[64:] + mm(high, wl[odd])))
        plane = jnp.concatenate(
            [sides[0][:, :256], sides[1][:, :256], sides[0][:, 256:], sides[1][:, 256:]], axis=1
        )
        stacked = jnp.concatenate(
            [
                jnp.concatenate([plane[:32, :HALF], plane[32:, :HALF]], axis=1),
                jnp.concatenate([plane[:32, HALF:], plane[32:, HALF:]], axis=1),
            ],
            axis=0,
        )
        return product(x_ref[0], stacked)

    ref = partbuf.at[pl.ds(0, 31)]
    pltpu.make_async_copy(ref, ref, part_recv).wait()
    for copy in near:
        copy.start()
    total = jnp.sum(partbuf[...], axis=0)
    lane1 = lane_of((1, 128))

    def pick(row, k):
        return jnp.sum(jnp.where(lane1 == k, row, 0.0), axis=1, keepdims=True)

    members = pick(total, 6)
    load = [pick(total, c) / members for c in range(6)]
    trace = load[0] + load[1] + load[2]
    d = [load[c] - trace / 3.0 if c < 3 else load[c] for c in range(6)]
    own_steps = steps_ref[group * 32 + me]
    rates = [jnp.where(k < own_steps, relax_rate, 0.0).astype(f32) for k in range(KMAX)]
    size = norm_of(d)

    @pl.loop(0, 4)
    def _(t):
        lame, shear = moduli(t * 8, 8)
        field[0, at(t * 8, 8), :] = (lame + (2.0 / 3.0) * shear).reshape(64, 128)
        scale, _ = relaxed(shear, size, rates)
        field[1, at(t * 8, 8), :] = (2.0 * shear * scale).reshape(64, 128)

    spectrum = forward()
    spectrum_a, spectrum_b = spectrum[:, :HALF], spectrum[:, HALF:]
    mix = d[0] * spec_ref[1]
    for c in range(1, 6):
        mix = mix + d[c] * spec_ref[1 + c]
    scaled = spec_ref[0]
    steady = (1.0 - green_ratio) * trace
    phi = [scaled * spectrum_b[:32], scaled * spectrum_b[32:]]
    pressure = [
        scaled * (steady * spectrum_a[:32]) - mix * phi[0],
        scaled * (steady * spectrum_a[32:]) - mix * phi[1],
    ]
    waves = [spec_ref[7 + c] for c in range(3)]
    turned = [
        d[0] * waves[0] + d[5] * waves[1] + d[4] * waves[2],
        d[5] * waves[0] + d[1] * waves[1] + d[3] * waves[2],
        d[4] * waves[0] + d[3] * waves[1] + d[2] * waves[2],
    ]
    slopes = [
        [waves[c] * pressure[k] + turned[c] * phi[k] for k in range(2)] for c in range(3)
    ]
    mixed = jnp.concatenate(
        [
            jnp.concatenate([-slopes[c][1] for c in range(3)], axis=1),
            jnp.concatenate([slopes[c][0] for c in range(3)], axis=1),
        ],
        axis=0,
    )
    back = product(x_ref[1], mixed)
    sides = []
    for odd in range(2):
        lines = jnp.concatenate(
            [
                jnp.concatenate(
                    [back[h : h + 32, c * HALF + odd * 256 :][:, :256] for h in (0, 32)], axis=1
                )
                for c in range(3)
            ],
            axis=0,
        )
        high, low = split(lines)
        both = mm(jnp.concatenate([high, low], axis=0), vh[odd])
        sides.append(both[:96] + (both[96:] + mm(high, vl[odd])))
    space = jnp.concatenate([sides[0] + sides[1], sides[0] - sides[1]], axis=1)
    for c in range(3):
        for s in range(8):
            disp_u[c, pl.ds(s, 32, stride=8), :] = space[
                c * 32 : c * 32 + 32, s * 128 : s * 128 + 128
            ]

    source, target = row_of((128, 128)), lane_of((128, 128))
    line = source // VOX == target // VOX
    ahead = line & ((target + 1) % VOX == source % VOX)
    behind = line & ((target + VOX - 1) % VOX == source % VOX)
    z_matrix = (jnp.where(ahead, 0.5, 0.0) - jnp.where(behind, 0.5, 0.0)).astype(bf16)

    def voxel(t, sums):
        x = t * BLOCK
        ux, uy, uz = (planes(disp_u, c, x, BLOCK) for c in range(3))
        dx = [x_slope(disp_u, c, x, BLOCK, u) for c, u in enumerate((ux, uy, uz))]
        high, low = split(jnp.concatenate([ux, uy, uz], axis=0).reshape(24 * BLOCK, 128))
        dz = (mm(high, z_matrix) + mm(low, z_matrix)).reshape(3, BLOCK, 8, 128)
        change = [
            -dx[0],
            -yc(uy),
            -dz[2],
            -0.5 * (yc(uz) + dz[1]),
            -0.5 * (dx[2] + dz[0]),
            -0.5 * (dx[1] + yc(ux)),
        ]
        for k in range(3):
            pair = jnp.concatenate(change[2 * k : 2 * k + 2], axis=1)
            flu[pl.ds(x, BLOCK), pl.ds(k * 16, 16), :] = pair.astype(wire)
        lame, shear = moduli(x, BLOCK)
        e = [load[c] + change[c] for c in range(6)]
        tr = e[0] + e[1] + e[2]
        dv = [e[c] - tr / 3.0 if c < 3 else e[c] for c in range(6)]
        scale, f = relaxed(shear, norm_of(dv), rates)
        twice = 2.0 * shear * scale
        bulk = (lame + (2.0 / 3.0) * shear) * tr
        new = [bulk + twice * dv[c] if c < 3 else twice * dv[c] for c in range(6)]
        new += [lame, shear / (1.0 + f)]
        return tuple(a + jnp.sum(b, axis=0) for a, b in zip(sums, new))

    zero = jnp.zeros((8, 128), f32)
    sums = lax.fori_loop(0, 32 // BLOCK, voxel, (zero,) * 8)
    column = jnp.concatenate([jnp.sum(a, axis=0, keepdims=True) for a in sums], axis=0)
    column = jnp.sum(column, axis=1, keepdims=True) * (1.0 / VOX**3)
    lane8, row8 = lane_of((8, 128)), row_of((8, 128))
    own_row = jnp.sum(
        jnp.where(lane8 == row8 + group * 16, column, 0.0), axis=0, keepdims=True
    )
    for c in range(6):
        own_row = own_row + jnp.where(lane1 == group * 16 + 8 + c, load[c], 0.0)

    rowbuf[3] = own_row
    rows_out = []
    for i in range(1, 4):
        rows_out.append(
            pltpu.make_async_remote_copy(
                src_ref=rowbuf.at[3],
                dst_ref=rowbuf.at[i - 1],
                send_sem=y_send.at[i - 1],
                recv_sem=y_recv.at[i - 1],
                device_id={"grp": lax.rem(group + i, 4)},
                device_id_type=MESH,
            )
        )
        rows_out[-1].start()
    for copy in rows_out:
        copy.wait_recv()
    joined[0] = rowbuf[0] + rowbuf[1] + rowbuf[2] + rowbuf[3]
    everyone(lambda peer: joined.at[0], respbuf, resp_send, resp_recv)
    respbuf[me] = joined[0]
    everyone(lambda peer: flu.at[peer], flubuf, flu_send, flu_recv)
    flubuf[me] = flu[me]

    for copy in near:
        copy.wait_recv()
    exists = [(me * count + j >= 3).astype(f32) * (me * count + j < 67).astype(f32) for j in range(8)]

    def extended(own, near_ref, c):
        def get(ref, p):
            return ref[c, pl.ds(p, 1)] if c is not None else ref[pl.ds(p, 1)]

        lowest = get(near_ref.at[0], 1) if c is None else get(near_ref.at[1], 0)
        planes = [lowest, get(near_ref.at[1], 0), get(near_ref.at[1], 1)]
        planes += [get(own, 0), get(own, 1)]
        planes += [get(near_ref.at[2], 0), get(near_ref.at[2], 1), get(near_ref.at[3], 0)]
        return planes

    def masked(planes):
        return jnp.concatenate([p * m for p, m in zip(planes, exists)], axis=0)

    around = [masked(extended(disp_ref, nb_disp, c)) for c in range(3)]
    outside = [masked(extended(force_ref, nb_force, c)) for c in range(3)]
    given = [
        (outside[c][1:] - spring_rate * around[c][1:])
        * jnp.concatenate([jnp.full((1, 8, 128), m) for m in exists[1:]], axis=0)
        for c in range(3)
    ]
    samples = extended(samp_ref, nb_samp, None)

    all_arrived(respbuf, resp_recv)
    gathered = jnp.concatenate([respbuf[r] for r in range(32)], axis=0)
    gathered = jnp.concatenate([gathered, jnp.zeros((96, 128), f32)], axis=0).T
    cells = []
    for c in range(8):
        row = jnp.concatenate(
            [gathered[g * 16 + c : g * 16 + c + 1, :32] for g in range(4)], axis=1
        )
        source = jnp.broadcast_to(row, (8, 128))
        cells.append(
            masked(
                [
                    jnp.take_along_axis(source, s[0], axis=1, mode="promise_in_bounds")[None]
                    for s in samples
                ]
            )
        )
    lame, shear = cells[6], cells[7]
    pull = force_of(cells[:6])
    inside = jnp.concatenate([jnp.full((1, 8, 128), m) for m in exists[1:]], axis=0)
    res = [given[c] - pull[c] * inside for c in range(3)]

    def stiff(w, low):
        n = w[0].shape[0]
        strain = strain_of(w)
        stress = stress_of(strain, lame[low : low + n - 1], shear[low : low + n - 1])
        pull = force_of(stress)
        mask = jnp.concatenate(
            [jnp.full((1, 8, 128), m) for m in exists[low + 1 : low + n - 1]], axis=0
        )
        return [(pull[c] + spring_rate * w[c][1:-1]) * mask for c in range(3)]

    k1 = stiff(res, 1)
    k2 = stiff(k1, 2)
    r_own = [a[2:4] for a in res]
    k1_own = [a[1:3] for a in k1]
    k2_own = [a[0:2] for a in k2]
    energy_strain = strain_of(k2)
    energy_stress = stress_of(energy_strain, lame[3:5], shear[3:5])

    def dotted(a, b):
        total = a[0] * b[0]
        for c in range(1, 3):
            total = total + a[c] * b[c]
        return jnp.sum(jnp.sum(total, axis=0), axis=0, keepdims=True)

    energy = energy_strain[0] * energy_stress[0]
    for c in range(1, 6):
        energy = energy + (1.0 if c < 3 else 2.0) * energy_strain[c] * energy_stress[c]
    energy = jnp.sum(jnp.sum(energy, axis=0), axis=0, keepdims=True) + spring_rate * dotted(
        k2_own, k2_own
    )
    rows = [
        dotted(r_own, r_own),
        dotted(r_own, k1_own),
        dotted(k1_own, k1_own),
        dotted(k1_own, k2_own),
        dotted(k2_own, k2_own),
        energy,
        jnp.zeros((2, 128), f32),
    ]
    column = jnp.sum(jnp.concatenate(rows, axis=0), axis=1, keepdims=True)
    moment[0] = jnp.sum(jnp.where(lane8 == row8, column, 0.0), axis=0, keepdims=True)
    everyone(lambda peer: moment.at[0], momentbuf, mom_send, mom_recv)
    momentbuf[me] = moment[0]

    def owner(r, acc):
        taken = jnp.where(slot_ref[group * 32 + r] == me, 1.0, 0.0).astype(f32)
        return acc + taken * respbuf[r]

    row = lax.fori_loop(0, 32, owner, jnp.zeros((1, 128), f32))
    shifted = jnp.zeros((1, 128), f32)
    for g in range(4):
        here = (group == g).astype(f32)
        shifted = shifted + here * roll(row, -16 * g, 1)
    row_out[...] = shifted[:, :8]

    table = jnp.concatenate([respbuf[r] for r in range(32)], axis=0)
    lane32 = lane_of((32, 128))
    group_load = [
        jnp.sum(jnp.where(lane32 == group * 16 + 8 + c, table, 0.0), axis=1, keepdims=True)
        for c in range(6)
    ]
    all_arrived(flubuf, flu_recv)
    for r in range(32):
        block = flubuf[r].astype(f32)
        for c in range(6):
            micro_out[pl.ds((c * 32 + r) * 8, 8), :] = (
                group_load[c][r : r + 1] + block[c * 8 : c * 8 + 8]
            )

    all_arrived(momentbuf, mom_recv)
    total = jnp.sum(momentbuf[...], axis=0)
    m = [pick(total, k) for k in range(6)]

    def form(a, b, first):
        out = 0.0
        for i, p in enumerate(a):
            for j, q in enumerate(b):
                out = out + p * q * m[i + j + first]
        return out

    rr = m[0]
    alpha0 = rr / m[1]
    r1 = (jnp.ones_like(rr), -alpha0)
    rr1 = form(r1, r1, 0)
    beta0 = rr1 / rr
    p1 = (1.0 + beta0, -alpha0)
    alpha1 = rr1 / form(p1, p1, 1)
    r2 = (jnp.ones_like(rr), -alpha0 - alpha1 * p1[0], alpha1 * alpha0)
    rr2 = form(r2, r2, 0)
    beta1 = rr2 / rr1
    p2 = (r2[0] + beta1 * p1[0], r2[1] + beta1 * p1[1], r2[2])
    alpha2 = rr2 / form(p2, p2, 1)
    weight = (
        alpha0 + alpha1 * p1[0] + alpha2 * p2[0],
        alpha1 * p1[1] + alpha2 * p2[1],
        alpha2 * p2[2],
    )
    for c in range(3):
        new = disp_ref[c] + (
            weight[0] * r_own[c] + weight[1] * k1_own[c] + weight[2] * k2_own[c]
        )
        for p in range(count):
            for q in range(4):
                disp_out[c, p, pl.ds(q, 8, stride=4), :] = new[p][:, q * 32 : q * 32 + 32]

    pl.when(me > 0)(first_plane.wait_send)
    for copy in near:
        copy.wait_send()
    for copy in rows_out:
        copy.wait_send()
    for buffer, sem in (
        (modbuf, mod_send), (partbuf, part_send), (respbuf, resp_send),
        (flubuf, flu_send), (momentbuf, mom_send),
    ):
        ref = buffer.at[pl.ds(0, 31)]
        pltpu.make_async_copy(ref, ref, sem).wait()


def leave(a, b, c, a_out, b_out, c_out, sem):
    step = c.shape[0] // PIECES
    pairs = [(a, a_out), (b, b_out)]
    pairs += [(c.at[pl.ds(k * step, step)], c_out.at[pl.ds(k * step, step)]) for k in range(PIECES)]
    copies = [pltpu.make_async_copy(*pair, sem.at[k]) for k, pair in enumerate(pairs)]
    for copy in copies:
        copy.start()
    for copy in copies:
        copy.wait()


def shards(
    displacement, external_force, element_sample, lame_field, shear_field, plastic_steps, owner_slot
):
    count = displacement.shape[1]
    disp, sample = (3, count, 8, 128), (count, 8, 128)
    wt, vt, vz, x, spec = (jnp.asarray(t) for t in tables())
    operands = (
        displacement,
        wt,
        lame_field.reshape(32, 1024),
        shear_field.reshape(32, 1024),
        external_force,
        element_sample,
        vt,
        vz,
        x,
        spec,
    )
    scalars = (plastic_steps, owner_slot)
    vmem = pl.BlockSpec(memory_space=pltpu.VMEM)
    hbm = pl.BlockSpec(memory_space=pltpu.HBM)
    dma = pltpu.SemaphoreType.DMA
    disp_next, row, micro = pl.pallas_call(
        kernel,
        out_shape=(
            jax.ShapeDtypeStruct(displacement.shape, f32),
            jax.ShapeDtypeStruct((1, 8), f32),
            jax.ShapeDtypeStruct((6 * 32 * 8, 128), f32),
        ),
        in_specs=[hbm] * 12,
        out_specs=(vmem,) * 3,
        scratch_shapes=[
            *(pltpu.VMEM(a.shape, a.dtype) for a in operands),
            *(pltpu.SMEM(a.shape, a.dtype) for a in scalars),
            dma((12,)),
            pltpu.VMEM(disp, f32),
            pltpu.VMEM(disp, f32),
            pltpu.VMEM(sample, jnp.int32),
            pltpu.VMEM((32, 16, 128), bf16),
            pltpu.VMEM((512, 128), f32),
            pltpu.VMEM((3, 8, 128), f32),
            pltpu.VMEM((4,) + disp, f32),
            pltpu.VMEM((4,) + disp, f32),
            pltpu.VMEM((4,) + sample, jnp.int32),
            pltpu.VMEM((32, 16, 128), bf16),
            pltpu.VMEM((32, 1, 128), f32),
            pltpu.VMEM((32, 1, 128), f32),
            pltpu.VMEM((count, 64, 128), f32),
            pltpu.VMEM((32, count * 1024), bf16),
            *(pltpu.VMEM((2, HALF, HALF), bf16),) * 4,
            pltpu.VMEM((2, 256, 128), f32),
            pltpu.VMEM((3, 256, 128), f32),
            pltpu.VMEM((32, 48, 128), wire),
            pltpu.VMEM((32, 48, 128), wire),
            pltpu.VMEM((4, 1, 128), f32),
            pltpu.VMEM((1, 1, 128), f32),
            pltpu.VMEM((32, 1, 128), f32),
            pltpu.VMEM((1, 1, 128), f32),
            pltpu.VMEM((32, 1, 128), f32),
            pltpu.SemaphoreType.REGULAR, dma((2,)), dma((3, 4)), dma((3, 4)), dma, dma, dma, dma,
            dma((3,)), dma((3,)), dma, dma, dma, dma, dma, dma,
        ],
        compiler_params=pltpu.CompilerParams(collective_id=0, has_side_effects=True, vmem_limit_bytes=24 << 20),
    )(*[pltpu.with_memory_space_constraint(a, pltpu.HBM) for a in operands + scalars])
    results = (disp_next, row, micro)
    disp_next, row, micro = pl.pallas_call(
        leave,
        out_shape=tuple(jax.ShapeDtypeStruct(a.shape, a.dtype) for a in results),
        in_specs=[pl.BlockSpec(memory_space=pl.ANY)] * 3,
        out_specs=(pl.BlockSpec(memory_space=pltpu.HBM),) * 3,
        scratch_shapes=[dma((PIECES + 2,))],
        compiler_params=pltpu.CompilerParams(vmem_limit_bytes=1 << 20),
    )(*results)
    return disp_next, row, micro.reshape(6, 32, 1, 1024)


def solution(mesh):
    in_specs = (
        P(None, "dev", None, None),
        P(None, "dev", None, None),
        P("dev", None, None),
        P("grp", "dev", None),
        P("grp", "dev", None),
        P(),
        P(),
    )
    out_specs = (P(None, "dev", None, None), P(("grp", "dev"), None), P(None, "grp", "dev", None))
    return jax.shard_map(shards, mesh=mesh, in_specs=in_specs, out_specs=out_specs, check_vma=False)
```

```python
import jax
import jax.numpy as jnp
import numpy as np
from jax import lax
from jax.experimental import pallas as pl
from jax.experimental.pallas import tpu as pltpu
from jax.sharding import PartitionSpec as P

VOX = 32
HALF = 512
BLOCK = 32
PIECES = 1
KMAX = 4
MESH = pl.DeviceIdType.MESH
NEAR = (-2, -1, 1, 2)

shear_ref = 1.65
lame_ref = 1.25
green_ratio = (lame_ref + shear_ref) / (lame_ref + 2.0 * shear_ref)
relax_rate = 0.35
spring_rate = 0.2
wire = jnp.bfloat16
f32 = jnp.float32
bf16 = jnp.bfloat16


def tables():
    n = np.arange(VOX)
    theta = 2.0 * np.pi / VOX
    order = np.concatenate([n[::2], n[1::2]])
    ky = np.repeat(order, 16)
    kz = np.tile(np.arange(16), VOX)
    yy = np.repeat(n[:16], VOX)
    zz = np.tile(n, 16)
    k16 = np.arange(16)

    def zeta(z, k):
        angle = theta * (z * k % VOX)
        return (
            np.where(k == 0, 1.0, np.cos(angle)),
            np.where(k == 0, (-1.0) ** z, -np.sin(angle)),
        )

    cy, sy = np.cos(theta * (np.outer(n, ky) % VOX)), np.sin(theta * (np.outer(n, ky) % VOX))
    zr, zi = zeta(n[:, None], kz[None, :])
    cv, sv = np.cos(theta * (np.outer(order, yy) % VOX)), np.sin(theta * (np.outer(order, yy) % VOX))
    vr, vi = zeta(zz[None, :], k16[:, None])
    c, s = np.cos(theta * (np.outer(n, n) % VOX)), np.sin(theta * (np.outer(n, n) % VOX))
    x = np.block([[c, s], [-s, c]])

    def wave(k):
        return np.where(k % 16 == 0, 0.0, np.sin(theta * k))

    one = np.ones((VOX, HALF))
    xx, xy, xz = wave(n)[:, None] * one, wave(ky)[None] * one, wave(kz)[None] * one
    square = xx * xx + xy * xy + xz * xz
    inverse = np.where(square > 0, 1.0 / np.where(square > 0, square, 1.0), 0.0)
    weight = np.where(kz == 0, 1.0, 2.0)[None] * one
    scaled = -(1.0 / shear_ref) * inverse * weight / VOX**3
    pairs = (xx * xx, xy * xy, xz * xz, 2 * xy * xz, 2 * xx * xz, 2 * xx * xy)
    spectral = np.stack([scaled] + [green_ratio * p * inverse for p in pairs] + [xx, xy, xz])
    to = lambda a: np.asarray(a, np.float32)
    return (
        to(np.stack([cy, sy, zr, zi])),
        to(np.stack([cv, sv])),
        to(np.stack([vr, vi])),
        to(np.stack([x, x.T])),
        to(spectral),
    )


def split(a):
    high = a.astype(bf16)
    return high, (a - high.astype(f32)).astype(bf16)


def mm(a, b):
    return jnp.dot(a, b, preferred_element_type=f32)


def product(a, b):
    ah, al = split(a)
    bh, bl = split(b)
    return mm(jnp.concatenate([ah, al, ah], axis=1), jnp.concatenate([bh, bh, bl], axis=0))


def lane_of(shape):
    return lax.broadcasted_iota(jnp.int32, shape, len(shape) - 1)


def row_of(shape):
    return lax.broadcasted_iota(jnp.int32, shape, len(shape) - 2)


def roll(a, shift, axis):
    return pltpu.roll(a, shift % a.shape[axis], axis)


def shifts(v, sign):
    lane, row = lane_of(v.shape), row_of(v.shape)
    edge = lane % VOX == (VOX - 1 if sign > 0 else 0)
    inner = lane < 96 if sign > 0 else lane >= VOX
    last = row == (7 if sign > 0 else 0)

    def along_y(moved):
        return jnp.where(inner, moved, jnp.where(last, 0.0, roll(moved, -sign, 1)))

    z = jnp.where(edge, 0.0, roll(v, -sign, 2))
    y = along_y(roll(v, -sign * VOX, 2))
    both = jnp.where(edge, 0.0, along_y(roll(v, -sign * (VOX + 1), 2)))
    return z, y, both


def yc(v):
    lane = lane_of(v.shape)
    up = roll(v, -VOX, 2)
    up = jnp.where(lane < 96, up, roll(up, -1, 1))
    down = roll(v, VOX, 2)
    down = jnp.where(lane >= VOX, down, roll(down, 1, 1))
    return 0.5 * (up - down)


def spans(distance):
    return min(distance, 4 - distance)


OTHERS = sorted(
    ((a, b, c) for a in range(4) for b in range(4) for c in range(2) if (a, b, c) != (0, 0, 0)),
    key=lambda p: (-spans(p[0]) - spans(p[1]), -p[2], p),
)


def strain_of(fields):
    slopes = []
    for w in fields:
        z, y, yz = shifts(w, 1)
        near, far = w + z, y + yz
        a, b = 0.25 * (near + far), 0.5 * (far - near)
        c = 0.5 * ((z + yz) - (w + y))
        slopes.append((a[1:] - a[:-1], 0.5 * (b[1:] + b[:-1]), 0.5 * (c[1:] + c[:-1])))
    x, y, z = slopes
    return (
        x[0],
        y[1],
        z[2],
        0.5 * (z[1] + y[2]),
        0.5 * (z[0] + x[2]),
        0.5 * (y[0] + x[1]),
    )


def force_of(stress):
    xx, yy, zz, yz, xz, xy = stress
    result = []
    for along_x, along_y, along_z in ((xx, xy, xz), (xy, yy, yz), (xz, yz, zz)):
        z, y, yz = shifts(along_x, -1)
        first = 0.25 * ((along_x + z) + (y + yz))
        both = along_y + along_z
        less = along_z - along_y
        z, y, _ = shifts(less, -1)
        _, _, yz = shifts(both, -1)
        rest = 0.5 * ((yz - y) + (z - both))
        result.append((first[:-1] - first[1:]) + 0.5 * (rest[1:] + rest[:-1]))
    return result


def stress_of(strain, lame, shear):
    spread = lame * (strain[0] + strain[1] + strain[2])
    twice = 2.0 * shear
    return [twice * e + spread for e in strain[:3]] + [twice * e for e in strain[3:]]


def norm_of(d):
    return d[0] * d[0] + d[1] * d[1] + d[2] * d[2] + 2.0 * (d[3] * d[3] + d[4] * d[4] + d[5] * d[5])


def relaxed(mu, size, rates):
    base = mu * mu * size
    scale = jnp.ones_like(mu)
    for rate in rates:
        f = base * scale * scale
        scale = scale * (1.0 - rate * (f / (1.0 + f)))
    return scale, base * scale * scale


def kernel(
    disp_in, wt_in, lame_in, shear_in, force_in, samp_in, vt_in, vz_in, x_in, spec_in, steps_in, slot_in,
    disp_out, row_out, micro_out,
    disp_raw, wt_ref, lame_raw, shear_raw, force_raw, samp_raw, vt_ref, vz_ref, x_ref, spec_ref,
    steps_ref, slot_ref, in_sem,
    disp_ref, force_ref, samp_ref, mod_ref, modwide,
    nb_first, nb_last, nb_mark, nb_disp, nb_force, nb_samp, modbuf, part, partbuf, strainrow, one_hot_ref, sums_ref,
    wh, wl, vh, vl, field, disp_u, flu, flubuf,
    rowbuf, joined, respbuf, moment, momentbuf,
    ready, first_send, first_recv, near_send, near_recv, mod_send, mod_recv, part_send, part_recv,
    y_send, y_recv, resp_send, resp_recv, flu_send, flu_recv, mom_send, mom_recv,
):
    me = lax.axis_index("dev")
    group = lax.axis_index("grp")
    count = disp_raw.shape[1]

    me_x, me_z, me_c = me // 8, lax.rem(me // 2, 4), lax.rem(me, 2)
    at_x = [lax.rem(me_x + k, 4) * 8 for k in range(4)]
    at_z = [lax.rem(me_z + k, 4) * 2 for k in range(4)]
    at_c = [me_c, 1 - me_c]
    peers = [at_x[a] + at_z[b] + at_c[c] for a, b, c in OTHERS]

    loads = [
        pltpu.make_async_copy(source, target, in_sem.at[k])
        for k, (source, target) in enumerate(
            (
                (disp_in, disp_raw), (wt_in, wt_ref), (lame_in, lame_raw), (shear_in, shear_raw),
                (force_in, force_raw), (samp_in, samp_raw), (vt_in, vt_ref), (vz_in, vz_ref),
                (x_in, x_ref), (spec_in, spec_ref), (steps_in, steps_ref), (slot_in, slot_ref),
            )
        )
    ]
    loads[0].start()
    loads[5].start()

    barrier = pltpu.get_barrier_semaphore()
    layer = [peer for peer, (a, _, _) in zip(peers, OTHERS) if a == 0]
    entry = [peer for peer, (_, b, c) in zip(peers, OTHERS) if (b, c) == (0, 0)] + layer
    entry += [lax.rem(me + 1, 32), lax.rem(me + 31, 32)]
    for peer in entry:
        pl.semaphore_signal(barrier, inc=1, device_id={"dev": peer}, device_id_type=MESH)
    for i in range(1, 4):
        pl.semaphore_signal(
            barrier, inc=1, device_id={"grp": lax.rem(group + i, 4)}, device_id_type=MESH
        )
    for k in (1, 2, 3, 4, *range(6, 12)):
        loads[k].start()

    def dense(raw, out):
        for index in np.ndindex(raw.shape[:-2]):
            out[index] = jnp.concatenate(
                [raw[(*index, pl.ds(q, 8, stride=4), slice(None))] for q in range(4)], axis=1
            )

    loads[0].wait()
    dense(disp_raw, disp_ref)
    loads[5].wait()
    dense(samp_raw, samp_ref)
    pl.semaphore_wait(barrier, len(entry) + 3)

    lowest, highest = lax.rem(me, 8) == 0, lax.rem(me, 8) == 7
    upper, lower = lowest & (me > 0), highest & (me < 31)
    above, below = lax.rem(me + 1, 32), lax.rem(me + 31, 32)

    def bordering(k, source, target, device):
        return pltpu.make_async_remote_copy(
            src_ref=source,
            dst_ref=target,
            send_sem=first_send.at[k],
            recv_sem=first_recv.at[k],
            device_id={"dev": device},
            device_id_type=MESH,
        )

    first_plane = bordering(0, disp_ref.at[:, 0], nb_first, below)
    last_planes = (
        bordering(1, disp_ref.at[:, count - 1], nb_last, above),
        bordering(2, samp_ref.at[count - 1], nb_mark, above),
    )
    pl.when(jnp.logical_not(lowest))(first_plane.start)
    for copy in last_planes:
        pl.when(lower)(copy.start)
    for peer in layer:
        pl.semaphore_signal(ready, inc=1, device_id={"dev": peer}, device_id_type=MESH)
    for k in range(2, 5):
        loads[k].wait()
    dense(force_raw, force_ref)
    for k, raw in enumerate((lame_raw, shear_raw)):
        wide = raw[...].astype(f32)
        for t in range(8):
            modwide[pl.ds(k * 8 + t, 32, stride=16), :] = wide[:, t * 128 : t * 128 + 128]
    for r in range(32):
        mod_ref[r] = modwide[pl.ds(r * 16, 16), :].astype(bf16)

    part[...] = jnp.zeros_like(part)
    for plane in range(count):
        strainrow[plane, pl.ds(48, 8), :] = jnp.ones((8, 128), f32)
        strainrow[plane, pl.ds(56, 8), :] = jnp.zeros((8, 128), f32)

    near = []
    for k, (source, target) in enumerate(
        ((disp_ref, nb_disp), (force_ref, nb_force), (samp_ref, nb_samp))
    ):
        for o, offset in enumerate(NEAR):
            if offset == 2 and k < 2:
                continue
            part_of = pl.ds(0 if offset == -2 else count - 1, 1) if abs(offset) == 2 else pl.ds(0, count)
            index = (part_of,) if k == 2 else (slice(None), part_of)
            near.append(
                pltpu.make_async_remote_copy(
                    src_ref=source.at[index],
                    dst_ref=target.at[(3 - o, *index)],
                    send_sem=near_send.at[k, o],
                    recv_sem=near_recv.at[k, 3 - o],
                    device_id={"dev": lax.rem(me + offset + 32, 32)},
                    device_id_type=MESH,
                )
            )

    def everyone(source, target, send, recv):
        for peer in peers:
            pltpu.make_async_remote_copy(
                src_ref=source(peer),
                dst_ref=target.at[me],
                send_sem=send,
                recv_sem=recv,
                device_id={"dev": peer},
                device_id_type=MESH,
            ).start()

    def all_arrived(target, recv):
        ref = target.at[pl.ds(0, 31)]
        pltpu.make_async_copy(ref, ref, recv).wait()

    loads[1].wait()

    @pl.loop(0, 16)
    def _(y):
        c, s = wt_ref[0, pl.ds(y, 1), :], wt_ref[1, pl.ds(y, 1), :]
        zr, zi = wt_ref[2], wt_ref[3]
        rows = pl.ds(pl.multiple_of(y * 32, 32), 32)
        for k, block in enumerate((c * zr + s * zi, c * zi - s * zr)):
            high, low = split(block)
            for odd in range(2):
                lanes = slice(odd * 256, odd * 256 + 256)
                wh[odd, rows, pl.ds(k * 256, 256)] = high[:, lanes]
                wl[odd, rows, pl.ds(k * 256, 256)] = low[:, lanes]

    def hot_of(sample, s, counted):
        hit = jnp.broadcast_to(sample[s : s + 1], (32, 128)) == row_of((32, 128)) + group * 32
        return jnp.where(hit, counted, 0.0).astype(bf16)

    own_last = jnp.where(lower, 0.0, 1.0).astype(f32)
    one_hot_ref[...] = jnp.concatenate(
        [hot_of(samp_ref[p], s, (1.0, own_last)[p // (count - 1)]) for p in range(count) for s in range(8)],
        axis=1,
    )
    pl.semaphore_wait(ready, len(layer))
    everyone(lambda peer: mod_ref.at[peer], modbuf, mod_send, mod_recv)
    modbuf[me] = mod_ref[me]

    def sums_of(strain, one_hot):
        n = strain[0].shape[0]
        rows_high, rows_low = [], []
        for p in range(n):
            for c in range(6):
                strainrow[p, pl.ds(c * 8, 8), :] = strain[c][p]
        for p in range(n):
            for s in range(8):
                high, low = split(strainrow[p, pl.ds(s, 8, stride=8), :])
                rows_high.append(high)
                rows_low.append(low)

        def against(rows):
            return lax.dot_general(
                one_hot,
                jnp.concatenate(rows, axis=1),
                (((1,), (1,)), ((), ())),
                preferred_element_type=f32,
            )

        return against(rows_high) + against(rows_low)

    pl.when(jnp.logical_not(highest))(first_plane.wait_recv)
    fields = [
        jnp.concatenate([disp_ref[c], jnp.where(highest, 0.0, nb_first[pl.ds(c, 1)])], axis=0)
        for c in range(3)
    ]
    sums_ref[:, pl.ds(0, 8)] = sums_of(strain_of(fields), one_hot_ref[...])

    @pl.when(upper)
    def _():
        for copy in last_planes:
            copy.wait_recv()
        between = [
            jnp.concatenate([nb_last[pl.ds(c, 1)], disp_ref[c, pl.ds(0, 1)]], axis=0) for c in range(3)
        ]
        hots = jnp.concatenate([hot_of(nb_mark, s, 1.0) for s in range(8)], axis=1)
        sums_ref[:, pl.ds(0, 8)] += sums_of(strain_of(between), hots)

    sums = sums_ref[:, pl.ds(0, 8)]
    for r in range(32):
        part[r, :, pl.ds(0, 8)] = sums[r : r + 1]
    everyone(lambda peer: part.at[peer], partbuf, part_send, part_recv)
    partbuf[me] = part[me]
    for k in range(6, 12):
        loads[k].wait()

    for odd in range(2):

        @pl.loop(0, 16)
        def _(k):
            row = pl.ds(odd * 16 + k, 1)
            c, s = vt_ref[0, row, :], vt_ref[1, row, :]
            zr, zi = vz_ref[0], vz_ref[1]
            for p, block in enumerate((c * zr + s * zi, c * zi - s * zr)):
                rows = pl.ds(pl.multiple_of(p * 256 + k * 16, 16), 16)
                high, low = split(block)
                vh[odd, rows, :] = high
                vl[odd, rows, :] = low

    ref = modbuf.at[pl.ds(0, 31)]
    pltpu.make_async_copy(ref, ref, mod_recv).wait()

    def moduli(x, n):
        both = modbuf[pl.ds(x, n)].astype(f32)
        return both[:, :8], both[:, 8:]

    def at(x, n):
        return pl.ds(pl.multiple_of(x * 8, 8), n * 8)

    def planes(ref, k, x, n):
        return ref[k, at(x, n), :].reshape(n, 8, 128)

    def x_slope(ref, k, x, n, v):
        after = planes(ref, k, lax.rem(x + n, 32), 1)
        before = planes(ref, k, lax.rem(x + 31, 32), 1)
        up = jnp.concatenate([v[1:], after], axis=0)
        down = jnp.concatenate([before, v[:-1]], axis=0)
        return 0.5 * (up - down)

    def forward():
        rows = jnp.concatenate(
            [
                jnp.concatenate([field[k, pl.ds(s, 32, stride=8), :] for k in range(2)], axis=0)
                for s in range(8)
            ],
            axis=1,
        )
        halves = [rows[:, :HALF] + rows[:, HALF:], rows[:, :HALF] - rows[:, HALF:]]
        sides = []
        for odd, half in enumerate(halves):
            high, low = split(half)
            both = mm(jnp.concatenate([high, low], axis=0), wh[odd])
            sides.append(both[:64] + (both[64:] + mm(high, wl[odd])))
        plane = jnp.concatenate(
            [sides[0][:, :256], sides[1][:, :256], sides[0][:, 256:], sides[1][:, 256:]], axis=1
        )
        stacked = jnp.concatenate(
            [
                jnp.concatenate([plane[:32, :HALF], plane[32:, :HALF]], axis=1),
                jnp.concatenate([plane[:32, HALF:], plane[32:, HALF:]], axis=1),
            ],
            axis=0,
        )
        return product(x_ref[0], stacked)

    ref = partbuf.at[pl.ds(0, 31)]
    pltpu.make_async_copy(ref, ref, part_recv).wait()
    for copy in near:
        copy.start()
    total = jnp.sum(partbuf[...], axis=0)
    lane1 = lane_of((1, 128))

    def pick(row, k):
        return jnp.sum(jnp.where(lane1 == k, row, 0.0), axis=1, keepdims=True)

    members = pick(total, 6)
    load = [pick(total, c) / members for c in range(6)]
    trace = load[0] + load[1] + load[2]
    d = [load[c] - trace / 3.0 if c < 3 else load[c] for c in range(6)]
    own_steps = steps_ref[group * 32 + me]
    rates = [jnp.where(k < own_steps, relax_rate, 0.0).astype(f32) for k in range(KMAX)]
    size = norm_of(d)

    @pl.loop(0, 4)
    def _(t):
        lame, shear = moduli(t * 8, 8)
        field[0, at(t * 8, 8), :] = (lame + (2.0 / 3.0) * shear).reshape(64, 128)
        scale, _ = relaxed(shear, size, rates)
        field[1, at(t * 8, 8), :] = (2.0 * shear * scale).reshape(64, 128)

    spectrum = forward()
    spectrum_a, spectrum_b = spectrum[:, :HALF], spectrum[:, HALF:]
    mix = d[0] * spec_ref[1]
    for c in range(1, 6):
        mix = mix + d[c] * spec_ref[1 + c]
    scaled = spec_ref[0]
    steady = (1.0 - green_ratio) * trace
    phi = [scaled * spectrum_b[:32], scaled * spectrum_b[32:]]
    pressure = [
        scaled * (steady * spectrum_a[:32]) - mix * phi[0],
        scaled * (steady * spectrum_a[32:]) - mix * phi[1],
    ]
    waves = [spec_ref[7 + c] for c in range(3)]
    turned = [
        d[0] * waves[0] + d[5] * waves[1] + d[4] * waves[2],
        d[5] * waves[0] + d[1] * waves[1] + d[3] * waves[2],
        d[4] * waves[0] + d[3] * waves[1] + d[2] * waves[2],
    ]
    slopes = [
        [waves[c] * pressure[k] + turned[c] * phi[k] for k in range(2)] for c in range(3)
    ]
    mixed = jnp.concatenate(
        [
            jnp.concatenate([-slopes[c][1] for c in range(3)], axis=1),
            jnp.concatenate([slopes[c][0] for c in range(3)], axis=1),
        ],
        axis=0,
    )
    back = product(x_ref[1], mixed)
    sides = []
    for odd in range(2):
        lines = jnp.concatenate(
            [
                jnp.concatenate(
                    [back[h : h + 32, c * HALF + odd * 256 :][:, :256] for h in (0, 32)], axis=1
                )
                for c in range(3)
            ],
            axis=0,
        )
        high, low = split(lines)
        both = mm(jnp.concatenate([high, low], axis=0), vh[odd])
        sides.append(both[:96] + (both[96:] + mm(high, vl[odd])))
    space = jnp.concatenate([sides[0] + sides[1], sides[0] - sides[1]], axis=1)
    for c in range(3):
        for s in range(8):
            disp_u[c, pl.ds(s, 32, stride=8), :] = space[
                c * 32 : c * 32 + 32, s * 128 : s * 128 + 128
            ]

    source, target = row_of((128, 128)), lane_of((128, 128))
    line = source // VOX == target // VOX
    ahead = line & ((target + 1) % VOX == source % VOX)
    behind = line & ((target + VOX - 1) % VOX == source % VOX)
    z_matrix = (jnp.where(ahead, 0.5, 0.0) - jnp.where(behind, 0.5, 0.0)).astype(bf16)

    def voxel(t, sums):
        x = t * BLOCK
        ux, uy, uz = (planes(disp_u, c, x, BLOCK) for c in range(3))
        dx = [x_slope(disp_u, c, x, BLOCK, u) for c, u in enumerate((ux, uy, uz))]
        high, low = split(jnp.concatenate([ux, uy, uz], axis=0).reshape(24 * BLOCK, 128))
        dz = (mm(high, z_matrix) + mm(low, z_matrix)).reshape(3, BLOCK, 8, 128)
        change = [
            -dx[0],
            -yc(uy),
            -dz[2],
            -0.5 * (yc(uz) + dz[1]),
            -0.5 * (dx[2] + dz[0]),
            -0.5 * (dx[1] + yc(ux)),
        ]
        for k in range(3):
            pair = jnp.concatenate(change[2 * k : 2 * k + 2], axis=1)
            flu[pl.ds(x, BLOCK), pl.ds(k * 16, 16), :] = pair.astype(wire)
        lame, shear = moduli(x, BLOCK)
        e = [load[c] + change[c] for c in range(6)]
        tr = e[0] + e[1] + e[2]
        dv = [e[c] - tr / 3.0 if c < 3 else e[c] for c in range(6)]
        scale, f = relaxed(shear, norm_of(dv), rates)
        twice = 2.0 * shear * scale
        bulk = (lame + (2.0 / 3.0) * shear) * tr
        new = [bulk + twice * dv[c] if c < 3 else twice * dv[c] for c in range(6)]
        new += [lame, shear / (1.0 + f)]
        return tuple(a + jnp.sum(b, axis=0) for a, b in zip(sums, new))

    zero = jnp.zeros((8, 128), f32)
    sums = lax.fori_loop(0, 32 // BLOCK, voxel, (zero,) * 8)
    column = jnp.concatenate([jnp.sum(a, axis=0, keepdims=True) for a in sums], axis=0)
    column = jnp.sum(column, axis=1, keepdims=True) * (1.0 / VOX**3)
    lane8, row8 = lane_of((8, 128)), row_of((8, 128))
    own_row = jnp.sum(
        jnp.where(lane8 == row8 + group * 16, column, 0.0), axis=0, keepdims=True
    )
    for c in range(6):
        own_row = own_row + jnp.where(lane1 == group * 16 + 8 + c, load[c], 0.0)

    rowbuf[3] = own_row
    rows_out = []
    for i in range(1, 4):
        rows_out.append(
            pltpu.make_async_remote_copy(
                src_ref=rowbuf.at[3],
                dst_ref=rowbuf.at[i - 1],
                send_sem=y_send.at[i - 1],
                recv_sem=y_recv.at[i - 1],
                device_id={"grp": lax.rem(group + i, 4)},
                device_id_type=MESH,
            )
        )
        rows_out[-1].start()
    for copy in rows_out:
        copy.wait_recv()
    joined[0] = rowbuf[0] + rowbuf[1] + rowbuf[2] + rowbuf[3]
    everyone(lambda peer: joined.at[0], respbuf, resp_send, resp_recv)
    respbuf[me] = joined[0]
    everyone(lambda peer: flu.at[peer], flubuf, flu_send, flu_recv)
    flubuf[me] = flu[me]

    for copy in near:
        copy.wait_recv()
    exists = [(me * count + j >= 3).astype(f32) * (me * count + j < 67).astype(f32) for j in range(8)]

    def extended(own, near_ref, c):
        def get(ref, p):
            return ref[c, pl.ds(p, 1)] if c is not None else ref[pl.ds(p, 1)]

        lowest = get(near_ref.at[0], 1) if c is None else get(near_ref.at[1], 0)
        planes = [lowest, get(near_ref.at[1], 0), get(near_ref.at[1], 1)]
        planes += [get(own, 0), get(own, 1)]
        planes += [get(near_ref.at[2], 0), get(near_ref.at[2], 1), get(near_ref.at[3], 0)]
        return planes

    def masked(planes):
        return jnp.concatenate([p * m for p, m in zip(planes, exists)], axis=0)

    around = [masked(extended(disp_ref, nb_disp, c)) for c in range(3)]
    outside = [masked(extended(force_ref, nb_force, c)) for c in range(3)]
    given = [
        (outside[c][1:] - spring_rate * around[c][1:])
        * jnp.concatenate([jnp.full((1, 8, 128), m) for m in exists[1:]], axis=0)
        for c in range(3)
    ]
    samples = extended(samp_ref, nb_samp, None)

    all_arrived(respbuf, resp_recv)
    gathered = jnp.concatenate([respbuf[r] for r in range(32)], axis=0)
    gathered = jnp.concatenate([gathered, jnp.zeros((96, 128), f32)], axis=0).T
    cells = []
    for c in range(8):
        row = jnp.concatenate(
            [gathered[g * 16 + c : g * 16 + c + 1, :32] for g in range(4)], axis=1
        )
        source = jnp.broadcast_to(row, (8, 128))
        cells.append(
            masked(
                [
                    jnp.take_along_axis(source, s[0], axis=1, mode="promise_in_bounds")[None]
                    for s in samples
                ]
            )
        )
    lame, shear = cells[6], cells[7]
    pull = force_of(cells[:6])
    inside = jnp.concatenate([jnp.full((1, 8, 128), m) for m in exists[1:]], axis=0)
    res = [given[c] - pull[c] * inside for c in range(3)]

    def stiff(w, low):
        n = w[0].shape[0]
        strain = strain_of(w)
        stress = stress_of(strain, lame[low : low + n - 1], shear[low : low + n - 1])
        pull = force_of(stress)
        mask = jnp.concatenate(
            [jnp.full((1, 8, 128), m) for m in exists[low + 1 : low + n - 1]], axis=0
        )
        return [(pull[c] + spring_rate * w[c][1:-1]) * mask for c in range(3)]

    k1 = stiff(res, 1)
    k2 = stiff(k1, 2)
    r_own = [a[2:4] for a in res]
    k1_own = [a[1:3] for a in k1]
    k2_own = [a[0:2] for a in k2]
    energy_strain = strain_of(k2)
    energy_stress = stress_of(energy_strain, lame[3:5], shear[3:5])

    def dotted(a, b):
        total = a[0] * b[0]
        for c in range(1, 3):
            total = total + a[c] * b[c]
        return jnp.sum(jnp.sum(total, axis=0), axis=0, keepdims=True)

    energy = energy_strain[0] * energy_stress[0]
    for c in range(1, 6):
        energy = energy + (1.0 if c < 3 else 2.0) * energy_strain[c] * energy_stress[c]
    energy = jnp.sum(jnp.sum(energy, axis=0), axis=0, keepdims=True) + spring_rate * dotted(
        k2_own, k2_own
    )
    rows = [
        dotted(r_own, r_own),
        dotted(r_own, k1_own),
        dotted(k1_own, k1_own),
        dotted(k1_own, k2_own),
        dotted(k2_own, k2_own),
        energy,
        jnp.zeros((2, 128), f32),
    ]
    column = jnp.sum(jnp.concatenate(rows, axis=0), axis=1, keepdims=True)
    moment[0] = jnp.sum(jnp.where(lane8 == row8, column, 0.0), axis=0, keepdims=True)
    everyone(lambda peer: moment.at[0], momentbuf, mom_send, mom_recv)
    momentbuf[me] = moment[0]

    def owner(r, acc):
        taken = jnp.where(slot_ref[group * 32 + r] == me, 1.0, 0.0).astype(f32)
        return acc + taken * respbuf[r]

    row = lax.fori_loop(0, 32, owner, jnp.zeros((1, 128), f32))
    shifted = jnp.zeros((1, 128), f32)
    for g in range(4):
        here = (group == g).astype(f32)
        shifted = shifted + here * roll(row, -16 * g, 1)
    row_out[...] = shifted[:, :8]

    table = jnp.concatenate([respbuf[r] for r in range(32)], axis=0)
    lane32 = lane_of((32, 128))
    group_load = [
        jnp.sum(jnp.where(lane32 == group * 16 + 8 + c, table, 0.0), axis=1, keepdims=True)
        for c in range(6)
    ]
    all_arrived(flubuf, flu_recv)
    for r in range(32):
        block = flubuf[r].astype(f32)
        for c in range(6):
            micro_out[pl.ds((c * 32 + r) * 8, 8), :] = (
                group_load[c][r : r + 1] + block[c * 8 : c * 8 + 8]
            )

    all_arrived(momentbuf, mom_recv)
    total = jnp.sum(momentbuf[...], axis=0)
    m = [pick(total, k) for k in range(6)]

    def form(a, b, first):
        out = 0.0
        for i, p in enumerate(a):
            for j, q in enumerate(b):
                out = out + p * q * m[i + j + first]
        return out

    rr = m[0]
    alpha0 = rr / m[1]
    r1 = (jnp.ones_like(rr), -alpha0)
    rr1 = form(r1, r1, 0)
    beta0 = rr1 / rr
    p1 = (1.0 + beta0, -alpha0)
    alpha1 = rr1 / form(p1, p1, 1)
    r2 = (jnp.ones_like(rr), -alpha0 - alpha1 * p1[0], alpha1 * alpha0)
    rr2 = form(r2, r2, 0)
    beta1 = rr2 / rr1
    p2 = (r2[0] + beta1 * p1[0], r2[1] + beta1 * p1[1], r2[2])
    alpha2 = rr2 / form(p2, p2, 1)
    weight = (
        alpha0 + alpha1 * p1[0] + alpha2 * p2[0],
        alpha1 * p1[1] + alpha2 * p2[1],
        alpha2 * p2[2],
    )
    for c in range(3):
        new = disp_ref[c] + (
            weight[0] * r_own[c] + weight[1] * k1_own[c] + weight[2] * k2_own[c]
        )
        for p in range(count):
            for q in range(4):
                disp_out[c, p, pl.ds(q, 8, stride=4), :] = new[p][:, q * 32 : q * 32 + 32]

    pl.when(jnp.logical_not(lowest))(first_plane.wait_send)
    for copy in last_planes:
        pl.when(lower)(copy.wait_send)
    for copy in near:
        copy.wait_send()
    for copy in rows_out:
        copy.wait_send()
    for buffer, sem in (
        (modbuf, mod_send), (partbuf, part_send), (respbuf, resp_send),
        (flubuf, flu_send), (momentbuf, mom_send),
    ):
        ref = buffer.at[pl.ds(0, 31)]
        pltpu.make_async_copy(ref, ref, sem).wait()


def leave(a, b, c, a_out, b_out, c_out, sem):
    step = c.shape[0] // PIECES
    pairs = [(a, a_out), (b, b_out)]
    pairs += [(c.at[pl.ds(k * step, step)], c_out.at[pl.ds(k * step, step)]) for k in range(PIECES)]
    copies = [pltpu.make_async_copy(*pair, sem.at[k]) for k, pair in enumerate(pairs)]
    for copy in copies:
        copy.start()
    for copy in copies:
        copy.wait()


def shards(
    displacement, external_force, element_sample, lame_field, shear_field, plastic_steps, owner_slot
):
    count = displacement.shape[1]
    disp, sample = (3, count, 8, 128), (count, 8, 128)
    wt, vt, vz, x, spec = (jnp.asarray(t) for t in tables())
    operands = (
        displacement,
        wt,
        lame_field.reshape(32, 1024),
        shear_field.reshape(32, 1024),
        external_force,
        element_sample,
        vt,
        vz,
        x,
        spec,
    )
    scalars = (plastic_steps, owner_slot)
    vmem = pl.BlockSpec(memory_space=pltpu.VMEM)
    hbm = pl.BlockSpec(memory_space=pltpu.HBM)
    dma = pltpu.SemaphoreType.DMA
    disp_next, row, micro = pl.pallas_call(
        kernel,
        out_shape=(
            jax.ShapeDtypeStruct(displacement.shape, f32),
            jax.ShapeDtypeStruct((1, 8), f32),
            jax.ShapeDtypeStruct((6 * 32 * 8, 128), f32),
        ),
        in_specs=[hbm] * 12,
        out_specs=(vmem,) * 3,
        scratch_shapes=[
            *(pltpu.VMEM(a.shape, a.dtype) for a in operands),
            *(pltpu.SMEM(a.shape, a.dtype) for a in scalars),
            dma((12,)),
            pltpu.VMEM(disp, f32),
            pltpu.VMEM(disp, f32),
            pltpu.VMEM(sample, jnp.int32),
            pltpu.VMEM((32, 16, 128), bf16),
            pltpu.VMEM((512, 128), f32),
            pltpu.VMEM((3, 8, 128), f32),
            pltpu.VMEM((3, 8, 128), f32),
            pltpu.VMEM((8, 128), jnp.int32),
            pltpu.VMEM((4,) + disp, f32),
            pltpu.VMEM((4,) + disp, f32),
            pltpu.VMEM((4,) + sample, jnp.int32),
            pltpu.VMEM((32, 16, 128), bf16),
            pltpu.VMEM((32, 1, 128), f32),
            pltpu.VMEM((32, 1, 128), f32),
            pltpu.VMEM((count, 64, 128), f32),
            pltpu.VMEM((32, count * 1024), bf16),
            pltpu.VMEM((32, 128), f32),
            *(pltpu.VMEM((2, HALF, HALF), bf16),) * 4,
            pltpu.VMEM((2, 256, 128), f32),
            pltpu.VMEM((3, 256, 128), f32),
            pltpu.VMEM((32, 48, 128), wire),
            pltpu.VMEM((32, 48, 128), wire),
            pltpu.VMEM((4, 1, 128), f32),
            pltpu.VMEM((1, 1, 128), f32),
            pltpu.VMEM((32, 1, 128), f32),
            pltpu.VMEM((1, 1, 128), f32),
            pltpu.VMEM((32, 1, 128), f32),
            pltpu.SemaphoreType.REGULAR, dma((3,)), dma((3,)), dma((3, 4)), dma((3, 4)), dma, dma, dma, dma,
            dma((3,)), dma((3,)), dma, dma, dma, dma, dma, dma,
        ],
        compiler_params=pltpu.CompilerParams(collective_id=0, has_side_effects=True, vmem_limit_bytes=24 << 20),
    )(*[pltpu.with_memory_space_constraint(a, pltpu.HBM) for a in operands + scalars])
    results = (disp_next, row, micro)
    disp_next, row, micro = pl.pallas_call(
        leave,
        out_shape=tuple(jax.ShapeDtypeStruct(a.shape, a.dtype) for a in results),
        in_specs=[pl.BlockSpec(memory_space=pl.ANY)] * 3,
        out_specs=(pl.BlockSpec(memory_space=pltpu.HBM),) * 3,
        scratch_shapes=[dma((PIECES + 2,))],
        compiler_params=pltpu.CompilerParams(vmem_limit_bytes=1 << 20),
    )(*results)
    return disp_next, row, micro.reshape(6, 32, 1, 1024)


def solution(mesh):
    in_specs = (
        P(None, "dev", None, None),
        P(None, "dev", None, None),
        P("dev", None, None),
        P("grp", "dev", None),
        P("grp", "dev", None),
        P(),
        P(),
    )
    out_specs = (P(None, "dev", None, None), P(("grp", "dev"), None), P(None, "grp", "dev", None))
    return jax.shard_map(shards, mesh=mesh, in_specs=in_specs, out_specs=out_specs, check_vma=False)
```

```python
import jax
import jax.numpy as jnp
import numpy as np
from jax import lax
from jax.experimental import pallas as pl
from jax.experimental.pallas import tpu as pltpu
from jax.sharding import PartitionSpec as P

VOX = 32
HALF = 512
BLOCK = 32
PIECES = 1
KMAX = 4
MESH = pl.DeviceIdType.MESH
NEAR = (-2, -1, 1, 2)

shear_ref = 1.65
lame_ref = 1.25
green_ratio = (lame_ref + shear_ref) / (lame_ref + 2.0 * shear_ref)
relax_rate = 0.35
spring_rate = 0.2
wire = jnp.bfloat16
f32 = jnp.float32
bf16 = jnp.bfloat16


def tables():
    n = np.arange(VOX)
    theta = 2.0 * np.pi / VOX
    order = np.concatenate([n[::4], n[2::4], n[1::2]])
    ky = np.repeat(order, 16)
    kz = np.tile(np.arange(16), VOX)
    yy = np.repeat(n[:16], VOX)
    zz = np.tile(n, 16)
    k16 = np.arange(16)

    def zeta(z, k):
        angle = theta * (z * k % VOX)
        return (
            np.where(k == 0, 1.0, np.cos(angle)),
            np.where(k == 0, (-1.0) ** z, -np.sin(angle)),
        )

    cy, sy = np.cos(theta * (np.outer(n, ky) % VOX)), np.sin(theta * (np.outer(n, ky) % VOX))
    zr, zi = zeta(n[:, None], kz[None, :])
    cv, sv = np.cos(theta * (np.outer(order, yy) % VOX)), np.sin(theta * (np.outer(order, yy) % VOX))
    vr, vi = zeta(zz[None, :], k16[:, None])
    c, s = np.cos(theta * (np.outer(n, n) % VOX)), np.sin(theta * (np.outer(n, n) % VOX))
    x = np.block([[c, s], [-s, c]])

    def wave(k):
        return np.where(k % 16 == 0, 0.0, np.sin(theta * k))

    one = np.ones((VOX, HALF))
    xx, xy, xz = wave(n)[:, None] * one, wave(ky)[None] * one, wave(kz)[None] * one
    square = xx * xx + xy * xy + xz * xz
    inverse = np.where(square > 0, 1.0 / np.where(square > 0, square, 1.0), 0.0)
    weight = np.where(kz == 0, 1.0, 2.0)[None] * one
    scaled = -(1.0 / shear_ref) * inverse * weight / VOX**3
    pairs = (xx * xx, xy * xy, xz * xz, 2 * xy * xz, 2 * xx * xz, 2 * xx * xy)
    spectral = np.stack([scaled] + [green_ratio * p * inverse for p in pairs] + [xx, xy, xz])
    to = lambda a: np.asarray(a, np.float32)
    return (
        to(np.stack([cy, sy, zr, zi])),
        to(np.stack([cv, sv])),
        to(np.stack([vr, vi])),
        to(np.stack([x, x.T])),
        to(spectral),
    )


def split(a):
    high = a.astype(bf16)
    return high, (a - high.astype(f32)).astype(bf16)


def mm(a, b):
    return jnp.dot(a, b, preferred_element_type=f32)


def product(a, b):
    ah, al = split(a)
    bh, bl = split(b)
    return mm(jnp.concatenate([ah, al, ah], axis=1), jnp.concatenate([bh, bh, bl], axis=0))


def lane_of(shape):
    return lax.broadcasted_iota(jnp.int32, shape, len(shape) - 1)


def row_of(shape):
    return lax.broadcasted_iota(jnp.int32, shape, len(shape) - 2)


def roll(a, shift, axis):
    return pltpu.roll(a, shift % a.shape[axis], axis)


def shifts(v, sign):
    lane, row = lane_of(v.shape), row_of(v.shape)
    edge = lane % VOX == (VOX - 1 if sign > 0 else 0)
    inner = lane < 96 if sign > 0 else lane >= VOX
    last = row == (7 if sign > 0 else 0)

    def along_y(moved):
        return jnp.where(inner, moved, jnp.where(last, 0.0, roll(moved, -sign, 1)))

    z = jnp.where(edge, 0.0, roll(v, -sign, 2))
    y = along_y(roll(v, -sign * VOX, 2))
    both = jnp.where(edge, 0.0, along_y(roll(v, -sign * (VOX + 1), 2)))
    return z, y, both


def yc(v):
    lane = lane_of(v.shape)
    up = roll(v, -VOX, 2)
    up = jnp.where(lane < 96, up, roll(up, -1, 1))
    down = roll(v, VOX, 2)
    down = jnp.where(lane >= VOX, down, roll(down, 1, 1))
    return 0.5 * (up - down)


def spans(distance):
    return min(distance, 4 - distance)


OTHERS = sorted(
    ((a, b, c) for a in range(4) for b in range(4) for c in range(2) if (a, b, c) != (0, 0, 0)),
    key=lambda p: (-spans(p[0]) - spans(p[1]), -p[2], p),
)


def strain_of(fields):
    slopes = []
    for w in fields:
        z, y, yz = shifts(w, 1)
        near, far = w + z, y + yz
        a, b = 0.25 * (near + far), 0.5 * (far - near)
        c = 0.5 * ((z + yz) - (w + y))
        slopes.append((a[1:] - a[:-1], 0.5 * (b[1:] + b[:-1]), 0.5 * (c[1:] + c[:-1])))
    x, y, z = slopes
    return (
        x[0],
        y[1],
        z[2],
        0.5 * (z[1] + y[2]),
        0.5 * (z[0] + x[2]),
        0.5 * (y[0] + x[1]),
    )


def force_of(stress):
    xx, yy, zz, yz, xz, xy = stress
    result = []
    for along_x, along_y, along_z in ((xx, xy, xz), (xy, yy, yz), (xz, yz, zz)):
        z, y, yz = shifts(along_x, -1)
        first = 0.25 * ((along_x + z) + (y + yz))
        both = along_y + along_z
        less = along_z - along_y
        z, y, _ = shifts(less, -1)
        _, _, yz = shifts(both, -1)
        rest = 0.5 * ((yz - y) + (z - both))
        result.append((first[:-1] - first[1:]) + 0.5 * (rest[1:] + rest[:-1]))
    return result


def stress_of(strain, lame, shear):
    spread = lame * (strain[0] + strain[1] + strain[2])
    twice = 2.0 * shear
    return [twice * e + spread for e in strain[:3]] + [twice * e for e in strain[3:]]


def norm_of(d):
    return d[0] * d[0] + d[1] * d[1] + d[2] * d[2] + 2.0 * (d[3] * d[3] + d[4] * d[4] + d[5] * d[5])


def relaxed(mu, size, rates):
    base = mu * mu * size
    scale = jnp.ones_like(mu)
    for rate in rates:
        f = base * scale * scale
        scale = scale * (1.0 - rate * (f / (1.0 + f)))
    return scale, base * scale * scale


def kernel(
    disp_in, wt_in, lame_in, shear_in, force_in, samp_in, vt_in, vz_in, x_in, spec_in, steps_in, slot_in,
    disp_out, row_out, micro_out,
    disp_raw, wt_ref, lame_raw, shear_raw, force_raw, samp_raw, vt_ref, vz_ref, x_ref, spec_ref,
    steps_ref, slot_ref, in_sem,
    disp_ref, force_ref, samp_ref, mod_ref, modwide,
    nb_first, nb_last, nb_mark, nb, nb_samp, modbuf, part, partbuf, strainrow, one_hot_ref, sums_ref,
    wh, wl, vh, vl, weh, wel, veh, vel, field, disp_u, flu, flubuf,
    rowbuf, joined, respbuf, moment, momentbuf,
    ready, first_send, first_recv, near_send, near_recv, mod_send, mod_recv, part_send, part_recv,
    y_send, y_recv, resp_send, resp_recv, flu_send, flu_recv, mom_send, mom_recv,
):
    me = lax.axis_index("dev")
    group = lax.axis_index("grp")
    count = disp_raw.shape[1]

    me_x, me_z, me_c = me // 8, lax.rem(me // 2, 4), lax.rem(me, 2)
    at_x = [lax.rem(me_x + k, 4) * 8 for k in range(4)]
    at_z = [lax.rem(me_z + k, 4) * 2 for k in range(4)]
    at_c = [me_c, 1 - me_c]
    peers = [at_x[a] + at_z[b] + at_c[c] for a, b, c in OTHERS]

    loads = [
        pltpu.make_async_copy(source, target, in_sem.at[k])
        for k, (source, target) in enumerate(
            (
                (disp_in, disp_raw), (wt_in, wt_ref), (lame_in, lame_raw), (shear_in, shear_raw),
                (force_in, force_raw), (samp_in, samp_raw), (vt_in, vt_ref), (vz_in, vz_ref),
                (x_in, x_ref), (spec_in, spec_ref), (steps_in, steps_ref), (slot_in, slot_ref),
            )
        )
    ]
    loads[0].start()
    loads[5].start()

    barrier = pltpu.get_barrier_semaphore()
    layer = [peer for peer, (a, _, _) in zip(peers, OTHERS) if a == 0]
    entry = [peer for peer, (_, b, c) in zip(peers, OTHERS) if (b, c) == (0, 0)] + layer
    entry += [lax.rem(me + 1, 32), lax.rem(me + 31, 32)]
    for peer in entry:
        pl.semaphore_signal(barrier, inc=1, device_id={"dev": peer}, device_id_type=MESH)
    for i in range(1, 4):
        pl.semaphore_signal(
            barrier, inc=1, device_id={"grp": lax.rem(group + i, 4)}, device_id_type=MESH
        )
    for k in (1, 2, 3, 4, *range(6, 12)):
        loads[k].start()

    def dense(raw, out):
        for index in np.ndindex(raw.shape[:-2]):
            out[index] = jnp.concatenate(
                [raw[(*index, pl.ds(q, 8, stride=4), slice(None))] for q in range(4)], axis=1
            )

    loads[0].wait()
    dense(disp_raw, disp_ref)
    loads[5].wait()
    dense(samp_raw, samp_ref)
    pl.semaphore_wait(barrier, len(entry) + 3)

    lowest, highest = lax.rem(me, 8) == 0, lax.rem(me, 8) == 7
    upper, lower = lowest & (me > 0), highest & (me < 31)
    above, below = lax.rem(me + 1, 32), lax.rem(me + 31, 32)

    def bordering(k, source, target, device):
        return pltpu.make_async_remote_copy(
            src_ref=source,
            dst_ref=target,
            send_sem=first_send.at[k],
            recv_sem=first_recv.at[k],
            device_id={"dev": device},
            device_id_type=MESH,
        )

    first_plane = bordering(0, disp_ref.at[:, 0], nb_first, below)
    last_planes = (
        bordering(1, disp_ref.at[:, count - 1], nb_last, above),
        bordering(2, samp_ref.at[count - 1], nb_mark, above),
    )
    pl.when(jnp.logical_not(lowest))(first_plane.start)
    for copy in last_planes:
        pl.when(lower)(copy.start)
    for peer in layer:
        pl.semaphore_signal(ready, inc=1, device_id={"dev": peer}, device_id_type=MESH)
    for k in range(2, 5):
        loads[k].wait()
    dense(force_raw, force_ref)
    for k, raw in enumerate((lame_raw, shear_raw)):
        wide = raw[...].astype(f32)
        for t in range(8):
            modwide[pl.ds(k * 8 + t, 32, stride=16), :] = wide[:, t * 128 : t * 128 + 128]
    for r in range(32):
        mod_ref[r] = modwide[pl.ds(r * 16, 16), :].astype(bf16)

    part[...] = jnp.zeros_like(part)
    for plane in range(count):
        strainrow[plane, pl.ds(48, 8), :] = jnp.ones((8, 128), f32)
        strainrow[plane, pl.ds(56, 8), :] = jnp.zeros((8, 128), f32)

    places = {-1: (0, 6, 1), 1: (6, 6, 1 + count), 2: (12, 3, 1 + 2 * count), -2: (None, 0, 0)}
    near = []
    for offset, (start, _, sample_start) in places.items():
        device = lax.rem(me - offset + 32, 32)
        plane = {2: 0, -2: count - 1}.get(offset)

        def send(source, target, k, device=device):
            near.append(
                pltpu.make_async_remote_copy(
                    src_ref=source,
                    dst_ref=target,
                    send_sem=near_send.at[k],
                    recv_sem=near_recv.at[k],
                    device_id={"dev": device},
                    device_id_type=MESH,
                )
            )

        width = count if plane is None else 1
        cut_out = pl.ds(0 if plane is None else plane, width)
        if start is not None:
            for k, source in enumerate((disp_ref, force_ref)):
                for c in range(3):
                    send(source.at[c, cut_out], nb.at[pl.ds(k * 15 + start + c * width, width)], 0)
        send(samp_ref.at[cut_out], nb_samp.at[pl.ds(sample_start, width)], 1)

    def everyone(source, target, send, recv):
        for peer in peers:
            pltpu.make_async_remote_copy(
                src_ref=source(peer),
                dst_ref=target.at[me],
                send_sem=send,
                recv_sem=recv,
                device_id={"dev": peer},
                device_id_type=MESH,
            ).start()

    def all_arrived(target, recv):
        ref = target.at[pl.ds(0, 31)]
        pltpu.make_async_copy(ref, ref, recv).wait()

    loads[1].wait()

    @pl.loop(0, 16)
    def _(y):
        c, s = wt_ref[0, pl.ds(y, 1), :], wt_ref[1, pl.ds(y, 1), :]
        zr, zi = wt_ref[2], wt_ref[3]
        rows = pl.ds(pl.multiple_of(y * 32, 32), 32)
        blocks = [split(b) for b in (c * zr + s * zi, c * zi - s * zr)]
        for k, (high, low) in enumerate(blocks):
            wh[rows, pl.ds(k * 256, 256)] = high[:, 256:]
            wl[rows, pl.ds(k * 256, 256)] = low[:, 256:]

        @pl.when(y < 8)
        def _():
            for k, (high, low) in enumerate(blocks):
                for q in range(2):
                    lanes = slice(q * 128, q * 128 + 128)
                    weh[q, rows, pl.ds(k * 128, 128)] = high[:, lanes]
                    wel[q, rows, pl.ds(k * 128, 128)] = low[:, lanes]

    def hot_of(sample, s, counted):
        hit = jnp.broadcast_to(sample[s : s + 1], (32, 128)) == row_of((32, 128)) + group * 32
        return jnp.where(hit, counted, 0.0).astype(bf16)

    own_last = jnp.where(lower, 0.0, 1.0).astype(f32)
    one_hot_ref[...] = jnp.concatenate(
        [hot_of(samp_ref[p], s, (1.0, own_last)[p // (count - 1)]) for p in range(count) for s in range(8)],
        axis=1,
    )
    pl.semaphore_wait(ready, len(layer))
    everyone(lambda peer: mod_ref.at[peer], modbuf, mod_send, mod_recv)
    modbuf[me] = mod_ref[me]

    def sums_of(strain, one_hot):
        n = strain[0].shape[0]
        rows_high, rows_low = [], []
        for p in range(n):
            for c in range(6):
                strainrow[p, pl.ds(c * 8, 8), :] = strain[c][p]
        for p in range(n):
            for s in range(8):
                high, low = split(strainrow[p, pl.ds(s, 8, stride=8), :])
                rows_high.append(high)
                rows_low.append(low)

        def against(rows):
            return lax.dot_general(
                one_hot,
                jnp.concatenate(rows, axis=1),
                (((1,), (1,)), ((), ())),
                preferred_element_type=f32,
            )

        return against(rows_high) + against(rows_low)

    pl.when(jnp.logical_not(highest))(first_plane.wait_recv)
    fields = [
        jnp.concatenate([disp_ref[c], jnp.where(highest, 0.0, nb_first[pl.ds(c, 1)])], axis=0)
        for c in range(3)
    ]
    sums_ref[:, pl.ds(0, 8)] = sums_of(strain_of(fields), one_hot_ref[...])

    @pl.when(upper)
    def _():
        for copy in last_planes:
            copy.wait_recv()
        between = [
            jnp.concatenate([nb_last[pl.ds(c, 1)], disp_ref[c, pl.ds(0, 1)]], axis=0) for c in range(3)
        ]
        hots = jnp.concatenate([hot_of(nb_mark, s, 1.0) for s in range(8)], axis=1)
        sums_ref[:, pl.ds(0, 8)] += sums_of(strain_of(between), hots)

    sums = sums_ref[:, pl.ds(0, 8)]
    for r in range(32):
        part[r, :, pl.ds(0, 8)] = sums[r : r + 1]
    everyone(lambda peer: part.at[peer], partbuf, part_send, part_recv)
    partbuf[me] = part[me]
    for k in range(6, 12):
        loads[k].wait()

    def back_rows(k, lanes):
        row = pl.ds(k, 1)
        c, s = vt_ref[0, row, pl.ds(0, lanes)], vt_ref[1, row, pl.ds(0, lanes)]
        zr, zi = vz_ref[0, :, pl.ds(0, lanes)], vz_ref[1, :, pl.ds(0, lanes)]
        return split(c * zr + s * zi), split(c * zi - s * zr)

    @pl.loop(0, 16)
    def _(k):
        for p, (high, low) in enumerate(back_rows(16 + k, HALF)):
            rows = pl.ds(pl.multiple_of(p * 256 + k * 16, 16), 16)
            vh[rows, :] = high
            vl[rows, :] = low

    for q in range(2):

        @pl.loop(0, 8)
        def _(k):
            for p, (high, low) in enumerate(back_rows(q * 8 + k, 256)):
                rows = pl.ds(pl.multiple_of(p * 128 + k * 16, 16), 16)
                veh[q, rows, :] = high
                vel[q, rows, :] = low

    ref = modbuf.at[pl.ds(0, 31)]
    pltpu.make_async_copy(ref, ref, mod_recv).wait()

    def moduli(x, n):
        both = modbuf[pl.ds(x, n)].astype(f32)
        return both[:, :8], both[:, 8:]

    def at(x, n):
        return pl.ds(pl.multiple_of(x * 8, 8), n * 8)

    def planes(ref, k, x, n):
        return ref[k, at(x, n), :].reshape(n, 8, 128)

    def x_slope(ref, k, x, n, v):
        after = planes(ref, k, lax.rem(x + n, 32), 1)
        before = planes(ref, k, lax.rem(x + 31, 32), 1)
        up = jnp.concatenate([v[1:], after], axis=0)
        down = jnp.concatenate([before, v[:-1]], axis=0)
        return 0.5 * (up - down)

    def forward():
        rows = jnp.concatenate(
            [
                jnp.concatenate([field[k, pl.ds(s, 32, stride=8), :] for k in range(2)], axis=0)
                for s in range(8)
            ],
            axis=1,
        )
        even, odd = rows[:, :HALF] + rows[:, HALF:], rows[:, :HALF] - rows[:, HALF:]

        def part_of(data, high_ref, low_ref):
            high, low = split(data)
            both = mm(jnp.concatenate([high, low], axis=0), high_ref[...])
            return both[:64] + (both[64:] + mm(high, low_ref[...]))

        sides = [
            part_of(even[:, :256] + even[:, 256:], weh.at[0], wel.at[0]),
            part_of(even[:, :256] - even[:, 256:], weh.at[1], wel.at[1]),
            part_of(odd, wh, wl),
        ]
        plane = jnp.concatenate(
            [side[:, : side.shape[1] // 2] for side in sides]
            + [side[:, side.shape[1] // 2 :] for side in sides],
            axis=1,
        )
        stacked = jnp.concatenate(
            [
                jnp.concatenate([plane[:32, :HALF], plane[32:, :HALF]], axis=1),
                jnp.concatenate([plane[:32, HALF:], plane[32:, HALF:]], axis=1),
            ],
            axis=0,
        )
        return product(x_ref[0], stacked)

    ref = partbuf.at[pl.ds(0, 31)]
    pltpu.make_async_copy(ref, ref, part_recv).wait()
    total = jnp.sum(partbuf[...], axis=0)
    lane1 = lane_of((1, 128))

    def pick(row, k):
        return jnp.sum(jnp.where(lane1 == k, row, 0.0), axis=1, keepdims=True)

    members = pick(total, 6)
    load = [pick(total, c) / members for c in range(6)]
    trace = load[0] + load[1] + load[2]
    d = [load[c] - trace / 3.0 if c < 3 else load[c] for c in range(6)]
    own_steps = steps_ref[group * 32 + me]
    rates = [jnp.where(k < own_steps, relax_rate, 0.0).astype(f32) for k in range(KMAX)]
    size = norm_of(d)

    @pl.loop(0, 4)
    def _(t):
        lame, shear = moduli(t * 8, 8)
        field[0, at(t * 8, 8), :] = (lame + (2.0 / 3.0) * shear).reshape(64, 128)
        scale, _ = relaxed(shear, size, rates)
        field[1, at(t * 8, 8), :] = (2.0 * shear * scale).reshape(64, 128)

    spectrum = forward()
    spectrum_a, spectrum_b = spectrum[:, :HALF], spectrum[:, HALF:]
    mix = d[0] * spec_ref[1]
    for c in range(1, 6):
        mix = mix + d[c] * spec_ref[1 + c]
    scaled = spec_ref[0]
    steady = (1.0 - green_ratio) * trace
    phi = [scaled * spectrum_b[:32], scaled * spectrum_b[32:]]
    pressure = [
        scaled * (steady * spectrum_a[:32]) - mix * phi[0],
        scaled * (steady * spectrum_a[32:]) - mix * phi[1],
    ]
    waves = [spec_ref[7 + c] for c in range(3)]
    turned = [
        d[0] * waves[0] + d[5] * waves[1] + d[4] * waves[2],
        d[5] * waves[0] + d[1] * waves[1] + d[3] * waves[2],
        d[4] * waves[0] + d[3] * waves[1] + d[2] * waves[2],
    ]
    slopes = [
        [waves[c] * pressure[k] + turned[c] * phi[k] for k in range(2)] for c in range(3)
    ]
    mixed = jnp.concatenate(
        [
            jnp.concatenate([-slopes[c][1] for c in range(3)], axis=1),
            jnp.concatenate([slopes[c][0] for c in range(3)], axis=1),
        ],
        axis=0,
    )
    back = product(x_ref[1], mixed)
    def side_of(start, width, high_ref, low_ref):
        lines = jnp.concatenate(
            [
                jnp.concatenate(
                    [back[h : h + 32, c * HALF + start :][:, :width] for h in (0, 32)], axis=1
                )
                for c in range(3)
            ],
            axis=0,
        )
        high, low = split(lines)
        both = mm(jnp.concatenate([high, low], axis=0), high_ref[...])
        return both[:96] + (both[96:] + mm(high, low_ref[...]))

    first, second = (side_of(q * 128, 128, veh.at[q], vel.at[q]) for q in range(2))
    even = jnp.concatenate([first + second, first - second], axis=1)
    odd = side_of(256, 256, vh, vl)
    space = jnp.concatenate([even + odd, even - odd], axis=1)
    for c in range(3):
        for s in range(8):
            disp_u[c, pl.ds(s, 32, stride=8), :] = space[
                c * 32 : c * 32 + 32, s * 128 : s * 128 + 128
            ]

    source, target = row_of((128, 128)), lane_of((128, 128))
    line = source // VOX == target // VOX
    ahead = line & ((target + 1) % VOX == source % VOX)
    behind = line & ((target + VOX - 1) % VOX == source % VOX)
    z_matrix = (jnp.where(ahead, 0.5, 0.0) - jnp.where(behind, 0.5, 0.0)).astype(bf16)

    def voxel(t, sums):
        x = t * BLOCK
        ux, uy, uz = (planes(disp_u, c, x, BLOCK) for c in range(3))
        dx = [x_slope(disp_u, c, x, BLOCK, u) for c, u in enumerate((ux, uy, uz))]
        high, low = split(jnp.concatenate([ux, uy, uz], axis=0).reshape(24 * BLOCK, 128))
        dz = (mm(high, z_matrix) + mm(low, z_matrix)).reshape(3, BLOCK, 8, 128)
        change = [
            -dx[0],
            -yc(uy),
            -dz[2],
            -0.5 * (yc(uz) + dz[1]),
            -0.5 * (dx[2] + dz[0]),
            -0.5 * (dx[1] + yc(ux)),
        ]
        for k in range(3):
            pair = jnp.concatenate(change[2 * k : 2 * k + 2], axis=1)
            flu[pl.ds(x, BLOCK), pl.ds(k * 16, 16), :] = pair.astype(wire)
        lame, shear = moduli(x, BLOCK)
        e = [load[c] + change[c] for c in range(6)]
        tr = e[0] + e[1] + e[2]
        dv = [e[c] - tr / 3.0 if c < 3 else e[c] for c in range(6)]
        scale, f = relaxed(shear, norm_of(dv), rates)
        twice = 2.0 * shear * scale
        bulk = (lame + (2.0 / 3.0) * shear) * tr
        new = [bulk + twice * dv[c] if c < 3 else twice * dv[c] for c in range(6)]
        new += [lame, shear / (1.0 + f)]
        return tuple(a + jnp.sum(b, axis=0) for a, b in zip(sums, new))

    zero = jnp.zeros((8, 128), f32)
    sums = lax.fori_loop(0, 32 // BLOCK, voxel, (zero,) * 8)
    column = jnp.concatenate([jnp.sum(a, axis=0, keepdims=True) for a in sums], axis=0)
    column = jnp.sum(column, axis=1, keepdims=True) * (1.0 / VOX**3)
    lane8, row8 = lane_of((8, 128)), row_of((8, 128))
    own_row = jnp.sum(
        jnp.where(lane8 == row8 + group * 16, column, 0.0), axis=0, keepdims=True
    )
    for c in range(6):
        own_row = own_row + jnp.where(lane1 == group * 16 + 8 + c, load[c], 0.0)

    rowbuf[3] = own_row
    for i in range(1, 4):
        (
            pltpu.make_async_remote_copy(
                src_ref=rowbuf.at[3],
                dst_ref=rowbuf.at[i - 1],
                send_sem=y_send,
                recv_sem=y_recv,
                device_id={"grp": lax.rem(group + i, 4)},
                device_id_type=MESH,
            )
        ).start()
    arrived = rowbuf.at[pl.ds(0, 3)]
    for copy in near:
        copy.start()
    pltpu.make_async_copy(arrived, arrived, y_recv).wait()
    joined[0] = rowbuf[0] + rowbuf[1] + rowbuf[2] + rowbuf[3]
    everyone(lambda peer: joined.at[0], respbuf, resp_send, resp_recv)
    respbuf[me] = joined[0]
    everyone(lambda peer: flu.at[peer], flubuf, flu_send, flu_recv)
    flubuf[me] = flu[me]

    pltpu.make_async_copy(nb, nb, near_recv.at[0]).wait()
    pltpu.make_async_copy(nb_samp, nb_samp, near_recv.at[1]).wait()
    exists = [(me * count + j >= 3).astype(f32) * (me * count + j < 67).astype(f32) for j in range(8)]

    def around_of(own, k, c):
        below = [nb[pl.ds(k * 15 + c * 2 + p, 1)] for p in (0, 0, 1)]
        above = [nb[pl.ds(k * 15 + 6 + c * 2 + p, 1)] for p in range(2)]
        return [*below, own[c, pl.ds(0, 1)], own[c, pl.ds(1, 1)], *above, nb[pl.ds(k * 15 + 12 + c, 1)]]

    def masked(planes):
        return jnp.concatenate([p * m for p, m in zip(planes, exists)], axis=0)

    around = [masked(around_of(disp_ref, 0, c)) for c in range(3)]
    outside = [masked(around_of(force_ref, 1, c)) for c in range(3)]
    given = [
        (outside[c][1:] - spring_rate * around[c][1:])
        * jnp.concatenate([jnp.full((1, 8, 128), m) for m in exists[1:]], axis=0)
        for c in range(3)
    ]
    samples = [nb_samp[pl.ds(j, 1)] for j in range(3)]
    samples += [samp_ref[pl.ds(p, 1)] for p in range(2)]
    samples += [nb_samp[pl.ds(j, 1)] for j in range(3, 6)]

    all_arrived(respbuf, resp_recv)
    gathered = jnp.concatenate([respbuf[r] for r in range(32)], axis=0)
    gathered = jnp.concatenate([gathered, jnp.zeros((96, 128), f32)], axis=0).T
    cells = []
    for c in range(8):
        row = jnp.concatenate(
            [gathered[g * 16 + c : g * 16 + c + 1, :32] for g in range(4)], axis=1
        )
        source = jnp.broadcast_to(row, (8, 128))
        cells.append(
            masked(
                [
                    jnp.take_along_axis(source, s[0], axis=1, mode="promise_in_bounds")[None]
                    for s in samples
                ]
            )
        )
    lame, shear = cells[6], cells[7]
    pull = force_of(cells[:6])
    inside = jnp.concatenate([jnp.full((1, 8, 128), m) for m in exists[1:]], axis=0)
    res = [given[c] - pull[c] * inside for c in range(3)]

    def stiff(w, low):
        n = w[0].shape[0]
        strain = strain_of(w)
        stress = stress_of(strain, lame[low : low + n - 1], shear[low : low + n - 1])
        pull = force_of(stress)
        mask = jnp.concatenate(
            [jnp.full((1, 8, 128), m) for m in exists[low + 1 : low + n - 1]], axis=0
        )
        return [(pull[c] + spring_rate * w[c][1:-1]) * mask for c in range(3)]

    k1 = stiff(res, 1)
    k2 = stiff(k1, 2)
    r_own = [a[2:4] for a in res]
    k1_own = [a[1:3] for a in k1]
    k2_own = [a[0:2] for a in k2]
    energy_strain = strain_of(k2)
    energy_stress = stress_of(energy_strain, lame[3:5], shear[3:5])

    def dotted(a, b):
        total = a[0] * b[0]
        for c in range(1, 3):
            total = total + a[c] * b[c]
        return jnp.sum(jnp.sum(total, axis=0), axis=0, keepdims=True)

    energy = energy_strain[0] * energy_stress[0]
    for c in range(1, 6):
        energy = energy + (1.0 if c < 3 else 2.0) * energy_strain[c] * energy_stress[c]
    energy = jnp.sum(jnp.sum(energy, axis=0), axis=0, keepdims=True) + spring_rate * dotted(
        k2_own, k2_own
    )
    rows = [
        dotted(r_own, r_own),
        dotted(r_own, k1_own),
        dotted(k1_own, k1_own),
        dotted(k1_own, k2_own),
        dotted(k2_own, k2_own),
        energy,
        jnp.zeros((2, 128), f32),
    ]
    column = jnp.sum(jnp.concatenate(rows, axis=0), axis=1, keepdims=True)
    moment[0] = jnp.sum(jnp.where(lane8 == row8, column, 0.0), axis=0, keepdims=True)
    everyone(lambda peer: moment.at[0], momentbuf, mom_send, mom_recv)
    momentbuf[me] = moment[0]

    def owner(r, acc):
        taken = jnp.where(slot_ref[group * 32 + r] == me, 1.0, 0.0).astype(f32)
        return acc + taken * respbuf[r]

    row = lax.fori_loop(0, 32, owner, jnp.zeros((1, 128), f32))
    shifted = jnp.zeros((1, 128), f32)
    for g in range(4):
        here = (group == g).astype(f32)
        shifted = shifted + here * roll(row, -16 * g, 1)
    row_out[...] = shifted[:, :8]

    table = jnp.concatenate([respbuf[r] for r in range(32)], axis=0)
    lane32 = lane_of((32, 128))
    group_load = [
        jnp.sum(jnp.where(lane32 == group * 16 + 8 + c, table, 0.0), axis=1, keepdims=True)
        for c in range(6)
    ]
    all_arrived(flubuf, flu_recv)
    for r in range(32):
        block = flubuf[r].astype(f32)
        for c in range(6):
            micro_out[pl.ds((c * 32 + r) * 8, 8), :] = (
                group_load[c][r : r + 1] + block[c * 8 : c * 8 + 8]
            )

    all_arrived(momentbuf, mom_recv)
    total = jnp.sum(momentbuf[...], axis=0)
    m = [pick(total, k) for k in range(6)]

    def form(a, b, first):
        out = 0.0
        for i, p in enumerate(a):
            for j, q in enumerate(b):
                out = out + p * q * m[i + j + first]
        return out

    rr = m[0]
    alpha0 = rr / m[1]
    r1 = (jnp.ones_like(rr), -alpha0)
    rr1 = form(r1, r1, 0)
    beta0 = rr1 / rr
    p1 = (1.0 + beta0, -alpha0)
    alpha1 = rr1 / form(p1, p1, 1)
    r2 = (jnp.ones_like(rr), -alpha0 - alpha1 * p1[0], alpha1 * alpha0)
    rr2 = form(r2, r2, 0)
    beta1 = rr2 / rr1
    p2 = (r2[0] + beta1 * p1[0], r2[1] + beta1 * p1[1], r2[2])
    alpha2 = rr2 / form(p2, p2, 1)
    weight = (
        alpha0 + alpha1 * p1[0] + alpha2 * p2[0],
        alpha1 * p1[1] + alpha2 * p2[1],
        alpha2 * p2[2],
    )
    for c in range(3):
        new = disp_ref[c] + (
            weight[0] * r_own[c] + weight[1] * k1_own[c] + weight[2] * k2_own[c]
        )
        for p in range(count):
            for q in range(4):
                disp_out[c, p, pl.ds(q, 8, stride=4), :] = new[p][:, q * 32 : q * 32 + 32]

    pl.when(jnp.logical_not(lowest))(first_plane.wait_send)
    for copy in last_planes:
        pl.when(lower)(copy.wait_send)
    pltpu.make_async_copy(nb, nb, near_send.at[0]).wait()
    pltpu.make_async_copy(nb_samp, nb_samp, near_send.at[1]).wait()
    pltpu.make_async_copy(arrived, arrived, y_send).wait()
    for buffer, sem in (
        (modbuf, mod_send), (partbuf, part_send), (respbuf, resp_send),
        (flubuf, flu_send), (momentbuf, mom_send),
    ):
        ref = buffer.at[pl.ds(0, 31)]
        pltpu.make_async_copy(ref, ref, sem).wait()


def leave(a, b, c, a_out, b_out, c_out, sem):
    step = c.shape[0] // PIECES
    pairs = [(a, a_out), (b, b_out)]
    pairs += [(c.at[pl.ds(k * step, step)], c_out.at[pl.ds(k * step, step)]) for k in range(PIECES)]
    copies = [pltpu.make_async_copy(*pair, sem.at[k]) for k, pair in enumerate(pairs)]
    for copy in copies:
        copy.start()
    for copy in copies:
        copy.wait()


def shards(
    displacement, external_force, element_sample, lame_field, shear_field, plastic_steps, owner_slot
):
    count = displacement.shape[1]
    disp, sample = (3, count, 8, 128), (count, 8, 128)
    wt, vt, vz, x, spec = (jnp.asarray(t) for t in tables())
    operands = (
        displacement,
        wt,
        lame_field.reshape(32, 1024),
        shear_field.reshape(32, 1024),
        external_force,
        element_sample,
        vt,
        vz,
        x,
        spec,
    )
    scalars = (plastic_steps, owner_slot)
    vmem = pl.BlockSpec(memory_space=pltpu.VMEM)
    hbm = pl.BlockSpec(memory_space=pltpu.HBM)
    dma = pltpu.SemaphoreType.DMA
    disp_next, row, micro = pl.pallas_call(
        kernel,
        out_shape=(
            jax.ShapeDtypeStruct(displacement.shape, f32),
            jax.ShapeDtypeStruct((1, 8), f32),
            jax.ShapeDtypeStruct((6 * 32 * 8, 128), f32),
        ),
        in_specs=[hbm] * 12,
        out_specs=(vmem,) * 3,
        scratch_shapes=[
            *(pltpu.VMEM(a.shape, a.dtype) for a in operands),
            *(pltpu.SMEM(a.shape, a.dtype) for a in scalars),
            dma((12,)),
            pltpu.VMEM(disp, f32),
            pltpu.VMEM(disp, f32),
            pltpu.VMEM(sample, jnp.int32),
            pltpu.VMEM((32, 16, 128), bf16),
            pltpu.VMEM((512, 128), f32),
            pltpu.VMEM((3, 8, 128), f32),
            pltpu.VMEM((3, 8, 128), f32),
            pltpu.VMEM((8, 128), jnp.int32),
            pltpu.VMEM((30, 8, 128), f32),
            pltpu.VMEM((6, 8, 128), jnp.int32),
            pltpu.VMEM((32, 16, 128), bf16),
            pltpu.VMEM((32, 1, 128), f32),
            pltpu.VMEM((32, 1, 128), f32),
            pltpu.VMEM((count, 64, 128), f32),
            pltpu.VMEM((32, count * 1024), bf16),
            pltpu.VMEM((32, 128), f32),
            *(pltpu.VMEM((HALF, HALF), bf16),) * 4,
            *(pltpu.VMEM((2, 256, 256), bf16),) * 4,
            pltpu.VMEM((2, 256, 128), f32),
            pltpu.VMEM((3, 256, 128), f32),
            pltpu.VMEM((32, 48, 128), wire),
            pltpu.VMEM((32, 48, 128), wire),
            pltpu.VMEM((4, 1, 128), f32),
            pltpu.VMEM((1, 1, 128), f32),
            pltpu.VMEM((32, 1, 128), f32),
            pltpu.VMEM((1, 1, 128), f32),
            pltpu.VMEM((32, 1, 128), f32),
            pltpu.SemaphoreType.REGULAR, dma((3,)), dma((3,)), dma((2,)), dma((2,)), dma, dma, dma, dma,
            dma, dma, dma, dma, dma, dma, dma, dma,
        ],
        compiler_params=pltpu.CompilerParams(collective_id=0, has_side_effects=True, vmem_limit_bytes=24 << 20),
    )(*[pltpu.with_memory_space_constraint(a, pltpu.HBM) for a in operands + scalars])
    results = (disp_next, row, micro)
    disp_next, row, micro = pl.pallas_call(
        leave,
        out_shape=tuple(jax.ShapeDtypeStruct(a.shape, a.dtype) for a in results),
        in_specs=[pl.BlockSpec(memory_space=pl.ANY)] * 3,
        out_specs=(pl.BlockSpec(memory_space=pltpu.HBM),) * 3,
        scratch_shapes=[dma((PIECES + 2,))],
        compiler_params=pltpu.CompilerParams(vmem_limit_bytes=1 << 20),
    )(*results)
    return disp_next, row, micro.reshape(6, 32, 1, 1024)


def solution(mesh):
    in_specs = (
        P(None, "dev", None, None),
        P(None, "dev", None, None),
        P("dev", None, None),
        P("grp", "dev", None),
        P("grp", "dev", None),
        P(),
        P(),
    )
    out_specs = (P(None, "dev", None, None), P(("grp", "dev"), None), P(None, "grp", "dev", None))
    return jax.shard_map(shards, mesh=mesh, in_specs=in_specs, out_specs=out_specs, check_vma=False)
```

```python
import jax
import jax.numpy as jnp
import numpy as np
from jax import lax
from jax.experimental import pallas as pl
from jax.experimental.pallas import tpu as pltpu
from jax.sharding import PartitionSpec as P

VOX = 32
HALF = 512
BLOCK = 32
PIECES = 1
KMAX = 4
MESH = pl.DeviceIdType.MESH
NEAR = (-2, -1, 1, 2)

shear_ref = 1.65
lame_ref = 1.25
green_ratio = (lame_ref + shear_ref) / (lame_ref + 2.0 * shear_ref)
relax_rate = 0.35
spring_rate = 0.2
wire = jnp.bfloat16
f32 = jnp.float32
bf16 = jnp.bfloat16


def tables():
    n = np.arange(VOX)
    theta = 2.0 * np.pi / VOX
    order = np.concatenate([n[::4], n[2::4], n[1::2]])
    ky = np.repeat(order, 16)
    kz = np.tile(np.arange(16), VOX)
    yy = np.repeat(n[:16], VOX)
    zz = np.tile(n, 16)
    k16 = np.arange(16)

    def zeta(z, k):
        angle = theta * (z * k % VOX)
        return (
            np.where(k == 0, 1.0, np.cos(angle)),
            np.where(k == 0, (-1.0) ** z, -np.sin(angle)),
        )

    cy, sy = np.cos(theta * (np.outer(n, ky) % VOX)), np.sin(theta * (np.outer(n, ky) % VOX))
    zr, zi = zeta(n[:, None], kz[None, :])
    cv, sv = np.cos(theta * (np.outer(order, yy) % VOX)), np.sin(theta * (np.outer(order, yy) % VOX))
    vr, vi = zeta(zz[None, :], k16[:, None])
    c, s = np.cos(theta * (np.outer(n, n) % VOX)), np.sin(theta * (np.outer(n, n) % VOX))
    x = np.block([[c, s], [-s, c]])

    def wave(k):
        return np.where(k % 16 == 0, 0.0, np.sin(theta * k))

    one = np.ones((VOX, HALF))
    xx, xy, xz = wave(n)[:, None] * one, wave(ky)[None] * one, wave(kz)[None] * one
    square = xx * xx + xy * xy + xz * xz
    inverse = np.where(square > 0, 1.0 / np.where(square > 0, square, 1.0), 0.0)
    weight = np.where(kz == 0, 1.0, 2.0)[None] * one
    scaled = -(1.0 / shear_ref) * inverse * weight / VOX**3
    pairs = (xx * xx, xy * xy, xz * xz, 2 * xy * xz, 2 * xx * xz, 2 * xx * xy)
    spectral = np.stack([scaled] + [green_ratio * p * inverse for p in pairs] + [xx, xy, xz])
    to = lambda a: np.asarray(a, np.float32)
    return (
        to(np.stack([cy, sy, zr, zi])),
        to(np.stack([cv, sv])),
        to(np.stack([vr, vi])),
        to(np.stack([x, x.T])),
        to(spectral),
    )


def split(a):
    high = a.astype(bf16)
    return high, (a - high.astype(f32)).astype(bf16)


def mm(a, b):
    return jnp.dot(a, b, preferred_element_type=f32)


def product(a, b):
    ah, al = split(a)
    bh, bl = split(b)
    return mm(jnp.concatenate([ah, al, ah], axis=1), jnp.concatenate([bh, bh, bl], axis=0))


def lane_of(shape):
    return lax.broadcasted_iota(jnp.int32, shape, len(shape) - 1)


def row_of(shape):
    return lax.broadcasted_iota(jnp.int32, shape, len(shape) - 2)


def roll(a, shift, axis):
    return pltpu.roll(a, shift % a.shape[axis], axis)


def shifts(v, sign):
    lane, row = lane_of(v.shape), row_of(v.shape)
    edge = lane % VOX == (VOX - 1 if sign > 0 else 0)
    inner = lane < 96 if sign > 0 else lane >= VOX
    last = row == (7 if sign > 0 else 0)

    def along_y(moved):
        return jnp.where(inner, moved, jnp.where(last, 0.0, roll(moved, -sign, 1)))

    z = jnp.where(edge, 0.0, roll(v, -sign, 2))
    y = along_y(roll(v, -sign * VOX, 2))
    both = jnp.where(edge, 0.0, along_y(roll(v, -sign * (VOX + 1), 2)))
    return z, y, both


def yc(v):
    lane = lane_of(v.shape)
    up = roll(v, -VOX, 2)
    up = jnp.where(lane < 96, up, roll(up, -1, 1))
    down = roll(v, VOX, 2)
    down = jnp.where(lane >= VOX, down, roll(down, 1, 1))
    return 0.5 * (up - down)


def spans(distance):
    return min(distance, 4 - distance)


OTHERS = sorted(
    ((a, b, c) for a in range(4) for b in range(4) for c in range(2) if (a, b, c) != (0, 0, 0)),
    key=lambda p: (-spans(p[0]) - spans(p[1]), -p[2], p),
)


def strain_of(fields):
    slopes = []
    for w in fields:
        z, y, yz = shifts(w, 1)
        near, far = w + z, y + yz
        a, b = 0.25 * (near + far), 0.5 * (far - near)
        c = 0.5 * ((z + yz) - (w + y))
        slopes.append((a[1:] - a[:-1], 0.5 * (b[1:] + b[:-1]), 0.5 * (c[1:] + c[:-1])))
    x, y, z = slopes
    return (
        x[0],
        y[1],
        z[2],
        0.5 * (z[1] + y[2]),
        0.5 * (z[0] + x[2]),
        0.5 * (y[0] + x[1]),
    )


def force_of(stress):
    xx, yy, zz, yz, xz, xy = stress
    result = []
    for along_x, along_y, along_z in ((xx, xy, xz), (xy, yy, yz), (xz, yz, zz)):
        z, y, yz = shifts(along_x, -1)
        first = 0.25 * ((along_x + z) + (y + yz))
        both = along_y + along_z
        less = along_z - along_y
        z, y, _ = shifts(less, -1)
        _, _, yz = shifts(both, -1)
        rest = 0.5 * ((yz - y) + (z - both))
        result.append((first[:-1] - first[1:]) + 0.5 * (rest[1:] + rest[:-1]))
    return result


def stress_of(strain, lame, shear):
    spread = lame * (strain[0] + strain[1] + strain[2])
    twice = 2.0 * shear
    return [twice * e + spread for e in strain[:3]] + [twice * e for e in strain[3:]]


def norm_of(d):
    return d[0] * d[0] + d[1] * d[1] + d[2] * d[2] + 2.0 * (d[3] * d[3] + d[4] * d[4] + d[5] * d[5])


def relaxed(mu, size, rates):
    base = mu * mu * size
    scale = jnp.ones_like(mu)
    for rate in rates:
        f = base * scale * scale
        scale = scale * ((1.0 - rate) + rate / (1.0 + f))
    return scale, base * scale * scale


def kernel(
    disp_in, wt_in, lame_in, shear_in, force_in, samp_in, vt_in, vz_in, x_in, spec_in, steps_in, slot_in,
    disp_out, row_out, micro_out,
    disp_raw, wt_ref, lame_raw, shear_raw, force_raw, samp_raw, vt_ref, vz_ref, x_ref, spec_ref,
    steps_ref, slot_ref, in_sem,
    disp_ref, force_ref, samp_ref, mod_ref, modwide,
    nb_first, nb_last, nb_mark, nb, nb_samp, modbuf, part, partbuf, strainrow, one_hot_ref, sums_ref,
    wh, wl, vh, vl, weh, wel, veh, vel, field, disp_u, flu, flubuf,
    rowbuf, joined, respbuf, moment, momentbuf,
    ready, first_send, first_recv, near_send, near_recv, mod_send, mod_recv, part_send, part_recv,
    y_send, y_recv, resp_send, resp_recv, flu_send, flu_recv, mom_send, mom_recv,
):
    me = lax.axis_index("dev")
    group = lax.axis_index("grp")
    count = disp_raw.shape[1]

    me_x, me_z, me_c = me // 8, lax.rem(me // 2, 4), lax.rem(me, 2)
    at_x = [lax.rem(me_x + k, 4) * 8 for k in range(4)]
    at_z = [lax.rem(me_z + k, 4) * 2 for k in range(4)]
    at_c = [me_c, 1 - me_c]
    peers = [at_x[a] + at_z[b] + at_c[c] for a, b, c in OTHERS]

    loads = [
        pltpu.make_async_copy(source, target, in_sem.at[k])
        for k, (source, target) in enumerate(
            (
                (disp_in, disp_raw), (wt_in, wt_ref), (lame_in, lame_raw), (shear_in, shear_raw),
                (force_in, force_raw), (samp_in, samp_raw), (vt_in, vt_ref), (vz_in, vz_ref),
                (x_in, x_ref), (spec_in, spec_ref), (steps_in, steps_ref), (slot_in, slot_ref),
            )
        )
    ]
    loads[0].start()
    loads[5].start()

    barrier = pltpu.get_barrier_semaphore()
    layer = [peer for peer, (a, _, _) in zip(peers, OTHERS) if a == 0]
    entry = [peer for peer, (_, b, c) in zip(peers, OTHERS) if (b, c) == (0, 0)] + layer
    entry += [lax.rem(me + 1, 32), lax.rem(me + 31, 32)]
    for peer in entry:
        pl.semaphore_signal(barrier, inc=1, device_id={"dev": peer}, device_id_type=MESH)
    for i in range(1, 4):
        pl.semaphore_signal(
            barrier, inc=1, device_id={"grp": lax.rem(group + i, 4)}, device_id_type=MESH
        )
    for k in (1, 2, 3, 4, *range(6, 12)):
        loads[k].start()

    def dense(raw, out):
        for index in np.ndindex(raw.shape[:-2]):
            out[index] = jnp.concatenate(
                [raw[(*index, pl.ds(q, 8, stride=4), slice(None))] for q in range(4)], axis=1
            )

    loads[0].wait()
    dense(disp_raw, disp_ref)
    loads[5].wait()
    dense(samp_raw, samp_ref)
    pl.semaphore_wait(barrier, len(entry) + 3)

    lowest, highest = lax.rem(me, 8) == 0, lax.rem(me, 8) == 7
    upper, lower = lowest & (me > 0), highest & (me < 31)
    above, below = lax.rem(me + 1, 32), lax.rem(me + 31, 32)

    def bordering(k, source, target, device):
        return pltpu.make_async_remote_copy(
            src_ref=source,
            dst_ref=target,
            send_sem=first_send.at[k],
            recv_sem=first_recv.at[k],
            device_id={"dev": device},
            device_id_type=MESH,
        )

    first_plane = bordering(0, disp_ref.at[:, 0], nb_first, below)
    last_planes = (
        bordering(1, disp_ref.at[:, count - 1], nb_last, above),
        bordering(2, samp_ref.at[count - 1], nb_mark, above),
    )
    pl.when(jnp.logical_not(lowest))(first_plane.start)
    for copy in last_planes:
        pl.when(lower)(copy.start)
    for peer in layer:
        pl.semaphore_signal(ready, inc=1, device_id={"dev": peer}, device_id_type=MESH)
    for k in range(2, 5):
        loads[k].wait()
    dense(force_raw, force_ref)
    for k, raw in enumerate((lame_raw, shear_raw)):
        wide = raw[...].astype(f32)
        for t in range(8):
            modwide[pl.ds(k * 8 + t, 32, stride=16), :] = wide[:, t * 128 : t * 128 + 128]
    for r in range(32):
        mod_ref[r] = modwide[pl.ds(r * 16, 16), :].astype(bf16)

    part[...] = jnp.zeros_like(part)
    for plane in range(count):
        strainrow[plane, pl.ds(48, 8), :] = jnp.ones((8, 128), f32)
        strainrow[plane, pl.ds(56, 8), :] = jnp.zeros((8, 128), f32)

    places = {-1: (0, 6, 1), 1: (6, 6, 1 + count), 2: (12, 3, 1 + 2 * count), -2: (None, 0, 0)}
    near = []
    for offset, (start, _, sample_start) in places.items():
        device = lax.rem(me - offset + 32, 32)
        plane = {2: 0, -2: count - 1}.get(offset)

        def send(source, target, k, device=device):
            near.append(
                pltpu.make_async_remote_copy(
                    src_ref=source,
                    dst_ref=target,
                    send_sem=near_send.at[k],
                    recv_sem=near_recv.at[k],
                    device_id={"dev": device},
                    device_id_type=MESH,
                )
            )

        width = count if plane is None else 1
        cut_out = pl.ds(0 if plane is None else plane, width)
        if start is not None:
            for k, source in enumerate((disp_ref, force_ref)):
                for c in range(3):
                    send(source.at[c, cut_out], nb.at[pl.ds(k * 15 + start + c * width, width)], 0)
        send(samp_ref.at[cut_out], nb_samp.at[pl.ds(sample_start, width)], 1)

    def everyone(source, target, send, recv):
        for peer in peers:
            pltpu.make_async_remote_copy(
                src_ref=source(peer),
                dst_ref=target.at[me],
                send_sem=send,
                recv_sem=recv,
                device_id={"dev": peer},
                device_id_type=MESH,
            ).start()

    def all_arrived(target, recv):
        ref = target.at[pl.ds(0, 31)]
        pltpu.make_async_copy(ref, ref, recv).wait()

    loads[1].wait()

    @pl.loop(0, 16)
    def _(y):
        c, s = wt_ref[0, pl.ds(y, 1), :], wt_ref[1, pl.ds(y, 1), :]
        zr, zi = wt_ref[2], wt_ref[3]
        rows = pl.ds(pl.multiple_of(y * 32, 32), 32)
        blocks = [split(b) for b in (c * zr + s * zi, c * zi - s * zr)]
        for k, (high, low) in enumerate(blocks):
            wh[rows, pl.ds(k * 256, 256)] = high[:, 256:]
            wl[rows, pl.ds(k * 256, 256)] = low[:, 256:]

        @pl.when(y < 8)
        def _():
            for k, (high, low) in enumerate(blocks):
                for q in range(2):
                    lanes = slice(q * 128, q * 128 + 128)
                    weh[q, rows, pl.ds(k * 128, 128)] = high[:, lanes]
                    wel[q, rows, pl.ds(k * 128, 128)] = low[:, lanes]

    def hot_of(sample, s, counted):
        hit = jnp.broadcast_to(sample[s : s + 1], (32, 128)) == row_of((32, 128)) + group * 32
        return jnp.where(hit, counted, 0.0).astype(bf16)

    own_last = jnp.where(lower, 0.0, 1.0).astype(f32)
    one_hot_ref[...] = jnp.concatenate(
        [hot_of(samp_ref[p], s, (1.0, own_last)[p // (count - 1)]) for p in range(count) for s in range(8)],
        axis=1,
    )
    pl.semaphore_wait(ready, len(layer))
    everyone(lambda peer: mod_ref.at[peer], modbuf, mod_send, mod_recv)
    modbuf[me] = mod_ref[me]

    def sums_of(strain, one_hot):
        n = strain[0].shape[0]
        rows_high, rows_low = [], []
        for p in range(n):
            for c in range(6):
                strainrow[p, pl.ds(c * 8, 8), :] = strain[c][p]
        for p in range(n):
            for s in range(8):
                high, low = split(strainrow[p, pl.ds(s, 8, stride=8), :])
                rows_high.append(high)
                rows_low.append(low)

        def against(rows):
            return lax.dot_general(
                one_hot,
                jnp.concatenate(rows, axis=1),
                (((1,), (1,)), ((), ())),
                preferred_element_type=f32,
            )

        return against(rows_high) + against(rows_low)

    pl.when(jnp.logical_not(highest))(first_plane.wait_recv)
    fields = [
        jnp.concatenate([disp_ref[c], jnp.where(highest, 0.0, nb_first[pl.ds(c, 1)])], axis=0)
        for c in range(3)
    ]
    sums_ref[:, pl.ds(0, 8)] = sums_of(strain_of(fields), one_hot_ref[...])

    @pl.when(upper)
    def _():
        for copy in last_planes:
            copy.wait_recv()
        between = [
            jnp.concatenate([nb_last[pl.ds(c, 1)], disp_ref[c, pl.ds(0, 1)]], axis=0) for c in range(3)
        ]
        hots = jnp.concatenate([hot_of(nb_mark, s, 1.0) for s in range(8)], axis=1)
        sums_ref[:, pl.ds(0, 8)] += sums_of(strain_of(between), hots)

    sums = sums_ref[:, pl.ds(0, 8)]
    for r in range(32):
        part[r, :, pl.ds(0, 8)] = sums[r : r + 1]
    everyone(lambda peer: part.at[peer], partbuf, part_send, part_recv)
    partbuf[me] = part[me]
    for k in range(6, 12):
        loads[k].wait()

    def back_rows(k, lanes):
        row = pl.ds(k, 1)
        c, s = vt_ref[0, row, pl.ds(0, lanes)], vt_ref[1, row, pl.ds(0, lanes)]
        zr, zi = vz_ref[0, :, pl.ds(0, lanes)], vz_ref[1, :, pl.ds(0, lanes)]
        return split(c * zr + s * zi), split(c * zi - s * zr)

    @pl.loop(0, 16)
    def _(k):
        for p, (high, low) in enumerate(back_rows(16 + k, HALF)):
            rows = pl.ds(pl.multiple_of(p * 256 + k * 16, 16), 16)
            vh[rows, :] = high
            vl[rows, :] = low

    for q in range(2):

        @pl.loop(0, 8)
        def _(k):
            for p, (high, low) in enumerate(back_rows(q * 8 + k, 256)):
                rows = pl.ds(pl.multiple_of(p * 128 + k * 16, 16), 16)
                veh[q, rows, :] = high
                vel[q, rows, :] = low

    ref = modbuf.at[pl.ds(0, 31)]
    pltpu.make_async_copy(ref, ref, mod_recv).wait()

    def moduli(x, n):
        both = modbuf[pl.ds(x, n)].astype(f32)
        return both[:, :8], both[:, 8:]

    def at(x, n):
        return pl.ds(pl.multiple_of(x * 8, 8), n * 8)

    def planes(ref, k, x, n):
        return ref[k, at(x, n), :].reshape(n, 8, 128)

    def x_slope(ref, k, x, n, v):
        after = planes(ref, k, lax.rem(x + n, 32), 1)
        before = planes(ref, k, lax.rem(x + 31, 32), 1)
        up = jnp.concatenate([v[1:], after], axis=0)
        down = jnp.concatenate([before, v[:-1]], axis=0)
        return 0.5 * (up - down)

    def forward():
        rows = jnp.concatenate(
            [
                jnp.concatenate([field[k, pl.ds(s, 32, stride=8), :] for k in range(2)], axis=0)
                for s in range(8)
            ],
            axis=1,
        )
        even, odd = rows[:, :HALF] + rows[:, HALF:], rows[:, :HALF] - rows[:, HALF:]

        def part_of(data, high_ref, low_ref):
            high, low = split(data)
            both = mm(jnp.concatenate([high, low], axis=0), high_ref[...])
            return both[:64] + (both[64:] + mm(high, low_ref[...]))

        sides = [
            part_of(even[:, :256] + even[:, 256:], weh.at[0], wel.at[0]),
            part_of(even[:, :256] - even[:, 256:], weh.at[1], wel.at[1]),
            part_of(odd, wh, wl),
        ]
        plane = jnp.concatenate(
            [side[:, : side.shape[1] // 2] for side in sides]
            + [side[:, side.shape[1] // 2 :] for side in sides],
            axis=1,
        )
        stacked = jnp.concatenate(
            [
                jnp.concatenate([plane[:32, :HALF], plane[32:, :HALF]], axis=1),
                jnp.concatenate([plane[:32, HALF:], plane[32:, HALF:]], axis=1),
            ],
            axis=0,
        )
        return product(x_ref[0], stacked)

    lame, shear = moduli(0, 32)
    field[0] = (lame + (2.0 / 3.0) * shear).reshape(256, 128)

    ref = partbuf.at[pl.ds(0, 31)]
    pltpu.make_async_copy(ref, ref, part_recv).wait()
    total = jnp.sum(partbuf[...], axis=0)
    lane1 = lane_of((1, 128))

    def pick(row, k):
        return jnp.sum(jnp.where(lane1 == k, row, 0.0), axis=1, keepdims=True)

    members = pick(total, 6)
    load = [pick(total, c) / members for c in range(6)]
    trace = load[0] + load[1] + load[2]
    d = [load[c] - trace / 3.0 if c < 3 else load[c] for c in range(6)]
    own_steps = steps_ref[group * 32 + me]
    rates = [jnp.where(k < own_steps, relax_rate, 0.0).astype(f32) for k in range(KMAX)]
    size = norm_of(d)

    _, shear = moduli(0, 32)
    scale, _ = relaxed(shear, size, rates)
    field[1] = (2.0 * shear * scale).reshape(256, 128)
    spectrum = forward()
    spectrum_a, spectrum_b = spectrum[:, :HALF], spectrum[:, HALF:]
    mix = d[0] * spec_ref[1]
    for c in range(1, 6):
        mix = mix + d[c] * spec_ref[1 + c]
    scaled = spec_ref[0]
    steady = (1.0 - green_ratio) * trace
    phi = [scaled * spectrum_b[:32], scaled * spectrum_b[32:]]
    pressure = [
        scaled * (steady * spectrum_a[:32]) - mix * phi[0],
        scaled * (steady * spectrum_a[32:]) - mix * phi[1],
    ]
    waves = [spec_ref[7 + c] for c in range(3)]
    turned = [
        d[0] * waves[0] + d[5] * waves[1] + d[4] * waves[2],
        d[5] * waves[0] + d[1] * waves[1] + d[3] * waves[2],
        d[4] * waves[0] + d[3] * waves[1] + d[2] * waves[2],
    ]
    slopes = [
        [waves[c] * pressure[k] + turned[c] * phi[k] for k in range(2)] for c in range(3)
    ]
    mixed = jnp.concatenate(
        [
            jnp.concatenate([-slopes[c][1] for c in range(3)], axis=1),
            jnp.concatenate([slopes[c][0] for c in range(3)], axis=1),
        ],
        axis=0,
    )
    back = product(x_ref[1], mixed)
    def side_of(start, width, high_ref, low_ref):
        lines = jnp.concatenate(
            [
                jnp.concatenate(
                    [back[h : h + 32, c * HALF + start :][:, :width] for h in (0, 32)], axis=1
                )
                for c in range(3)
            ],
            axis=0,
        )
        high, low = split(lines)
        both = mm(jnp.concatenate([high, low], axis=0), high_ref[...])
        return both[:96] + (both[96:] + mm(high, low_ref[...]))

    first, second = (side_of(q * 128, 128, veh.at[q], vel.at[q]) for q in range(2))
    even = jnp.concatenate([first + second, first - second], axis=1)
    odd = side_of(256, 256, vh, vl)
    space = jnp.concatenate([even + odd, even - odd], axis=1)
    for c in range(3):
        for s in range(8):
            disp_u[c, pl.ds(s, 32, stride=8), :] = space[
                c * 32 : c * 32 + 32, s * 128 : s * 128 + 128
            ]

    source, target = row_of((128, 128)), lane_of((128, 128))
    line = source // VOX == target // VOX
    ahead = line & ((target + 1) % VOX == source % VOX)
    behind = line & ((target + VOX - 1) % VOX == source % VOX)
    z_matrix = (jnp.where(ahead, 0.5, 0.0) - jnp.where(behind, 0.5, 0.0)).astype(bf16)

    def voxel(t, sums):
        x = t * BLOCK
        ux, uy, uz = (planes(disp_u, c, x, BLOCK) for c in range(3))
        dx = [x_slope(disp_u, c, x, BLOCK, u) for c, u in enumerate((ux, uy, uz))]
        high, low = split(jnp.concatenate([ux, uy, uz], axis=0).reshape(24 * BLOCK, 128))
        dz = (mm(high, z_matrix) + mm(low, z_matrix)).reshape(3, BLOCK, 8, 128)
        change = [
            -dx[0],
            -yc(uy),
            -dz[2],
            -0.5 * (yc(uz) + dz[1]),
            -0.5 * (dx[2] + dz[0]),
            -0.5 * (dx[1] + yc(ux)),
        ]
        for k in range(3):
            pair = jnp.concatenate(change[2 * k : 2 * k + 2], axis=1)
            flu[pl.ds(x, BLOCK), pl.ds(k * 16, 16), :] = pair.astype(wire)
        lame, shear = moduli(x, BLOCK)
        e = [load[c] + change[c] for c in range(6)]
        tr = e[0] + e[1] + e[2]
        dv = [e[c] - tr / 3.0 if c < 3 else e[c] for c in range(6)]
        scale, f = relaxed(shear, norm_of(dv), rates)
        twice = 2.0 * shear * scale
        bulk = (lame + (2.0 / 3.0) * shear) * tr
        new = [bulk + twice * dv[c] if c < 3 else twice * dv[c] for c in range(6)]
        new += [lame, shear / (1.0 + f)]
        return tuple(a + jnp.sum(b, axis=0) for a, b in zip(sums, new))

    zero = jnp.zeros((8, 128), f32)
    sums = lax.fori_loop(0, 32 // BLOCK, voxel, (zero,) * 8)
    column = jnp.concatenate([jnp.sum(a, axis=0, keepdims=True) for a in sums], axis=0)
    column = jnp.sum(column, axis=1, keepdims=True) * (1.0 / VOX**3)
    lane8, row8 = lane_of((8, 128)), row_of((8, 128))
    own_row = jnp.sum(
        jnp.where(lane8 == row8 + group * 16, column, 0.0), axis=0, keepdims=True
    )
    for c in range(6):
        own_row = own_row + jnp.where(lane1 == group * 16 + 8 + c, load[c], 0.0)

    rowbuf[3] = own_row
    for i in range(1, 4):
        (
            pltpu.make_async_remote_copy(
                src_ref=rowbuf.at[3],
                dst_ref=rowbuf.at[i - 1],
                send_sem=y_send,
                recv_sem=y_recv,
                device_id={"grp": lax.rem(group + i, 4)},
                device_id_type=MESH,
            )
        ).start()
    arrived = rowbuf.at[pl.ds(0, 3)]
    for copy in near:
        copy.start()
    pltpu.make_async_copy(arrived, arrived, y_recv).wait()
    joined[0] = rowbuf[0] + rowbuf[1] + rowbuf[2] + rowbuf[3]
    everyone(lambda peer: joined.at[0], respbuf, resp_send, resp_recv)
    respbuf[me] = joined[0]
    everyone(lambda peer: flu.at[peer], flubuf, flu_send, flu_recv)
    flubuf[me] = flu[me]

    pltpu.make_async_copy(nb, nb, near_recv.at[0]).wait()
    pltpu.make_async_copy(nb_samp, nb_samp, near_recv.at[1]).wait()
    exists = [(me * count + j >= 3).astype(f32) * (me * count + j < 67).astype(f32) for j in range(8)]

    def around_of(own, k, c):
        below = [nb[pl.ds(k * 15 + c * 2 + p, 1)] for p in (0, 0, 1)]
        above = [nb[pl.ds(k * 15 + 6 + c * 2 + p, 1)] for p in range(2)]
        return [*below, own[c, pl.ds(0, 1)], own[c, pl.ds(1, 1)], *above, nb[pl.ds(k * 15 + 12 + c, 1)]]

    def masked(planes):
        return jnp.concatenate([p * m for p, m in zip(planes, exists)], axis=0)

    around = [masked(around_of(disp_ref, 0, c)) for c in range(3)]
    outside = [masked(around_of(force_ref, 1, c)) for c in range(3)]
    given = [
        (outside[c][1:] - spring_rate * around[c][1:])
        * jnp.concatenate([jnp.full((1, 8, 128), m) for m in exists[1:]], axis=0)
        for c in range(3)
    ]
    samples = [nb_samp[pl.ds(j, 1)] for j in range(3)]
    samples += [samp_ref[pl.ds(p, 1)] for p in range(2)]
    samples += [nb_samp[pl.ds(j, 1)] for j in range(3, 6)]

    all_arrived(respbuf, resp_recv)
    gathered = jnp.concatenate([respbuf[r] for r in range(32)], axis=0)
    gathered = jnp.concatenate([gathered, jnp.zeros((96, 128), f32)], axis=0).T
    cells = []
    for c in range(8):
        row = jnp.concatenate(
            [gathered[g * 16 + c : g * 16 + c + 1, :32] for g in range(4)], axis=1
        )
        source = jnp.broadcast_to(row, (8, 128))
        cells.append(
            masked(
                [
                    jnp.take_along_axis(source, s[0], axis=1, mode="promise_in_bounds")[None]
                    for s in samples
                ]
            )
        )
    lame, shear = cells[6], cells[7]
    pull = force_of(cells[:6])
    inside = jnp.concatenate([jnp.full((1, 8, 128), m) for m in exists[1:]], axis=0)
    res = [given[c] - pull[c] * inside for c in range(3)]

    def stiff(w, low):
        n = w[0].shape[0]
        strain = strain_of(w)
        stress = stress_of(strain, lame[low : low + n - 1], shear[low : low + n - 1])
        pull = force_of(stress)
        mask = jnp.concatenate(
            [jnp.full((1, 8, 128), m) for m in exists[low + 1 : low + n - 1]], axis=0
        )
        return [(pull[c] + spring_rate * w[c][1:-1]) * mask for c in range(3)]

    k1 = stiff(res, 1)
    k2 = stiff(k1, 2)
    r_own = [a[2:4] for a in res]
    k1_own = [a[1:3] for a in k1]
    k2_own = [a[0:2] for a in k2]
    energy_strain = strain_of(k2)
    energy_stress = stress_of(energy_strain, lame[3:5], shear[3:5])

    def dotted(a, b):
        total = a[0] * b[0]
        for c in range(1, 3):
            total = total + a[c] * b[c]
        return jnp.sum(jnp.sum(total, axis=0), axis=0, keepdims=True)

    energy = energy_strain[0] * energy_stress[0]
    for c in range(1, 6):
        energy = energy + (1.0 if c < 3 else 2.0) * energy_strain[c] * energy_stress[c]
    energy = jnp.sum(jnp.sum(energy, axis=0), axis=0, keepdims=True) + spring_rate * dotted(
        k2_own, k2_own
    )
    rows = [
        dotted(r_own, r_own),
        dotted(r_own, k1_own),
        dotted(k1_own, k1_own),
        dotted(k1_own, k2_own),
        dotted(k2_own, k2_own),
        energy,
        jnp.zeros((2, 128), f32),
    ]
    column = jnp.sum(jnp.concatenate(rows, axis=0), axis=1, keepdims=True)
    moment[0] = jnp.sum(jnp.where(lane8 == row8, column, 0.0), axis=0, keepdims=True)
    everyone(lambda peer: moment.at[0], momentbuf, mom_send, mom_recv)
    momentbuf[me] = moment[0]

    def owner(r, acc):
        taken = jnp.where(slot_ref[group * 32 + r] == me, 1.0, 0.0).astype(f32)
        return acc + taken * respbuf[r]

    row = lax.fori_loop(0, 32, owner, jnp.zeros((1, 128), f32))
    shifted = jnp.zeros((1, 128), f32)
    for g in range(4):
        here = (group == g).astype(f32)
        shifted = shifted + here * roll(row, -16 * g, 1)
    row_out[...] = shifted[:, :8]

    table = jnp.concatenate([respbuf[r] for r in range(32)], axis=0)
    lane32 = lane_of((32, 128))
    group_load = [
        jnp.sum(jnp.where(lane32 == group * 16 + 8 + c, table, 0.0), axis=1, keepdims=True)
        for c in range(6)
    ]
    all_arrived(flubuf, flu_recv)
    for r in range(32):
        block = flubuf[r].astype(f32)
        for c in range(6):
            micro_out[pl.ds((c * 32 + r) * 8, 8), :] = (
                group_load[c][r : r + 1] + block[c * 8 : c * 8 + 8]
            )

    all_arrived(momentbuf, mom_recv)
    total = jnp.sum(momentbuf[...], axis=0)
    m = [pick(total, k) for k in range(6)]

    def form(a, b, first):
        out = 0.0
        for i, p in enumerate(a):
            for j, q in enumerate(b):
                out = out + p * q * m[i + j + first]
        return out

    rr = m[0]
    alpha0 = rr / m[1]
    r1 = (jnp.ones_like(rr), -alpha0)
    rr1 = form(r1, r1, 0)
    beta0 = rr1 / rr
    p1 = (1.0 + beta0, -alpha0)
    alpha1 = rr1 / form(p1, p1, 1)
    r2 = (jnp.ones_like(rr), -alpha0 - alpha1 * p1[0], alpha1 * alpha0)
    rr2 = form(r2, r2, 0)
    beta1 = rr2 / rr1
    p2 = (r2[0] + beta1 * p1[0], r2[1] + beta1 * p1[1], r2[2])
    alpha2 = rr2 / form(p2, p2, 1)
    weight = (
        alpha0 + alpha1 * p1[0] + alpha2 * p2[0],
        alpha1 * p1[1] + alpha2 * p2[1],
        alpha2 * p2[2],
    )
    for c in range(3):
        new = disp_ref[c] + (
            weight[0] * r_own[c] + weight[1] * k1_own[c] + weight[2] * k2_own[c]
        )
        for p in range(count):
            for q in range(4):
                disp_out[c, p, pl.ds(q, 8, stride=4), :] = new[p][:, q * 32 : q * 32 + 32]

    pl.when(jnp.logical_not(lowest))(first_plane.wait_send)
    for copy in last_planes:
        pl.when(lower)(copy.wait_send)
    pltpu.make_async_copy(nb, nb, near_send.at[0]).wait()
    pltpu.make_async_copy(nb_samp, nb_samp, near_send.at[1]).wait()
    pltpu.make_async_copy(arrived, arrived, y_send).wait()
    for buffer, sem in (
        (modbuf, mod_send), (partbuf, part_send), (respbuf, resp_send),
        (flubuf, flu_send), (momentbuf, mom_send),
    ):
        ref = buffer.at[pl.ds(0, 31)]
        pltpu.make_async_copy(ref, ref, sem).wait()


def leave(a, b, c, a_out, b_out, c_out, sem):
    step = c.shape[0] // PIECES
    pairs = [(a, a_out), (b, b_out)]
    pairs += [(c.at[pl.ds(k * step, step)], c_out.at[pl.ds(k * step, step)]) for k in range(PIECES)]
    copies = [pltpu.make_async_copy(*pair, sem.at[k]) for k, pair in enumerate(pairs)]
    for copy in copies:
        copy.start()
    for copy in copies:
        copy.wait()


def shards(
    displacement, external_force, element_sample, lame_field, shear_field, plastic_steps, owner_slot
):
    count = displacement.shape[1]
    disp, sample = (3, count, 8, 128), (count, 8, 128)
    wt, vt, vz, x, spec = (jnp.asarray(t) for t in tables())
    operands = (
        displacement,
        wt,
        lame_field.reshape(32, 1024),
        shear_field.reshape(32, 1024),
        external_force,
        element_sample,
        vt,
        vz,
        x,
        spec,
    )
    scalars = (plastic_steps, owner_slot)
    vmem = pl.BlockSpec(memory_space=pltpu.VMEM)
    hbm = pl.BlockSpec(memory_space=pltpu.HBM)
    dma = pltpu.SemaphoreType.DMA
    disp_next, row, micro = pl.pallas_call(
        kernel,
        out_shape=(
            jax.ShapeDtypeStruct(displacement.shape, f32),
            jax.ShapeDtypeStruct((1, 8), f32),
            jax.ShapeDtypeStruct((6 * 32 * 8, 128), f32),
        ),
        in_specs=[hbm] * 12,
        out_specs=(vmem,) * 3,
        scratch_shapes=[
            *(pltpu.VMEM(a.shape, a.dtype) for a in operands),
            *(pltpu.SMEM(a.shape, a.dtype) for a in scalars),
            dma((12,)),
            pltpu.VMEM(disp, f32),
            pltpu.VMEM(disp, f32),
            pltpu.VMEM(sample, jnp.int32),
            pltpu.VMEM((32, 16, 128), bf16),
            pltpu.VMEM((512, 128), f32),
            pltpu.VMEM((3, 8, 128), f32),
            pltpu.VMEM((3, 8, 128), f32),
            pltpu.VMEM((8, 128), jnp.int32),
            pltpu.VMEM((30, 8, 128), f32),
            pltpu.VMEM((6, 8, 128), jnp.int32),
            pltpu.VMEM((32, 16, 128), bf16),
            pltpu.VMEM((32, 1, 128), f32),
            pltpu.VMEM((32, 1, 128), f32),
            pltpu.VMEM((count, 64, 128), f32),
            pltpu.VMEM((32, count * 1024), bf16),
            pltpu.VMEM((32, 128), f32),
            *(pltpu.VMEM((HALF, HALF), bf16),) * 4,
            *(pltpu.VMEM((2, 256, 256), bf16),) * 4,
            pltpu.VMEM((2, 256, 128), f32),
            pltpu.VMEM((3, 256, 128), f32),
            pltpu.VMEM((32, 48, 128), wire),
            pltpu.VMEM((32, 48, 128), wire),
            pltpu.VMEM((4, 1, 128), f32),
            pltpu.VMEM((1, 1, 128), f32),
            pltpu.VMEM((32, 1, 128), f32),
            pltpu.VMEM((1, 1, 128), f32),
            pltpu.VMEM((32, 1, 128), f32),
            pltpu.SemaphoreType.REGULAR, dma((3,)), dma((3,)), dma((2,)), dma((2,)), dma, dma, dma, dma,
            dma, dma, dma, dma, dma, dma, dma, dma,
        ],
        compiler_params=pltpu.CompilerParams(collective_id=0, has_side_effects=True, vmem_limit_bytes=24 << 20),
    )(*[pltpu.with_memory_space_constraint(a, pltpu.HBM) for a in operands + scalars])
    results = (disp_next, row, micro)
    disp_next, row, micro = pl.pallas_call(
        leave,
        out_shape=tuple(jax.ShapeDtypeStruct(a.shape, a.dtype) for a in results),
        in_specs=[pl.BlockSpec(memory_space=pl.ANY)] * 3,
        out_specs=(pl.BlockSpec(memory_space=pltpu.HBM),) * 3,
        scratch_shapes=[dma((PIECES + 2,))],
        compiler_params=pltpu.CompilerParams(vmem_limit_bytes=1 << 20),
    )(*results)
    return disp_next, row, micro.reshape(6, 32, 1, 1024)


def solution(mesh):
    in_specs = (
        P(None, "dev", None, None),
        P(None, "dev", None, None),
        P("dev", None, None),
        P("grp", "dev", None),
        P("grp", "dev", None),
        P(),
        P(),
    )
    out_specs = (P(None, "dev", None, None), P(("grp", "dev"), None), P(None, "grp", "dev", None))
    return jax.shard_map(shards, mesh=mesh, in_specs=in_specs, out_specs=out_specs, check_vma=False)
```

```python
import jax
import jax.numpy as jnp
import numpy as np
from jax import lax
from jax.experimental import pallas as pl
from jax.experimental.pallas import tpu as pltpu
from jax.sharding import PartitionSpec as P

VOX = 32
HALF = 512
BLOCK = 32
PIECES = 1
KMAX = 4
MESH = pl.DeviceIdType.MESH
NEAR = (-2, -1, 1, 2)

shear_ref = 1.65
lame_ref = 1.25
green_ratio = (lame_ref + shear_ref) / (lame_ref + 2.0 * shear_ref)
relax_rate = 0.35
spring_rate = 0.2
wire = jnp.bfloat16
f32 = jnp.float32
bf16 = jnp.bfloat16


def tables():
    n = np.arange(VOX)
    theta = 2.0 * np.pi / VOX
    order = np.concatenate([n[::4], n[2::4], n[1::2]])
    ky = np.repeat(order, 16)
    kz = np.tile(np.arange(16), VOX)
    yy = np.repeat(n[:16], VOX)
    zz = np.tile(n, 16)
    k16 = np.arange(16)

    def zeta(z, k):
        angle = theta * (z * k % VOX)
        return (
            np.where(k == 0, 1.0, np.cos(angle)),
            np.where(k == 0, (-1.0) ** z, -np.sin(angle)),
        )

    cy, sy = np.cos(theta * (np.outer(n, ky) % VOX)), np.sin(theta * (np.outer(n, ky) % VOX))
    zr, zi = zeta(n[:, None], kz[None, :])
    cv, sv = np.cos(theta * (np.outer(order, yy) % VOX)), np.sin(theta * (np.outer(order, yy) % VOX))
    vr, vi = zeta(zz[None, :], k16[:, None])
    c, s = np.cos(theta * (np.outer(n, n) % VOX)), np.sin(theta * (np.outer(n, n) % VOX))
    x = np.block([[c, s], [-s, c]])

    def wave(k):
        return np.where(k % 16 == 0, 0.0, np.sin(theta * k))

    one = np.ones((VOX, HALF))
    xx, xy, xz = wave(n)[:, None] * one, wave(ky)[None] * one, wave(kz)[None] * one
    square = xx * xx + xy * xy + xz * xz
    inverse = np.where(square > 0, 1.0 / np.where(square > 0, square, 1.0), 0.0)
    weight = np.where(kz == 0, 1.0, 2.0)[None] * one
    scaled = -(1.0 / shear_ref) * inverse * weight / VOX**3
    pairs = (xx * xx, xy * xy, xz * xz, 2 * xy * xz, 2 * xx * xz, 2 * xx * xy)
    spectral = np.stack([scaled] + [green_ratio * p * inverse for p in pairs] + [xx, xy, xz])
    to = lambda a: np.asarray(a, np.float32)
    return (
        to(np.stack([cy, sy, zr, zi])),
        to(np.stack([cv, sv])),
        to(np.stack([vr, vi])),
        to(np.stack([x, x.T])),
        to(spectral),
    )


def split(a):
    high = a.astype(bf16)
    return high, (a - high.astype(f32)).astype(bf16)


def mm(a, b):
    return jnp.dot(a, b, preferred_element_type=f32)


def product(a, b):
    ah, al = split(a)
    bh, bl = split(b)
    return mm(jnp.concatenate([ah, al, ah], axis=1), jnp.concatenate([bh, bh, bl], axis=0))


def lane_of(shape):
    return lax.broadcasted_iota(jnp.int32, shape, len(shape) - 1)


def row_of(shape):
    return lax.broadcasted_iota(jnp.int32, shape, len(shape) - 2)


def roll(a, shift, axis):
    return pltpu.roll(a, shift % a.shape[axis], axis)


def shifts(v, sign):
    lane, row = lane_of(v.shape), row_of(v.shape)
    edge = lane % VOX == (VOX - 1 if sign > 0 else 0)
    inner = lane < 96 if sign > 0 else lane >= VOX
    last = row == (7 if sign > 0 else 0)

    def along_y(moved):
        return jnp.where(inner, moved, jnp.where(last, 0.0, roll(moved, -sign, 1)))

    z = jnp.where(edge, 0.0, roll(v, -sign, 2))
    y = along_y(roll(v, -sign * VOX, 2))
    both = jnp.where(edge, 0.0, along_y(roll(v, -sign * (VOX + 1), 2)))
    return z, y, both


def yc(v):
    lane = lane_of(v.shape)
    up = roll(v, -VOX, 2)
    up = jnp.where(lane < 96, up, roll(up, -1, 1))
    down = roll(v, VOX, 2)
    down = jnp.where(lane >= VOX, down, roll(down, 1, 1))
    return 0.5 * (up - down)


def spans(distance):
    return min(distance, 4 - distance)


OTHERS = sorted(
    ((a, b, c) for a in range(4) for b in range(4) for c in range(2) if (a, b, c) != (0, 0, 0)),
    key=lambda p: (-spans(p[0]) - spans(p[1]), -p[2], p),
)


def strain_of(fields):
    slopes = []
    for w in fields:
        z, y, yz = shifts(w, 1)
        near, far = w + z, y + yz
        a, b = 0.25 * (near + far), 0.5 * (far - near)
        c = 0.5 * ((z + yz) - (w + y))
        slopes.append((a[1:] - a[:-1], 0.5 * (b[1:] + b[:-1]), 0.5 * (c[1:] + c[:-1])))
    x, y, z = slopes
    return (
        x[0],
        y[1],
        z[2],
        0.5 * (z[1] + y[2]),
        0.5 * (z[0] + x[2]),
        0.5 * (y[0] + x[1]),
    )


def force_of(stress):
    xx, yy, zz, yz, xz, xy = stress
    result = []
    for along_x, along_y, along_z in ((xx, xy, xz), (xy, yy, yz), (xz, yz, zz)):
        z, y, yz = shifts(along_x, -1)
        first = 0.25 * ((along_x + z) + (y + yz))
        both = along_y + along_z
        less = along_z - along_y
        z, y, _ = shifts(less, -1)
        _, _, yz = shifts(both, -1)
        rest = 0.5 * ((yz - y) + (z - both))
        result.append((first[:-1] - first[1:]) + 0.5 * (rest[1:] + rest[:-1]))
    return result


def stress_of(strain, lame, shear):
    spread = lame * (strain[0] + strain[1] + strain[2])
    twice = 2.0 * shear
    return [twice * e + spread for e in strain[:3]] + [twice * e for e in strain[3:]]


def norm_of(d):
    return d[0] * d[0] + d[1] * d[1] + d[2] * d[2] + 2.0 * (d[3] * d[3] + d[4] * d[4] + d[5] * d[5])


def relaxed(mu, size, rates):
    base = mu * mu * size
    scale = jnp.ones_like(mu)
    for rate in rates:
        f = base * scale * scale
        scale = scale * ((1.0 - rate) + rate / (1.0 + f))
    return scale, base * scale * scale


def kernel(
    disp_in, wt_in, lame_in, shear_in, force_in, samp_in, vt_in, vz_in, x_in, spec_in, steps_in, slot_in,
    disp_out, row_out, micro_out,
    disp_raw, wt_ref, lame_raw, shear_raw, force_raw, samp_raw, vt_ref, vz_ref, x_ref, spec_ref,
    steps_ref, slot_ref, in_sem,
    disp_ref, force_ref, samp_ref, mod_ref, modwide,
    nb_first, nb_last, nb_mark, nb, nb_samp, sized, modbuf, partbuf, strainrow, one_hot_ref, sums_ref,
    wh, wl, vh, vl, weh, wel, veh, vel, field, disp_u, flu, flubuf,
    rowbuf, joined, respbuf, moment, momentbuf,
    ready, first_send, first_recv, near_send, near_recv, mod_send, mod_recv, part_send, part_recv,
    y_send, y_recv, resp_send, resp_recv, flu_send, flu_recv, mom_send, mom_recv,
):
    me = lax.axis_index("dev")
    group = lax.axis_index("grp")
    count = disp_raw.shape[1]

    me_x, me_z, me_c = me // 8, lax.rem(me // 2, 4), lax.rem(me, 2)
    at_x = [lax.rem(me_x + k, 4) * 8 for k in range(4)]
    at_z = [lax.rem(me_z + k, 4) * 2 for k in range(4)]
    at_c = [me_c, 1 - me_c]
    peers = [at_x[a] + at_z[b] + at_c[c] for a, b, c in OTHERS]

    loads = [
        pltpu.make_async_copy(source, target, in_sem.at[k])
        for k, (source, target) in enumerate(
            (
                (disp_in, disp_raw), (wt_in, wt_ref), (lame_in, lame_raw), (shear_in, shear_raw),
                (force_in, force_raw), (samp_in, samp_raw), (vt_in, vt_ref), (vz_in, vz_ref),
                (x_in, x_ref), (spec_in, spec_ref), (steps_in, steps_ref), (slot_in, slot_ref),
            )
        )
    ]
    loads[0].start()
    loads[5].start()

    barrier = pltpu.get_barrier_semaphore()
    layer = [peer for peer, (a, _, _) in zip(peers, OTHERS) if a == 0]
    entry = [peer for peer, (_, b, c) in zip(peers, OTHERS) if (b, c) == (0, 0)] + layer
    entry += [lax.rem(me + 1, 32), lax.rem(me + 31, 32)]
    for peer in entry:
        pl.semaphore_signal(barrier, inc=1, device_id={"dev": peer}, device_id_type=MESH)
    for i in range(1, 4):
        pl.semaphore_signal(
            barrier, inc=1, device_id={"grp": lax.rem(group + i, 4)}, device_id_type=MESH
        )
    for k in (1, 2, 3, 4, *range(6, 12)):
        loads[k].start()

    def dense(raw, out):
        for index in np.ndindex(raw.shape[:-2]):
            out[index] = jnp.concatenate(
                [raw[(*index, pl.ds(q, 8, stride=4), slice(None))] for q in range(4)], axis=1
            )

    loads[0].wait()
    dense(disp_raw, disp_ref)
    loads[5].wait()
    dense(samp_raw, samp_ref)
    pl.semaphore_wait(barrier, len(entry) + 3)

    lowest, highest = lax.rem(me, 8) == 0, lax.rem(me, 8) == 7
    upper, lower = lowest & (me > 0), highest & (me < 31)
    above, below = lax.rem(me + 1, 32), lax.rem(me + 31, 32)

    def bordering(k, source, target, device):
        return pltpu.make_async_remote_copy(
            src_ref=source,
            dst_ref=target,
            send_sem=first_send.at[k],
            recv_sem=first_recv.at[k],
            device_id={"dev": device},
            device_id_type=MESH,
        )

    first_plane = bordering(0, disp_ref.at[:, 0], nb_first, below)
    last_planes = (
        bordering(1, disp_ref.at[:, count - 1], nb_last, above),
        bordering(2, samp_ref.at[count - 1], nb_mark, above),
    )
    pl.when(jnp.logical_not(lowest))(first_plane.start)
    for copy in last_planes:
        pl.when(lower)(copy.start)
    for peer in layer:
        pl.semaphore_signal(ready, inc=1, device_id={"dev": peer}, device_id_type=MESH)
    for k in range(2, 5):
        loads[k].wait()
    dense(force_raw, force_ref)
    for k, raw in enumerate((lame_raw, shear_raw)):
        wide = raw[...].astype(f32)
        for t in range(8):
            modwide[pl.ds(k * 8 + t, 32, stride=16), :] = wide[:, t * 128 : t * 128 + 128]
    for r in range(32):
        mod_ref[r] = modwide[pl.ds(r * 16, 16), :].astype(bf16)

    sums_ref[...] = jnp.zeros_like(sums_ref)
    for plane in range(count):
        strainrow[plane, pl.ds(48, 8), :] = jnp.ones((8, 128), f32)
        strainrow[plane, pl.ds(56, 8), :] = jnp.zeros((8, 128), f32)

    places = {-1: (0, 6, 1), 1: (6, 6, 1 + count), 2: (12, 3, 1 + 2 * count), -2: (None, 0, 0)}
    near = []
    for offset, (start, _, sample_start) in places.items():
        device = lax.rem(me - offset + 32, 32)
        plane = {2: 0, -2: count - 1}.get(offset)

        def send(source, target, k, device=device):
            near.append(
                pltpu.make_async_remote_copy(
                    src_ref=source,
                    dst_ref=target,
                    send_sem=near_send.at[k],
                    recv_sem=near_recv.at[k],
                    device_id={"dev": device},
                    device_id_type=MESH,
                )
            )

        width = count if plane is None else 1
        cut_out = pl.ds(0 if plane is None else plane, width)
        if start is not None:
            for k, source in enumerate((disp_ref, force_ref)):
                for c in range(3):
                    send(source.at[c, cut_out], nb.at[pl.ds(k * 15 + start + c * width, width)], 0)
        send(samp_ref.at[cut_out], nb_samp.at[pl.ds(sample_start, width)], 1)

    def everyone(source, target, send, recv):
        for peer in peers:
            pltpu.make_async_remote_copy(
                src_ref=source(peer),
                dst_ref=target.at[me] if len(target.shape) == 3 else target.at[pl.ds(me, 1)],
                send_sem=send,
                recv_sem=recv,
                device_id={"dev": peer},
                device_id_type=MESH,
            ).start()

    def all_arrived(target, recv):
        ref = target.at[pl.ds(0, 31)] if len(target.shape) == 3 else sized.at[pl.ds(0, 31)]
        pltpu.make_async_copy(ref, ref, recv).wait()

    loads[1].wait()

    @pl.loop(0, 16)
    def _(y):
        c, s = wt_ref[0, pl.ds(y, 1), :], wt_ref[1, pl.ds(y, 1), :]
        zr, zi = wt_ref[2], wt_ref[3]
        rows = pl.ds(pl.multiple_of(y * 32, 32), 32)
        blocks = [split(b) for b in (c * zr + s * zi, c * zi - s * zr)]
        for k, (high, low) in enumerate(blocks):
            wh[rows, pl.ds(k * 256, 256)] = high[:, 256:]
            wl[rows, pl.ds(k * 256, 256)] = low[:, 256:]

        @pl.when(y < 8)
        def _():
            for k, (high, low) in enumerate(blocks):
                for q in range(2):
                    lanes = slice(q * 128, q * 128 + 128)
                    weh[q, rows, pl.ds(k * 128, 128)] = high[:, lanes]
                    wel[q, rows, pl.ds(k * 128, 128)] = low[:, lanes]

    def hot_of(sample, s, counted):
        hit = jnp.broadcast_to(sample[s : s + 1], (32, 128)) == row_of((32, 128)) + group * 32
        return jnp.where(hit, counted, 0.0).astype(bf16)

    own_last = jnp.where(lower, 0.0, 1.0).astype(f32)
    one_hot_ref[...] = jnp.concatenate(
        [hot_of(samp_ref[p], s, (1.0, own_last)[p // (count - 1)]) for p in range(count) for s in range(8)],
        axis=1,
    )
    pl.semaphore_wait(ready, len(layer))
    everyone(lambda peer: mod_ref.at[peer], modbuf, mod_send, mod_recv)
    modbuf[me] = mod_ref[me]

    def sums_of(strain, one_hot):
        n = strain[0].shape[0]
        rows_high, rows_low = [], []
        for p in range(n):
            for c in range(6):
                strainrow[p, pl.ds(c * 8, 8), :] = strain[c][p]
        for p in range(n):
            for s in range(8):
                high, low = split(strainrow[p, pl.ds(s, 8, stride=8), :])
                rows_high.append(high)
                rows_low.append(low)

        def against(rows):
            return lax.dot_general(
                one_hot,
                jnp.concatenate(rows, axis=1),
                (((1,), (1,)), ((), ())),
                preferred_element_type=f32,
            )

        return against(rows_high) + against(rows_low)

    pl.when(jnp.logical_not(highest))(first_plane.wait_recv)
    fields = [
        jnp.concatenate([disp_ref[c], jnp.where(highest, 0.0, nb_first[pl.ds(c, 1)])], axis=0)
        for c in range(3)
    ]
    sums_ref[:, pl.ds(0, 8)] = sums_of(strain_of(fields), one_hot_ref[...])

    @pl.when(upper)
    def _():
        for copy in last_planes:
            copy.wait_recv()
        between = [
            jnp.concatenate([nb_last[pl.ds(c, 1)], disp_ref[c, pl.ds(0, 1)]], axis=0) for c in range(3)
        ]
        hots = jnp.concatenate([hot_of(nb_mark, s, 1.0) for s in range(8)], axis=1)
        sums_ref[:, pl.ds(0, 8)] += sums_of(strain_of(between), hots)

    everyone(lambda peer: sums_ref.at[pl.ds(peer, 1)], partbuf, part_send, part_recv)
    partbuf[pl.ds(me, 1), :] = sums_ref[pl.ds(me, 1), :]
    for k in range(6, 12):
        loads[k].wait()

    def back_rows(k, lanes):
        row = pl.ds(k, 1)
        c, s = vt_ref[0, row, pl.ds(0, lanes)], vt_ref[1, row, pl.ds(0, lanes)]
        zr, zi = vz_ref[0, :, pl.ds(0, lanes)], vz_ref[1, :, pl.ds(0, lanes)]
        return split(c * zr + s * zi), split(c * zi - s * zr)

    @pl.loop(0, 16)
    def _(k):
        for p, (high, low) in enumerate(back_rows(16 + k, HALF)):
            rows = pl.ds(pl.multiple_of(p * 256 + k * 16, 16), 16)
            vh[rows, :] = high
            vl[rows, :] = low

    for q in range(2):

        @pl.loop(0, 8)
        def _(k):
            for p, (high, low) in enumerate(back_rows(q * 8 + k, 256)):
                rows = pl.ds(pl.multiple_of(p * 128 + k * 16, 16), 16)
                veh[q, rows, :] = high
                vel[q, rows, :] = low

    ref = modbuf.at[pl.ds(0, 31)]
    pltpu.make_async_copy(ref, ref, mod_recv).wait()

    def moduli(x, n):
        both = modbuf[pl.ds(x, n)].astype(f32)
        return both[:, :8], both[:, 8:]

    def at(x, n):
        return pl.ds(pl.multiple_of(x * 8, 8), n * 8)

    def planes(ref, k, x, n):
        return ref[k, at(x, n), :].reshape(n, 8, 128)

    def x_slope(ref, k, x, n, v):
        after = planes(ref, k, lax.rem(x + n, 32), 1)
        before = planes(ref, k, lax.rem(x + 31, 32), 1)
        up = jnp.concatenate([v[1:], after], axis=0)
        down = jnp.concatenate([before, v[:-1]], axis=0)
        return 0.5 * (up - down)

    def forward():
        rows = jnp.concatenate(
            [
                jnp.concatenate([field[k, pl.ds(s, 32, stride=8), :] for k in range(2)], axis=0)
                for s in range(8)
            ],
            axis=1,
        )
        even, odd = rows[:, :HALF] + rows[:, HALF:], rows[:, :HALF] - rows[:, HALF:]

        def part_of(data, high_ref, low_ref):
            high, low = split(data)
            both = mm(jnp.concatenate([high, low], axis=0), high_ref[...])
            return both[:64] + (both[64:] + mm(high, low_ref[...]))

        sides = [
            part_of(even[:, :256] + even[:, 256:], weh.at[0], wel.at[0]),
            part_of(even[:, :256] - even[:, 256:], weh.at[1], wel.at[1]),
            part_of(odd, wh, wl),
        ]
        plane = jnp.concatenate(
            [side[:, : side.shape[1] // 2] for side in sides]
            + [side[:, side.shape[1] // 2 :] for side in sides],
            axis=1,
        )
        stacked = jnp.concatenate(
            [
                jnp.concatenate([plane[:32, :HALF], plane[32:, :HALF]], axis=1),
                jnp.concatenate([plane[:32, HALF:], plane[32:, HALF:]], axis=1),
            ],
            axis=0,
        )
        return product(x_ref[0], stacked)

    lame, shear = moduli(0, 32)
    field[0] = (lame + (2.0 / 3.0) * shear).reshape(256, 128)

    all_arrived(partbuf, part_recv)
    total = jnp.sum(partbuf[...], axis=0, keepdims=True)
    lane1 = lane_of((1, 128))

    def pick(row, k):
        return jnp.sum(jnp.where(lane1 == k, row, 0.0), axis=1, keepdims=True)

    members = pick(total, 6)
    load = [pick(total, c) / members for c in range(6)]
    trace = load[0] + load[1] + load[2]
    d = [load[c] - trace / 3.0 if c < 3 else load[c] for c in range(6)]
    own_steps = steps_ref[group * 32 + me]
    rates = [jnp.where(k < own_steps, relax_rate, 0.0).astype(f32) for k in range(KMAX)]
    size = norm_of(d)

    _, shear = moduli(0, 32)
    scale, _ = relaxed(shear, size, rates)
    field[1] = (2.0 * shear * scale).reshape(256, 128)
    spectrum = forward()
    spectrum_a, spectrum_b = spectrum[:, :HALF], spectrum[:, HALF:]
    mix = d[0] * spec_ref[1]
    for c in range(1, 6):
        mix = mix + d[c] * spec_ref[1 + c]
    scaled = spec_ref[0]
    steady = (1.0 - green_ratio) * trace
    phi = [scaled * spectrum_b[:32], scaled * spectrum_b[32:]]
    pressure = [
        scaled * (steady * spectrum_a[:32]) - mix * phi[0],
        scaled * (steady * spectrum_a[32:]) - mix * phi[1],
    ]
    waves = [spec_ref[7 + c] for c in range(3)]
    turned = [
        d[0] * waves[0] + d[5] * waves[1] + d[4] * waves[2],
        d[5] * waves[0] + d[1] * waves[1] + d[3] * waves[2],
        d[4] * waves[0] + d[3] * waves[1] + d[2] * waves[2],
    ]
    slopes = [
        [waves[c] * pressure[k] + turned[c] * phi[k] for k in range(2)] for c in range(3)
    ]
    mixed = jnp.concatenate(
        [
            jnp.concatenate([-slopes[c][1] for c in range(3)], axis=1),
            jnp.concatenate([slopes[c][0] for c in range(3)], axis=1),
        ],
        axis=0,
    )
    back = product(x_ref[1], mixed)
    def side_of(start, width, high_ref, low_ref):
        lines = jnp.concatenate(
            [
                jnp.concatenate(
                    [back[h : h + 32, c * HALF + start :][:, :width] for h in (0, 32)], axis=1
                )
                for c in range(3)
            ],
            axis=0,
        )
        high, low = split(lines)
        both = mm(jnp.concatenate([high, low], axis=0), high_ref[...])
        return both[:96] + (both[96:] + mm(high, low_ref[...]))

    first, second = (side_of(q * 128, 128, veh.at[q], vel.at[q]) for q in range(2))
    even = jnp.concatenate([first + second, first - second], axis=1)
    odd = side_of(256, 256, vh, vl)
    space = jnp.concatenate([even + odd, even - odd], axis=1)
    for c in range(3):
        for s in range(8):
            disp_u[c, pl.ds(s, 32, stride=8), :] = space[
                c * 32 : c * 32 + 32, s * 128 : s * 128 + 128
            ]

    source, target = row_of((128, 128)), lane_of((128, 128))
    line = source // VOX == target // VOX
    ahead = line & ((target + 1) % VOX == source % VOX)
    behind = line & ((target + VOX - 1) % VOX == source % VOX)
    z_matrix = (jnp.where(ahead, 0.5, 0.0) - jnp.where(behind, 0.5, 0.0)).astype(bf16)

    def voxel(t, sums):
        x = t * BLOCK
        ux, uy, uz = (planes(disp_u, c, x, BLOCK) for c in range(3))
        dx = [x_slope(disp_u, c, x, BLOCK, u) for c, u in enumerate((ux, uy, uz))]
        high, low = split(jnp.concatenate([ux, uy, uz], axis=0).reshape(24 * BLOCK, 128))
        dz = (mm(high, z_matrix) + mm(low, z_matrix)).reshape(3, BLOCK, 8, 128)
        change = [
            -dx[0],
            -yc(uy),
            -dz[2],
            -0.5 * (yc(uz) + dz[1]),
            -0.5 * (dx[2] + dz[0]),
            -0.5 * (dx[1] + yc(ux)),
        ]
        for k in range(3):
            pair = jnp.concatenate(change[2 * k : 2 * k + 2], axis=1)
            flu[pl.ds(x, BLOCK), pl.ds(k * 16, 16), :] = pair.astype(wire)
        lame, shear = moduli(x, BLOCK)
        e = [load[c] + change[c] for c in range(6)]
        tr = e[0] + e[1] + e[2]
        dv = [e[c] - tr / 3.0 if c < 3 else e[c] for c in range(6)]
        scale, f = relaxed(shear, norm_of(dv), rates)
        twice = 2.0 * shear * scale
        bulk = (lame + (2.0 / 3.0) * shear) * tr
        new = [bulk + twice * dv[c] if c < 3 else twice * dv[c] for c in range(6)]
        new += [lame, shear / (1.0 + f)]
        return tuple(a + jnp.sum(b, axis=0) for a, b in zip(sums, new))

    zero = jnp.zeros((8, 128), f32)
    sums = lax.fori_loop(0, 32 // BLOCK, voxel, (zero,) * 8)
    column = jnp.concatenate([jnp.sum(a, axis=0, keepdims=True) for a in sums], axis=0)
    column = jnp.sum(column, axis=1, keepdims=True) * (1.0 / VOX**3)
    lane8, row8 = lane_of((8, 128)), row_of((8, 128))
    own_row = jnp.sum(
        jnp.where(lane8 == row8 + group * 16, column, 0.0), axis=0, keepdims=True
    )
    for c in range(6):
        own_row = own_row + jnp.where(lane1 == group * 16 + 8 + c, load[c], 0.0)

    rowbuf[3] = own_row
    for i in range(1, 4):
        (
            pltpu.make_async_remote_copy(
                src_ref=rowbuf.at[3],
                dst_ref=rowbuf.at[i - 1],
                send_sem=y_send,
                recv_sem=y_recv,
                device_id={"grp": lax.rem(group + i, 4)},
                device_id_type=MESH,
            )
        ).start()
    arrived = rowbuf.at[pl.ds(0, 3)]
    for copy in near:
        copy.start()
    pltpu.make_async_copy(arrived, arrived, y_recv).wait()
    joined[0] = rowbuf[0] + rowbuf[1] + rowbuf[2] + rowbuf[3]
    everyone(lambda peer: joined.at[0], respbuf, resp_send, resp_recv)
    respbuf[pl.ds(me, 1), :] = joined[0]
    everyone(lambda peer: flu.at[peer], flubuf, flu_send, flu_recv)
    flubuf[me] = flu[me]

    pltpu.make_async_copy(nb, nb, near_recv.at[0]).wait()
    pltpu.make_async_copy(nb_samp, nb_samp, near_recv.at[1]).wait()
    exists = [(me * count + j >= 3).astype(f32) * (me * count + j < 67).astype(f32) for j in range(8)]

    def around_of(own, k, c):
        below = [nb[pl.ds(k * 15 + c * 2 + p, 1)] for p in (0, 0, 1)]
        above = [nb[pl.ds(k * 15 + 6 + c * 2 + p, 1)] for p in range(2)]
        return [*below, own[c, pl.ds(0, 1)], own[c, pl.ds(1, 1)], *above, nb[pl.ds(k * 15 + 12 + c, 1)]]

    def masked(planes):
        return jnp.concatenate([p * m for p, m in zip(planes, exists)], axis=0)

    around = [masked(around_of(disp_ref, 0, c)) for c in range(3)]
    outside = [masked(around_of(force_ref, 1, c)) for c in range(3)]
    given = [
        (outside[c][1:] - spring_rate * around[c][1:])
        * jnp.concatenate([jnp.full((1, 8, 128), m) for m in exists[1:]], axis=0)
        for c in range(3)
    ]
    samples = [nb_samp[pl.ds(j, 1)] for j in range(3)]
    samples += [samp_ref[pl.ds(p, 1)] for p in range(2)]
    samples += [nb_samp[pl.ds(j, 1)] for j in range(3, 6)]

    all_arrived(respbuf, resp_recv)
    gathered = jnp.concatenate([respbuf[...], jnp.zeros((96, 128), f32)], axis=0).T
    cells = []
    for c in range(8):
        row = jnp.concatenate(
            [gathered[g * 16 + c : g * 16 + c + 1, :32] for g in range(4)], axis=1
        )
        source = jnp.broadcast_to(row, (8, 128))
        cells.append(
            masked(
                [
                    jnp.take_along_axis(source, s[0], axis=1, mode="promise_in_bounds")[None]
                    for s in samples
                ]
            )
        )
    lame, shear = cells[6], cells[7]
    pull = force_of(cells[:6])
    inside = jnp.concatenate([jnp.full((1, 8, 128), m) for m in exists[1:]], axis=0)
    res = [given[c] - pull[c] * inside for c in range(3)]

    def stiff(w, low):
        n = w[0].shape[0]
        strain = strain_of(w)
        stress = stress_of(strain, lame[low : low + n - 1], shear[low : low + n - 1])
        pull = force_of(stress)
        mask = jnp.concatenate(
            [jnp.full((1, 8, 128), m) for m in exists[low + 1 : low + n - 1]], axis=0
        )
        return [(pull[c] + spring_rate * w[c][1:-1]) * mask for c in range(3)]

    k1 = stiff(res, 1)
    k2 = stiff(k1, 2)
    r_own = [a[2:4] for a in res]
    k1_own = [a[1:3] for a in k1]
    k2_own = [a[0:2] for a in k2]
    energy_strain = strain_of(k2)
    energy_stress = stress_of(energy_strain, lame[3:5], shear[3:5])

    def dotted(a, b):
        total = a[0] * b[0]
        for c in range(1, 3):
            total = total + a[c] * b[c]
        return jnp.sum(jnp.sum(total, axis=0), axis=0, keepdims=True)

    energy = energy_strain[0] * energy_stress[0]
    for c in range(1, 6):
        energy = energy + (1.0 if c < 3 else 2.0) * energy_strain[c] * energy_stress[c]
    energy = jnp.sum(jnp.sum(energy, axis=0), axis=0, keepdims=True) + spring_rate * dotted(
        k2_own, k2_own
    )
    rows = [
        dotted(r_own, r_own),
        dotted(r_own, k1_own),
        dotted(k1_own, k1_own),
        dotted(k1_own, k2_own),
        dotted(k2_own, k2_own),
        energy,
        jnp.zeros((2, 128), f32),
    ]
    column = jnp.sum(jnp.concatenate(rows, axis=0), axis=1, keepdims=True)
    moment[0] = jnp.sum(jnp.where(lane8 == row8, column, 0.0), axis=0, keepdims=True)
    everyone(lambda peer: moment.at[0], momentbuf, mom_send, mom_recv)
    momentbuf[pl.ds(me, 1), :] = moment[0]

    def owner(r, acc):
        taken = jnp.where(slot_ref[group * 32 + r] == me, 1.0, 0.0).astype(f32)
        return acc + taken * respbuf[pl.ds(r, 1), :]

    row = lax.fori_loop(0, 32, owner, jnp.zeros((1, 128), f32))
    shifted = jnp.zeros((1, 128), f32)
    for g in range(4):
        here = (group == g).astype(f32)
        shifted = shifted + here * roll(row, -16 * g, 1)
    row_out[...] = shifted[:, :8]

    table = respbuf[...]
    lane32 = lane_of((32, 128))
    group_load = [
        jnp.sum(jnp.where(lane32 == group * 16 + 8 + c, table, 0.0), axis=1, keepdims=True)
        for c in range(6)
    ]
    all_arrived(flubuf, flu_recv)
    for r in range(32):
        block = flubuf[r].astype(f32)
        for c in range(6):
            micro_out[pl.ds((c * 32 + r) * 8, 8), :] = (
                group_load[c][r : r + 1] + block[c * 8 : c * 8 + 8]
            )

    all_arrived(momentbuf, mom_recv)
    total = jnp.sum(momentbuf[...], axis=0, keepdims=True)
    m = [pick(total, k) for k in range(6)]

    def form(a, b, first):
        out = 0.0
        for i, p in enumerate(a):
            for j, q in enumerate(b):
                out = out + p * q * m[i + j + first]
        return out

    rr = m[0]
    alpha0 = rr / m[1]
    r1 = (jnp.ones_like(rr), -alpha0)
    rr1 = form(r1, r1, 0)
    beta0 = rr1 / rr
    p1 = (1.0 + beta0, -alpha0)
    alpha1 = rr1 / form(p1, p1, 1)
    r2 = (jnp.ones_like(rr), -alpha0 - alpha1 * p1[0], alpha1 * alpha0)
    rr2 = form(r2, r2, 0)
    beta1 = rr2 / rr1
    p2 = (r2[0] + beta1 * p1[0], r2[1] + beta1 * p1[1], r2[2])
    alpha2 = rr2 / form(p2, p2, 1)
    weight = (
        alpha0 + alpha1 * p1[0] + alpha2 * p2[0],
        alpha1 * p1[1] + alpha2 * p2[1],
        alpha2 * p2[2],
    )
    for c in range(3):
        new = disp_ref[c] + (
            weight[0] * r_own[c] + weight[1] * k1_own[c] + weight[2] * k2_own[c]
        )
        for p in range(count):
            for q in range(4):
                disp_out[c, p, pl.ds(q, 8, stride=4), :] = new[p][:, q * 32 : q * 32 + 32]

    pl.when(jnp.logical_not(lowest))(first_plane.wait_send)
    for copy in last_planes:
        pl.when(lower)(copy.wait_send)
    pltpu.make_async_copy(nb, nb, near_send.at[0]).wait()
    pltpu.make_async_copy(nb_samp, nb_samp, near_send.at[1]).wait()
    pltpu.make_async_copy(arrived, arrived, y_send).wait()
    for buffer, sem in (
        (modbuf, mod_send), (partbuf, part_send), (respbuf, resp_send),
        (flubuf, flu_send), (momentbuf, mom_send),
    ):
        all_arrived(buffer, sem)


def leave(a, b, c, a_out, b_out, c_out, sem):
    step = c.shape[0] // PIECES
    pairs = [(a, a_out), (b, b_out)]
    pairs += [(c.at[pl.ds(k * step, step)], c_out.at[pl.ds(k * step, step)]) for k in range(PIECES)]
    copies = [pltpu.make_async_copy(*pair, sem.at[k]) for k, pair in enumerate(pairs)]
    for copy in copies:
        copy.start()
    for copy in copies:
        copy.wait()


def shards(
    displacement, external_force, element_sample, lame_field, shear_field, plastic_steps, owner_slot
):
    count = displacement.shape[1]
    disp, sample = (3, count, 8, 128), (count, 8, 128)
    wt, vt, vz, x, spec = (jnp.asarray(t) for t in tables())
    operands = (
        displacement,
        wt,
        lame_field.reshape(32, 1024),
        shear_field.reshape(32, 1024),
        external_force,
        element_sample,
        vt,
        vz,
        x,
        spec,
    )
    scalars = (plastic_steps, owner_slot)
    vmem = pl.BlockSpec(memory_space=pltpu.VMEM)
    hbm = pl.BlockSpec(memory_space=pltpu.HBM)
    dma = pltpu.SemaphoreType.DMA
    disp_next, row, micro = pl.pallas_call(
        kernel,
        out_shape=(
            jax.ShapeDtypeStruct(displacement.shape, f32),
            jax.ShapeDtypeStruct((1, 8), f32),
            jax.ShapeDtypeStruct((6 * 32 * 8, 128), f32),
        ),
        in_specs=[hbm] * 12,
        out_specs=(vmem,) * 3,
        scratch_shapes=[
            *(pltpu.VMEM(a.shape, a.dtype) for a in operands),
            *(pltpu.SMEM(a.shape, a.dtype) for a in scalars),
            dma((12,)),
            pltpu.VMEM(disp, f32),
            pltpu.VMEM(disp, f32),
            pltpu.VMEM(sample, jnp.int32),
            pltpu.VMEM((32, 16, 128), bf16),
            pltpu.VMEM((512, 128), f32),
            pltpu.VMEM((3, 8, 128), f32),
            pltpu.VMEM((3, 8, 128), f32),
            pltpu.VMEM((8, 128), jnp.int32),
            pltpu.VMEM((30, 8, 128), f32),
            pltpu.VMEM((6, 8, 128), jnp.int32),
            pltpu.VMEM((32, 1, 128), f32),
            pltpu.VMEM((32, 16, 128), bf16),
            pltpu.VMEM((32, 128), f32),
            pltpu.VMEM((count, 64, 128), f32),
            pltpu.VMEM((32, count * 1024), bf16),
            pltpu.VMEM((32, 128), f32),
            *(pltpu.VMEM((HALF, HALF), bf16),) * 4,
            *(pltpu.VMEM((2, 256, 256), bf16),) * 4,
            pltpu.VMEM((2, 256, 128), f32),
            pltpu.VMEM((3, 256, 128), f32),
            pltpu.VMEM((32, 48, 128), wire),
            pltpu.VMEM((32, 48, 128), wire),
            pltpu.VMEM((4, 1, 128), f32),
            pltpu.VMEM((1, 1, 128), f32),
            pltpu.VMEM((32, 128), f32),
            pltpu.VMEM((1, 1, 128), f32),
            pltpu.VMEM((32, 128), f32),
            pltpu.SemaphoreType.REGULAR, dma((3,)), dma((3,)), dma((2,)), dma((2,)), dma, dma, dma, dma,
            dma, dma, dma, dma, dma, dma, dma, dma,
        ],
        compiler_params=pltpu.CompilerParams(collective_id=0, has_side_effects=True, vmem_limit_bytes=24 << 20),
    )(*[pltpu.with_memory_space_constraint(a, pltpu.HBM) for a in operands + scalars])
    results = (disp_next, row, micro)
    disp_next, row, micro = pl.pallas_call(
        leave,
        out_shape=tuple(jax.ShapeDtypeStruct(a.shape, a.dtype) for a in results),
        in_specs=[pl.BlockSpec(memory_space=pl.ANY)] * 3,
        out_specs=(pl.BlockSpec(memory_space=pltpu.HBM),) * 3,
        scratch_shapes=[dma((PIECES + 2,))],
        compiler_params=pltpu.CompilerParams(vmem_limit_bytes=1 << 20),
    )(*results)
    return disp_next, row, micro.reshape(6, 32, 1, 1024)


def solution(mesh):
    in_specs = (
        P(None, "dev", None, None),
        P(None, "dev", None, None),
        P("dev", None, None),
        P("grp", "dev", None),
        P("grp", "dev", None),
        P(),
        P(),
    )
    out_specs = (P(None, "dev", None, None), P(("grp", "dev"), None), P(None, "grp", "dev", None))
    return jax.shard_map(shards, mesh=mesh, in_specs=in_specs, out_specs=out_specs, check_vma=False)
```

```python
import jax
import jax.numpy as jnp
import numpy as np
from jax import lax
from jax.experimental import pallas as pl
from jax.experimental.pallas import tpu as pltpu
from jax.sharding import PartitionSpec as P

VOX = 32
HALF = 512
BLOCK = 32
PIECES = 1
KMAX = 4
MESH = pl.DeviceIdType.MESH
NEAR = (-2, -1, 1, 2)

shear_ref = 1.65
lame_ref = 1.25
green_ratio = (lame_ref + shear_ref) / (lame_ref + 2.0 * shear_ref)
relax_rate = 0.35
spring_rate = 0.2
wire = jnp.bfloat16
f32 = jnp.float32
bf16 = jnp.bfloat16


def tables():
    n = np.arange(VOX)
    theta = 2.0 * np.pi / VOX
    order = np.concatenate([n[::4], n[2::4], n[1::2]])
    ky = np.repeat(order, 16)
    kz = np.tile(np.arange(16), VOX)
    yy = np.repeat(n[:16], VOX)
    zz = np.tile(n, 16)
    k16 = np.arange(16)

    def zeta(z, k):
        angle = theta * (z * k % VOX)
        return (
            np.where(k == 0, 1.0, np.cos(angle)),
            np.where(k == 0, (-1.0) ** z, -np.sin(angle)),
        )

    cy, sy = np.cos(theta * (np.outer(n, ky) % VOX)), np.sin(theta * (np.outer(n, ky) % VOX))
    zr, zi = zeta(n[:, None], kz[None, :])
    cv, sv = np.cos(theta * (np.outer(order, yy) % VOX)), np.sin(theta * (np.outer(order, yy) % VOX))
    vr, vi = zeta(zz[None, :], k16[:, None])
    c, s = np.cos(theta * (np.outer(n, n) % VOX)), np.sin(theta * (np.outer(n, n) % VOX))
    x = np.block([[c, s], [-s, c]])

    def wave(k):
        return np.where(k % 16 == 0, 0.0, np.sin(theta * k))

    one = np.ones((VOX, HALF))
    xx, xy, xz = wave(n)[:, None] * one, wave(ky)[None] * one, wave(kz)[None] * one
    square = xx * xx + xy * xy + xz * xz
    inverse = np.where(square > 0, 1.0 / np.where(square > 0, square, 1.0), 0.0)
    weight = np.where(kz == 0, 1.0, 2.0)[None] * one
    scaled = -(1.0 / shear_ref) * inverse * weight / VOX**3
    pairs = (xx * xx, xy * xy, xz * xz, 2 * xy * xz, 2 * xx * xz, 2 * xx * xy)
    spectral = np.stack([scaled] + [green_ratio * p * inverse for p in pairs] + [xx, xy, xz])
    to = lambda a: np.asarray(a, np.float32)
    return (
        to(np.stack([cy, sy, zr, zi])),
        to(np.stack([cv, sv])),
        to(np.stack([vr, vi])),
        to(np.stack([x, x.T])),
        to(spectral),
    )


def split(a):
    high = a.astype(bf16)
    return high, (a - high.astype(f32)).astype(bf16)


def mm(a, b):
    return jnp.dot(a, b, preferred_element_type=f32)


def product(a, b):
    ah, al = split(a)
    bh, bl = split(b)
    return mm(jnp.concatenate([ah, al, ah], axis=1), jnp.concatenate([bh, bh, bl], axis=0))


def lane_of(shape):
    return lax.broadcasted_iota(jnp.int32, shape, len(shape) - 1)


def row_of(shape):
    return lax.broadcasted_iota(jnp.int32, shape, len(shape) - 2)


def roll(a, shift, axis):
    return pltpu.roll(a, shift % a.shape[axis], axis)


def shifts(v, sign):
    lane, row = lane_of(v.shape), row_of(v.shape)
    edge = lane % VOX == (VOX - 1 if sign > 0 else 0)
    inner = lane < 96 if sign > 0 else lane >= VOX
    last = row == (7 if sign > 0 else 0)

    def along_y(moved):
        return jnp.where(inner, moved, jnp.where(last, 0.0, roll(moved, -sign, 1)))

    z = jnp.where(edge, 0.0, roll(v, -sign, 2))
    y = along_y(roll(v, -sign * VOX, 2))
    both = jnp.where(edge, 0.0, along_y(roll(v, -sign * (VOX + 1), 2)))
    return z, y, both


def yc(v):
    lane = lane_of(v.shape)
    up = roll(v, -VOX, 2)
    up = jnp.where(lane < 96, up, roll(up, -1, 1))
    down = roll(v, VOX, 2)
    down = jnp.where(lane >= VOX, down, roll(down, 1, 1))
    return 0.5 * (up - down)


def spans(distance):
    return min(distance, 4 - distance)


OTHERS = sorted(
    ((a, b, c) for a in range(4) for b in range(4) for c in range(2) if (a, b, c) != (0, 0, 0)),
    key=lambda p: (-spans(p[0]) - spans(p[1]), -p[2], p),
)


def strain_of(fields):
    slopes = []
    for w in fields:
        z, y, yz = shifts(w, 1)
        near, far = w + z, y + yz
        a, b = 0.25 * (near + far), 0.5 * (far - near)
        c = 0.5 * ((z + yz) - (w + y))
        slopes.append((a[1:] - a[:-1], 0.5 * (b[1:] + b[:-1]), 0.5 * (c[1:] + c[:-1])))
    x, y, z = slopes
    return (
        x[0],
        y[1],
        z[2],
        0.5 * (z[1] + y[2]),
        0.5 * (z[0] + x[2]),
        0.5 * (y[0] + x[1]),
    )


def force_of(stress):
    xx, yy, zz, yz, xz, xy = stress
    result = []
    for along_x, along_y, along_z in ((xx, xy, xz), (xy, yy, yz), (xz, yz, zz)):
        z, y, yz = shifts(along_x, -1)
        first = 0.25 * ((along_x + z) + (y + yz))
        both = along_y + along_z
        less = along_z - along_y
        z, y, _ = shifts(less, -1)
        _, _, yz = shifts(both, -1)
        rest = 0.5 * ((yz - y) + (z - both))
        result.append((first[:-1] - first[1:]) + 0.5 * (rest[1:] + rest[:-1]))
    return result


def stress_of(strain, lame, shear):
    spread = lame * (strain[0] + strain[1] + strain[2])
    twice = 2.0 * shear
    return [twice * e + spread for e in strain[:3]] + [twice * e for e in strain[3:]]


def norm_of(d):
    return d[0] * d[0] + d[1] * d[1] + d[2] * d[2] + 2.0 * (d[3] * d[3] + d[4] * d[4] + d[5] * d[5])


def relaxed(mu, size, rates):
    base = mu * mu * size
    scale = jnp.ones_like(mu)
    for rate in rates:
        f = base * scale * scale
        scale = scale * ((1.0 - rate) + rate / (1.0 + f))
    return scale, base * scale * scale


def kernel(
    disp_in, wt_in, lame_in, shear_in, force_in, samp_in, vt_in, vz_in, x_in, spec_in, steps_in, slot_in,
    disp_out, row_out, micro_out,
    disp_raw, wt_ref, lame_raw, shear_raw, force_raw, samp_raw, vt_ref, vz_ref, x_ref, spec_ref,
    steps_ref, slot_ref, in_sem,
    disp_ref, force_ref, samp_ref, mod_ref, modwide,
    nb_first, nb_last, nb_mark, nb, nb_samp, sized, modbuf, partbuf, strainrow, one_hot_ref, sums_ref,
    wh, wl, vh, vl, weh, wel, veh, vel, field, disp_u, flu, flubuf,
    rowbuf, joined, respbuf, moment, momentbuf,
    ready, first_send, first_recv, near_send, near_recv, mod_send, mod_recv, part_send, part_recv,
    y_send, y_recv, resp_send, resp_recv, flu_send, flu_recv, mom_send, mom_recv,
):
    me = lax.axis_index("dev")
    group = lax.axis_index("grp")
    count = disp_raw.shape[1]

    me_x, me_z, me_c = me // 8, lax.rem(me // 2, 4), lax.rem(me, 2)
    at_x = [lax.rem(me_x + k, 4) * 8 for k in range(4)]
    at_z = [lax.rem(me_z + k, 4) * 2 for k in range(4)]
    at_c = [me_c, 1 - me_c]
    peers = [at_x[a] + at_z[b] + at_c[c] for a, b, c in OTHERS]

    loads = [
        pltpu.make_async_copy(source, target, in_sem.at[k])
        for k, (source, target) in enumerate(
            (
                (disp_in, disp_raw), (wt_in, wt_ref), (lame_in, lame_raw), (shear_in, shear_raw),
                (force_in, force_raw), (samp_in, samp_raw), (vt_in, vt_ref), (vz_in, vz_ref),
                (x_in, x_ref), (spec_in, spec_ref), (steps_in, steps_ref), (slot_in, slot_ref),
            )
        )
    ]
    loads[0].start()
    loads[5].start()

    barrier = pltpu.get_barrier_semaphore()
    layer = [peer for peer, (a, _, _) in zip(peers, OTHERS) if a == 0]
    entry = [peer for peer, (_, b, c) in zip(peers, OTHERS) if (b, c) == (0, 0)] + layer
    entry += [lax.rem(me + 1, 32), lax.rem(me + 31, 32)]
    for peer in entry:
        pl.semaphore_signal(barrier, inc=1, device_id={"dev": peer}, device_id_type=MESH)
    for i in range(1, 4):
        pl.semaphore_signal(
            barrier, inc=1, device_id={"grp": lax.rem(group + i, 4)}, device_id_type=MESH
        )
    for k in (1, 2, 3, 4, *range(6, 12)):
        loads[k].start()

    def dense(raw, out):
        for index in np.ndindex(raw.shape[:-2]):
            out[index] = jnp.concatenate(
                [raw[(*index, pl.ds(q, 8, stride=4), slice(None))] for q in range(4)], axis=1
            )

    loads[0].wait()
    dense(disp_raw, disp_ref)
    loads[5].wait()
    dense(samp_raw, samp_ref)
    pl.semaphore_wait(barrier, len(entry) + 3)

    lowest, highest = lax.rem(me, 8) == 0, lax.rem(me, 8) == 7
    upper, lower = lowest & (me > 0), highest & (me < 31)
    above, below = lax.rem(me + 1, 32), lax.rem(me + 31, 32)

    def bordering(k, source, target, device):
        return pltpu.make_async_remote_copy(
            src_ref=source,
            dst_ref=target,
            send_sem=first_send.at[k],
            recv_sem=first_recv.at[k],
            device_id={"dev": device},
            device_id_type=MESH,
        )

    first_plane = bordering(0, disp_ref.at[:, 0], nb_first, below)
    last_planes = (
        bordering(1, disp_ref.at[:, count - 1], nb_last, above),
        bordering(2, samp_ref.at[count - 1], nb_mark, above),
    )
    pl.when(jnp.logical_not(lowest))(first_plane.start)
    for copy in last_planes:
        pl.when(lower)(copy.start)
    for peer in layer:
        pl.semaphore_signal(ready, inc=1, device_id={"dev": peer}, device_id_type=MESH)
    for k in range(2, 5):
        loads[k].wait()
    dense(force_raw, force_ref)
    for k, raw in enumerate((lame_raw, shear_raw)):
        wide = raw[...].astype(f32)
        for t in range(8):
            modwide[pl.ds(k * 8 + t, 32, stride=16), :] = wide[:, t * 128 : t * 128 + 128]
    for r in range(32):
        mod_ref[r] = modwide[pl.ds(r * 16, 16), :].astype(bf16)

    sums_ref[...] = jnp.zeros_like(sums_ref)
    for plane in range(count):
        strainrow[plane, pl.ds(48, 8), :] = jnp.ones((8, 128), f32)
        strainrow[plane, pl.ds(56, 8), :] = jnp.zeros((8, 128), f32)

    places = {-1: (0, 6, 1), 1: (6, 6, 1 + count), 2: (12, 3, 1 + 2 * count), -2: (None, 0, 0)}
    near = []
    for offset, (start, _, sample_start) in places.items():
        device = lax.rem(me - offset + 32, 32)
        plane = {2: 0, -2: count - 1}.get(offset)

        def send(source, target, k, device=device):
            near.append(
                pltpu.make_async_remote_copy(
                    src_ref=source,
                    dst_ref=target,
                    send_sem=near_send.at[k],
                    recv_sem=near_recv.at[k],
                    device_id={"dev": device},
                    device_id_type=MESH,
                )
            )

        width = count if plane is None else 1
        cut_out = pl.ds(0 if plane is None else plane, width)
        if start is not None:
            for k, source in enumerate((disp_ref, force_ref)):
                for c in range(3):
                    send(source.at[c, cut_out], nb.at[pl.ds(k * 15 + start + c * width, width)], 0)
        send(samp_ref.at[cut_out], nb_samp.at[pl.ds(sample_start, width)], 1)

    def everyone(source, target, send, recv, some=None):
        for peer in peers if some is None else some:
            pltpu.make_async_remote_copy(
                src_ref=source(peer),
                dst_ref=target.at[me] if len(target.shape) == 3 else target.at[pl.ds(me, 1)],
                send_sem=send,
                recv_sem=recv,
                device_id={"dev": peer},
                device_id_type=MESH,
            ).start()

    def all_arrived(target, recv):
        ref = target.at[pl.ds(0, 31)] if len(target.shape) == 3 else sized.at[pl.ds(0, 31)]
        pltpu.make_async_copy(ref, ref, recv).wait()

    known = [k for k, (a, b, c) in enumerate(OTHERS) if a == 0 or (b, c) == (0, 0)]
    unknown = [peer for k, peer in enumerate(peers) if k not in known]
    everyone(
        lambda peer: mod_ref.at[peer], modbuf, mod_send, mod_recv, [peers[k] for k in known]
    )

    loads[1].wait()

    @pl.loop(0, 16)
    def _(y):
        c, s = wt_ref[0, pl.ds(y, 1), :], wt_ref[1, pl.ds(y, 1), :]
        zr, zi = wt_ref[2], wt_ref[3]
        rows = pl.ds(pl.multiple_of(y * 32, 32), 32)
        blocks = [split(b) for b in (c * zr + s * zi, c * zi - s * zr)]
        for k, (high, low) in enumerate(blocks):
            wh[rows, pl.ds(k * 256, 256)] = high[:, 256:]
            wl[rows, pl.ds(k * 256, 256)] = low[:, 256:]

        @pl.when(y < 8)
        def _():
            for k, (high, low) in enumerate(blocks):
                for q in range(2):
                    lanes = slice(q * 128, q * 128 + 128)
                    weh[q, rows, pl.ds(k * 128, 128)] = high[:, lanes]
                    wel[q, rows, pl.ds(k * 128, 128)] = low[:, lanes]

    def hot_of(sample, s, counted):
        hit = jnp.broadcast_to(sample[s : s + 1], (32, 128)) == row_of((32, 128)) + group * 32
        return jnp.where(hit, counted, 0.0).astype(bf16)

    own_last = jnp.where(lower, 0.0, 1.0).astype(f32)
    one_hot_ref[...] = jnp.concatenate(
        [hot_of(samp_ref[p], s, (1.0, own_last)[p // (count - 1)]) for p in range(count) for s in range(8)],
        axis=1,
    )
    pl.semaphore_wait(ready, len(layer))
    everyone(lambda peer: mod_ref.at[peer], modbuf, mod_send, mod_recv, unknown)
    modbuf[me] = mod_ref[me]

    def sums_of(strain, one_hot):
        n = strain[0].shape[0]
        rows_high, rows_low = [], []
        for p in range(n):
            for c in range(6):
                strainrow[p, pl.ds(c * 8, 8), :] = strain[c][p]
        for p in range(n):
            for s in range(8):
                high, low = split(strainrow[p, pl.ds(s, 8, stride=8), :])
                rows_high.append(high)
                rows_low.append(low)

        def against(rows):
            return lax.dot_general(
                one_hot,
                jnp.concatenate(rows, axis=1),
                (((1,), (1,)), ((), ())),
                preferred_element_type=f32,
            )

        return against(rows_high) + against(rows_low)

    pl.when(jnp.logical_not(highest))(first_plane.wait_recv)
    fields = [
        jnp.concatenate([disp_ref[c], jnp.where(highest, 0.0, nb_first[pl.ds(c, 1)])], axis=0)
        for c in range(3)
    ]
    sums_ref[:, pl.ds(0, 8)] = sums_of(strain_of(fields), one_hot_ref[...])

    @pl.when(upper)
    def _():
        for copy in last_planes:
            copy.wait_recv()
        between = [
            jnp.concatenate([nb_last[pl.ds(c, 1)], disp_ref[c, pl.ds(0, 1)]], axis=0) for c in range(3)
        ]
        hots = jnp.concatenate([hot_of(nb_mark, s, 1.0) for s in range(8)], axis=1)
        sums_ref[:, pl.ds(0, 8)] += sums_of(strain_of(between), hots)

    everyone(lambda peer: sums_ref.at[pl.ds(peer, 1)], partbuf, part_send, part_recv)
    partbuf[pl.ds(me, 1), :] = sums_ref[pl.ds(me, 1), :]
    for k in range(6, 12):
        loads[k].wait()

    def back_rows(k, lanes):
        row = pl.ds(k, 1)
        c, s = vt_ref[0, row, pl.ds(0, lanes)], vt_ref[1, row, pl.ds(0, lanes)]
        zr, zi = vz_ref[0, :, pl.ds(0, lanes)], vz_ref[1, :, pl.ds(0, lanes)]
        return split(c * zr + s * zi), split(c * zi - s * zr)

    @pl.loop(0, 16)
    def _(k):
        for p, (high, low) in enumerate(back_rows(16 + k, HALF)):
            rows = pl.ds(pl.multiple_of(p * 256 + k * 16, 16), 16)
            vh[rows, :] = high
            vl[rows, :] = low

    for q in range(2):

        @pl.loop(0, 8)
        def _(k):
            for p, (high, low) in enumerate(back_rows(q * 8 + k, 256)):
                rows = pl.ds(pl.multiple_of(p * 128 + k * 16, 16), 16)
                veh[q, rows, :] = high
                vel[q, rows, :] = low

    ref = modbuf.at[pl.ds(0, 31)]
    pltpu.make_async_copy(ref, ref, mod_recv).wait()

    def moduli(x, n):
        both = modbuf[pl.ds(x, n)].astype(f32)
        return both[:, :8], both[:, 8:]

    def at(x, n):
        return pl.ds(pl.multiple_of(x * 8, 8), n * 8)

    def planes(ref, k, x, n):
        return ref[k, at(x, n), :].reshape(n, 8, 128)

    def x_slope(ref, k, x, n, v):
        after = planes(ref, k, lax.rem(x + n, 32), 1)
        before = planes(ref, k, lax.rem(x + 31, 32), 1)
        up = jnp.concatenate([v[1:], after], axis=0)
        down = jnp.concatenate([before, v[:-1]], axis=0)
        return 0.5 * (up - down)

    def forward():
        rows = jnp.concatenate(
            [
                jnp.concatenate([field[k, pl.ds(s, 32, stride=8), :] for k in range(2)], axis=0)
                for s in range(8)
            ],
            axis=1,
        )
        even, odd = rows[:, :HALF] + rows[:, HALF:], rows[:, :HALF] - rows[:, HALF:]

        def part_of(data, high_ref, low_ref):
            high, low = split(data)
            both = mm(jnp.concatenate([high, low], axis=0), high_ref[...])
            return both[:64] + (both[64:] + mm(high, low_ref[...]))

        sides = [
            part_of(even[:, :256] + even[:, 256:], weh.at[0], wel.at[0]),
            part_of(even[:, :256] - even[:, 256:], weh.at[1], wel.at[1]),
            part_of(odd, wh, wl),
        ]
        plane = jnp.concatenate(
            [side[:, : side.shape[1] // 2] for side in sides]
            + [side[:, side.shape[1] // 2 :] for side in sides],
            axis=1,
        )
        stacked = jnp.concatenate(
            [
                jnp.concatenate([plane[:32, :HALF], plane[32:, :HALF]], axis=1),
                jnp.concatenate([plane[:32, HALF:], plane[32:, HALF:]], axis=1),
            ],
            axis=0,
        )
        return product(x_ref[0], stacked)

    lame, shear = moduli(0, 32)
    field[0] = (lame + (2.0 / 3.0) * shear).reshape(256, 128)

    all_arrived(partbuf, part_recv)
    total = jnp.sum(partbuf[...], axis=0, keepdims=True)
    lane1 = lane_of((1, 128))

    def pick(row, k):
        return jnp.sum(jnp.where(lane1 == k, row, 0.0), axis=1, keepdims=True)

    members = pick(total, 6)
    load = [pick(total, c) / members for c in range(6)]
    trace = load[0] + load[1] + load[2]
    d = [load[c] - trace / 3.0 if c < 3 else load[c] for c in range(6)]
    own_steps = steps_ref[group * 32 + me]
    rates = [jnp.where(k < own_steps, relax_rate, 0.0).astype(f32) for k in range(KMAX)]
    size = norm_of(d)

    _, shear = moduli(0, 32)
    scale, _ = relaxed(shear, size, rates)
    field[1] = (2.0 * shear * scale).reshape(256, 128)
    spectrum = forward()
    spectrum_a, spectrum_b = spectrum[:, :HALF], spectrum[:, HALF:]
    mix = d[0] * spec_ref[1]
    for c in range(1, 6):
        mix = mix + d[c] * spec_ref[1 + c]
    scaled = spec_ref[0]
    steady = (1.0 - green_ratio) * trace
    phi = [scaled * spectrum_b[:32], scaled * spectrum_b[32:]]
    pressure = [
        scaled * (steady * spectrum_a[:32]) - mix * phi[0],
        scaled * (steady * spectrum_a[32:]) - mix * phi[1],
    ]
    waves = [spec_ref[7 + c] for c in range(3)]
    turned = [
        d[0] * waves[0] + d[5] * waves[1] + d[4] * waves[2],
        d[5] * waves[0] + d[1] * waves[1] + d[3] * waves[2],
        d[4] * waves[0] + d[3] * waves[1] + d[2] * waves[2],
    ]
    slopes = [
        [waves[c] * pressure[k] + turned[c] * phi[k] for k in range(2)] for c in range(3)
    ]
    mixed = jnp.concatenate(
        [
            jnp.concatenate([-slopes[c][1] for c in range(3)], axis=1),
            jnp.concatenate([slopes[c][0] for c in range(3)], axis=1),
        ],
        axis=0,
    )
    back = product(x_ref[1], mixed)
    def side_of(start, width, high_ref, low_ref):
        lines = jnp.concatenate(
            [
                jnp.concatenate(
                    [back[h : h + 32, c * HALF + start :][:, :width] for h in (0, 32)], axis=1
                )
                for c in range(3)
            ],
            axis=0,
        )
        high, low = split(lines)
        both = mm(jnp.concatenate([high, low], axis=0), high_ref[...])
        return both[:96] + (both[96:] + mm(high, low_ref[...]))

    first, second = (side_of(q * 128, 128, veh.at[q], vel.at[q]) for q in range(2))
    even = jnp.concatenate([first + second, first - second], axis=1)
    odd = side_of(256, 256, vh, vl)
    space = jnp.concatenate([even + odd, even - odd], axis=1)
    for c in range(3):
        for s in range(8):
            disp_u[c, pl.ds(s, 32, stride=8), :] = space[
                c * 32 : c * 32 + 32, s * 128 : s * 128 + 128
            ]

    source, target = row_of((128, 128)), lane_of((128, 128))
    line = source // VOX == target // VOX
    ahead = line & ((target + 1) % VOX == source % VOX)
    behind = line & ((target + VOX - 1) % VOX == source % VOX)
    z_matrix = (jnp.where(ahead, 0.5, 0.0) - jnp.where(behind, 0.5, 0.0)).astype(bf16)

    def voxel(t, sums):
        x = t * BLOCK
        ux, uy, uz = (planes(disp_u, c, x, BLOCK) for c in range(3))
        dx = [x_slope(disp_u, c, x, BLOCK, u) for c, u in enumerate((ux, uy, uz))]
        high, low = split(jnp.concatenate([ux, uy, uz], axis=0).reshape(24 * BLOCK, 128))
        dz = (mm(high, z_matrix) + mm(low, z_matrix)).reshape(3, BLOCK, 8, 128)
        change = [
            -dx[0],
            -yc(uy),
            -dz[2],
            -0.5 * (yc(uz) + dz[1]),
            -0.5 * (dx[2] + dz[0]),
            -0.5 * (dx[1] + yc(ux)),
        ]
        for k in range(3):
            pair = jnp.concatenate(change[2 * k : 2 * k + 2], axis=1)
            flu[pl.ds(x, BLOCK), pl.ds(k * 16, 16), :] = pair.astype(wire)
        lame, shear = moduli(x, BLOCK)
        e = [load[c] + change[c] for c in range(6)]
        tr = e[0] + e[1] + e[2]
        dv = [e[c] - tr / 3.0 if c < 3 else e[c] for c in range(6)]
        scale, f = relaxed(shear, norm_of(dv), rates)
        twice = 2.0 * shear * scale
        bulk = (lame + (2.0 / 3.0) * shear) * tr
        new = [bulk + twice * dv[c] if c < 3 else twice * dv[c] for c in range(6)]
        new += [lame, shear / (1.0 + f)]
        return tuple(a + jnp.sum(b, axis=0) for a, b in zip(sums, new))

    zero = jnp.zeros((8, 128), f32)
    sums = lax.fori_loop(0, 32 // BLOCK, voxel, (zero,) * 8)
    column = jnp.concatenate([jnp.sum(a, axis=0, keepdims=True) for a in sums], axis=0)
    column = jnp.sum(column, axis=1, keepdims=True) * (1.0 / VOX**3)
    lane8, row8 = lane_of((8, 128)), row_of((8, 128))
    own_row = jnp.sum(
        jnp.where(lane8 == row8 + group * 16, column, 0.0), axis=0, keepdims=True
    )
    for c in range(6):
        own_row = own_row + jnp.where(lane1 == group * 16 + 8 + c, load[c], 0.0)

    rowbuf[3] = own_row
    for i in range(1, 4):
        (
            pltpu.make_async_remote_copy(
                src_ref=rowbuf.at[3],
                dst_ref=rowbuf.at[i - 1],
                send_sem=y_send,
                recv_sem=y_recv,
                device_id={"grp": lax.rem(group + i, 4)},
                device_id_type=MESH,
            )
        ).start()
    arrived = rowbuf.at[pl.ds(0, 3)]
    for copy in near:
        copy.start()
    pltpu.make_async_copy(arrived, arrived, y_recv).wait()
    joined[0] = rowbuf[0] + rowbuf[1] + rowbuf[2] + rowbuf[3]
    everyone(lambda peer: joined.at[0], respbuf, resp_send, resp_recv)
    respbuf[pl.ds(me, 1), :] = joined[0]
    everyone(lambda peer: flu.at[peer], flubuf, flu_send, flu_recv)
    flubuf[me] = flu[me]

    pltpu.make_async_copy(nb, nb, near_recv.at[0]).wait()
    pltpu.make_async_copy(nb_samp, nb_samp, near_recv.at[1]).wait()
    exists = [(me * count + j >= 3).astype(f32) * (me * count + j < 67).astype(f32) for j in range(8)]

    def around_of(own, k, c):
        below = [nb[pl.ds(k * 15 + c * 2 + p, 1)] for p in (0, 0, 1)]
        above = [nb[pl.ds(k * 15 + 6 + c * 2 + p, 1)] for p in range(2)]
        return [*below, own[c, pl.ds(0, 1)], own[c, pl.ds(1, 1)], *above, nb[pl.ds(k * 15 + 12 + c, 1)]]

    def masked(planes):
        return jnp.concatenate([p * m for p, m in zip(planes, exists)], axis=0)

    around = [masked(around_of(disp_ref, 0, c)) for c in range(3)]
    outside = [masked(around_of(force_ref, 1, c)) for c in range(3)]
    given = [
        (outside[c][1:] - spring_rate * around[c][1:])
        * jnp.concatenate([jnp.full((1, 8, 128), m) for m in exists[1:]], axis=0)
        for c in range(3)
    ]
    samples = [nb_samp[pl.ds(j, 1)] for j in range(3)]
    samples += [samp_ref[pl.ds(p, 1)] for p in range(2)]
    samples += [nb_samp[pl.ds(j, 1)] for j in range(3, 6)]

    all_arrived(respbuf, resp_recv)
    gathered = jnp.concatenate([respbuf[...], jnp.zeros((96, 128), f32)], axis=0).T
    cells = []
    for c in range(8):
        row = jnp.concatenate(
            [gathered[g * 16 + c : g * 16 + c + 1, :32] for g in range(4)], axis=1
        )
        source = jnp.broadcast_to(row, (8, 128))
        cells.append(
            masked(
                [
                    jnp.take_along_axis(source, s[0], axis=1, mode="promise_in_bounds")[None]
                    for s in samples
                ]
            )
        )
    lame, shear = cells[6], cells[7]
    pull = force_of(cells[:6])
    inside = jnp.concatenate([jnp.full((1, 8, 128), m) for m in exists[1:]], axis=0)
    res = [given[c] - pull[c] * inside for c in range(3)]

    def stiff(w, low):
        n = w[0].shape[0]
        strain = strain_of(w)
        stress = stress_of(strain, lame[low : low + n - 1], shear[low : low + n - 1])
        pull = force_of(stress)
        mask = jnp.concatenate(
            [jnp.full((1, 8, 128), m) for m in exists[low + 1 : low + n - 1]], axis=0
        )
        return [(pull[c] + spring_rate * w[c][1:-1]) * mask for c in range(3)]

    k1 = stiff(res, 1)
    k2 = stiff(k1, 2)
    r_own = [a[2:4] for a in res]
    k1_own = [a[1:3] for a in k1]
    k2_own = [a[0:2] for a in k2]
    energy_strain = strain_of(k2)
    energy_stress = stress_of(energy_strain, lame[3:5], shear[3:5])

    def dotted(a, b):
        total = a[0] * b[0]
        for c in range(1, 3):
            total = total + a[c] * b[c]
        return jnp.sum(jnp.sum(total, axis=0), axis=0, keepdims=True)

    energy = energy_strain[0] * energy_stress[0]
    for c in range(1, 6):
        energy = energy + (1.0 if c < 3 else 2.0) * energy_strain[c] * energy_stress[c]
    energy = jnp.sum(jnp.sum(energy, axis=0), axis=0, keepdims=True) + spring_rate * dotted(
        k2_own, k2_own
    )
    rows = [
        dotted(r_own, r_own),
        dotted(r_own, k1_own),
        dotted(k1_own, k1_own),
        dotted(k1_own, k2_own),
        dotted(k2_own, k2_own),
        energy,
        jnp.zeros((2, 128), f32),
    ]
    column = jnp.sum(jnp.concatenate(rows, axis=0), axis=1, keepdims=True)
    moment[0] = jnp.sum(jnp.where(lane8 == row8, column, 0.0), axis=0, keepdims=True)
    everyone(lambda peer: moment.at[0], momentbuf, mom_send, mom_recv)
    momentbuf[pl.ds(me, 1), :] = moment[0]

    def owner(r, acc):
        taken = jnp.where(slot_ref[group * 32 + r] == me, 1.0, 0.0).astype(f32)
        return acc + taken * respbuf[pl.ds(r, 1), :]

    row = lax.fori_loop(0, 32, owner, jnp.zeros((1, 128), f32))
    shifted = jnp.zeros((1, 128), f32)
    for g in range(4):
        here = (group == g).astype(f32)
        shifted = shifted + here * roll(row, -16 * g, 1)
    row_out[...] = shifted[:, :8]

    table = respbuf[...]
    lane32 = lane_of((32, 128))
    group_load = [
        jnp.sum(jnp.where(lane32 == group * 16 + 8 + c, table, 0.0), axis=1, keepdims=True)
        for c in range(6)
    ]
    all_arrived(flubuf, flu_recv)
    for r in range(32):
        block = flubuf[r].astype(f32)
        for c in range(6):
            micro_out[pl.ds((c * 32 + r) * 8, 8), :] = (
                group_load[c][r : r + 1] + block[c * 8 : c * 8 + 8]
            )

    all_arrived(momentbuf, mom_recv)
    total = jnp.sum(momentbuf[...], axis=0, keepdims=True)
    m = [pick(total, k) for k in range(6)]

    def form(a, b, first):
        out = 0.0
        for i, p in enumerate(a):
            for j, q in enumerate(b):
                out = out + p * q * m[i + j + first]
        return out

    rr = m[0]
    alpha0 = rr / m[1]
    r1 = (jnp.ones_like(rr), -alpha0)
    rr1 = form(r1, r1, 0)
    beta0 = rr1 / rr
    p1 = (1.0 + beta0, -alpha0)
    alpha1 = rr1 / form(p1, p1, 1)
    r2 = (jnp.ones_like(rr), -alpha0 - alpha1 * p1[0], alpha1 * alpha0)
    rr2 = form(r2, r2, 0)
    beta1 = rr2 / rr1
    p2 = (r2[0] + beta1 * p1[0], r2[1] + beta1 * p1[1], r2[2])
    alpha2 = rr2 / form(p2, p2, 1)
    weight = (
        alpha0 + alpha1 * p1[0] + alpha2 * p2[0],
        alpha1 * p1[1] + alpha2 * p2[1],
        alpha2 * p2[2],
    )
    for c in range(3):
        new = disp_ref[c] + (
            weight[0] * r_own[c] + weight[1] * k1_own[c] + weight[2] * k2_own[c]
        )
        for p in range(count):
            for q in range(4):
                disp_out[c, p, pl.ds(q, 8, stride=4), :] = new[p][:, q * 32 : q * 32 + 32]

    pl.when(jnp.logical_not(lowest))(first_plane.wait_send)
    for copy in last_planes:
        pl.when(lower)(copy.wait_send)
    pltpu.make_async_copy(nb, nb, near_send.at[0]).wait()
    pltpu.make_async_copy(nb_samp, nb_samp, near_send.at[1]).wait()
    pltpu.make_async_copy(arrived, arrived, y_send).wait()
    for buffer, sem in (
        (modbuf, mod_send), (partbuf, part_send), (respbuf, resp_send),
        (flubuf, flu_send), (momentbuf, mom_send),
    ):
        all_arrived(buffer, sem)


def leave(a, b, c, a_out, b_out, c_out, sem):
    step = c.shape[0] // PIECES
    pairs = [(a, a_out), (b, b_out)]
    pairs += [(c.at[pl.ds(k * step, step)], c_out.at[pl.ds(k * step, step)]) for k in range(PIECES)]
    copies = [pltpu.make_async_copy(*pair, sem.at[k]) for k, pair in enumerate(pairs)]
    for copy in copies:
        copy.start()
    for copy in copies:
        copy.wait()


def shards(
    displacement, external_force, element_sample, lame_field, shear_field, plastic_steps, owner_slot
):
    count = displacement.shape[1]
    disp, sample = (3, count, 8, 128), (count, 8, 128)
    wt, vt, vz, x, spec = (jnp.asarray(t) for t in tables())
    operands = (
        displacement,
        wt,
        lame_field.reshape(32, 1024),
        shear_field.reshape(32, 1024),
        external_force,
        element_sample,
        vt,
        vz,
        x,
        spec,
    )
    scalars = (plastic_steps, owner_slot)
    vmem = pl.BlockSpec(memory_space=pltpu.VMEM)
    hbm = pl.BlockSpec(memory_space=pltpu.HBM)
    dma = pltpu.SemaphoreType.DMA
    disp_next, row, micro = pl.pallas_call(
        kernel,
        out_shape=(
            jax.ShapeDtypeStruct(displacement.shape, f32),
            jax.ShapeDtypeStruct((1, 8), f32),
            jax.ShapeDtypeStruct((6 * 32 * 8, 128), f32),
        ),
        in_specs=[hbm] * 12,
        out_specs=(vmem,) * 3,
        scratch_shapes=[
            *(pltpu.VMEM(a.shape, a.dtype) for a in operands),
            *(pltpu.SMEM(a.shape, a.dtype) for a in scalars),
            dma((12,)),
            pltpu.VMEM(disp, f32),
            pltpu.VMEM(disp, f32),
            pltpu.VMEM(sample, jnp.int32),
            pltpu.VMEM((32, 16, 128), bf16),
            pltpu.VMEM((512, 128), f32),
            pltpu.VMEM((3, 8, 128), f32),
            pltpu.VMEM((3, 8, 128), f32),
            pltpu.VMEM((8, 128), jnp.int32),
            pltpu.VMEM((30, 8, 128), f32),
            pltpu.VMEM((6, 8, 128), jnp.int32),
            pltpu.VMEM((32, 1, 128), f32),
            pltpu.VMEM((32, 16, 128), bf16),
            pltpu.VMEM((32, 128), f32),
            pltpu.VMEM((count, 64, 128), f32),
            pltpu.VMEM((32, count * 1024), bf16),
            pltpu.VMEM((32, 128), f32),
            *(pltpu.VMEM((HALF, HALF), bf16),) * 4,
            *(pltpu.VMEM((2, 256, 256), bf16),) * 4,
            pltpu.VMEM((2, 256, 128), f32),
            pltpu.VMEM((3, 256, 128), f32),
            pltpu.VMEM((32, 48, 128), wire),
            pltpu.VMEM((32, 48, 128), wire),
            pltpu.VMEM((4, 1, 128), f32),
            pltpu.VMEM((1, 1, 128), f32),
            pltpu.VMEM((32, 128), f32),
            pltpu.VMEM((1, 1, 128), f32),
            pltpu.VMEM((32, 128), f32),
            pltpu.SemaphoreType.REGULAR, dma((3,)), dma((3,)), dma((2,)), dma((2,)), dma, dma, dma, dma,
            dma, dma, dma, dma, dma, dma, dma, dma,
        ],
        compiler_params=pltpu.CompilerParams(collective_id=0, has_side_effects=True, vmem_limit_bytes=24 << 20),
    )(*[pltpu.with_memory_space_constraint(a, pltpu.HBM) for a in operands + scalars])
    results = (disp_next, row, micro)
    disp_next, row, micro = pl.pallas_call(
        leave,
        out_shape=tuple(jax.ShapeDtypeStruct(a.shape, a.dtype) for a in results),
        in_specs=[pl.BlockSpec(memory_space=pl.ANY)] * 3,
        out_specs=(pl.BlockSpec(memory_space=pltpu.HBM),) * 3,
        scratch_shapes=[dma((PIECES + 2,))],
        compiler_params=pltpu.CompilerParams(vmem_limit_bytes=1 << 20),
    )(*results)
    return disp_next, row, micro.reshape(6, 32, 1, 1024)


def solution(mesh):
    in_specs = (
        P(None, "dev", None, None),
        P(None, "dev", None, None),
        P("dev", None, None),
        P("grp", "dev", None),
        P("grp", "dev", None),
        P(),
        P(),
    )
    out_specs = (P(None, "dev", None, None), P(("grp", "dev"), None), P(None, "grp", "dev", None))
    return jax.shard_map(shards, mesh=mesh, in_specs=in_specs, out_specs=out_specs, check_vma=False)
```
